32 devices in a mesh: dp: 8 (over y, x, core), tensor: 4 (over z).
Axes of the slice: x: 2, y: 2, z: 4, core: 2. Of those that a mesh axis runs over, the one named last changes fastest.
Arguments:
- hidden_in: float32 [8192, 2048], P(('dp', 'tensor')), may hold values from -6 to 6
- positions: int32 [8192], P('dp'), may hold values from 0 to 4095
- norm_gains: bfloat16 [1, 2, 2048], P(None, None, ('dp', 'tensor')), may hold values from 0.25 to 1.75
- w_query: bfloat16 [1, 2048, 2048], P(None, 'dp', 'tensor'), may hold values from -0.125 to 0.125
- w_key: bfloat16 [1, 2048, 256], P(None, ('dp', 'tensor')), may hold values from -0.125 to 0.125
- w_value: bfloat16 [1, 2048, 256], P(None, ('dp', 'tensor')), may hold values from -0.125 to 0.125
- w_out: bfloat16 [1, 2048, 2048], P(None, 'tensor', 'dp'), may hold values from -0.5 to 0.5
- w_gate: bfloat16 [1, 2048, 5632], P(None, 'dp', 'tensor'), may hold values from -0.125 to 0.125
- w_up: bfloat16 [1, 2048, 5632], P(None, 'dp', 'tensor'), may hold values from -0.125 to 0.125
- w_down: bfloat16 [1, 5632, 2048], P(None, 'tensor', 'dp'), may hold values from -0.078125 to 0.078125
- out_grad: float32 [8192, 2048], P(('dp', 'tensor')), may hold values from -6 to 6
Outputs:
- hidden_out: float32 [8192, 2048], P(('dp', 'tensor'))
- grad_in: float32 [8192, 2048], P(('dp', 'tensor'))
- grad_gains: float32 [1, 2, 2048], P(None, None, ('dp', 'tensor'))
- grad_query: float32 [1, 2048, 2048], P(None, 'dp', 'tensor')
- grad_key: float32 [1, 2048, 256], P(None, ('dp', 'tensor'))
- grad_value: float32 [1, 2048, 256], P(None, ('dp', 'tensor'))
- grad_out: float32 [1, 2048, 2048], P(None, 'tensor', 'dp')
- grad_gate: float32 [1, 2048, 5632], P(None, 'dp', 'tensor')
- grad_up: float32 [1, 2048, 5632], P(None, 'dp', 'tensor')
- grad_down: float32 [1, 5632, 2048], P(None, 'tensor', 'dp')
The draws below stay inside these ranges and needn't reach their ends.
All inputs are finite; a program needn't handle non-finite values.
Results may differ from the reference program's by a relative error of at most 0.019.
Values may be sent and summed in bfloat16 or wider, within the bound.
A program may use at most 192 MiB of HBM per device.

```python
import jax
import jax.numpy as jnp
from jax import lax

D = 2048
H = 32
KV = 4
HD = 64
FF = 5632
LAYERS = 1
SEQ = 128
TOKENS = 8192


def place_ends(result, rng, low, top_value):
    longest = result.shape.index(max(result.shape))
    spots = []
    for shift in (0, 1):
        where = [jax.random.randint(jax.random.fold_in(rng, axis), (), 0, length) for axis, length in enumerate(result.shape)]
        where[longest] = (where[longest] + shift) % result.shape[longest]
        spots.append(tuple(where))
    return result.at[spots[0]].set(low).at[spots[1]].set(top_value)


def level_of(key, extent, shards, least, top_value):
    loudness = 1.0
    for dim, blocks in shards:
        draws = jax.random.uniform(jax.random.fold_in(jax.random.fold_in(key, 6), dim), (blocks,), jnp.float32, least / len(shards), top_value / len(shards))
        loudness = loudness * jnp.repeat(jnp.exp(draws), extent[dim] // blocks).reshape((-1,) + (1,) * (len(extent) - 1 - dim))
    return loudness


def noise(stream_key, dims, scale, limit, cuts=(), kind=jnp.bfloat16):
    drawn = jax.random.normal(stream_key, dims, jnp.float32) * scale
    if len(cuts) > 0:
        drawn = level_of(stream_key, dims, cuts, -0.22, 0.18) * drawn
    return jnp.clip(drawn, min=-limit, max=limit).astype(kind)


def setup_inputs(seed: int = 0) -> dict:
    arg_keys = jax.random.split(jax.random.key(seed), 12)
    return {
        "hidden_in": noise(arg_keys[0], (TOKENS, D), 1.0, 6.0, ((0, 32),), jnp.float32),
        "positions": place_ends(jax.random.randint(arg_keys[1], (TOKENS,), 0, 4096), jax.random.fold_in(arg_keys[1], 1), 0, 4095).astype(jnp.int32),
        "norm_gains": jnp.clip(1.0 + 0.15 * jax.random.normal(arg_keys[2], (LAYERS, 2, D), jnp.float32), 0.25, 1.75).astype(jnp.bfloat16),
        "w_query": noise(arg_keys[3], (LAYERS, D, H * HD), D ** -0.5, 0.125, ((1, 8), (2, 4))),
        "w_key": noise(arg_keys[4], (LAYERS, D, KV * HD), D ** -0.5, 0.125, ((1, 32),)),
        "w_value": noise(arg_keys[5], (LAYERS, D, KV * HD), D ** -0.5, 0.125, ((1, 32),)),
        "w_out": noise(arg_keys[6], (LAYERS, H * HD, D), (H * HD // 16) ** -0.5, 0.5, ((1, 4), (2, 8))),
        "w_gate": noise(arg_keys[7], (LAYERS, D, FF), D ** -0.5, 0.125, ((1, 8), (2, 4))),
        "w_up": noise(arg_keys[8], (LAYERS, D, FF), D ** -0.5, 0.125, ((1, 8), (2, 4))),
        "w_down": noise(arg_keys[9], (LAYERS, FF, D), FF ** -0.5, 0.078125, ((1, 4), (2, 8))),
        "out_grad": noise(arg_keys[10], (TOKENS, D), 1.0, 6.0, ((0, 32),), jnp.float32),
    }


NORM_EPS = 1e-05
NEG_BIG = -1e+30

def rms_normed(row_vals, gain_vec):
    inv_rms = lax.rsqrt(lax.optimization_barrier(jnp.mean(row_vals * row_vals, -1, keepdims=True)) + NORM_EPS)
    return (row_vals * inv_rms * gain_vec.astype(jnp.float32)).astype(jnp.bfloat16)

def rms_back(row_vals, gain_vec, grad_normed):
    inv_rms = lax.rsqrt(lax.optimization_barrier(jnp.mean(row_vals * row_vals, -1, keepdims=True)) + NORM_EPS)
    weighted = grad_normed * gain_vec.astype(jnp.float32)
    grad_gain = lax.optimization_barrier(jnp.sum(grad_normed * row_vals * inv_rms, 0))
    grad_rows = inv_rms * weighted - row_vals * inv_rms ** 3 * lax.optimization_barrier(jnp.mean(weighted * row_vals, -1, keepdims=True))
    return (grad_rows, grad_gain)

def rope_tables(positions):
    inv_freq = 10000.0 ** (-(jnp.arange(HD // 2, dtype=jnp.float32) * 2.0 / HD))
    angles = positions.astype(jnp.float32)[:, None] * inv_freq[None, :]
    return (jnp.cos(angles), jnp.sin(angles))

def rotate(row_vals, cosine_tab, sine_tab):
    row_total = row_vals.shape[0]
    shaped = row_vals.reshape(row_total, -1, HD)
    front_half = shaped[..., :HD // 2]
    back_half = shaped[..., HD // 2:]
    cos_part = cosine_tab[:, None, :]
    sin_part = sine_tab[:, None, :]
    turned = jnp.concatenate([front_half * cos_part - back_half * sin_part, back_half * cos_part + front_half * sin_part], -1)
    return turned.reshape(row_total, -1)

def rotate_back(row_vals, cosine_tab, sine_tab):
    row_total = row_vals.shape[0]
    shaped = row_vals.reshape(row_total, -1, HD)
    front_half = shaped[..., :HD // 2]
    back_half = shaped[..., HD // 2:]
    cos_part = cosine_tab[:, None, :]
    sin_part = sine_tab[:, None, :]
    turned = jnp.concatenate([front_half * cos_part + back_half * sin_part, back_half * cos_part - front_half * sin_part], -1)
    return turned.reshape(row_total, -1)

def head_major(values_in, seq_len):
    head_count = values_in.shape[1] // HD
    return values_in.reshape(seq_len, head_count, HD).transpose(1, 0, 2).reshape(head_count * seq_len, HD)

def seq_major(values_in, seq_len):
    head_count = values_in.shape[0] // seq_len
    return values_in.reshape(head_count, seq_len, HD).transpose(1, 0, 2).reshape(seq_len, head_count * HD)

def causal_scores(query_rows, key_rows):
    seq_len = key_rows.shape[0]
    scores = jnp.dot(query_rows, key_rows.T, preferred_element_type=jnp.float32) * HD ** (-0.5)
    row_pos = lax.broadcasted_iota(jnp.int32, scores.shape, 0) % seq_len
    col_pos = lax.broadcasted_iota(jnp.int32, scores.shape, 1)
    return jnp.where(col_pos <= row_pos, scores, NEG_BIG)

def attend_forward(query_rows, key_rows, value_rows):
    scores = causal_scores(query_rows, key_rows)
    row_max = lax.optimization_barrier(jnp.max(scores, -1, keepdims=True))
    log_total = row_max[:, 0] + jnp.log(lax.optimization_barrier(jnp.sum(jnp.exp(scores - row_max), -1)))
    attn_prob = jnp.exp(scores - log_total[:, None]).astype(jnp.bfloat16)
    return (jnp.dot(attn_prob, value_rows, preferred_element_type=jnp.float32), log_total)

def attend_backward(query_rows, key_rows, value_rows, log_total, grad_rows):
    seq_len = key_rows.shape[0]
    head_count = query_rows.shape[0] // seq_len
    scores = causal_scores(query_rows, key_rows)
    attn_prob = jnp.exp(scores - log_total[:, None])
    prob_bf = attn_prob.astype(jnp.bfloat16)
    grad_prob = jnp.dot(grad_rows, value_rows.T, preferred_element_type=jnp.float32)
    delta = lax.optimization_barrier(jnp.sum(attn_prob * grad_prob, -1, keepdims=True))
    grad_scores = (attn_prob * (grad_prob - delta) * HD ** (-0.5)).astype(jnp.bfloat16)
    grad_query = jnp.dot(grad_scores, key_rows, preferred_element_type=jnp.float32)
    scores_3d = grad_scores.reshape(head_count, seq_len, seq_len).astype(jnp.float32)
    query_3d = query_rows.reshape(head_count, seq_len, HD).astype(jnp.float32)
    prob_3d = prob_bf.reshape(head_count, seq_len, seq_len).astype(jnp.float32)
    grad_3d = grad_rows.reshape(head_count, seq_len, HD).astype(jnp.float32)
    grad_key = jnp.einsum('hqk,hqd->hkd', scores_3d, query_3d, precision=lax.Precision.HIGHEST)
    grad_value = jnp.einsum('hqk,hqd->hkd', prob_3d, grad_3d, precision=lax.Precision.HIGHEST)
    return (grad_query, grad_key.reshape(head_count * seq_len, HD), grad_value.reshape(head_count * seq_len, HD))

def split_groups(row_vals, width):
    return row_vals.reshape(SEQ, KV, width).transpose(1, 0, 2)

def join_groups(group_vals):
    return group_vals.transpose(1, 0, 2).reshape(SEQ, -1)

def sequence_forward(pieces):
    query_seq, key_seq, value_seq = pieces
    group = H // KV

    def one_group(inner):
        query_grp, key_grp, value_grp = inner
        attended, log_total = attend_forward(head_major(query_grp, SEQ), key_grp, value_grp)
        return (seq_major(attended, SEQ).astype(jnp.bfloat16), log_total)
    attended, log_total = lax.map(one_group, (split_groups(query_seq, group * HD), split_groups(key_seq, HD), split_groups(value_seq, HD)))
    return (join_groups(attended), log_total)

def sequence_backward(pieces):
    query_seq, key_seq, value_seq, log_seq, grad_seq = pieces
    group = H // KV

    def one_group(inner):
        query_grp, key_grp, value_grp, log_grp, grad_grp = inner
        grad_query, grad_key, grad_value = attend_backward(head_major(query_grp, SEQ), key_grp, value_grp, log_grp, head_major(grad_grp, SEQ))
        return (seq_major(grad_query, SEQ), seq_major(grad_key, SEQ), seq_major(grad_value, SEQ))
    grads = lax.map(one_group, (split_groups(query_seq, group * HD), split_groups(key_seq, HD), split_groups(value_seq, HD), log_seq, split_groups(grad_seq, group * HD)))
    return tuple((join_groups(piece) for piece in grads))

def expand_heads(weight_kv):
    group = H // KV
    spread = jnp.broadcast_to(weight_kv.reshape(D, KV, 1, HD), (D, KV, group, HD))
    return spread.reshape(D, H * HD)

def reduce_heads(grad_heads):
    return lax.optimization_barrier(jnp.sum(grad_heads.reshape(D, KV, H // KV, HD), 2)).reshape(D, KV * HD)

def layer_forward(residual, cosine_tab, sine_tab, gain_pair, wq, wk, wv, wo, wg, wu, wd):
    seq_count = residual.shape[0] // SEQ
    normed_one = rms_normed(residual, gain_pair[0])
    query_all = rotate(jnp.dot(normed_one, wq, preferred_element_type=jnp.float32), cosine_tab, sine_tab).astype(jnp.bfloat16)
    key_all = rotate(jnp.dot(normed_one, wk, preferred_element_type=jnp.float32), cosine_tab, sine_tab).astype(jnp.bfloat16)
    value_all = jnp.dot(normed_one, wv, preferred_element_type=jnp.float32).astype(jnp.bfloat16)
    attended, log_total = lax.map(sequence_forward, (query_all.reshape(seq_count, SEQ, -1), key_all.reshape(seq_count, SEQ, -1), value_all.reshape(seq_count, SEQ, -1)))
    attended = attended.reshape(residual.shape[0], -1)
    middle = residual + jnp.dot(attended, wo, preferred_element_type=jnp.float32)
    normed_two = rms_normed(middle, gain_pair[1])
    gate_pre = jnp.dot(normed_two, wg, preferred_element_type=jnp.float32)
    up_pre = jnp.dot(normed_two, wu, preferred_element_type=jnp.float32)
    hidden = (gate_pre * jax.nn.sigmoid(gate_pre) * up_pre).astype(jnp.bfloat16)
    output = middle + jnp.dot(hidden, wd, preferred_element_type=jnp.float32)
    return (output, (normed_one, query_all, key_all, value_all, attended, log_total, middle, normed_two, gate_pre, up_pre, hidden))

def reference(hidden_in, positions, norm_gains, w_query, w_key, w_value, w_out, w_gate, w_up, w_down, out_grad):
    cosine_tab, sine_tab = rope_tables(positions)
    seq_count = hidden_in.shape[0] // SEQ
    inputs = []
    residual = hidden_in
    for layer_index in range(LAYERS):
        inputs.append(residual)
        residual, _ = layer_forward(residual, cosine_tab, sine_tab, norm_gains[layer_index], w_query[layer_index], w_key[layer_index], w_value[layer_index], w_out[layer_index], w_gate[layer_index], w_up[layer_index], w_down[layer_index])
    hidden_out = residual
    cotangent = out_grad
    results = [None] * LAYERS
    for layer_index in reversed(range(LAYERS)):
        gain_pair = norm_gains[layer_index]
        wq, wk, wv = (w_query[layer_index], w_key[layer_index], w_value[layer_index])
        wo, wg, wu, wd = (w_out[layer_index], w_gate[layer_index], w_up[layer_index], w_down[layer_index])
        layer_in = inputs[layer_index]
        _, saved = layer_forward(layer_in, cosine_tab, sine_tab, gain_pair, wq, wk, wv, wo, wg, wu, wd)
        normed_one, query_all, key_all, value_all, attended, log_total, middle, normed_two, gate_pre, up_pre, hidden = saved
        top_bf = cotangent.astype(jnp.bfloat16)
        grad_down = jnp.dot(hidden.T, top_bf, preferred_element_type=jnp.float32)
        grad_hidden = jnp.dot(top_bf, wd.T, preferred_element_type=jnp.float32)
        sigmoid_gate = jax.nn.sigmoid(gate_pre)
        grad_gate_pre = (grad_hidden * up_pre * sigmoid_gate * (1.0 + gate_pre * (1.0 - sigmoid_gate))).astype(jnp.bfloat16)
        grad_up_pre = (grad_hidden * gate_pre * sigmoid_gate).astype(jnp.bfloat16)
        grad_gate = jnp.dot(normed_two.T, grad_gate_pre, preferred_element_type=jnp.float32)
        grad_up = jnp.dot(normed_two.T, grad_up_pre, preferred_element_type=jnp.float32)
        grad_normed_two = jnp.dot(grad_gate_pre, wg.T, preferred_element_type=jnp.float32) + jnp.dot(grad_up_pre, wu.T, preferred_element_type=jnp.float32)
        grad_mid_norm, grad_gain_two = rms_back(middle, gain_pair[1], grad_normed_two)
        grad_middle = cotangent + grad_mid_norm
        middle_bf = grad_middle.astype(jnp.bfloat16)
        grad_out = jnp.dot(attended.T, middle_bf, preferred_element_type=jnp.float32)
        grad_attended = jnp.dot(middle_bf, wo.T, preferred_element_type=jnp.float32).astype(jnp.bfloat16)
        grads = lax.map(sequence_backward, (query_all.reshape(seq_count, SEQ, -1), key_all.reshape(seq_count, SEQ, -1), value_all.reshape(seq_count, SEQ, -1), log_total, grad_attended.reshape(seq_count, SEQ, -1)))
        grad_q = rotate_back(grads[0].reshape(hidden_in.shape[0], -1), cosine_tab, sine_tab).astype(jnp.bfloat16)
        grad_k = rotate_back(grads[1].reshape(hidden_in.shape[0], -1), cosine_tab, sine_tab).astype(jnp.bfloat16)
        grad_v = grads[2].reshape(hidden_in.shape[0], -1).astype(jnp.bfloat16)
        grad_query = jnp.dot(normed_one.T, grad_q, preferred_element_type=jnp.float32)
        grad_key = reduce_heads(jnp.dot(normed_one.T, grad_k, preferred_element_type=jnp.float32))
        grad_value = reduce_heads(jnp.dot(normed_one.T, grad_v, preferred_element_type=jnp.float32))
        grad_normed_one = jnp.dot(grad_q, wq.T, preferred_element_type=jnp.float32) + jnp.dot(grad_k, expand_heads(wk).T, preferred_element_type=jnp.float32) + jnp.dot(grad_v, expand_heads(wv).T, preferred_element_type=jnp.float32)
        grad_in_norm, grad_gain_one = rms_back(layer_in, gain_pair[0], grad_normed_one)
        cotangent = grad_middle + grad_in_norm
        results[layer_index] = (jnp.stack([grad_gain_one, grad_gain_two]), grad_query, grad_key, grad_value, grad_out, grad_gate, grad_up, grad_down)
    stacked = [jnp.stack([results[index][kind] for index in range(LAYERS)]) for kind in range(8)]
    return (hidden_out, cotangent, stacked[0], stacked[1], stacked[2], stacked[3], stacked[4], stacked[5], stacked[6], stacked[7])
```

```python
import functools

import jax
import jax.numpy as jnp
from jax import lax
from jax.experimental import pallas as pl
from jax.experimental.pallas import tpu as pltpu
from jax.sharding import PartitionSpec as P

H = 32
KV = 4
HD = 64
SEQ = 128
NORM_EPS = 1e-05
NEG_BIG = -1e30
SCALE = HD ** (-0.5)
LANES = 128
F32 = jnp.float32
BF16 = jnp.bfloat16


def dot(a, b):
    return jnp.dot(a, b, preferred_element_type=F32)


def dot_nt(a, b):
    return lax.dot_general(a, b, (((1,), (1,)), ((), ())), preferred_element_type=F32)


def dot_tn(a, b):
    return lax.dot_general(a, b, (((0,), (0,)), ((), ())), preferred_element_type=F32)


class Natural:
    def __init__(self, nd, nt):
        self.nd, self.nt = nd, nt
        self.order = list(range(nd))
        self.groups = [list(range(nt)) + ["kv"]]

    def permute(self, rows):
        return rows

    def roll_slots(self, vals, axis, sign):
        return vals

    def slots(self, vals):
        every = lax.all_gather(vals, "tensor")
        return [every[j] for j in range(self.nt)]

    slots_far = slots

    def blocks(self, vals):
        every = lax.all_gather(vals, "dp")
        return [every[k] for k in range(self.nd)]

    def sum_slots(self, parts):
        stacked = jnp.stack(parts).astype(BF16)
        return lax.psum_scatter(stacked, "tensor", scatter_dimension=0).astype(F32)

    sum_slots_far = sum_slots

    def sum_blocks(self, make, axis, kind=BF16):
        part = make(0, self.nd).astype(kind)
        return lax.psum_scatter(part, "dp", scatter_dimension=axis, tiled=True).astype(F32)


class Linked:
    def __init__(self):
        self.nd, self.nt = 8, 4
        self.order = [0, 2, 4, 6, 1, 3, 5, 7]
        self.groups = [[0], [1, 3], [2, "kv"]]

    def flip(self, vals, bits):
        return lax.ppermute(vals, "dp", [(i, i ^ bits) for i in range(8)])

    def rotate(self, vals, by):
        return lax.ppermute(vals, "tensor", [(i, (i - by) % 4) for i in range(4)])

    def permute(self, rows):
        width = rows.shape[1] // 8
        here = lax.axis_index("dp")
        pieces = [
            lax.dynamic_slice_in_dim(rows, (here ^ k) * width, width, 1) for k in self.order
        ]
        return jnp.concatenate(pieces, 1)

    def unpermute(self, rows):
        width = rows.shape[1] // 8
        here = lax.axis_index("dp")
        pieces = []
        for k in range(8):
            rel = here ^ k
            place = jnp.where(rel % 2 == 0, rel // 2, 4 + rel // 2)
            pieces.append(lax.dynamic_slice_in_dim(rows, place * width, width, 1))
        return jnp.concatenate(pieces, 1)

    def roll_slots(self, vals, axis, sign):
        z = lax.axis_index("tensor")
        width = vals.shape[axis] // 4
        out = vals
        for by in (1, 2, 3):
            out = jnp.where(z == by, jnp.roll(vals, -sign * by * width, axis), out)
        return out

    def slots(self, vals):
        z = lax.axis_index("tensor")
        right, left = [], []
        r = l = vals
        for step in range(3):
            r = lax.ppermute(r, "tensor", [(i, i + 1) for i in range(step, 3)])
            l = lax.ppermute(l, "tensor", [(i, i - 1) for i in range(1, 4 - step)])
            right.append(r)
            left.append(l)
        return [
            vals,
            jnp.where(z <= 2, left[0], right[2]),
            jnp.where(z <= 1, left[1], right[1]),
            jnp.where(z >= 1, right[0], left[2]),
        ]

    def slots_far(self, vals):
        return [vals] + [self.rotate(vals, j) for j in (1, 2, 3)]

    def blocks(self, vals):
        half = vals.shape[0] // 2
        got = {0: vals, 2: self.flip(vals, 2), 4: self.flip(vals, 4)}
        upper = self.flip(got[2][:half], 4)
        lower = self.flip(got[4][half:], 2)
        got[1] = self.flip(vals, 1)
        got[3] = self.flip(got[2], 1)
        got[5] = self.flip(got[4], 1)
        got[6] = jnp.concatenate([upper, lower])
        got[7] = jnp.concatenate([self.flip(upper, 1), self.flip(lower, 1)])
        return [got[k] for k in self.order]

    def sum_slots(self, parts):
        r = l = None
        for step in (1, 2, 3):
            to_right = parts[4 - step] if r is None else parts[4 - step].astype(F32) + r
            to_left = parts[step] if l is None else parts[step].astype(F32) + l
            r = lax.ppermute(to_right.astype(BF16), "tensor", [(i, i + 1) for i in range(step)])
            l = lax.ppermute(
                to_left.astype(BF16), "tensor", [(i, i - 1) for i in range(4 - step, 4)]
            )
            r, l = r.astype(F32), l.astype(F32)
        return parts[0].astype(F32) + r + l

    def sum_slots_far(self, parts):
        total = parts[0].astype(F32)
        for j in (1, 2, 3):
            total = total + self.rotate(parts[j].astype(BF16), -j).astype(F32)
        return total

    def sum_blocks(self, make, axis, kind=BF16):
        other = self.flip(make(4, 4).astype(kind), 1)
        mine = (make(0, 4) + other.astype(F32)).astype(kind)
        width = mine.shape[axis] // 4
        half = (width if axis == 0 else mine.shape[0]) // 2

        def piece(chip, part):
            block = lax.slice_in_dim(mine, chip * width, (chip + 1) * width, axis=axis)
            return block[:half] if part == 0 else block[half:]

        along_x = self.flip(jnp.stack([piece(1, 0), piece(3, 0)]), 2).astype(F32)
        along_y = self.flip(jnp.stack([piece(2, 1), piece(3, 1)]), 4).astype(F32)
        then_y = self.flip((piece(2, 0).astype(F32) + along_x[1]).astype(kind), 4)
        then_x = self.flip((piece(1, 1).astype(F32) + along_y[1]).astype(kind), 2)
        upper = piece(0, 0).astype(F32) + along_x[0] + then_y.astype(F32)
        lower = piece(0, 1).astype(F32) + along_y[0] + then_x.astype(F32)
        return jnp.concatenate([upper, lower])


def lane_masks():
    lane = lax.broadcasted_iota(jnp.int32, (SEQ, LANES), 1)
    return lane % HD < HD // 2, lane < HD


def swap_halves(u, first):
    return jnp.where(first, pltpu.roll(u, LANES - HD // 2, 1), pltpu.roll(u, HD // 2, 1))


def twice(tile, index, low):
    turned = pltpu.roll(tile, HD, 1)
    return jnp.where(low, tile, turned) if index % 2 == 0 else jnp.where(low, turned, tile)


def causal_probs(query, key):
    scores = dot_nt(query, key) * SCALE
    rows = lax.broadcasted_iota(jnp.int32, scores.shape, 0)
    cols = lax.broadcasted_iota(jnp.int32, scores.shape, 1)
    scores = jnp.where(cols <= rows, scores, NEG_BIG)
    weights = jnp.exp(scores - jnp.max(scores, -1, keepdims=True))
    return weights * (1.0 / jnp.sum(weights, -1, keepdims=True))


def layout_of(groups, slot_width):
    places = {}
    for index, group in enumerate(groups):
        offset = 0
        for item in group:
            places[item] = (index, offset)
            offset += slot_width if item != "kv" else 2 * KV * HD
    return places


def attend_kernel(groups, slot_width, cos_ref, sin_ref, *refs):
    ins = refs[: len(groups)]
    q_out, kv_out, o_out = refs[len(groups) :]
    places = layout_of(groups, slot_width)
    cos, sin = cos_ref[...], sin_ref[...]
    first, low = lane_masks()

    def turn(u):
        return u * cos + swap_halves(u, first) * sin

    where_kv, kv_at = places["kv"]
    keys, vals_low, vals_high = [], [], []
    for tile in range(KV // 2):
        at = kv_at + tile * LANES
        key = turn(ins[where_kv][:, at : at + LANES])
        val = ins[where_kv][:, at + KV * HD : at + KV * HD + LANES]
        kv_out[:, tile * LANES : (tile + 1) * LANES] = key.astype(BF16)
        kv_out[:, KV * HD + tile * LANES : KV * HD + (tile + 1) * LANES] = val.astype(BF16)
        for index in (0, 1):
            keys.append(twice(key, index, low).astype(BF16))
            both = twice(val, index, low)
            vals_low.append(jnp.where(low, both, 0.0).astype(BF16))
            vals_high.append(jnp.where(low, 0.0, both).astype(BF16))
    for slot in range(H * HD // slot_width):
        which, offset = places[slot]
        for pair in range(slot_width // LANES):
            group = (slot * slot_width + pair * LANES) // (H // KV * HD)
            query = turn(ins[which][:, offset + pair * LANES : offset + (pair + 1) * LANES])
            p_low = causal_probs(jnp.where(low, query, 0.0).astype(BF16), keys[group])
            p_high = causal_probs(jnp.where(low, 0.0, query).astype(BF16), keys[group])
            at = slot * slot_width + pair * LANES
            q_out[:, at : at + LANES] = query.astype(BF16)
            o_out[:, at : at + LANES] = (
                dot(p_low.astype(BF16), vals_low[group]) + dot(p_high.astype(BF16), vals_high[group])
            ).astype(BF16)


def attend_back_kernel(groups, slot_width, cos_ref, sin_ref, q_ref, kv_ref, da_ref, *outs):
    places = layout_of(groups, slot_width)
    cos, sin = cos_ref[...], sin_ref[...]
    first, low = lane_masks()

    def turn_back(u):
        return (u * cos - swap_halves(u, first) * sin).astype(BF16)

    where_kv, kv_at = places["kv"]
    pair_total = H // KV * HD // LANES
    held = {}
    for group in range(KV):
        tile_at = group // 2 * LANES
        key = twice(kv_ref[:, tile_at : tile_at + LANES].astype(F32), group, low)
        val_at = KV * HD + tile_at
        val = twice(kv_ref[:, val_at : val_at + LANES].astype(F32), group, low).astype(BF16)
        key_low = jnp.where(low, key, 0.0).astype(BF16)
        key_high = jnp.where(low, 0.0, key).astype(BF16)
        key = key.astype(BF16)
        dk = jnp.zeros((SEQ, LANES), F32)
        dv = jnp.zeros((SEQ, LANES), F32)
        for pair in range(pair_total):
            at = group * pair_total * LANES + pair * LANES
            query = q_ref[:, at : at + LANES].astype(F32)
            grad = da_ref[:, at : at + LANES].astype(F32)
            dq = None
            for is_low in (True, False):
                if is_low:
                    query_h = jnp.where(low, query, 0.0).astype(BF16)
                    grad_h = jnp.where(low, grad, 0.0).astype(BF16)
                else:
                    query_h = jnp.where(low, 0.0, query).astype(BF16)
                    grad_h = jnp.where(low, 0.0, grad).astype(BF16)
                prob = causal_probs(query_h, key)
                grad_prob = dot_nt(grad_h, val)
                delta = jnp.sum(prob * grad_prob, -1, keepdims=True)
                ds = (prob * (grad_prob - delta) * SCALE).astype(BF16)
                term = dot(ds, key_low if is_low else key_high)
                dq = term if dq is None else dq + term
                dk = dk + dot_tn(ds, query_h)
                dv = dv + dot_tn(prob.astype(BF16), grad_h)
            slot, inner = divmod(at, slot_width)
            which, offset = places[slot]
            outs[which][:, offset + inner : offset + inner + LANES] = turn_back(dq)
        held[group] = (dk + pltpu.roll(dk, HD, 1), dv + pltpu.roll(dv, HD, 1))
    for tile in range(KV // 2):
        at = kv_at + tile * LANES
        dk = jnp.where(low, held[2 * tile][0], held[2 * tile + 1][0])
        dv = jnp.where(low, held[2 * tile][1], held[2 * tile + 1][1])
        outs[where_kv][:, at : at + LANES] = turn_back(dk)
        outs[where_kv][:, at + KV * HD : at + KV * HD + LANES] = dv.astype(BF16)


def group_widths(groups, slot_width):
    return [sum(slot_width if item != "kv" else 2 * KV * HD for item in g) for g in groups]


def row_spec(width):
    return pl.BlockSpec((SEQ, width), lambda i: (i, 0))


def attend(groups, slot_width, cos, sin, parts):
    rows = cos.shape[0]
    widths = group_widths(groups, slot_width)
    shapes = [(rows, H * HD), (rows, 2 * KV * HD), (rows, H * HD)]
    return pl.pallas_call(
        functools.partial(attend_kernel, groups, slot_width),
        grid=(rows // SEQ,),
        in_specs=[row_spec(LANES)] * 2 + [row_spec(w) for w in widths],
        out_specs=[row_spec(s[1]) for s in shapes],
        out_shape=[jax.ShapeDtypeStruct(s, BF16) for s in shapes],
        name="attend",
    )(cos, sin, *parts)


def attend_back(groups, slot_width, cos, sin, query, key_val, grad):
    rows = cos.shape[0]
    widths = group_widths(groups, slot_width)
    return pl.pallas_call(
        functools.partial(attend_back_kernel, groups, slot_width),
        grid=(rows // SEQ,),
        in_specs=[row_spec(LANES)] * 2 + [row_spec(H * HD), row_spec(2 * KV * HD), row_spec(H * HD)],
        out_specs=[row_spec(w) for w in widths],
        out_shape=[jax.ShapeDtypeStruct((rows, w), BF16) for w in widths],
        name="attend_back",
    )(cos, sin, query, key_val, grad)


def norm_scale(rows):
    return lax.rsqrt(jnp.mean(rows * rows, -1, keepdims=True) + NORM_EPS)


def norm_back(rows, gain, grad_normed):
    inv = norm_scale(rows)
    weighted = grad_normed * gain
    grad_gain = jnp.sum(grad_normed * rows * inv, 0)
    grad_rows = inv * weighted - rows * inv**3 * jnp.mean(weighted * rows, -1, keepdims=True)
    return grad_rows, grad_gain


def rope_tables(positions):
    half = jnp.arange(LANES, dtype=jnp.int32) % (HD // 2)
    inv_freq = 10000.0 ** (-(half.astype(F32) * 2.0 / HD))
    angles = positions.astype(F32)[:, None] * inv_freq[None, :]
    sign = jnp.where(jnp.arange(LANES) % HD < HD // 2, -1.0, 1.0).astype(F32)
    return jnp.cos(angles), jnp.sin(angles) * sign[None, :]


def on_device(
    comm, hidden_in, positions, norm_gains, w_query, w_key, w_value, w_out, w_gate, w_up, w_down, out_grad
):
    rows_dev, width = hidden_in.shape
    nt, nd = comm.nt, comm.nd
    slot_width = w_query.shape[2]
    ff = w_gate.shape[2]
    kv_rows = w_key.shape[1]
    unpermute = getattr(comm, "unpermute", comm.permute)
    z = lax.axis_index("tensor")

    wq_slots = comm.slots_far(w_query[0])
    kv_slots = comm.slots_far(jnp.concatenate([w_key[0], w_value[0]], 1))
    gain_slots = comm.slots_far(norm_gains[0])
    wkv = comm.roll_slots(jnp.concatenate(kv_slots), 0, -1)
    wkv = jnp.concatenate(
        [comm.roll_slots(wkv[:, : KV * HD], 1, 1), comm.roll_slots(wkv[:, KV * HD :], 1, 1)], 1
    )
    gains = jnp.concatenate(
        comm.blocks(comm.roll_slots(jnp.concatenate(gain_slots, 1), 1, -1)), 1
    ).astype(F32)
    sources = {**dict(enumerate(wq_slots)), "kv": wkv}
    w_groups = [
        jnp.concatenate(comm.blocks(jnp.concatenate([sources[item] for item in group], 1)))
        for group in comm.groups
    ]
    wo_slots = comm.slots_far(w_out[0])
    wo = jnp.concatenate(comm.blocks(jnp.concatenate(wo_slots)), 1)

    wgu = jnp.concatenate(comm.blocks(jnp.concatenate([w_gate[0], w_up[0]], 1)))
    wd = jnp.concatenate(comm.blocks(w_down[0]), 1)

    x = comm.permute(hidden_in)
    g = comm.permute(out_grad)
    my_positions = lax.dynamic_slice_in_dim(positions, z * rows_dev, rows_dev)
    cos, sin = rope_tables(my_positions)

    normed_one = (x * norm_scale(x) * gains[0]).astype(BF16)
    parts = [dot(normed_one, w) for w in w_groups]
    query, key_val, attended = attend(comm.groups, slot_width, cos, sin, parts)
    middle = x + dot(attended, wo)

    normed_two = (middle * norm_scale(middle) * gains[1]).astype(BF16)
    n2 = jnp.concatenate(comm.slots(normed_two))
    top = jnp.concatenate(comm.slots(g.astype(BF16)))
    gate_up = dot(n2, wgu)
    gate_pre, up_pre = gate_up[:, :ff], gate_up[:, ff:]
    sig = jax.nn.sigmoid(gate_pre)
    hidden = (gate_pre * sig * up_pre).astype(BF16)
    grad_hidden = dot_nt(top, wd)
    grad_gate_pre = (grad_hidden * up_pre * sig * (1.0 + gate_pre * (1.0 - sig))).astype(BF16)
    grad_up_pre = (grad_hidden * gate_pre * sig).astype(BF16)
    grad_gu_pre = jnp.concatenate([grad_gate_pre, grad_up_pre], 1)

    def slots_of(rows):
        return [rows[j * rows_dev : (j + 1) * rows_dev] for j in range(nt)]

    grad_n2 = comm.sum_slots(slots_of(dot_nt(grad_gu_pre, wgu).astype(BF16)))
    output = middle + comm.sum_slots(slots_of(dot(hidden, wd).astype(BF16)))
    block = width // nd

    def cols(rows, start, count):
        return rows[:, start * block : (start + count) * block]

    grad_down = comm.sum_blocks(lambda s, c: dot_tn(hidden, cols(top, s, c)), 1)
    grad_gu = comm.sum_blocks(lambda s, c: dot_tn(cols(n2, s, c), grad_gu_pre), 0)

    grad_mid_norm, gain_two = norm_back(middle, gains[1], grad_n2)
    grad_middle = g + grad_mid_norm
    mid_bf = grad_middle.astype(BF16)
    grad_attended = dot_nt(mid_bf, wo).astype(BF16)
    grad_parts = attend_back(comm.groups, slot_width, cos, sin, query, key_val, grad_attended)
    grad_n1 = sum(dot_nt(part, w) for part, w in zip(grad_parts, w_groups))
    grad_in_norm, gain_one = norm_back(x, gains[0], grad_n1)
    grad_in = grad_middle + grad_in_norm

    grad_wo = comm.sum_blocks(lambda s, c: dot_tn(attended, cols(mid_bf, s, c)), 1)
    grad_out = comm.sum_slots_far(
        [grad_wo[j * slot_width : (j + 1) * slot_width] for j in range(nt)]
    )
    grad_all = jnp.concatenate(grad_parts, 1)
    grad_qkv = comm.sum_blocks(lambda s, c: dot_tn(cols(normed_one, s, c), grad_all), 0)
    widths = group_widths(comm.groups, slot_width)
    places = layout_of(comm.groups, slot_width)
    starts = [sum(widths[:i]) for i in range(len(widths))]

    def piece(item, size):
        which, offset = places[item]
        return grad_qkv[:, starts[which] + offset : starts[which] + offset + size]

    grad_query = comm.sum_slots_far([piece(j, slot_width) for j in range(nt)])
    grad_kv = piece("kv", 2 * KV * HD)
    grad_kv = jnp.concatenate(
        [comm.roll_slots(grad_kv[:, : KV * HD], 1, -1), comm.roll_slots(grad_kv[:, KV * HD :], 1, -1)], 1
    )
    grad_kv = comm.roll_slots(grad_kv, 0, 1)
    grad_kv = comm.sum_slots_far([grad_kv[j * kv_rows : (j + 1) * kv_rows] for j in range(nt)])

    gain_parts = jnp.stack([gain_one, gain_two])
    gain_sum = comm.sum_blocks(lambda s, c: cols(gain_parts, s, c), 1, F32)
    gain_sum = comm.roll_slots(gain_sum, 1, 1)
    own = width // nd // nt
    grad_gains = comm.sum_slots_far([gain_sum[:, j * own : (j + 1) * own] for j in range(nt)])

    return (
        unpermute(output),
        unpermute(grad_in),
        grad_gains[None],
        grad_query[None],
        grad_kv[None, :, : KV * HD],
        grad_kv[None, :, KV * HD :],
        grad_out[None],
        grad_gu[None, :, :ff],
        grad_gu[None, :, ff:],
        grad_down[None],
    )


def solution(mesh):
    nd, nt = mesh.shape["dp"], mesh.shape["tensor"]
    comm = Linked() if (nd, nt) == (8, 4) else Natural(nd, nt)
    rows = P(("dp", "tensor"), None)
    wide = P(None, "dp", "tensor")
    tall = P(None, "tensor", "dp")
    flat = P(None, ("dp", "tensor"), None)
    gain = P(None, None, ("dp", "tensor"))
    return jax.shard_map(
        functools.partial(on_device, comm),
        mesh=mesh,
        in_specs=(rows, P("dp"), gain, wide, flat, flat, tall, wide, wide, tall, rows),
        out_specs=(rows, rows, gain, wide, flat, flat, tall, wide, wide, tall),
        check_vma=False,
    )
```

```python
import functools

import jax
import jax.numpy as jnp
from jax import lax
from jax.experimental import pallas as pl
from jax.experimental.pallas import tpu as pltpu
from jax.sharding import PartitionSpec as P

H = 32
KV = 4
HD = 64
SEQ = 128
NORM_EPS = 1e-05
NEG_BIG = -1e30
SCALE = HD ** (-0.5)
LANES = 128
F32 = jnp.float32
BF16 = jnp.bfloat16


def dot(a, b):
    return jnp.dot(a, b, preferred_element_type=F32)


def dot_nt(a, b):
    return lax.dot_general(a, b, (((1,), (1,)), ((), ())), preferred_element_type=F32)


def dot_tn(a, b):
    return lax.dot_general(a, b, (((0,), (0,)), ((), ())), preferred_element_type=F32)


class Natural:
    def __init__(self, nd, nt):
        self.nd, self.nt = nd, nt

    def sum_rows(self, part):
        return lax.psum_scatter(part, "tensor", scatter_dimension=0, tiled=True).astype(F32)

    def sum_tensor(self, part, axis):
        return lax.psum_scatter(part.astype(BF16), "tensor", scatter_dimension=axis, tiled=True).astype(F32)

    def sum_blocks(self, left, right, axis, kind=BF16):
        part = (right if left is None else dot_tn(left, right)).astype(kind)
        return lax.psum_scatter(part, "dp", scatter_dimension=axis, tiled=True).astype(F32)


class Linked:
    order = [0, 2, 4, 6, 1, 3, 5, 7]

    def flip(self, vals, bits):
        return lax.ppermute(vals, "dp", [(i, i ^ bits) for i in range(8)])

    def permute(self, rows):
        width = rows.shape[1] // 8
        here = lax.axis_index("dp")
        return jnp.concatenate(
            [lax.dynamic_slice_in_dim(rows, (here ^ k) * width, width, 1) for k in self.order], 1
        )

    def slots_of(self, vals, axis):
        z = lax.axis_index("tensor")
        size = vals.shape[axis] // 4
        return [lax.dynamic_slice_in_dim(vals, (z + j) % 4 * size, size, axis) for j in range(4)]

    def sum_rows(self, part):
        parts = self.slots_of(part, 0)
        r = l = None
        for step in (1, 2, 3):
            to_right = parts[4 - step] if r is None else parts[4 - step].astype(F32) + r
            to_left = parts[step] if l is None else parts[step].astype(F32) + l
            r = lax.ppermute(to_right.astype(BF16), "tensor", [(i, i + 1) for i in range(step)])
            l = lax.ppermute(to_left.astype(BF16), "tensor", [(i, i - 1) for i in range(4 - step, 4)])
            r, l = r.astype(F32), l.astype(F32)
        return parts[0].astype(F32) + r + l

    def sum_tensor(self, part, axis):
        if part.shape[axis] // 4 % 128 and axis == 1:
            z = lax.axis_index("tensor")
            size = part.shape[1] // 4
            rolled = part
            for by in (1, 2, 3):
                rolled = jnp.where(z == by, jnp.roll(part, -by * size, 1), rolled)
            parts = [rolled[:, j * size : (j + 1) * size] for j in range(4)]
        else:
            parts = self.slots_of(part, axis)
        total = parts[0]
        for j in (1, 2, 3):
            sent = lax.ppermute(parts[j].astype(BF16), "tensor", [(i, (i + j) % 4) for i in range(4)])
            total = total + sent.astype(F32)
        return total

    def sum_blocks(self, left, right, axis, kind=BF16):
        if axis == 0:
            left = self.permute(left)
        else:
            right = self.permute(right)

        def make(half):
            picked = left if axis == 0 else right
            size = picked.shape[1] // 2
            picked = picked[:, half * size : (half + 1) * size]
            if left is None:
                return picked
            return dot_tn(picked, right) if axis == 0 else dot_tn(left, picked)

        other = self.flip(make(1).astype(kind), 1)
        mine = (make(0) + other.astype(F32)).astype(kind)
        width = mine.shape[axis] // 4
        half = (width if axis == 0 else mine.shape[0]) // 2

        def piece(chip, part):
            block = lax.slice_in_dim(mine, chip * width, (chip + 1) * width, axis=axis)
            return block[:half] if part == 0 else block[half:]

        along_x = self.flip(jnp.stack([piece(1, 0), piece(3, 0)]), 2).astype(F32)
        along_y = self.flip(jnp.stack([piece(2, 1), piece(3, 1)]), 4).astype(F32)
        then_y = self.flip((piece(2, 0).astype(F32) + along_x[1]).astype(kind), 4)
        then_x = self.flip((piece(1, 1).astype(F32) + along_y[1]).astype(kind), 2)
        upper = piece(0, 0).astype(F32) + along_x[0] + then_y.astype(F32)
        lower = piece(0, 1).astype(F32) + along_y[0] + then_x.astype(F32)
        return jnp.concatenate([upper, lower])


def lane_masks():
    lane = lax.broadcasted_iota(jnp.int32, (SEQ, LANES), 1)
    return lane % HD < HD // 2, lane < HD


def swap_halves(u, first):
    return jnp.where(first, pltpu.roll(u, LANES - HD // 2, 1), pltpu.roll(u, HD // 2, 1))


def twice(tile, index, low):
    turned = pltpu.roll(tile, HD, 1)
    return jnp.where(low, tile, turned) if index % 2 == 0 else jnp.where(low, turned, tile)


def causal_probs(query, key):
    scores = dot_nt(query, key) * SCALE
    rows = lax.broadcasted_iota(jnp.int32, scores.shape, 0)
    cols = lax.broadcasted_iota(jnp.int32, scores.shape, 1)
    scores = jnp.where(cols <= rows, scores, NEG_BIG)
    weights = jnp.exp(scores - jnp.max(scores, -1, keepdims=True))
    return weights * (1.0 / jnp.sum(weights, -1, keepdims=True))


def attend_sequence(cos, sin, load, kv_at, q_out, kv_out, o_out, at):
    first, low = lane_masks()

    def turn(u):
        return u * cos + swap_halves(u, first) * sin

    keys, vals_low, vals_high = [], [], []
    for tile in range(KV // 2):
        key = turn(load(kv_at + tile * LANES))
        val = load(kv_at + KV * HD + tile * LANES)
        kv_out[at, tile * LANES : (tile + 1) * LANES] = key.astype(BF16)
        kv_out[at, KV * HD + tile * LANES : KV * HD + (tile + 1) * LANES] = val.astype(BF16)
        for index in (0, 1):
            keys.append(twice(key, index, low).astype(BF16))
            both = twice(val, index, low)
            vals_low.append(jnp.where(low, both, 0.0).astype(BF16))
            vals_high.append(jnp.where(low, 0.0, both).astype(BF16))
    for pair in range(H // 2):
        group = pair * LANES // (H // KV * HD)
        query = turn(load(pair * LANES))
        p_low = causal_probs(jnp.where(low, query, 0.0).astype(BF16), keys[group])
        p_high = causal_probs(jnp.where(low, 0.0, query).astype(BF16), keys[group])
        q_out[at, pair * LANES : (pair + 1) * LANES] = query.astype(BF16)
        o_out[at, pair * LANES : (pair + 1) * LANES] = (
            dot(p_low.astype(BF16), vals_low[group]) + dot(p_high.astype(BF16), vals_high[group])
        ).astype(BF16)


def attend_back_sequence(cos, sin, q_ref, kv_ref, da_ref, dqkv_out, at):
    first, low = lane_masks()

    def turn_back(u):
        return (u * cos - swap_halves(u, first) * sin).astype(BF16)

    pair_total = H // KV * HD // LANES
    width = H * HD
    held = {}
    for group in range(KV):
        tile_at = group // 2 * LANES
        key = twice(kv_ref[at, tile_at : tile_at + LANES].astype(F32), group, low)
        val_at = KV * HD + tile_at
        val = twice(kv_ref[at, val_at : val_at + LANES].astype(F32), group, low).astype(BF16)
        key_low = jnp.where(low, key, 0.0).astype(BF16)
        key_high = jnp.where(low, 0.0, key).astype(BF16)
        key = key.astype(BF16)
        dk = jnp.zeros((SEQ, LANES), F32)
        dv = jnp.zeros((SEQ, LANES), F32)
        for pair in range(group * pair_total, (group + 1) * pair_total):
            query = q_ref[at, pair * LANES : (pair + 1) * LANES].astype(F32)
            grad = da_ref[at, pair * LANES : (pair + 1) * LANES].astype(F32)
            dq = None
            for is_low in (True, False):
                if is_low:
                    query_h = jnp.where(low, query, 0.0).astype(BF16)
                    grad_h = jnp.where(low, grad, 0.0).astype(BF16)
                else:
                    query_h = jnp.where(low, 0.0, query).astype(BF16)
                    grad_h = jnp.where(low, 0.0, grad).astype(BF16)
                prob = causal_probs(query_h, key)
                grad_prob = dot_nt(grad_h, val)
                delta = jnp.sum(prob * grad_prob, -1, keepdims=True)
                ds = (prob * (grad_prob - delta) * SCALE).astype(BF16)
                term = dot(ds, key_low if is_low else key_high)
                dq = term if dq is None else dq + term
                dk = dk + dot_tn(ds, query_h)
                dv = dv + dot_tn(prob.astype(BF16), grad_h)
            dqkv_out[at, pair * LANES : (pair + 1) * LANES] = turn_back(dq)
        held[group] = (dk + pltpu.roll(dk, HD, 1), dv + pltpu.roll(dv, HD, 1))
    for tile in range(KV // 2):
        col = width + tile * LANES
        dk = jnp.where(low, held[2 * tile][0], held[2 * tile + 1][0])
        dv = jnp.where(low, held[2 * tile][1], held[2 * tile + 1][1])
        dqkv_out[at, col : col + LANES] = turn_back(dk)
        dqkv_out[at, col + KV * HD : col + KV * HD + LANES] = dv.astype(BF16)


def attend_kernel(cos_ref, sin_ref, qkv_ref, q_out, kv_out, o_out):
    attend_sequence(
        cos_ref[...], sin_ref[...], lambda c: qkv_ref[:, c : c + LANES], H * HD, q_out, kv_out, o_out, slice(None)
    )


def attend_back_kernel(cos_ref, sin_ref, q_ref, kv_ref, da_ref, dqkv_out):
    attend_back_sequence(cos_ref[...], sin_ref[...], q_ref, kv_ref, da_ref, dqkv_out, slice(None))


def by_sequence(body, name, ins, widths):
    rows = ins[0].shape[0]
    spec = lambda w: pl.BlockSpec((SEQ, w), lambda i: (i, 0))
    return pl.pallas_call(
        body,
        grid=(rows // SEQ,),
        in_specs=[spec(a.shape[1]) for a in ins],
        out_specs=[spec(w) for w in widths],
        out_shape=[jax.ShapeDtypeStruct((rows, w), BF16) for w in widths],
        name=name,
    )(*ins)


def attend(cos, sin, qkv):
    return by_sequence(attend_kernel, "attend", (cos, sin, qkv), (H * HD, 2 * KV * HD, H * HD))


def attend_back(cos, sin, query, key_val, grad):
    return by_sequence(
        attend_back_kernel, "attend_back", (cos, sin, query, key_val, grad), (H * HD + 2 * KV * HD,)
    )[0]


def norm_scale(rows):
    return lax.rsqrt(jnp.mean(rows * rows, -1, keepdims=True) + NORM_EPS)


def norm_back(rows, gain, grad_normed):
    inv = norm_scale(rows)
    weighted = grad_normed * gain
    grad_gain = jnp.sum(grad_normed * rows * inv, 0)
    grad_rows = inv * weighted - rows * inv**3 * jnp.mean(weighted * rows, -1, keepdims=True)
    return grad_rows, grad_gain


def rope_tables(positions):
    half = jnp.arange(LANES, dtype=jnp.int32) % (HD // 2)
    inv_freq = 10000.0 ** (-(half.astype(F32) * 2.0 / HD))
    angles = positions.astype(F32)[:, None] * inv_freq[None, :]
    sign = jnp.where(jnp.arange(LANES) % HD < HD // 2, -1.0, 1.0).astype(F32)
    return jnp.cos(angles), jnp.sin(angles) * sign[None, :]


MESH = pl.DeviceIdType.MESH
KV_ROWS = 64
GAIN_ROWS = 16


class Links:
    def __init__(self):
        self.d, self.z = lax.axis_index("dp"), lax.axis_index("tensor")
        core, x, y = self.d % 2, self.d // 2 % 2, self.d // 4
        self.dc = self.d + 1 - 2 * core
        step_x, step_y = 2 - 4 * x, 4 - 8 * y
        self.dx, self.dy, self.dxy = self.d + step_x, self.d + step_y, self.d + step_x + step_y
        self.dcx, self.dcy, self.dcxy = self.dc + step_x, self.dc + step_y, self.dc + step_x + step_y

    def barrier(self):
        z = self.z
        sem = pltpu.get_barrier_semaphore()

        def greet(d, zz):
            pl.semaphore_signal(sem, inc=1, device_id=(d, zz), device_id_type=MESH)

        for d in (self.dx, self.dy, self.dc):
            greet(d, z)
        pl.when(z > 0)(lambda: greet(self.d, z - 1))
        pl.when(z < 3)(lambda: greet(self.d, z + 1))
        pl.semaphore_wait(sem, 3 + (z + 2) // 3 + (5 - z) // 3)


class Sender:
    def __init__(self, links, send_sem, recv_sem):
        self.links, self.send_sem, self.recv_sem = links, send_sem, recv_sem

    def copy(self, src, dst, at, to):
        return pltpu.make_async_remote_copy(
            src_ref=src,
            dst_ref=dst,
            send_sem=self.send_sem.at[at],
            recv_sem=self.recv_sem.at[at],
            device_id=to,
            device_id_type=MESH,
        )

    def start(self, src, dst, at, to):
        self.copy(src, dst, at, to).start()

    def landed(self, region, at):
        self.copy(region, region, at, (self.links.dc, self.links.z)).wait_recv()

    def sent(self, region, at):
        self.copy(region, region, at, (self.links.dc, self.links.z)).wait_send()


class Spread:
    def __init__(self, sender, region, base):
        self.s, self.region, self.base = sender, region, base

    def own(self, p, src):
        k, r, b = self.s.links, self.region, self.base + 9 * p
        mine = r(k.d, p, None)
        self.s.start(src, mine, b, (k.dx, k.z))
        self.s.start(src, mine, b + 1, (k.dy, k.z))
        self.s.start(src, mine, b + 2, (k.dc, k.z))

    def near(self, p):
        k, r, b = self.s.links, self.region, self.base + 9 * p
        self.s.landed(r(k.dx, p, None), b)
        self.s.start(r(k.dx, p, 0), r(k.dx, p, 0), b + 3, (k.dy, k.z))
        self.s.start(r(k.dx, p, None), r(k.dx, p, None), b + 5, (k.dc, k.z))
        self.s.landed(r(k.dy, p, None), b + 1)
        self.s.start(r(k.dy, p, 1), r(k.dy, p, 1), b + 4, (k.dx, k.z))
        self.s.start(r(k.dy, p, None), r(k.dy, p, None), b + 6, (k.dc, k.z))

    def far(self, p):
        k, r, b = self.s.links, self.region, self.base + 9 * p
        for part in (0, 1):
            self.s.landed(r(k.dxy, p, part), b + 3 + part)
            self.s.start(r(k.dxy, p, part), r(k.dxy, p, part), b + 7 + part, (k.dc, k.z))

    def finish(self, p):
        k, r, b = self.s.links, self.region, self.base + 9 * p
        self.s.landed(r(k.dc, p, None), b + 2)
        self.s.landed(r(k.dcx, p, None), b + 5)
        self.s.landed(r(k.dcy, p, None), b + 6)
        for part in (0, 1):
            self.s.landed(r(k.dcxy, p, part), b + 7 + part)

    def drain(self, p):
        k, r, b = self.s.links, self.region, self.base + 9 * p
        for i in (0, 1, 2):
            self.s.sent(r(k.d, p, None), b + i)
        self.s.sent(r(k.dx, p, 0), b + 3)
        self.s.sent(r(k.dy, p, 1), b + 4)
        self.s.sent(r(k.dx, p, None), b + 5)
        self.s.sent(r(k.dy, p, None), b + 6)
        for part in (0, 1):
            self.s.sent(r(k.dxy, p, part), b + 7 + part)


class Line:
    def __init__(self, sender, region, base):
        self.s, self.region, self.base = sender, region, base

    def _send(self, src, p, way, step):
        k = self.s.links
        self.s.start(src, self.region(p), self.base + 2 * (step - 1) + way, (k.d, k.z + 1 - 2 * way))

    def own(self, src):
        z = self.s.links.z
        pl.when(z < 3)(lambda: self._send(src, z, 0, 1))
        pl.when(z > 0)(lambda: self._send(src, z, 1, 1))

    def each(self, step, action):
        z = self.s.links.z
        pl.when(z >= step)(lambda: action(z - step, 0))
        pl.when(z + step <= 3)(lambda: action(z + step, 1))

    def arrive(self, step, then=None):
        z = self.s.links.z

        def action(p, way):
            self.s.landed(self.region(p), self.base + 2 * (step - 1) + way)
            if step < 3:
                ahead = z < 3 if way == 0 else z > 0
                pl.when(ahead)(lambda: self._send(self.region(p), p, way, step + 1))
            if then is not None:
                then(p)

        self.each(step, action)

    def drain(self):
        z = self.s.links.z
        for step in (1, 2, 3):
            for way in (0, 1):
                came = z - (step - 1) if way == 0 else z + (step - 1)
                ok = jnp.logical_and(z < 3, z >= step - 1) if way == 0 else jnp.logical_and(z > 0, z <= 4 - step)
                pl.when(ok)(
                    functools.partial(self.s.sent, self.region(came), self.base + 2 * (step - 1) + way)
                )


def forward_kernel(
    x_ref, g_ref, cos_ref, sin_ref, att_ref, wo_ref, gu_ref, wd_ref,
    wa_all, wo_all, gu_all, wd_all, n2_all, top_all, wqkv_all,
    q_out, kv_out, o_out, mid_out, gain_out,
    n1, qkv, w_buf, wkv_buf, gain_buf, wo_buf, n2, top, send_sem, recv_sem, local_sem,
):
    rows, width = x_ref.shape
    slot_width = att_ref.shape[1]
    block = width // 8
    links = Links()
    d, z = links.d, links.z
    s = Sender(links, send_sem, recv_sem)
    cut_a = att_ref.shape[0] // 32 * 16
    cuts_a = ((0, cut_a), (cut_a, att_ref.shape[0] - cut_a))

    def at_a(dd, p, part):
        if part is None:
            return wa_all.at[dd, p]
        return wa_all.at[dd, p, pl.ds(*cuts_a[part])]

    def at_b(dd, p, part):
        start, size = (0, slot_width) if part is None else (part * slot_width // 2, slot_width // 2)
        return wo_all.at[
            pl.ds(pl.multiple_of(p * slot_width + start, 16), size),
            pl.ds(pl.multiple_of(dd * block, 128), block),
        ]

    def at_gu(dd, p, part):
        start, size = (0, block) if part is None else (part * block // 2, block // 2)
        return gu_all.at[pl.ds(pl.multiple_of(dd * block + start, 16), size)]

    ff = wd_ref.shape[0]

    def at_wd(dd, p, part):
        start, size = (0, ff) if part is None else (part * ff // 2, ff // 2)
        return wd_all.at[pl.ds(start, size), pl.ds(pl.multiple_of(dd * block, 128), block)]

    def rows_of(ref):
        return lambda p: ref.at[pl.ds(pl.multiple_of(p * rows, 16), rows)]

    spread_a, spread_b = Spread(s, at_a, 0), Spread(s, at_b, 36)
    spread_gu, spread_wd = Spread(s, at_gu, 72), Spread(s, at_wd, 81)
    line_a = Line(s, lambda p: at_a(d, p, None), 90)
    line_b = Line(s, lambda p: at_b(d, p, None), 96)
    line_n, line_t = Line(s, rows_of(n2_all), 102), Line(s, rows_of(top_all), 108)

    def keep(src, dst, at):
        pltpu.make_async_copy(src, dst, local_sem.at[at]).start()

    def kept(src, dst, at):
        pltpu.make_async_copy(src, dst, local_sem.at[at]).wait()

    links.barrier()

    line_a.own(att_ref)
    spread_a.own(z, att_ref)
    keep(att_ref, at_a(d, z, None), 0)
    keep(wo_ref, at_b(d, z, None), 1)
    keep(gu_ref, at_gu(d, 0, None), 2)
    keep(wd_ref, at_wd(d, 0, None), 3)
    top[...] = g_ref[...].astype(BF16)
    line_a.arrive(1, lambda p: spread_a.own(p, at_a(d, p, None)))
    spread_a.near(z)
    line_a.arrive(2, lambda p: spread_a.own(p, at_a(d, p, None)))
    line_b.own(wo_ref)
    line_a.each(1, lambda p, way: spread_a.near(p))
    spread_a.far(z)
    line_a.arrive(3, lambda p: spread_a.own(p, at_a(d, p, None)))
    line_b.arrive(1)
    line_a.each(2, lambda p, way: spread_a.near(p))
    line_a.each(1, lambda p, way: spread_a.far(p))
    spread_b.own(z, wo_ref)
    line_b.each(1, lambda p, way: spread_b.own(p, at_b(d, p, None)))
    line_a.each(3, lambda p, way: spread_a.near(p))
    line_b.arrive(2, lambda p: spread_b.own(p, at_b(d, p, None)))
    line_a.each(2, lambda p, way: spread_a.far(p))
    line_b.arrive(3, lambda p: spread_b.own(p, at_b(d, p, None)))
    line_t.own(top)
    line_a.each(3, lambda p, way: spread_a.far(p))
    kept(att_ref, at_a(d, z, None), 0)
    for p in range(4):
        spread_a.finish(p)
    spread_gu.own(0, gu_ref)

    for p in range(4):
        keep(wa_all.at[:, p, pl.ds(0, block)], w_buf.at[p], 4 + p)
    keep(wa_all.at[:, :, pl.ds(block, KV_ROWS)], wkv_buf, 8)
    keep(wa_all.at[:, :, pl.ds(block + KV_ROWS, GAIN_ROWS), pl.ds(0, LANES)], gain_buf, 9)
    kept(wa_all.at[:, :, pl.ds(block + KV_ROWS, GAIN_ROWS), pl.ds(0, LANES)], gain_buf, 9)
    low_row = lax.broadcasted_iota(jnp.int32, (GAIN_ROWS, LANES), 1) < HD
    for dd in range(8):
        for half in (0, 1):
            first = gain_buf[dd, 2 * half].astype(F32)
            second = pltpu.roll(gain_buf[dd, 2 * half + 1].astype(F32), HD, 1)
            at = dd * block + half * LANES
            gain_out[:, at : at + LANES] = jnp.where(low_row, first, second)[:8]
    x = x_ref[...]
    n1[...] = (x * norm_scale(x) * gain_out[0:1]).astype(BF16)
    for p in range(4):
        kept(wa_all.at[:, p, pl.ds(0, block)], w_buf.at[p], 4 + p)
        qkv[:, p * slot_width : (p + 1) * slot_width] = dot(
            n1[...], w_buf[p].reshape(width, slot_width)
        )
        keep(w_buf.at[p], wqkv_all.at[:, :, pl.ds(p * slot_width, slot_width)], 4 + p)
    kept(wa_all.at[:, :, pl.ds(block, KV_ROWS)], wkv_buf, 8)
    qkv[:, width:] = dot(n1[...], wkv_buf[...].reshape(width, 2 * KV * HD))
    for p in range(4):
        keep(
            wkv_buf.at[:, p],
            wqkv_all.at[:, pl.ds(p * KV_ROWS, KV_ROWS), pl.ds(width, 2 * KV * HD)],
            10 + p,
        )

    line_t.arrive(1)
    line_b_pieces = lambda action: [action(z)] + [line_b.each(i, lambda p, way: action(p)) for i in (1, 2, 3)]

    def sequence(i, carry):
        at = pl.ds(pl.multiple_of(i * SEQ, SEQ), SEQ)
        attend_sequence(
            cos_ref[at], sin_ref[at], lambda c: qkv[at, c : c + LANES], width, q_out, kv_out, o_out, at
        )

        @pl.when(i == 0)
        def _():
            line_b_pieces(spread_b.near)

        return carry

    lax.fori_loop(0, rows // SEQ, sequence, 0)
    line_t.arrive(2)
    line_b_pieces(spread_b.far)
    spread_wd.own(0, wd_ref)
    kept(wo_ref, at_b(d, z, None), 1)
    for p in range(4):
        spread_b.finish(p)
    keep(wo_all, wo_buf, 0)
    kept(wo_all, wo_buf, 0)

    def column(i, carry):
        at = pl.ds(pl.multiple_of(i * 256, 256), 256)
        mid_out[:, at] = x_ref[:, at] + dot(o_out[...], wo_buf[:, at])
        return carry

    lax.fori_loop(0, width // 256, column, 0)
    mid = mid_out[...]
    n2[...] = (mid * norm_scale(mid) * gain_out[1:2]).astype(BF16)

    line_n.own(n2)
    keep(n2, n2_all.at[pl.ds(pl.multiple_of(z * rows, 16), rows)], 8)
    keep(top, top_all.at[pl.ds(pl.multiple_of(z * rows, 16), rows)], 9)
    line_t.arrive(3)
    spread_gu.near(0)
    line_n.arrive(1)
    spread_gu.far(0)
    spread_wd.near(0)
    line_n.arrive(2)
    spread_wd.far(0)
    line_n.arrive(3)
    spread_gu.finish(0)
    spread_wd.finish(0)

    kept(gu_ref, at_gu(d, 0, None), 2)
    kept(wd_ref, at_wd(d, 0, None), 3)
    for p in range(4):
        kept(w_buf.at[p], wqkv_all.at[:, :, pl.ds(p * slot_width, slot_width)], 4 + p)
        kept(
            wkv_buf.at[:, p],
            wqkv_all.at[:, pl.ds(p * KV_ROWS, KV_ROWS), pl.ds(width, 2 * KV * HD)],
            10 + p,
        )
    kept(n2, n2_all.at[pl.ds(pl.multiple_of(z * rows, 16), rows)], 8)
    kept(top, top_all.at[pl.ds(pl.multiple_of(z * rows, 16), rows)], 9)
    for p in range(4):
        spread_a.drain(p)
        spread_b.drain(p)
    spread_gu.drain(0)
    spread_wd.drain(0)
    for line in (line_a, line_b, line_n, line_t):
        line.drain()


def forward_stage(x, g, cos, sin, att, wo, gu, wd):
    rows, width = x.shape
    slot_width = att.shape[1]
    block = width // 8
    kv_width = 2 * KV * HD
    ff = wd.shape[0]
    vmem = pl.BlockSpec(memory_space=pltpu.VMEM)
    hbm = pl.BlockSpec(memory_space=pltpu.HBM)
    shape = jax.ShapeDtypeStruct
    outs = [
        (hbm, shape((8, 4) + att.shape, BF16)),
        (hbm, shape((width, width), BF16)),
        (hbm, shape((width, gu.shape[1]), BF16)),
        (hbm, shape((ff, width), BF16)),
        (hbm, shape((4 * rows, width), BF16)),
        (hbm, shape((4 * rows, width), BF16)),
        (hbm, shape((8, block, width + kv_width), BF16)),
        (vmem, shape((rows, width), BF16)),
        (vmem, shape((rows, kv_width), BF16)),
        (vmem, shape((rows, width), BF16)),
        (vmem, shape((rows, width), F32)),
        (vmem, shape((8, width), F32)),
    ]
    return pl.pallas_call(
        forward_kernel,
        in_specs=[vmem] * 8,
        out_specs=[o[0] for o in outs],
        out_shape=[o[1] for o in outs],
        scratch_shapes=[
            pltpu.VMEM((rows, width), BF16),
            pltpu.VMEM((rows, width + kv_width), F32),
            pltpu.VMEM((4, 8, block, slot_width), BF16),
            pltpu.VMEM((8, 4, KV_ROWS, kv_width), BF16),
            pltpu.VMEM((8, 4, GAIN_ROWS, LANES), BF16),
            pltpu.VMEM((width, width), BF16),
            pltpu.VMEM((rows, width), BF16),
            pltpu.VMEM((rows, width), BF16),
            pltpu.SemaphoreType.DMA((114,)),
            pltpu.SemaphoreType.DMA((114,)),
            pltpu.SemaphoreType.DMA((14,)),
        ],
        compiler_params=pltpu.CompilerParams(
            collective_id=0, has_side_effects=True, vmem_limit_bytes=62 * 1024 * 1024
        ),
        name="forward",
    )(x, g, cos, sin, att, wo, gu, wd)


def plain_forward(x, g, cos, sin, w_query, w_kv, gains, w_out, w_gu, w_down):
    both = ("dp", "tensor")
    gather = lax.all_gather

    def whole(shard, dims):
        for dim, axis in dims:
            shard = gather(shard, axis, axis=dim, tiled=True)
        return shard

    wq = whole(w_query, ((1, "tensor"), (0, "dp")))
    wqkv = jnp.concatenate([wq, whole(w_kv, ((0, both),))], 1)
    gain = whole(gains, ((1, both),)).astype(F32)
    wo = whole(w_out, ((0, "tensor"), (1, "dp")))
    wgu = whole(w_gu, ((0, "dp"),))
    wd = whole(w_down, ((1, "dp"),))
    normed = (x * norm_scale(x) * gain[0]).astype(BF16)
    query, key_val, attended = attend(cos, sin, dot(normed, wqkv))
    middle = x + dot(attended, wo)
    normed_two = (middle * norm_scale(middle) * gain[1]).astype(BF16)
    n2 = gather(normed_two, "tensor", axis=0, tiled=True)
    top = gather(g.astype(BF16), "tensor", axis=0, tiled=True)
    return wqkv, gain, wo, wgu, wd, n2, top, query, key_val, attended, middle


def linked_forward(x, g, cos, sin, w_query, w_kv, gains, w_out, w_gu, w_down):
    rows, width = x.shape
    slot = w_query.shape[1]
    padded = jnp.pad(gains, ((0, GAIN_ROWS - 2), (0, slot - gains.shape[1])))
    piece = jnp.concatenate([w_query, w_kv, padded])
    (_, wo, wgu, wd, n2, top, wqkv, query, key_val, attended, middle, gain) = forward_stage(
        x, g, cos, sin, piece, w_out, w_gu, w_down
    )
    wqkv = wqkv.reshape(width, -1)
    return wqkv, gain[:2], wo, wgu, wd, n2, top, query, key_val, attended, middle


def on_device(
    linked, nd, nt,
    hidden_in, positions, norm_gains, w_query, w_key, w_value, w_out, w_gate, w_up, w_down, out_grad,
):
    x, g = hidden_in, out_grad
    rows, width = x.shape
    ff = w_gate.shape[2]
    kv_width = 2 * KV * HD
    z = lax.axis_index("tensor")
    comm = Linked() if linked else Natural(nd, nt)

    cos, sin = rope_tables(lax.dynamic_slice_in_dim(positions, z * rows, rows))
    forward = linked_forward if linked else plain_forward
    wqkv, gains, wo, wgu, wd, n2, top, query, key_val, attended, middle = forward(
        x, g, cos, sin,
        w_query[0],
        jnp.concatenate([w_key[0], w_value[0]], 1),
        norm_gains[0],
        w_out[0],
        jnp.concatenate([w_gate[0], w_up[0]], 1),
        w_down[0],
    )

    gate_up = dot(n2, wgu)
    gate_pre, up_pre = gate_up[:, :ff], gate_up[:, ff:]
    sig = jax.nn.sigmoid(gate_pre)
    hidden = (gate_pre * sig * up_pre).astype(BF16)
    grad_hidden = dot_nt(top, wd)
    grad_gate_pre = (grad_hidden * up_pre * sig * (1.0 + gate_pre * (1.0 - sig))).astype(BF16)
    grad_up_pre = (grad_hidden * gate_pre * sig).astype(BF16)
    grad_gu_pre = jnp.concatenate([grad_gate_pre, grad_up_pre], 1)

    grad_n2 = comm.sum_rows(dot_nt(grad_gu_pre, wgu).astype(BF16))
    output = middle + comm.sum_rows(dot(hidden, wd).astype(BF16))
    grad_down = comm.sum_blocks(hidden, top, 1)
    grad_gu = comm.sum_blocks(n2, grad_gu_pre, 0)

    grad_mid_norm, gain_two = norm_back(middle, gains[1], grad_n2)
    grad_middle = g + grad_mid_norm
    mid_bf = grad_middle.astype(BF16)
    grad_attended = dot_nt(mid_bf, wo).astype(BF16)
    grad_qkv_rows = attend_back(cos, sin, query, key_val, grad_attended)
    grad_n1 = dot_nt(grad_qkv_rows, wqkv)
    grad_in_norm, gain_one = norm_back(x, gains[0], grad_n1)
    grad_in = grad_middle + grad_in_norm

    normed_one = (x * norm_scale(x) * gains[0]).astype(BF16)
    grad_out = comm.sum_tensor(comm.sum_blocks(attended, mid_bf, 1), 0)
    grad_qkv = comm.sum_blocks(normed_one, grad_qkv_rows, 0)
    grad_query = comm.sum_tensor(grad_qkv[:, :width], 1)
    grad_kv = comm.sum_tensor(grad_qkv[:, width:], 0)
    grad_gains = comm.sum_tensor(comm.sum_blocks(None, jnp.stack([gain_one, gain_two]), 1, F32), 1)

    return (
        output,
        grad_in,
        grad_gains[None],
        grad_query[None],
        grad_kv[None, :, : KV * HD],
        grad_kv[None, :, KV * HD :],
        grad_out[None],
        grad_gu[None, :, :ff],
        grad_gu[None, :, ff:],
        grad_down[None],
    )


def solution(mesh):
    nd, nt = mesh.shape["dp"], mesh.shape["tensor"]
    rows = P(("dp", "tensor"), None)
    wide = P(None, "dp", "tensor")
    tall = P(None, "tensor", "dp")
    flat = P(None, ("dp", "tensor"), None)
    gain = P(None, None, ("dp", "tensor"))
    return jax.shard_map(
        functools.partial(on_device, (nd, nt) == (8, 4), nd, nt),
        mesh=mesh,
        in_specs=(rows, P("dp"), gain, wide, flat, flat, tall, wide, wide, tall, rows),
        out_specs=(rows, rows, gain, wide, flat, flat, tall, wide, wide, tall),
        check_vma=False,
    )
```

```python
import functools

import jax
import jax.numpy as jnp
from jax import lax
from jax.experimental import pallas as pl
from jax.experimental.pallas import tpu as pltpu
from jax.sharding import PartitionSpec as P

H = 32
KV = 4
HD = 64
SEQ = 128
NORM_EPS = 1e-05
NEG_BIG = -1e30
SCALE = HD ** (-0.5)
LANES = 128
F32 = jnp.float32
BF16 = jnp.bfloat16


def dot(a, b):
    return jnp.dot(a, b, preferred_element_type=F32)


def dot_nt(a, b):
    return lax.dot_general(a, b, (((1,), (1,)), ((), ())), preferred_element_type=F32)


def dot_tn(a, b):
    return lax.dot_general(a, b, (((0,), (0,)), ((), ())), preferred_element_type=F32)


def lane_masks():
    lane = lax.broadcasted_iota(jnp.int32, (SEQ, LANES), 1)
    return lane % HD < HD // 2, lane < HD


def swap_halves(u, first):
    return jnp.where(first, pltpu.roll(u, LANES - HD // 2, 1), pltpu.roll(u, HD // 2, 1))


def twice(tile, index, low):
    turned = pltpu.roll(tile, HD, 1)
    return jnp.where(low, tile, turned) if index % 2 == 0 else jnp.where(low, turned, tile)


def causal_probs(query, key):
    scores = dot_nt(query, key) * SCALE
    rows = lax.broadcasted_iota(jnp.int32, scores.shape, 0)
    cols = lax.broadcasted_iota(jnp.int32, scores.shape, 1)
    scores = jnp.where(cols <= rows, scores, NEG_BIG)
    weights = jnp.exp(scores - jnp.max(scores, -1, keepdims=True))
    return weights * (1.0 / jnp.sum(weights, -1, keepdims=True))


def attend_sequence(cos, sin, load, kv_at, q_out, kv_out, o_out, at):
    first, low = lane_masks()

    def turn(u):
        return u * cos + swap_halves(u, first) * sin

    keys, vals_low, vals_high = [], [], []
    for tile in range(KV // 2):
        key = turn(load(kv_at + tile * LANES))
        val = load(kv_at + KV * HD + tile * LANES)
        kv_out[at, tile * LANES : (tile + 1) * LANES] = key.astype(BF16)
        kv_out[at, KV * HD + tile * LANES : KV * HD + (tile + 1) * LANES] = val.astype(BF16)
        for index in (0, 1):
            keys.append(twice(key, index, low).astype(BF16))
            both = twice(val, index, low)
            vals_low.append(jnp.where(low, both, 0.0).astype(BF16))
            vals_high.append(jnp.where(low, 0.0, both).astype(BF16))
    for pair in range(H // 2):
        group = pair * LANES // (H // KV * HD)
        query = turn(load(pair * LANES))
        p_low = causal_probs(jnp.where(low, query, 0.0).astype(BF16), keys[group])
        p_high = causal_probs(jnp.where(low, 0.0, query).astype(BF16), keys[group])
        q_out[at, pair * LANES : (pair + 1) * LANES] = query.astype(BF16)
        o_out[at, pair * LANES : (pair + 1) * LANES] = (
            dot(p_low.astype(BF16), vals_low[group]) + dot(p_high.astype(BF16), vals_high[group])
        ).astype(BF16)


def attend_back_sequence(cos, sin, q_ref, kv_ref, da_ref, dqkv_out, at):
    first, low = lane_masks()

    def turn_back(u):
        return (u * cos - swap_halves(u, first) * sin).astype(BF16)

    pair_total = H // KV * HD // LANES
    width = H * HD
    held = {}
    for group in range(KV):
        tile_at = group // 2 * LANES
        key = twice(kv_ref[at, tile_at : tile_at + LANES].astype(F32), group, low)
        val_at = KV * HD + tile_at
        val = twice(kv_ref[at, val_at : val_at + LANES].astype(F32), group, low).astype(BF16)
        key_low = jnp.where(low, key, 0.0).astype(BF16)
        key_high = jnp.where(low, 0.0, key).astype(BF16)
        key = key.astype(BF16)
        dk = jnp.zeros((SEQ, LANES), F32)
        dv = jnp.zeros((SEQ, LANES), F32)
        for pair in range(group * pair_total, (group + 1) * pair_total):
            query = q_ref[at, pair * LANES : (pair + 1) * LANES].astype(F32)
            grad = da_ref[at, pair * LANES : (pair + 1) * LANES].astype(F32)
            dq = None
            for is_low in (True, False):
                if is_low:
                    query_h = jnp.where(low, query, 0.0).astype(BF16)
                    grad_h = jnp.where(low, grad, 0.0).astype(BF16)
                else:
                    query_h = jnp.where(low, 0.0, query).astype(BF16)
                    grad_h = jnp.where(low, 0.0, grad).astype(BF16)
                prob = causal_probs(query_h, key)
                grad_prob = dot_nt(grad_h, val)
                delta = jnp.sum(prob * grad_prob, -1, keepdims=True)
                ds = (prob * (grad_prob - delta) * SCALE).astype(BF16)
                term = dot(ds, key_low if is_low else key_high)
                dq = term if dq is None else dq + term
                dk = dk + dot_tn(ds, query_h)
                dv = dv + dot_tn(prob.astype(BF16), grad_h)
            dqkv_out[at, pair * LANES : (pair + 1) * LANES] = turn_back(dq)
        held[group] = (dk + pltpu.roll(dk, HD, 1), dv + pltpu.roll(dv, HD, 1))
    for tile in range(KV // 2):
        col = width + tile * LANES
        dk = jnp.where(low, held[2 * tile][0], held[2 * tile + 1][0])
        dv = jnp.where(low, held[2 * tile][1], held[2 * tile + 1][1])
        dqkv_out[at, col : col + LANES] = turn_back(dk)
        dqkv_out[at, col + KV * HD : col + KV * HD + LANES] = dv.astype(BF16)


def attend_kernel(cos_ref, sin_ref, qkv_ref, q_out, kv_out, o_out):
    attend_sequence(
        cos_ref[...], sin_ref[...], lambda c: qkv_ref[:, c : c + LANES], H * HD, q_out, kv_out, o_out, slice(None)
    )


def attend_back_kernel(cos_ref, sin_ref, q_ref, kv_ref, da_ref, dqkv_out):
    attend_back_sequence(cos_ref[...], sin_ref[...], q_ref, kv_ref, da_ref, dqkv_out, slice(None))


def by_sequence(body, name, ins, widths):
    rows = ins[0].shape[0]
    spec = lambda w: pl.BlockSpec((SEQ, w), lambda i: (i, 0))
    return pl.pallas_call(
        body,
        grid=(rows // SEQ,),
        in_specs=[spec(a.shape[1]) for a in ins],
        out_specs=[spec(w) for w in widths],
        out_shape=[jax.ShapeDtypeStruct((rows, w), BF16) for w in widths],
        name=name,
    )(*ins)


def attend(cos, sin, qkv):
    return by_sequence(attend_kernel, "attend", (cos, sin, qkv), (H * HD, 2 * KV * HD, H * HD))


def attend_back(cos, sin, query, key_val, grad):
    return by_sequence(
        attend_back_kernel, "attend_back", (cos, sin, query, key_val, grad), (H * HD + 2 * KV * HD,)
    )[0]


def norm_scale(rows):
    return lax.rsqrt(jnp.mean(rows * rows, -1, keepdims=True) + NORM_EPS)


def norm_back(rows, gain, grad_normed):
    inv = norm_scale(rows)
    weighted = grad_normed * gain
    grad_gain = jnp.sum(grad_normed * rows * inv, 0)
    grad_rows = inv * weighted - rows * inv**3 * jnp.mean(weighted * rows, -1, keepdims=True)
    return grad_rows, grad_gain


def rope_tables(positions):
    half = jnp.arange(LANES, dtype=jnp.int32) % (HD // 2)
    inv_freq = 10000.0 ** (-(half.astype(F32) * 2.0 / HD))
    angles = positions.astype(F32)[:, None] * inv_freq[None, :]
    sign = jnp.where(jnp.arange(LANES) % HD < HD // 2, -1.0, 1.0).astype(F32)
    return jnp.cos(angles), jnp.sin(angles) * sign[None, :]


MESH = pl.DeviceIdType.MESH
KV_ROWS = 64
GAIN_ROWS = 16


class Links:
    def __init__(self):
        self.d, self.z = lax.axis_index("dp"), lax.axis_index("tensor")
        core, x, y = self.d % 2, self.d // 2 % 2, self.d // 4
        self.dc = self.d + 1 - 2 * core
        step_x, step_y = 2 - 4 * x, 4 - 8 * y
        self.dx, self.dy, self.dxy = self.d + step_x, self.d + step_y, self.d + step_x + step_y
        self.dcx, self.dcy, self.dcxy = self.dc + step_x, self.dc + step_y, self.dc + step_x + step_y

    def barrier(self, far=False):
        z = self.z
        sem = pltpu.get_barrier_semaphore()

        def greet(d, zz):
            pl.semaphore_signal(sem, inc=1, device_id=(d, zz), device_id_type=MESH)

        for d in (self.dx, self.dy, self.dc):
            greet(d, z)
        if far:
            for j in (1, 2, 3):
                greet(self.d, (z + j) % 4)
            pl.semaphore_wait(sem, 6)
            return
        pl.when(z > 0)(lambda: greet(self.d, z - 1))
        pl.when(z < 3)(lambda: greet(self.d, z + 1))
        pl.semaphore_wait(sem, 3 + (z + 2) // 3 + (5 - z) // 3)


class Sender:
    def __init__(self, links, send_sem, recv_sem):
        self.links, self.send_sem, self.recv_sem = links, send_sem, recv_sem

    def copy(self, src, dst, at, to):
        return pltpu.make_async_remote_copy(
            src_ref=src,
            dst_ref=dst,
            send_sem=self.send_sem.at[at],
            recv_sem=self.recv_sem.at[at],
            device_id=to,
            device_id_type=MESH,
        )

    def start(self, src, dst, at, to):
        self.copy(src, dst, at, to).start()

    def landed(self, region, at):
        self.copy(region, region, at, (self.links.dc, self.links.z)).wait_recv()

    def sent(self, region, at):
        self.copy(region, region, at, (self.links.dc, self.links.z)).wait_send()


class Spread:
    def __init__(self, sender, region, base):
        self.s, self.region, self.base = sender, region, base

    def own(self, p, src):
        k, r, b = self.s.links, self.region, self.base + 9 * p
        mine = r(k.d, p, None)
        self.s.start(src, mine, b, (k.dx, k.z))
        self.s.start(src, mine, b + 1, (k.dy, k.z))
        self.s.start(src, mine, b + 2, (k.dc, k.z))

    def near(self, p):
        k, r, b = self.s.links, self.region, self.base + 9 * p
        self.s.landed(r(k.dx, p, None), b)
        self.s.start(r(k.dx, p, 0), r(k.dx, p, 0), b + 3, (k.dy, k.z))
        self.s.start(r(k.dx, p, None), r(k.dx, p, None), b + 5, (k.dc, k.z))
        self.s.landed(r(k.dy, p, None), b + 1)
        self.s.start(r(k.dy, p, 1), r(k.dy, p, 1), b + 4, (k.dx, k.z))
        self.s.start(r(k.dy, p, None), r(k.dy, p, None), b + 6, (k.dc, k.z))

    def far(self, p):
        k, r, b = self.s.links, self.region, self.base + 9 * p
        for part in (0, 1):
            self.s.landed(r(k.dxy, p, part), b + 3 + part)
            self.s.start(r(k.dxy, p, part), r(k.dxy, p, part), b + 7 + part, (k.dc, k.z))

    def finish(self, p):
        k, r, b = self.s.links, self.region, self.base + 9 * p
        self.s.landed(r(k.dc, p, None), b + 2)
        self.s.landed(r(k.dcx, p, None), b + 5)
        self.s.landed(r(k.dcy, p, None), b + 6)
        for part in (0, 1):
            self.s.landed(r(k.dcxy, p, part), b + 7 + part)

    def drain(self, p):
        k, r, b = self.s.links, self.region, self.base + 9 * p
        for i in (0, 1, 2):
            self.s.sent(r(k.d, p, None), b + i)
        self.s.sent(r(k.dx, p, 0), b + 3)
        self.s.sent(r(k.dy, p, 1), b + 4)
        self.s.sent(r(k.dx, p, None), b + 5)
        self.s.sent(r(k.dy, p, None), b + 6)
        for part in (0, 1):
            self.s.sent(r(k.dxy, p, part), b + 7 + part)


class Line:
    def __init__(self, sender, region, base):
        self.s, self.region, self.base = sender, region, base

    def _send(self, src, p, way, step):
        k = self.s.links
        self.s.start(src, self.region(p), self.base + 2 * (step - 1) + way, (k.d, k.z + 1 - 2 * way))

    def own(self, src):
        z = self.s.links.z
        pl.when(z < 3)(lambda: self._send(src, z, 0, 1))
        pl.when(z > 0)(lambda: self._send(src, z, 1, 1))

    def each(self, step, action):
        z = self.s.links.z
        pl.when(z >= step)(lambda: action(z - step, 0))
        pl.when(z + step <= 3)(lambda: action(z + step, 1))

    def arrive(self, step, then=None):
        z = self.s.links.z

        def action(p, way):
            self.s.landed(self.region(p), self.base + 2 * (step - 1) + way)
            if step < 3:
                ahead = z < 3 if way == 0 else z > 0
                pl.when(ahead)(lambda: self._send(self.region(p), p, way, step + 1))
            if then is not None:
                then(p)

        self.each(step, action)

    def drain(self):
        z = self.s.links.z
        for step in (1, 2, 3):
            for way in (0, 1):
                came = z - (step - 1) if way == 0 else z + (step - 1)
                ok = jnp.logical_and(z < 3, z >= step - 1) if way == 0 else jnp.logical_and(z > 0, z <= 4 - step)
                pl.when(ok)(
                    functools.partial(self.s.sent, self.region(came), self.base + 2 * (step - 1) + way)
                )


def forward_kernel(
    x_ref, g_ref, cos_ref, sin_ref, att_ref, wo_ref, gu_ref, wd_ref,
    wa_all, wo_all, gu_all, wd_all, n2_all, top_all, wqkv_all,
    q_out, kv_out, o_out, mid_out, gain_out,
    n1, qkv, w_buf, wkv_buf, gain_buf, wo_buf, n2, top, send_sem, recv_sem, local_sem,
):
    rows, width = x_ref.shape
    slot_width = att_ref.shape[1]
    block = width // 8
    links = Links()
    d, z = links.d, links.z
    s = Sender(links, send_sem, recv_sem)
    cut_a = att_ref.shape[0] // 32 * 16
    cuts_a = ((0, cut_a), (cut_a, att_ref.shape[0] - cut_a))

    def at_a(dd, p, part):
        if part is None:
            return wa_all.at[dd, p]
        return wa_all.at[dd, p, pl.ds(*cuts_a[part])]

    def at_b(dd, p, part):
        start, size = (0, slot_width) if part is None else (part * slot_width // 2, slot_width // 2)
        return wo_all.at[
            pl.ds(pl.multiple_of(p * slot_width + start, 16), size),
            pl.ds(pl.multiple_of(dd * block, 128), block),
        ]

    def at_gu(dd, p, part):
        start, size = (0, block) if part is None else (part * block // 2, block // 2)
        return gu_all.at[pl.ds(pl.multiple_of(dd * block + start, 16), size)]

    ff = wd_ref.shape[0]

    def at_wd(dd, p, part):
        start, size = (0, ff) if part is None else (part * ff // 2, ff // 2)
        return wd_all.at[pl.ds(start, size), pl.ds(pl.multiple_of(dd * block, 128), block)]

    def rows_of(ref):
        return lambda p: ref.at[pl.ds(pl.multiple_of(p * rows, 16), rows)]

    spread_a, spread_b = Spread(s, at_a, 0), Spread(s, at_b, 36)
    spread_gu, spread_wd = Spread(s, at_gu, 72), Spread(s, at_wd, 81)
    line_a = Line(s, lambda p: at_a(d, p, None), 90)
    line_b = Line(s, lambda p: at_b(d, p, None), 96)
    line_n, line_t = Line(s, rows_of(n2_all), 102), Line(s, rows_of(top_all), 108)

    def keep(src, dst, at):
        pltpu.make_async_copy(src, dst, local_sem.at[at]).start()

    def kept(src, dst, at):
        pltpu.make_async_copy(src, dst, local_sem.at[at]).wait()

    links.barrier()

    line_a.own(att_ref)
    spread_a.own(z, att_ref)
    keep(att_ref, at_a(d, z, None), 0)
    keep(wo_ref, at_b(d, z, None), 1)
    keep(gu_ref, at_gu(d, 0, None), 2)
    keep(wd_ref, at_wd(d, 0, None), 3)
    top[...] = g_ref[...].astype(BF16)
    line_a.arrive(1, lambda p: spread_a.own(p, at_a(d, p, None)))
    spread_a.near(z)
    line_a.arrive(2, lambda p: spread_a.own(p, at_a(d, p, None)))
    line_b.own(wo_ref)
    line_a.each(1, lambda p, way: spread_a.near(p))
    spread_a.far(z)
    line_a.arrive(3, lambda p: spread_a.own(p, at_a(d, p, None)))
    line_b.arrive(1)
    line_a.each(2, lambda p, way: spread_a.near(p))
    line_a.each(1, lambda p, way: spread_a.far(p))
    spread_b.own(z, wo_ref)
    line_b.each(1, lambda p, way: spread_b.own(p, at_b(d, p, None)))
    line_a.each(3, lambda p, way: spread_a.near(p))
    line_b.arrive(2, lambda p: spread_b.own(p, at_b(d, p, None)))
    line_a.each(2, lambda p, way: spread_a.far(p))
    line_b.arrive(3, lambda p: spread_b.own(p, at_b(d, p, None)))
    line_t.own(top)
    line_a.each(3, lambda p, way: spread_a.far(p))
    kept(att_ref, at_a(d, z, None), 0)
    for p in range(4):
        spread_a.finish(p)
    spread_gu.own(0, gu_ref)

    for p in range(4):
        keep(wa_all.at[:, p, pl.ds(0, block)], w_buf.at[p], 4 + p)
    keep(wa_all.at[:, :, pl.ds(block, KV_ROWS)], wkv_buf, 8)
    keep(wa_all.at[:, :, pl.ds(block + KV_ROWS, GAIN_ROWS), pl.ds(0, LANES)], gain_buf, 9)
    kept(wa_all.at[:, :, pl.ds(block + KV_ROWS, GAIN_ROWS), pl.ds(0, LANES)], gain_buf, 9)
    low_row = lax.broadcasted_iota(jnp.int32, (GAIN_ROWS, LANES), 1) < HD
    for dd in range(8):
        for half in (0, 1):
            first = gain_buf[dd, 2 * half].astype(F32)
            second = pltpu.roll(gain_buf[dd, 2 * half + 1].astype(F32), HD, 1)
            at = dd * block + half * LANES
            gain_out[:, at : at + LANES] = jnp.where(low_row, first, second)[:8]
    x = x_ref[...]
    n1[...] = (x * norm_scale(x) * gain_out[0:1]).astype(BF16)
    for p in range(4):
        kept(wa_all.at[:, p, pl.ds(0, block)], w_buf.at[p], 4 + p)
        qkv[:, p * slot_width : (p + 1) * slot_width] = dot(
            n1[...], w_buf[p].reshape(width, slot_width)
        )
        keep(w_buf.at[p], wqkv_all.at[:, :, pl.ds(p * slot_width, slot_width)], 4 + p)
    kept(wa_all.at[:, :, pl.ds(block, KV_ROWS)], wkv_buf, 8)
    qkv[:, width:] = dot(n1[...], wkv_buf[...].reshape(width, 2 * KV * HD))
    for p in range(4):
        keep(
            wkv_buf.at[:, p],
            wqkv_all.at[:, pl.ds(p * KV_ROWS, KV_ROWS), pl.ds(width, 2 * KV * HD)],
            10 + p,
        )

    line_t.arrive(1)
    line_b_pieces = lambda action: [action(z)] + [line_b.each(i, lambda p, way: action(p)) for i in (1, 2, 3)]

    def sequence(i, carry):
        at = pl.ds(pl.multiple_of(i * SEQ, SEQ), SEQ)
        attend_sequence(
            cos_ref[at], sin_ref[at], lambda c: qkv[at, c : c + LANES], width, q_out, kv_out, o_out, at
        )

        @pl.when(i == 0)
        def _():
            line_b_pieces(spread_b.near)

        return carry

    lax.fori_loop(0, rows // SEQ, sequence, 0)
    line_t.arrive(2)
    line_b_pieces(spread_b.far)
    spread_wd.own(0, wd_ref)
    kept(wo_ref, at_b(d, z, None), 1)
    for p in range(4):
        spread_b.finish(p)
    keep(wo_all, wo_buf, 0)
    kept(wo_all, wo_buf, 0)

    def column(i, carry):
        at = pl.ds(pl.multiple_of(i * 256, 256), 256)
        mid_out[:, at] = x_ref[:, at] + dot(o_out[...], wo_buf[:, at])
        return carry

    lax.fori_loop(0, width // 256, column, 0)
    mid = mid_out[...]
    n2[...] = (mid * norm_scale(mid) * gain_out[1:2]).astype(BF16)

    line_n.own(n2)
    keep(n2, n2_all.at[pl.ds(pl.multiple_of(z * rows, 16), rows)], 8)
    keep(top, top_all.at[pl.ds(pl.multiple_of(z * rows, 16), rows)], 9)
    line_t.arrive(3)
    spread_gu.near(0)
    line_n.arrive(1)
    spread_gu.far(0)
    spread_wd.near(0)
    line_n.arrive(2)
    spread_wd.far(0)
    line_n.arrive(3)
    spread_gu.finish(0)
    spread_wd.finish(0)

    kept(gu_ref, at_gu(d, 0, None), 2)
    kept(wd_ref, at_wd(d, 0, None), 3)
    for p in range(4):
        kept(w_buf.at[p], wqkv_all.at[:, :, pl.ds(p * slot_width, slot_width)], 4 + p)
        kept(
            wkv_buf.at[:, p],
            wqkv_all.at[:, pl.ds(p * KV_ROWS, KV_ROWS), pl.ds(width, 2 * KV * HD)],
            10 + p,
        )
    kept(n2, n2_all.at[pl.ds(pl.multiple_of(z * rows, 16), rows)], 8)
    kept(top, top_all.at[pl.ds(pl.multiple_of(z * rows, 16), rows)], 9)
    for p in range(4):
        spread_a.drain(p)
        spread_b.drain(p)
    spread_gu.drain(0)
    spread_wd.drain(0)
    for line in (line_a, line_b, line_n, line_t):
        line.drain()


def forward_stage(x, g, cos, sin, att, wo, gu, wd):
    rows, width = x.shape
    slot_width = att.shape[1]
    block = width // 8
    kv_width = 2 * KV * HD
    ff = wd.shape[0]
    vmem = pl.BlockSpec(memory_space=pltpu.VMEM)
    hbm = pl.BlockSpec(memory_space=pltpu.HBM)
    shape = jax.ShapeDtypeStruct
    outs = [
        (hbm, shape((8, 4) + att.shape, BF16)),
        (hbm, shape((width, width), BF16)),
        (hbm, shape((width, gu.shape[1]), BF16)),
        (hbm, shape((ff, width), BF16)),
        (hbm, shape((4 * rows, width), BF16)),
        (hbm, shape((4 * rows, width), BF16)),
        (hbm, shape((8, block, width + kv_width), BF16)),
        (vmem, shape((rows, width), BF16)),
        (vmem, shape((rows, kv_width), BF16)),
        (vmem, shape((rows, width), BF16)),
        (vmem, shape((rows, width), F32)),
        (vmem, shape((8, width), F32)),
    ]
    return pl.pallas_call(
        forward_kernel,
        in_specs=[vmem] * 8,
        out_specs=[o[0] for o in outs],
        out_shape=[o[1] for o in outs],
        scratch_shapes=[
            pltpu.VMEM((rows, width), BF16),
            pltpu.VMEM((rows, width + kv_width), F32),
            pltpu.VMEM((4, 8, block, slot_width), BF16),
            pltpu.VMEM((8, 4, KV_ROWS, kv_width), BF16),
            pltpu.VMEM((8, 4, GAIN_ROWS, LANES), BF16),
            pltpu.VMEM((width, width), BF16),
            pltpu.VMEM((rows, width), BF16),
            pltpu.VMEM((rows, width), BF16),
            pltpu.SemaphoreType.DMA((114,)),
            pltpu.SemaphoreType.DMA((114,)),
            pltpu.SemaphoreType.DMA((14,)),
        ],
        compiler_params=pltpu.CompilerParams(
            collective_id=0, has_side_effects=True, vmem_limit_bytes=62 * 1024 * 1024
        ),
        name="forward",
    )(x, g, cos, sin, att, wo, gu, wd)


def loop(count, body):
    def step(i, carry):
        body(i)
        return carry

    lax.fori_loop(0, count, step, 0)


class Local:
    def __init__(self, sem):
        self.sem, self.next = sem, 0

    def start(self, src, dst):
        copy = pltpu.make_async_copy(src, dst, self.sem.at[self.next])
        self.next += 1
        copy.start()
        return copy

    def load(self, src, dst):
        self.start(src, dst).wait()


class Reduce:
    def __init__(self, sender, local, compute, base, sends, kept, land, tmp, halves):
        self.s, self.local, self.compute, self.base = sender, local, compute, base
        self.sends, self.kept, self.land, self.tmp, self.halves = sends, kept, land, tmp, halves

    def half(self, ref, part):
        return ref.at[pl.ds(*self.halves[part])]

    def place(self, i):
        if i < 4:
            return self.land.at[i]
        return self.half(self.land.at[4 + (i - 4) // 2], i % 2)

    def partner(self):
        k = self.s.links
        count = self.sends.shape[0]
        for i, dest in enumerate((k.dcxy, k.dcx, k.dcy, k.dc)):
            if i >= count:
                self.s.sent(self.sends.at[i % count], self.base + i - count)
            self.compute(dest, None, self.sends.at[i % count])
            self.s.start(self.sends.at[i % count], self.place(i), self.base + i, (k.dc, k.z))

    def own(self):
        k, b = self.s.links, self.base
        to_x, to_y = (k.dx, k.z), (k.dy, k.z)
        for i, dest in enumerate((k.dxy, k.dx, k.dy, k.d)):
            self.s.landed(self.place(i), b + i)
            self.local.load(self.place(i), self.tmp)
            self.compute(dest, self.tmp, self.kept.at[i])
            kept = self.kept.at[i]
            if i == 0:
                self.s.start(self.half(kept, 0), self.place(4), b + 4, to_x)
                self.s.start(self.half(kept, 1), self.place(7), b + 7, to_y)
            elif i == 1:
                self.s.start(self.half(kept, 0), self.place(6), b + 6, to_x)
            elif i == 2:
                self.s.start(self.half(kept, 1), self.place(5), b + 5, to_y)

    def add(self, i, part, at):
        self.s.landed(self.place(at), self.base + at)
        self.local.load(self.place(at), self.half(self.tmp, part))
        start, size = self.halves[part]
        step = 32 if size % 32 == 0 else 16

        def rows(n):
            r = pl.ds(pl.multiple_of(start + n * step, 16), step)
            self.kept[i, r] = (self.kept[i, r].astype(F32) + self.tmp[r].astype(F32)).astype(BF16)

        loop(size // step, rows)

    def second(self):
        k, b = self.s.links, self.base
        self.add(2, 0, 4)
        self.s.start(self.half(self.kept.at[2], 0), self.place(8), b + 8, (k.dy, k.z))
        self.add(1, 1, 7)
        self.s.start(self.half(self.kept.at[1], 1), self.place(9), b + 9, (k.dx, k.z))

    def last(self):
        self.add(3, 0, 6)
        self.add(3, 1, 5)
        self.add(3, 0, 8)
        self.add(3, 1, 9)

    def drain(self):
        b, kept = self.base, self.kept
        count = self.sends.shape[0]
        for i in range(4 - count, 4):
            self.s.sent(self.sends.at[i % count], b + i)
        self.s.sent(self.half(kept.at[0], 0), b + 4)
        self.s.sent(self.half(kept.at[2], 1), b + 5)
        self.s.sent(self.half(kept.at[1], 0), b + 6)
        self.s.sent(self.half(kept.at[0], 1), b + 7)
        self.s.sent(self.half(kept.at[2], 0), b + 8)
        self.s.sent(self.half(kept.at[1], 1), b + 9)


class LineSum:
    def __init__(self, sender, local, part, sends, tmp, land, base):
        self.s, self.local, self.part, self.sends = sender, local, part, sends
        self.tmp, self.land, self.base = tmp, land, base
        self.rows = tmp.shape[0]

    def rows_of(self, t):
        return self.part.at[pl.ds(pl.multiple_of(t * self.rows, 16), self.rows)]

    def add(self, into, at):
        self.s.landed(self.land.at[at], self.base + at)
        self.local.load(self.land.at[at], self.tmp)

        def rows(n):
            r = pl.ds(pl.multiple_of(n * 32, 32), 32)
            self.sends[into, r] = (self.sends[into, r].astype(F32) + self.tmp[r].astype(F32)).astype(BF16)

        loop(self.rows // 32, rows)

    def ways(self, s):
        z = self.s.links.z
        right = (z <= s - 1, s - 1 - z, 2 * (s - 1), z + 4 - s, z >= 1, z + 1)
        left = (z >= 4 - s, s - 1, 2 * (s - 1) + 1, z - 4 + s, z <= 2, z - 1)
        return right, left

    def step(self, s):
        for sends, slot, place, holds, received, to in self.ways(s):

            @pl.when(sends)
            def _():
                self.local.load(self.rows_of(holds), self.sends.at[slot])
                if s > 1:
                    pl.when(received)(lambda: self.add(slot, place - 2))
                self.s.start(self.sends.at[slot], self.land.at[place], self.base + place, (self.s.links.d, to))

    def finish(self, write):
        z = self.s.links.z
        self.local.load(self.rows_of(z), self.sends.at[3])
        pl.when(z >= 1)(lambda: self.add(3, 4))
        pl.when(z <= 2)(lambda: self.add(3, 5))

        def rows(n):
            r = pl.ds(pl.multiple_of(n * 32, 32), 32)
            write(r, self.sends[3, r].astype(F32))

        loop(self.rows // 32, rows)

    def drain(self):
        for s in (1, 2, 3):
            for sends, slot, place, _, _, _ in self.ways(s):
                pl.when(sends)(functools.partial(self.s.sent, self.sends.at[slot], self.base + place))


def stream(local, count, source, bufs, body):
    first = local.next
    local.next += 2

    def copy(n, slot):
        return pltpu.make_async_copy(source(n), bufs.at[slot], local.sem.at[first + slot])

    copy(0, 0).start()

    def step(n):
        slot = n % 2
        copy(n, slot).wait()

        @pl.when(n + 1 < count)
        def _():
            copy(n + 1, 1 - slot).start()

        body(n, bufs.at[slot])

    loop(count, step)


def turned(ref):
    return jnp.transpose(ref[...].astype(F32)).astype(BF16)


def columns(ref, start, size):
    return ref.at[:, pl.ds(pl.multiple_of(start, 128), size)]


def block_of(local, source, cols, dest, block):
    if cols is None:
        return columns(source, dest * block, block)
    local.load(columns(source, dest * block, block), cols)
    return cols


def row_blocks(local, source, cols, left, right):
    block = left.shape[0]
    width = right.shape[1]

    def compute(dest, add, out):
        left[...] = turned(block_of(local, source, cols, dest, block))

        def chunk(n):
            c = pl.ds(pl.multiple_of(n * 256, 256), 256)
            total = dot(left[...], right[:, c])
            if add is not None:
                total = total + add[:, c].astype(F32)
            out[:, c] = total.astype(BF16)

        loop(width // 256, chunk)

    return compute


def column_blocks(local, left, source, cols, chunks, block):
    size = left.shape[0] // chunks

    def compute(dest, add, out):
        picked = block_of(local, source, cols, dest, block)

        def chunk(n):
            r = pl.ds(pl.multiple_of(n * size, 16), size)
            total = dot(left[r], picked[...])
            if add is not None:
                total = total + add[r].astype(F32)
            out[r] = total.astype(BF16)

        loop(chunks, chunk)

    return compute


def feed_back_kernel(
    part_ref, n2_ref, dgu_ref, dn2_out, ggu_out, land, line_land,
    dgu, cols, left, sends, kept, tmp, line_sends, line_tmp, send_sem, recv_sem, local_sem,
):
    links = Links()
    s = Sender(links, send_sem, recv_sem)
    local = Local(local_sem)
    block = left.shape[0]
    links.barrier()
    fetch = local.start(dgu_ref, dgu)
    line = LineSum(s, local, part_ref, line_sends, line_tmp, line_land, 10)
    line.step(1)
    fetch.wait()
    grads = Reduce(
        s, local, row_blocks(local, n2_ref, cols, left, dgu), 0, sends, kept, land, tmp,
        ((0, block // 2), (block // 2, block // 2)),
    )
    grads.partner()
    line.step(2)
    grads.own()
    line.step(3)
    grads.second()

    def write(r, total):
        dn2_out[r] = total

    line.finish(write)
    grads.last()

    def rows(n):
        r = pl.ds(pl.multiple_of(n * 16, 16), 16)
        ggu_out[r] = kept[3, r].astype(F32)

    loop(block // 16, rows)
    grads.drain()
    line.drain()


def feed_back(part, n2, dgu):
    rows, width = part.shape[0] // 4, part.shape[1]
    block, wide = width // 8, dgu.shape[1]
    vmem = pl.BlockSpec(memory_space=pltpu.VMEM)
    hbm = pl.BlockSpec(memory_space=pltpu.HBM)
    shape = jax.ShapeDtypeStruct
    return pl.pallas_call(
        feed_back_kernel,
        in_specs=[hbm] * 3,
        out_specs=[vmem, vmem, hbm, hbm],
        out_shape=[
            shape((rows, width), F32),
            shape((block, wide), F32),
            shape((7, block, wide), BF16),
            shape((6, rows, width), BF16),
        ],
        scratch_shapes=[
            pltpu.VMEM((4 * rows, wide), BF16),
            pltpu.VMEM((4 * rows, block), BF16),
            pltpu.VMEM((block, 4 * rows), BF16),
            pltpu.VMEM((4, block, wide), BF16),
            pltpu.VMEM((4, block, wide), BF16),
            pltpu.VMEM((block, wide), BF16),
            pltpu.VMEM((4, rows, width), BF16),
            pltpu.VMEM((rows, width), BF16),
            pltpu.SemaphoreType.DMA((16,)),
            pltpu.SemaphoreType.DMA((16,)),
            pltpu.SemaphoreType.DMA((40,)),
        ],
        compiler_params=pltpu.CompilerParams(
            collective_id=1, has_side_effects=True, vmem_limit_bytes=62 * 1024 * 1024
        ),
        name="feed_back",
    )(part, n2, dgu)[:2]


class Spread4:
    def __init__(self, sender, pick, land, base):
        self.s, self.pick, self.land, self.base = sender, pick, land, base

    def send(self):
        k = self.s.links
        for j in (1, 2, 3):
            to = (k.z + j) % 4
            self.s.start(self.pick(to), self.land.at[j - 1], self.base + j - 1, (k.d, to))

    def landed(self):
        for j in range(3):
            self.s.landed(self.land.at[j], self.base + j)

    def drain(self):
        z = self.s.links.z
        for j in (1, 2, 3):
            self.s.sent(self.pick((z + j) % 4), self.base + j - 1)


def norm_back_rows(rows_ref, at, gain, grad_normed):
    rows = rows_ref[at]
    inv = norm_scale(rows)
    weighted = grad_normed * gain
    scaled = grad_normed * rows * inv
    grad_rows = inv * weighted - rows * (inv * inv * inv) * jnp.mean(weighted * rows, -1, keepdims=True)
    return grad_rows, scaled


def attention_back_kernel(
    dn2_ref, mid_ref, x_ref, g_ref, gain_ref, cos_ref, sin_ref, q_ref, kv_ref, att_ref,
    hidden_ref, top_ref, wo_ref, wqkv_ref, out_part_ref,
    grad_in_out, hidden_out, gq_out, gkv_out, go_out, gd_out, gain_out,
    land_row, land_o, land_d, line_land,
    mid_bf, da, dqkv, n1, hidden_cols, hidden_t, att_t, w_chunk, cols_d, left_n,
    row_sends, row_kept, row_tmp, o_sends, o_kept, o_tmp, d_sends, d_kept, d_tmp,
    gain_part, gain_land, z_q, z_kv, z_o, line_sends, line_tmp,
    send_sem, recv_sem, local_sem,
):
    rows, width = x_ref.shape
    block = width // 8
    kv_width = 2 * KV * HD
    slot = width // 4
    links = Links()
    d, z = links.d, links.z
    s = Sender(links, send_sem, recv_sem)
    local = Local(local_sem)
    links.barrier(far=True)

    dn1 = hidden_out
    line = LineSum(s, local, out_part_ref, line_sends, line_tmp, line_land, 30)
    line.step(1)

    gain_part[...] = jnp.zeros_like(gain_part)
    step = 32

    def add_gain(row, scaled):
        for b in range(8):
            total = jnp.sum(scaled[:, b * block : (b + 1) * block], 0, keepdims=True)
            at = (b % 2, b // 2 % 2 * 2 + b // 4)
            gain_part[at[0], at[1], row : row + 1] += total

    def middle(n):
        r = pl.ds(pl.multiple_of(n * step, step), step)
        grad_rows, scaled = norm_back_rows(mid_ref, r, gain_ref[1:2], dn2_ref[r])
        grad = g_ref[r] + grad_rows
        grad_in_out[r] = grad
        mid_bf[r] = grad.astype(BF16)
        add_gain(1, scaled)
        rows_x = x_ref[r]
        n1[r] = (rows_x * norm_scale(rows_x) * gain_ref[0:1]).astype(BF16)

    loop(rows // step, middle)

    def transpose_into(src, dst):
        def part(n):
            c = pl.ds(pl.multiple_of(n * 128, 128), 128)
            dst[c] = jnp.transpose(src[:, c].astype(F32)).astype(BF16)

        loop(src.shape[1] // 128, part)

    transpose_into(att_ref, att_t)
    halves = lambda size: ((0, size // 2), (size // 2, size // 2))
    grad_o = Reduce(
        s, local, column_blocks(local, att_t, mid_bf, None, 4, block), 0, o_sends, o_kept, land_o, o_tmp, halves(width)
    )
    grad_o.partner()
    ff = hidden_t.shape[0]

    def turn_hidden(n, buf):
        hidden_t[pl.ds(pl.multiple_of(n * 128, 128), 128)] = turned(buf)

    stream(local, ff // 128, lambda n: columns(hidden_ref, n * 128, 128), hidden_cols, turn_hidden)
    grad_d = Reduce(
        s, local, column_blocks(local, hidden_t, top_ref, cols_d, 4, block), 10, d_sends, d_kept, land_d, d_tmp, halves(ff)
    )
    grad_o.own()
    grad_d.partner()

    def attended(n, buf):
        da[:, pl.ds(pl.multiple_of(n * 256, 256), 256)] = dot_nt(mid_bf[...], buf[...]).astype(BF16)

    row_chunk = lambda ref: lambda n: ref.at[pl.ds(pl.multiple_of(n * 256, 256), 256)]
    stream(local, width // 256, row_chunk(wo_ref), w_chunk.at[:, :, pl.ds(0, width)], attended)
    line.step(2)
    grad_d.own()

    def sequence(i):
        at = pl.ds(pl.multiple_of(i * SEQ, SEQ), SEQ)
        attend_back_sequence(cos_ref[at], sin_ref[at], q_ref, kv_ref, da, dqkv, at)

        @pl.when(i == 0)
        def _():
            grad_o.second()
            line.step(3)

    loop(rows // SEQ, sequence)
    grad_d.second()

    grad_row = Reduce(
        s, local, row_blocks(local, n1, None, left_n, dqkv), 20, row_sends, row_kept, land_row, row_tmp,
        halves(block),
    )
    grad_row.partner()
    grad_row.own()
    grad_o.last()
    send_o = Spread4(s, lambda p: o_kept.at[3, pl.ds(pl.multiple_of(p * slot, 16), slot)], z_o, 40)
    send_o.send()

    def projected(n, buf):
        dn1[:, pl.ds(pl.multiple_of(n * 256, 256), 256)] = dot_nt(dqkv[...], buf[...])

    stream(local, width // 256, row_chunk(wqkv_ref), w_chunk, projected)
    grad_row.second()

    def inward(n):
        r = pl.ds(pl.multiple_of(n * step, step), step)
        grad_rows, scaled = norm_back_rows(x_ref, r, gain_ref[0:1], dn1[r])
        grad_in_out[r] += grad_rows
        add_gain(0, scaled)

    loop(rows // step, inward)

    core, x_at, y_at = d % 2, d // 2 % 2, d // 4
    s.start(gain_part.at[1 - core], gain_land.at[pl.ds(0, 4)], 49, (links.dc, z))

    def write(r, total):
        hidden_out[r] = mid_ref[r] + total

    line.finish(write)
    s.landed(gain_land.at[pl.ds(0, 4)], 49)
    gain_part[core] += gain_land[0:4]
    other_x = pl.multiple_of(2 - 2 * x_at, 2)
    s.start(gain_part.at[core, pl.ds(other_x, 2)], gain_land.at[pl.ds(4, 2)], 50, (links.dx, z))
    grad_d.last()

    def down(n):
        r = pl.ds(pl.multiple_of(n * 16, 16), 16)
        gd_out[r] = d_kept[3, r].astype(F32)

    loop(ff // 16, down)
    s.landed(gain_land.at[pl.ds(4, 2)], 50)
    mine_x = 2 * x_at
    gain_part[core, pl.ds(mine_x, 2)] += gain_land[4:6]
    s.start(gain_part.at[core, mine_x + 1 - y_at], gain_land.at[6], 51, (links.dy, z))

    grad_row.last()
    send_q = Spread4(s, lambda p: row_kept.at[3, :, pl.ds(pl.multiple_of(p * slot, 128), slot)], z_q, 43)
    send_kv = Spread4(
        s, lambda p: row_kept.at[3, pl.ds(pl.multiple_of(p * KV_ROWS, 16), KV_ROWS), pl.ds(width, kv_width)], z_kv, 46
    )
    send_q.send()
    send_kv.send()
    s.landed(gain_land.at[6], 51)
    gain_part[core, mine_x + y_at] += gain_land[6]
    send_g = Spread4(s, lambda p: gain_part.at[core, mine_x + y_at], gain_land.at[pl.ds(7, 3)], 52)
    send_g.send()

    send_o.landed()

    def out_rows(n):
        r = pl.ds(pl.multiple_of(n * 16, 16), 16)
        mine = pl.ds(pl.multiple_of(z * slot + n * 16, 16), 16)
        go_out[r] = (
            o_kept[3, mine].astype(F32) + z_o[0, r].astype(F32) + z_o[1, r].astype(F32) + z_o[2, r].astype(F32)
        )

    loop(slot // 16, out_rows)
    send_q.landed()
    mine_q = pl.ds(pl.multiple_of(z * slot, 128), slot)

    def query_rows(n):
        r = pl.ds(pl.multiple_of(n * 16, 16), 16)
        gq_out[r] = (
            row_kept[3, r, mine_q].astype(F32)
            + z_q[0, r].astype(F32)
            + z_q[1, r].astype(F32)
            + z_q[2, r].astype(F32)
        )

    loop(block // 16, query_rows)
    send_kv.landed()
    mine_kv = pl.ds(pl.multiple_of(z * KV_ROWS, 16), KV_ROWS)
    gkv_out[...] = row_kept[3, mine_kv, width : width + kv_width].astype(F32) + (
        z_kv[0].astype(F32) + z_kv[1].astype(F32) + z_kv[2].astype(F32)
    )
    send_g.landed()
    gain_out[...] = gain_part[core, mine_x + y_at] + gain_land[7] + gain_land[8] + gain_land[9]

    for unit in (grad_o, grad_d, grad_row, line, send_o, send_q, send_kv, send_g):
        unit.drain()
    s.sent(gain_part.at[1 - core], 49)
    s.sent(gain_part.at[core, pl.ds(other_x, 2)], 50)
    s.sent(gain_part.at[core, mine_x + 1 - y_at], 51)


def attention_back(dn2, mid, x, g, gains, cos, sin, query, key_val, attended, hidden, top, wo, wqkv, out_part):
    rows, width = x.shape
    block, slot = width // 8, width // 4
    ff = hidden.shape[1]
    kv_width = 2 * KV * HD
    wide = width + kv_width
    vmem = pl.BlockSpec(memory_space=pltpu.VMEM)
    hbm = pl.BlockSpec(memory_space=pltpu.HBM)
    shape = jax.ShapeDtypeStruct
    outs = [
        (vmem, shape((rows, width), F32)),
        (vmem, shape((rows, width), F32)),
        (vmem, shape((block, slot), F32)),
        (vmem, shape((KV_ROWS, kv_width), F32)),
        (vmem, shape((slot, block), F32)),
        (vmem, shape((ff, block), F32)),
        (vmem, shape((8, block), F32)),
        (hbm, shape((7, block, wide), BF16)),
        (hbm, shape((7, width, block), BF16)),
        (hbm, shape((7, ff, block), BF16)),
        (hbm, shape((6, rows, width), BF16)),
    ]
    return pl.pallas_call(
        attention_back_kernel,
        in_specs=[vmem] * 10 + [hbm] * 5,
        out_specs=[o[0] for o in outs],
        out_shape=[o[1] for o in outs],
        scratch_shapes=[
            pltpu.VMEM((rows, width), BF16),
            pltpu.VMEM((rows, width), BF16),
            pltpu.VMEM((rows, wide), BF16),
            pltpu.VMEM((rows, width), BF16),
            pltpu.VMEM((2, 4 * rows, 128), BF16),
            pltpu.VMEM((ff, 4 * rows), BF16),
            pltpu.VMEM((width, rows), BF16),
            pltpu.VMEM((2, 256, wide), BF16),
            pltpu.VMEM((4 * rows, block), BF16),
            pltpu.VMEM((block, rows), BF16),
            pltpu.VMEM((2, block, wide), BF16),
            pltpu.VMEM((4, block, wide), BF16),
            pltpu.VMEM((block, wide), BF16),
            pltpu.VMEM((2, width, block), BF16),
            pltpu.VMEM((4, width, block), BF16),
            pltpu.VMEM((width, block), BF16),
            pltpu.VMEM((2, ff, block), BF16),
            pltpu.VMEM((4, ff, block), BF16),
            pltpu.VMEM((ff, block), BF16),
            pltpu.VMEM((2, 4, 8, block), F32),
            pltpu.VMEM((10, 8, block), F32),
            pltpu.VMEM((3, block, slot), BF16),
            pltpu.VMEM((3, KV_ROWS, kv_width), BF16),
            pltpu.VMEM((3, slot, block), BF16),
            pltpu.VMEM((4, rows, width), BF16),
            pltpu.VMEM((rows, width), BF16),
            pltpu.SemaphoreType.DMA((55,)),
            pltpu.SemaphoreType.DMA((55,)),
            pltpu.SemaphoreType.DMA((100,)),
        ],
        compiler_params=pltpu.CompilerParams(
            collective_id=2, has_side_effects=True, vmem_limit_bytes=65000 * 1024
        ),
        name="attention_back",
    )(dn2, mid, x, g, gains, cos, sin, query, key_val, attended, hidden, top, wo, wqkv, out_part)[:7]


def plain_forward(x, g, cos, sin, w_query, w_kv, gains, w_out, w_gu, w_down):
    both = ("dp", "tensor")
    gather = lax.all_gather

    def whole(shard, dims):
        for dim, axis in dims:
            shard = gather(shard, axis, axis=dim, tiled=True)
        return shard

    wq = whole(w_query, ((1, "tensor"), (0, "dp")))
    wqkv = jnp.concatenate([wq, whole(w_kv, ((0, both),))], 1)
    gain = whole(gains, ((1, both),)).astype(F32)
    wo = whole(w_out, ((0, "tensor"), (1, "dp")))
    wgu = whole(w_gu, ((0, "dp"),))
    wd = whole(w_down, ((1, "dp"),))
    normed = (x * norm_scale(x) * gain[0]).astype(BF16)
    query, key_val, attended = attend(cos, sin, dot(normed, wqkv))
    middle = x + dot(attended, wo)
    normed_two = (middle * norm_scale(middle) * gain[1]).astype(BF16)
    n2 = gather(normed_two, "tensor", axis=0, tiled=True)
    top = gather(g.astype(BF16), "tensor", axis=0, tiled=True)
    return wqkv, gain, wo, wgu, wd, n2, top, query, key_val, attended, middle


def linked_forward(x, g, cos, sin, w_query, w_kv, gains, w_out, w_gu, w_down):
    rows, width = x.shape
    slot = w_query.shape[1]
    padded = jnp.pad(gains, ((0, GAIN_ROWS - 2), (0, slot - gains.shape[1])))
    piece = jnp.concatenate([w_query, w_kv, padded])
    (_, wo, wgu, wd, n2, top, wqkv, query, key_val, attended, middle, gain) = forward_stage(
        x, g, cos, sin, piece, w_out, w_gu, w_down
    )
    wqkv = wqkv.reshape(width, -1)
    return wqkv, gain, wo, wgu, wd, n2, top, query, key_val, attended, middle


def plain_backward(
    dn2_part, out_part, n2, grad_gu_pre, hidden, top,
    middle, x, g, gains, cos, sin, query, key_val, attended, wo, wqkv,
):
    width = x.shape[1]

    def scatter(part, axis, dim):
        return lax.psum_scatter(part.astype(BF16), axis, scatter_dimension=dim, tiled=True).astype(F32)

    output = middle + scatter(out_part, "tensor", 0)
    grad_mid_norm, gain_two = norm_back(middle, gains[1], scatter(dn2_part, "tensor", 0))
    grad_middle = g + grad_mid_norm
    mid_bf = grad_middle.astype(BF16)
    grad_qkv_rows = attend_back(cos, sin, query, key_val, dot_nt(mid_bf, wo).astype(BF16))
    grad_in_norm, gain_one = norm_back(x, gains[0], dot_nt(grad_qkv_rows, wqkv))
    normed_one = (x * norm_scale(x) * gains[0]).astype(BF16)
    grad_qkv = scatter(dot_tn(normed_one, grad_qkv_rows), "dp", 0)
    gain_parts = lax.psum_scatter(jnp.stack([gain_one, gain_two]), "dp", scatter_dimension=1, tiled=True)
    return (
        output,
        grad_middle + grad_in_norm,
        lax.psum_scatter(gain_parts, "tensor", scatter_dimension=1, tiled=True),
        scatter(grad_qkv[:, :width], "tensor", 1),
        scatter(grad_qkv[:, width:], "tensor", 0),
        scatter(scatter(dot_tn(attended, mid_bf), "dp", 1), "tensor", 0),
        scatter(dot_tn(n2, grad_gu_pre), "dp", 0),
        scatter(dot_tn(hidden, top), "dp", 1),
    )


def linked_backward(
    dn2_part, out_part, n2, grad_gu_pre, hidden, top,
    middle, x, g, gains, cos, sin, query, key_val, attended, wo, wqkv,
):
    grad_n2, grad_gu = feed_back(dn2_part, n2, grad_gu_pre)
    grad_in, output, grad_query, grad_kv, grad_out, grad_down, gain_sum = attention_back(
        grad_n2, middle, x, g, gains, cos, sin, query, key_val, attended, hidden, top, wo, wqkv, out_part
    )
    own = gain_sum.shape[1] // 4
    grad_gains = lax.dynamic_slice(gain_sum, (0, lax.axis_index("tensor") * own), (2, own))
    return output, grad_in, grad_gains, grad_query, grad_kv, grad_out, grad_gu, grad_down


def on_device(
    linked,
    hidden_in, positions, norm_gains, w_query, w_key, w_value, w_out, w_gate, w_up, w_down, out_grad,
):
    x, g = hidden_in, out_grad
    rows, width = x.shape
    ff = w_gate.shape[2]
    kv_width = 2 * KV * HD
    z = lax.axis_index("tensor")

    cos, sin = rope_tables(lax.dynamic_slice_in_dim(positions, z * rows, rows))
    forward = linked_forward if linked else plain_forward
    wqkv, gains, wo, wgu, wd, n2, top, query, key_val, attended, middle = forward(
        x, g, cos, sin,
        w_query[0],
        jnp.concatenate([w_key[0], w_value[0]], 1),
        norm_gains[0],
        w_out[0],
        jnp.concatenate([w_gate[0], w_up[0]], 1),
        w_down[0],
    )

    gate_up = dot(n2, wgu)
    gate_pre, up_pre = gate_up[:, :ff], gate_up[:, ff:]
    sig = jax.nn.sigmoid(gate_pre)
    hidden = (gate_pre * sig * up_pre).astype(BF16)
    grad_hidden = dot_nt(top, wd)
    grad_gate_pre = (grad_hidden * up_pre * sig * (1.0 + gate_pre * (1.0 - sig))).astype(BF16)
    grad_up_pre = (grad_hidden * gate_pre * sig).astype(BF16)
    grad_gu_pre = jnp.concatenate([grad_gate_pre, grad_up_pre], 1)

    dn2_part = dot_nt(grad_gu_pre, wgu).astype(BF16)
    out_part = dot(hidden, wd).astype(BF16)
    backward = linked_backward if linked else plain_backward
    output, grad_in, grad_gains, grad_query, grad_kv, grad_out, grad_gu, grad_down = backward(
        dn2_part, out_part, n2, grad_gu_pre, hidden, top,
        middle, x, g, gains, cos, sin, query, key_val, attended, wo, wqkv,
    )

    return (
        output,
        grad_in,
        grad_gains[None],
        grad_query[None],
        grad_kv[None, :, : KV * HD],
        grad_kv[None, :, KV * HD :],
        grad_out[None],
        grad_gu[None, :, :ff],
        grad_gu[None, :, ff:],
        grad_down[None],
    )


def solution(mesh):
    nd, nt = mesh.shape["dp"], mesh.shape["tensor"]
    rows = P(("dp", "tensor"), None)
    wide = P(None, "dp", "tensor")
    tall = P(None, "tensor", "dp")
    flat = P(None, ("dp", "tensor"), None)
    gain = P(None, None, ("dp", "tensor"))
    return jax.shard_map(
        functools.partial(on_device, (nd, nt) == (8, 4)),
        mesh=mesh,
        in_specs=(rows, P("dp"), gain, wide, flat, flat, tall, wide, wide, tall, rows),
        out_specs=(rows, rows, gain, wide, flat, flat, tall, wide, wide, tall),
        check_vma=False,
    )
```

```python
import functools

import jax
import jax.numpy as jnp
from jax import lax
from jax.experimental import pallas as pl
from jax.experimental.pallas import tpu as pltpu
from jax.sharding import PartitionSpec as P

H = 32
KV = 4
HD = 64
SEQ = 128
NORM_EPS = 1e-05
NEG_BIG = -1e30
SCALE = HD ** (-0.5)
LANES = 128
F32 = jnp.float32
BF16 = jnp.bfloat16


def dot(a, b):
    return jnp.dot(a, b, preferred_element_type=F32)


def dot_nt(a, b):
    return lax.dot_general(a, b, (((1,), (1,)), ((), ())), preferred_element_type=F32)


def dot_tn(a, b):
    return lax.dot_general(a, b, (((0,), (0,)), ((), ())), preferred_element_type=F32)


def lane_masks():
    lane = lax.broadcasted_iota(jnp.int32, (SEQ, LANES), 1)
    return lane % HD < HD // 2, lane < HD


def swap_halves(u, first):
    return jnp.where(first, pltpu.roll(u, LANES - HD // 2, 1), pltpu.roll(u, HD // 2, 1))


def twice(tile, index, low):
    turned = pltpu.roll(tile, HD, 1)
    return jnp.where(low, tile, turned) if index % 2 == 0 else jnp.where(low, turned, tile)


def causal_probs(query, key):
    scores = dot_nt(query, key) * SCALE
    rows = lax.broadcasted_iota(jnp.int32, scores.shape, 0)
    cols = lax.broadcasted_iota(jnp.int32, scores.shape, 1)
    scores = jnp.where(cols <= rows, scores, NEG_BIG)
    weights = jnp.exp(scores - jnp.max(scores, -1, keepdims=True))
    return weights * (1.0 / jnp.sum(weights, -1, keepdims=True))


def attend_sequence(cos, sin, load, kv_at, q_out, kv_out, o_out, at):
    first, low = lane_masks()

    def turn(u):
        return u * cos + swap_halves(u, first) * sin

    keys, vals_low, vals_high = [], [], []
    for tile in range(KV // 2):
        key = turn(load(kv_at + tile * LANES))
        val = load(kv_at + KV * HD + tile * LANES)
        kv_out[at, tile * LANES : (tile + 1) * LANES] = key.astype(BF16)
        kv_out[at, KV * HD + tile * LANES : KV * HD + (tile + 1) * LANES] = val.astype(BF16)
        for index in (0, 1):
            keys.append(twice(key, index, low).astype(BF16))
            both = twice(val, index, low)
            vals_low.append(jnp.where(low, both, 0.0).astype(BF16))
            vals_high.append(jnp.where(low, 0.0, both).astype(BF16))
    for pair in range(H // 2):
        group = pair * LANES // (H // KV * HD)
        query = turn(load(pair * LANES))
        p_low = causal_probs(jnp.where(low, query, 0.0).astype(BF16), keys[group])
        p_high = causal_probs(jnp.where(low, 0.0, query).astype(BF16), keys[group])
        q_out[at, pair * LANES : (pair + 1) * LANES] = query.astype(BF16)
        o_out[at, pair * LANES : (pair + 1) * LANES] = (
            dot(p_low.astype(BF16), vals_low[group]) + dot(p_high.astype(BF16), vals_high[group])
        ).astype(BF16)


def attend_back_sequence(cos, sin, q_ref, kv_ref, da_ref, dqkv_out, at):
    first, low = lane_masks()

    def turn_back(u):
        return (u * cos - swap_halves(u, first) * sin).astype(BF16)

    pair_total = H // KV * HD // LANES
    width = H * HD
    held = {}
    for group in range(KV):
        tile_at = group // 2 * LANES
        key = twice(kv_ref[at, tile_at : tile_at + LANES].astype(F32), group, low)
        val_at = KV * HD + tile_at
        val = twice(kv_ref[at, val_at : val_at + LANES].astype(F32), group, low).astype(BF16)
        key_low = jnp.where(low, key, 0.0).astype(BF16)
        key_high = jnp.where(low, 0.0, key).astype(BF16)
        key = key.astype(BF16)
        dk = jnp.zeros((SEQ, LANES), F32)
        dv = jnp.zeros((SEQ, LANES), F32)
        for pair in range(group * pair_total, (group + 1) * pair_total):
            query = q_ref[at, pair * LANES : (pair + 1) * LANES].astype(F32)
            grad = da_ref[at, pair * LANES : (pair + 1) * LANES].astype(F32)
            dq = None
            for is_low in (True, False):
                if is_low:
                    query_h = jnp.where(low, query, 0.0).astype(BF16)
                    grad_h = jnp.where(low, grad, 0.0).astype(BF16)
                else:
                    query_h = jnp.where(low, 0.0, query).astype(BF16)
                    grad_h = jnp.where(low, 0.0, grad).astype(BF16)
                prob = causal_probs(query_h, key)
                grad_prob = dot_nt(grad_h, val)
                delta = jnp.sum(prob * grad_prob, -1, keepdims=True)
                ds = (prob * (grad_prob - delta) * SCALE).astype(BF16)
                term = dot(ds, key_low if is_low else key_high)
                dq = term if dq is None else dq + term
                dk = dk + dot_tn(ds, query_h)
                dv = dv + dot_tn(prob.astype(BF16), grad_h)
            dqkv_out[at, pair * LANES : (pair + 1) * LANES] = turn_back(dq)
        held[group] = (dk + pltpu.roll(dk, HD, 1), dv + pltpu.roll(dv, HD, 1))
    for tile in range(KV // 2):
        col = width + tile * LANES
        dk = jnp.where(low, held[2 * tile][0], held[2 * tile + 1][0])
        dv = jnp.where(low, held[2 * tile][1], held[2 * tile + 1][1])
        dqkv_out[at, col : col + LANES] = turn_back(dk)
        dqkv_out[at, col + KV * HD : col + KV * HD + LANES] = dv.astype(BF16)


def attend_back_group(cos, sin, group, q_ref, kv_ref, da_ref, dqkv_out, dkv_out, at):
    first, low = lane_masks()
    head_width = H // KV * HD
    mine = low == (group % 2 == 0)

    def both(tile):
        kept = jnp.where(mine, tile.astype(F32), 0.0)
        return kept + pltpu.roll(kept, HD, 1)

    tile = pl.ds(pl.multiple_of(group // 2 * LANES, LANES), LANES)
    val_tile = pl.ds(pl.multiple_of(KV * HD + group // 2 * LANES, LANES), LANES)
    key = both(kv_ref[at, tile])
    val = both(kv_ref[at, val_tile]).astype(BF16)
    key_low = jnp.where(low, key, 0.0).astype(BF16)
    key_high = jnp.where(low, 0.0, key).astype(BF16)
    key = key.astype(BF16)
    dk = jnp.zeros((SEQ, LANES), F32)
    dv = jnp.zeros((SEQ, LANES), F32)
    for pair in range(head_width // LANES):
        c = pl.ds(pl.multiple_of(group * head_width + pair * LANES, LANES), LANES)
        query = q_ref[at, c].astype(F32)
        grad = da_ref[at, c].astype(F32)
        dq = None
        for is_low in (True, False):
            pick = low if is_low else jnp.logical_not(low)
            query_h = jnp.where(pick, query, 0.0).astype(BF16)
            grad_h = jnp.where(pick, grad, 0.0).astype(BF16)
            prob = causal_probs(query_h, key)
            grad_prob = dot_nt(grad_h, val)
            delta = jnp.sum(prob * grad_prob, -1, keepdims=True)
            ds = (prob * (grad_prob - delta) * SCALE).astype(BF16)
            term = dot(ds, key_low if is_low else key_high)
            dq = term if dq is None else dq + term
            dk = dk + dot_tn(ds, query_h)
            dv = dv + dot_tn(prob.astype(BF16), grad_h)
        dqkv_out[at, c] = (dq * cos - swap_halves(dq, first) * sin).astype(BF16)
    dkv_out[at, tile] += jnp.where(mine, dk + pltpu.roll(dk, HD, 1), 0.0)
    dkv_out[at, val_tile] += jnp.where(mine, dv + pltpu.roll(dv, HD, 1), 0.0)


def attend_kernel(cos_ref, sin_ref, qkv_ref, q_out, kv_out, o_out):
    attend_sequence(
        cos_ref[...], sin_ref[...], lambda c: qkv_ref[:, c : c + LANES], H * HD, q_out, kv_out, o_out, slice(None)
    )


def attend_back_kernel(cos_ref, sin_ref, q_ref, kv_ref, da_ref, dqkv_out):
    attend_back_sequence(cos_ref[...], sin_ref[...], q_ref, kv_ref, da_ref, dqkv_out, slice(None))


def by_sequence(body, name, ins, widths):
    rows = ins[0].shape[0]
    spec = lambda w: pl.BlockSpec((SEQ, w), lambda i: (i, 0))
    return pl.pallas_call(
        body,
        grid=(rows // SEQ,),
        in_specs=[spec(a.shape[1]) for a in ins],
        out_specs=[spec(w) for w in widths],
        out_shape=[jax.ShapeDtypeStruct((rows, w), BF16) for w in widths],
        name=name,
    )(*ins)


def attend(cos, sin, qkv):
    return by_sequence(attend_kernel, "attend", (cos, sin, qkv), (H * HD, 2 * KV * HD, H * HD))


def attend_back(cos, sin, query, key_val, grad):
    return by_sequence(
        attend_back_kernel, "attend_back", (cos, sin, query, key_val, grad), (H * HD + 2 * KV * HD,)
    )[0]


def norm_scale(rows):
    return lax.rsqrt(jnp.mean(rows * rows, -1, keepdims=True) + NORM_EPS)


def norm_back(rows, gain, grad_normed):
    inv = norm_scale(rows)
    weighted = grad_normed * gain
    grad_gain = jnp.sum(grad_normed * rows * inv, 0)
    grad_rows = inv * weighted - rows * inv**3 * jnp.mean(weighted * rows, -1, keepdims=True)
    return grad_rows, grad_gain


def rope_tables(positions):
    half = jnp.arange(LANES, dtype=jnp.int32) % (HD // 2)
    inv_freq = 10000.0 ** (-(half.astype(F32) * 2.0 / HD))
    angles = positions.astype(F32)[:, None] * inv_freq[None, :]
    sign = jnp.where(jnp.arange(LANES) % HD < HD // 2, -1.0, 1.0).astype(F32)
    return jnp.cos(angles), jnp.sin(angles) * sign[None, :]


MESH = pl.DeviceIdType.MESH
KV_ROWS = 64
GAIN_ROWS = 16


class Links:
    def __init__(self):
        self.d, self.z = lax.axis_index("dp"), lax.axis_index("tensor")
        core, x, y = self.d % 2, self.d // 2 % 2, self.d // 4
        self.dc = self.d + 1 - 2 * core
        step_x, step_y = 2 - 4 * x, 4 - 8 * y
        self.dx, self.dy, self.dxy = self.d + step_x, self.d + step_y, self.d + step_x + step_y
        self.dcx, self.dcy, self.dcxy = self.dc + step_x, self.dc + step_y, self.dc + step_x + step_y

    def barrier(self, far=False):
        z = self.z
        sem = pltpu.get_barrier_semaphore()

        def greet(d, zz):
            pl.semaphore_signal(sem, inc=1, device_id=(d, zz), device_id_type=MESH)

        for d in (self.dx, self.dy, self.dc):
            greet(d, z)
        if far:
            for j in (1, 2, 3):
                greet(self.d, (z + j) % 4)
            pl.semaphore_wait(sem, 6)
            return
        pl.when(z > 0)(lambda: greet(self.d, z - 1))
        pl.when(z < 3)(lambda: greet(self.d, z + 1))
        pl.semaphore_wait(sem, 3 + (z + 2) // 3 + (5 - z) // 3)


class Sender:
    def __init__(self, links, send_sem, recv_sem):
        self.links, self.send_sem, self.recv_sem = links, send_sem, recv_sem

    def copy(self, src, dst, at, to):
        return pltpu.make_async_remote_copy(
            src_ref=src,
            dst_ref=dst,
            send_sem=self.send_sem.at[at],
            recv_sem=self.recv_sem.at[at],
            device_id=to,
            device_id_type=MESH,
        )

    def start(self, src, dst, at, to):
        self.copy(src, dst, at, to).start()

    def landed(self, region, at):
        self.copy(region, region, at, (self.links.dc, self.links.z)).wait_recv()

    def sent(self, region, at):
        self.copy(region, region, at, (self.links.dc, self.links.z)).wait_send()


class Spread:
    def __init__(self, sender, region, base):
        self.s, self.region, self.base = sender, region, base

    def own(self, p, src):
        k, r, b = self.s.links, self.region, self.base + 9 * p
        mine = r(k.d, p, None)
        self.s.start(src, mine, b, (k.dx, k.z))
        self.s.start(src, mine, b + 1, (k.dy, k.z))
        self.s.start(src, mine, b + 2, (k.dc, k.z))

    def near(self, p):
        k, r, b = self.s.links, self.region, self.base + 9 * p
        self.s.landed(r(k.dx, p, None), b)
        self.s.start(r(k.dx, p, 0), r(k.dx, p, 0), b + 3, (k.dy, k.z))
        self.s.start(r(k.dx, p, None), r(k.dx, p, None), b + 5, (k.dc, k.z))
        self.s.landed(r(k.dy, p, None), b + 1)
        self.s.start(r(k.dy, p, 1), r(k.dy, p, 1), b + 4, (k.dx, k.z))
        self.s.start(r(k.dy, p, None), r(k.dy, p, None), b + 6, (k.dc, k.z))

    def far(self, p):
        k, r, b = self.s.links, self.region, self.base + 9 * p
        for part in (0, 1):
            self.s.landed(r(k.dxy, p, part), b + 3 + part)
            self.s.start(r(k.dxy, p, part), r(k.dxy, p, part), b + 7 + part, (k.dc, k.z))

    def finish(self, p):
        k, r, b = self.s.links, self.region, self.base + 9 * p
        self.s.landed(r(k.dc, p, None), b + 2)
        self.s.landed(r(k.dcx, p, None), b + 5)
        self.s.landed(r(k.dcy, p, None), b + 6)
        for part in (0, 1):
            self.s.landed(r(k.dcxy, p, part), b + 7 + part)

    def drain(self, p):
        k, r, b = self.s.links, self.region, self.base + 9 * p
        for i in (0, 1, 2):
            self.s.sent(r(k.d, p, None), b + i)
        self.s.sent(r(k.dx, p, 0), b + 3)
        self.s.sent(r(k.dy, p, 1), b + 4)
        self.s.sent(r(k.dx, p, None), b + 5)
        self.s.sent(r(k.dy, p, None), b + 6)
        for part in (0, 1):
            self.s.sent(r(k.dxy, p, part), b + 7 + part)


class Line:
    def __init__(self, sender, region, base):
        self.s, self.region, self.base = sender, region, base

    def _send(self, src, p, way, step):
        k = self.s.links
        self.s.start(src, self.region(p), self.base + 2 * (step - 1) + way, (k.d, k.z + 1 - 2 * way))

    def own(self, src):
        z = self.s.links.z
        pl.when(z < 3)(lambda: self._send(src, z, 0, 1))
        pl.when(z > 0)(lambda: self._send(src, z, 1, 1))

    def each(self, step, action):
        z = self.s.links.z
        pl.when(z >= step)(lambda: action(z - step, 0))
        pl.when(z + step <= 3)(lambda: action(z + step, 1))

    def arrive(self, step, then=None):
        z = self.s.links.z

        def action(p, way):
            self.s.landed(self.region(p), self.base + 2 * (step - 1) + way)
            if step < 3:
                ahead = z < 3 if way == 0 else z > 0
                pl.when(ahead)(lambda: self._send(self.region(p), p, way, step + 1))
            if then is not None:
                then(p)

        self.each(step, action)

    def drain(self):
        z = self.s.links.z
        for step in (1, 2, 3):
            for way in (0, 1):
                came = z - (step - 1) if way == 0 else z + (step - 1)
                ok = jnp.logical_and(z < 3, z >= step - 1) if way == 0 else jnp.logical_and(z > 0, z <= 4 - step)
                pl.when(ok)(
                    functools.partial(self.s.sent, self.region(came), self.base + 2 * (step - 1) + way)
                )


def forward_kernel(
    x_ref, g_ref, cos_ref, sin_ref, att_ref, wo_ref, gu_ref, wd_ref,
    wa_all, wo_all, gu_all, wd_all, n2_all, top_all, wqkv_all, hidden_all, dgu_all, out_all, dn2_land,
    q_out, kv_out, o_out, mid_out, gain_out, dn2_out,
    n1, qkv, w_buf, wkv_buf, gain_buf, wo_buf, n2, top,
    n2_rows, top_rows, gate_up, grad_hidden, hidden, dgu, dn2_sends, out_rows,
    send_sem, recv_sem, local_sem,
):
    rows, width = x_ref.shape
    slot_width = att_ref.shape[1]
    block = width // 8
    links = Links()
    d, z = links.d, links.z
    s = Sender(links, send_sem, recv_sem)
    cut_a = att_ref.shape[0] // 32 * 16
    cuts_a = ((0, cut_a), (cut_a, att_ref.shape[0] - cut_a))

    def at_a(dd, p, part):
        if part is None:
            return wa_all.at[dd, p]
        return wa_all.at[dd, p, pl.ds(*cuts_a[part])]

    def at_b(dd, p, part):
        start, size = (0, slot_width) if part is None else (part * slot_width // 2, slot_width // 2)
        return wo_all.at[
            pl.ds(pl.multiple_of(p * slot_width + start, 16), size),
            pl.ds(pl.multiple_of(dd * block, 128), block),
        ]

    def at_gu(dd, p, part):
        start, size = (0, block) if part is None else (part * block // 2, block // 2)
        return gu_all.at[pl.ds(pl.multiple_of(dd * block + start, 16), size)]

    ff = wd_ref.shape[0]

    def at_wd(dd, p, part):
        start, size = (0, ff) if part is None else (part * ff // 2, ff // 2)
        return wd_all.at[pl.ds(start, size), pl.ds(pl.multiple_of(dd * block, 128), block)]

    def rows_of(ref):
        return lambda p: ref.at[pl.ds(pl.multiple_of(p * rows, 16), rows)]

    spread_a, spread_b = Spread(s, at_a, 0), Spread(s, at_b, 36)
    spread_gu, spread_wd = Spread(s, at_gu, 72), Spread(s, at_wd, 81)
    line_a = Line(s, lambda p: at_a(d, p, None), 90)
    line_b = Line(s, lambda p: at_b(d, p, None), 96)
    line_n, line_t = Line(s, rows_of(n2_all), 102), Line(s, rows_of(top_all), 108)

    def keep(src, dst, at):
        pltpu.make_async_copy(src, dst, local_sem.at[at]).start()

    def kept(src, dst, at):
        pltpu.make_async_copy(src, dst, local_sem.at[at]).wait()

    links.barrier(far=True)

    line_a.own(att_ref)
    spread_a.own(z, att_ref)
    keep(att_ref, at_a(d, z, None), 0)
    keep(wo_ref, at_b(d, z, None), 1)
    keep(gu_ref, at_gu(d, 0, None), 2)
    keep(wd_ref, at_wd(d, 0, None), 3)
    top[...] = g_ref[...].astype(BF16)
    line_a.arrive(1, lambda p: spread_a.own(p, at_a(d, p, None)))
    spread_a.near(z)
    line_a.arrive(2, lambda p: spread_a.own(p, at_a(d, p, None)))
    line_b.own(wo_ref)
    line_a.each(1, lambda p, way: spread_a.near(p))
    spread_a.far(z)
    line_a.arrive(3, lambda p: spread_a.own(p, at_a(d, p, None)))
    line_b.arrive(1)
    line_a.each(2, lambda p, way: spread_a.near(p))
    line_a.each(1, lambda p, way: spread_a.far(p))
    spread_b.own(z, wo_ref)
    line_b.each(1, lambda p, way: spread_b.own(p, at_b(d, p, None)))
    line_a.each(3, lambda p, way: spread_a.near(p))
    line_b.arrive(2, lambda p: spread_b.own(p, at_b(d, p, None)))
    line_a.each(2, lambda p, way: spread_a.far(p))
    line_b.arrive(3, lambda p: spread_b.own(p, at_b(d, p, None)))
    line_t.own(top)
    line_a.each(3, lambda p, way: spread_a.far(p))
    kept(att_ref, at_a(d, z, None), 0)
    for p in range(4):
        spread_a.finish(p)

    def kv_copy(dd, p):
        return wkv_buf.at[dd, p], wqkv_all.at[pl.ds(dd * block + p * KV_ROWS, KV_ROWS), pl.ds(width, 2 * KV * HD)]

    for p in range(4):
        for dd in range(8):
            pltpu.make_async_copy(
                wa_all.at[dd, p, pl.ds(0, block)], w_buf.at[p, pl.ds(dd * block, block)], local_sem.at[14 + 8 * p + dd]
            ).start()
    keep(wa_all.at[:, :, pl.ds(block, KV_ROWS)], wkv_buf, 8)
    keep(wa_all.at[:, :, pl.ds(block + KV_ROWS, GAIN_ROWS), pl.ds(0, LANES)], gain_buf, 9)
    kept(wa_all.at[:, :, pl.ds(block + KV_ROWS, GAIN_ROWS), pl.ds(0, LANES)], gain_buf, 9)
    low_row = lax.broadcasted_iota(jnp.int32, (GAIN_ROWS, LANES), 1) < HD
    for dd in range(8):
        for half in (0, 1):
            first = gain_buf[dd, 2 * half].astype(F32)
            second = pltpu.roll(gain_buf[dd, 2 * half + 1].astype(F32), HD, 1)
            at = dd * block + half * LANES
            gain_out[:, at : at + LANES] = jnp.where(low_row, first, second)[:8]
    x = x_ref[...]
    n1[...] = (x * norm_scale(x) * gain_out[0:1]).astype(BF16)
    for p in range(4):
        for dd in range(8):
            kept(wa_all.at[dd, p, pl.ds(0, block)], w_buf.at[p, pl.ds(dd * block, block)], 14 + 8 * p + dd)
        for c in range(0, slot_width, 256):
            qkv[:, p * slot_width + c : p * slot_width + c + 256] = dot(n1[...], w_buf[p, :, c : c + 256])
        keep(w_buf.at[p], wqkv_all.at[:, pl.ds(p * slot_width, slot_width)], 4 + p)
    kept(wa_all.at[:, :, pl.ds(block, KV_ROWS)], wkv_buf, 8)
    qkv[:, width:] = dot(n1[...], wkv_buf[...].reshape(width, 2 * KV * HD))
    for p in range(4):
        for dd in range(8):
            pltpu.make_async_copy(*kv_copy(dd, p), local_sem.at[46 + 8 * p + dd]).start()

    line_t.arrive(1)
    line_b_pieces = lambda action: [action(z)] + [line_b.each(i, lambda p, way: action(p)) for i in (1, 2, 3)]

    def sequence(i, carry):
        at = pl.ds(pl.multiple_of(i * SEQ, SEQ), SEQ)
        attend_sequence(
            cos_ref[at], sin_ref[at], lambda c: qkv[at, c : c + LANES], width, q_out, kv_out, o_out, at
        )

        @pl.when(i == 0)
        def _():
            line_b_pieces(spread_b.near)
            spread_gu.own(0, gu_ref)

        return carry

    lax.fori_loop(0, rows // SEQ, sequence, 0)
    line_t.arrive(2)
    line_b_pieces(spread_b.far)
    spread_wd.own(0, wd_ref)
    kept(wo_ref, at_b(d, z, None), 1)
    for p in range(4):
        spread_b.finish(p)
    keep(wo_all, wo_buf, 0)
    kept(wo_all, wo_buf, 0)

    def column(i, carry):
        at = pl.ds(pl.multiple_of(i * 256, 256), 256)
        mid_out[:, at] = x_ref[:, at] + dot(o_out[...], wo_buf[:, at])
        return carry

    lax.fori_loop(0, width // 256, column, 0)
    mid = mid_out[...]
    n2[...] = (mid * norm_scale(mid) * gain_out[1:2]).astype(BF16)

    line_n.own(n2)
    keep(n2, n2_all.at[pl.ds(pl.multiple_of(z * rows, 16), rows)], 8)
    keep(top, top_all.at[pl.ds(pl.multiple_of(z * rows, 16), rows)], 9)
    line_t.arrive(3)
    spread_gu.near(0)
    line_n.arrive(1)
    spread_gu.far(0)
    spread_wd.near(0)
    line_n.arrive(2)
    spread_wd.far(0)
    spread_gu.finish(0)
    spread_wd.finish(0)
    kept(gu_ref, at_gu(d, 0, None), 2)
    kept(wd_ref, at_wd(d, 0, None), 3)
    for p in range(4):
        kept(w_buf.at[p], wqkv_all.at[:, pl.ds(p * slot_width, slot_width)], 4 + p)
        for dd in range(8):
            kept(*kv_copy(dd, p), 46 + 8 * p + dd)
    kept(n2, n2_all.at[pl.ds(pl.multiple_of(z * rows, 16), rows)], 8)
    kept(top, top_all.at[pl.ds(pl.multiple_of(z * rows, 16), rows)], 9)

    wide = 2 * ff
    pieces = [(c, min(slot_width, wide - c)) for c in range(0, wide, slot_width)]
    gu_piece = lambda i, c, n: (columns(gu_all, c, n), w_buf.at[i, :, pl.ds(0, n)])
    for i, (c, n) in enumerate(pieces):
        keep(*gu_piece(i, c, n), 14 + i)
    wd_vmem = wo_buf.at[pl.ds(0, ff)]
    keep(wd_all, wd_vmem, 20)
    nearest = z - 1 + 2 * ((3 - z) // 3)
    farthest = 3 - 3 * (z // 2)
    between = 6 - z - nearest - farthest
    for i, (c, n) in enumerate(pieces):
        kept(*gu_piece(i, c, n), 14 + i)
    kept(wd_all, wd_vmem, 20)
    chunks = [(c, min(256, ff - c)) for c in range(0, ff, 256)]

    def feed(i):
        pl.when(i == 2)(lambda: line_n.arrive(3))
        second = (i + 2) // 3 - i // 2
        p = nearest * ((3 - i) // 3) + between * second + farthest * (i // 2 - i // 3) + z * (i // 3)
        at = pl.ds(pl.multiple_of(p * rows, 16), rows)
        keep(n2_all.at[at], n2_rows, 0)
        keep(top_all.at[at], top_rows, 1)
        kept(n2_all.at[at], n2_rows, 0)
        for c, n in pieces:
            for h in range(0, n, 256):
                gate_up[:, c + h : c + h + 256] = dot(n2_rows[...], w_buf[c // slot_width, :, h : h + 256])
        kept(top_all.at[at], top_rows, 1)
        for c, n in chunks:
            grad_hidden[:, c : c + n] = dot_nt(top_rows[...], wo_buf[c : c + n])

        @pl.when(i > 0)
        def _():
            kept(hidden, hidden_all.at[at], 2)
            kept(dgu, dgu_all.at[at], 3)

        def act(m):
            r = pl.ds(pl.multiple_of(m * 16, 16), 16)
            for c, n in chunks:
                gate, up, grad = gate_up[r, c : c + n], gate_up[r, ff + c : ff + c + n], grad_hidden[r, c : c + n]
                sig = 1.0 / (1.0 + jnp.exp(-gate))
                silu = gate * sig
                hidden[r, c : c + n] = (silu * up).astype(BF16)
                dgu[r, c : c + n] = (grad * up * sig * (1.0 + gate * (1.0 - sig))).astype(BF16)
                dgu[r, ff + c : ff + c + n] = (grad * silu).astype(BF16)

        loop(rows // 16, act)
        keep(hidden, hidden_all.at[at], 2)
        keep(dgu, dgu_all.at[at], 3)

        def back(m):
            r = pl.ds(pl.multiple_of(m * 256, 256), 256)
            total = None
            for j, (c, n) in enumerate(pieces):
                term = dot_nt(dgu[:, c : c + n], w_buf[j, r, :n])
                total = term if total is None else total + term

            @pl.when(i < 3)
            def _():
                dn2_sends[i, :, r] = total.astype(BF16)

            @pl.when(i == 3)
            def _():
                dn2_out[:, r] = total

        loop(width // 256, back)

        @pl.when(i < 3)
        def _():
            j = (p - z + 4) % 4 - 1
            s.start(dn2_sends.at[i], dn2_land.at[j], 114 + j, (d, p))

        pl.when(i > 0)(lambda: kept(out_rows, out_all.at[at], 7))

        def down(m):
            r = pl.ds(pl.multiple_of(m * 256, 256), 256)
            out_rows[:, r] = dot(hidden[...], wo_buf[:ff, r]).astype(BF16)

        loop(width // 256, down)
        keep(out_rows, out_all.at[at], 7)

    loop(4, feed)
    kept(hidden, hidden_all.at[pl.ds(0, rows)], 2)
    kept(dgu, dgu_all.at[pl.ds(0, rows)], 3)
    kept(out_rows, out_all.at[pl.ds(0, rows)], 7)
    for j in range(3):
        s.landed(dn2_land.at[j], 114 + j)
        keep(dn2_land.at[j], n2_rows, 0)
        kept(dn2_land.at[j], n2_rows, 0)

        def add(m):
            r = pl.ds(pl.multiple_of(m * 16, 16), 16)
            dn2_out[r] += n2_rows[r].astype(F32)

        loop(rows // 16, add)
        s.sent(dn2_sends.at[0], 114 + j)
    for p in range(4):
        spread_a.drain(p)
        spread_b.drain(p)
    spread_gu.drain(0)
    spread_wd.drain(0)
    for line in (line_a, line_b, line_n, line_t):
        line.drain()


def forward_stage(x, g, cos, sin, att, wo, gu, wd):
    rows, width = x.shape
    slot_width = att.shape[1]
    block = width // 8
    kv_width = 2 * KV * HD
    ff = wd.shape[0]
    vmem = pl.BlockSpec(memory_space=pltpu.VMEM)
    hbm = pl.BlockSpec(memory_space=pltpu.HBM)
    shape = jax.ShapeDtypeStruct
    outs = [
        (hbm, shape((8, 4) + att.shape, BF16)),
        (hbm, shape((width, width), BF16)),
        (hbm, shape((width, gu.shape[1]), BF16)),
        (hbm, shape((ff, width), BF16)),
        (hbm, shape((4 * rows, width), BF16)),
        (hbm, shape((4 * rows, width), BF16)),
        (hbm, shape((width, width + kv_width), BF16)),
        (hbm, shape((4 * rows, ff), BF16)),
        (hbm, shape((4 * rows, 2 * ff), BF16)),
        (hbm, shape((4 * rows, width), BF16)),
        (hbm, shape((3, rows, width), BF16)),
        (vmem, shape((rows, width), BF16)),
        (vmem, shape((rows, kv_width), BF16)),
        (vmem, shape((rows, width), BF16)),
        (vmem, shape((rows, width), F32)),
        (vmem, shape((8, width), F32)),
        (vmem, shape((rows, width), F32)),
    ]
    return pl.pallas_call(
        forward_kernel,
        in_specs=[vmem] * 8,
        out_specs=[o[0] for o in outs],
        out_shape=[o[1] for o in outs],
        scratch_shapes=[
            pltpu.VMEM((rows, width), BF16),
            pltpu.VMEM((rows, width + kv_width), F32),
            pltpu.VMEM((-(-2 * ff // slot_width), width, slot_width), BF16),
            pltpu.VMEM((8, 4, KV_ROWS, kv_width), BF16),
            pltpu.VMEM((8, 4, GAIN_ROWS, LANES), BF16),
            pltpu.VMEM((width, width), BF16),
            pltpu.VMEM((rows, width), BF16),
            pltpu.VMEM((rows, width), BF16),
            pltpu.VMEM((rows, width), BF16),
            pltpu.VMEM((rows, width), BF16),
            pltpu.VMEM((rows, 2 * ff), F32),
            pltpu.VMEM((rows, ff), F32),
            pltpu.VMEM((rows, ff), BF16),
            pltpu.VMEM((rows, 2 * ff), BF16),
            pltpu.VMEM((3, rows, width), BF16),
            pltpu.VMEM((rows, width), BF16),
            pltpu.SemaphoreType.DMA((117,)),
            pltpu.SemaphoreType.DMA((117,)),
            pltpu.SemaphoreType.DMA((78,)),
        ],
        compiler_params=pltpu.CompilerParams(
            collective_id=0, has_side_effects=True, vmem_limit_bytes=65000 * 1024
        ),
        name="forward",
    )(x, g, cos, sin, att, wo, gu, wd)


def loop(count, body):
    def step(i, carry):
        body(i)
        return carry

    lax.fori_loop(0, count, step, 0)


class Local:
    def __init__(self, sem):
        self.sem, self.next = sem, 0

    def start(self, src, dst):
        copy = pltpu.make_async_copy(src, dst, self.sem.at[self.next])
        self.next += 1
        copy.start()
        return copy

    def load(self, src, dst):
        self.start(src, dst).wait()


class Reduce:
    def __init__(self, sender, compute, base, sends, kept, land, halves):
        self.s, self.compute, self.base = sender, compute, base
        self.sends, self.kept, self.land, self.halves = sends, kept, land, halves

    def half(self, ref, part):
        return ref.at[pl.ds(*self.halves[part])]

    def place(self, i):
        if i < 4:
            return self.land.at[i]
        return self.half(self.land.at[4 + (i - 4) // 2], i % 2)

    def partner(self, i):
        k = self.s.links
        count = self.sends.shape[0]
        if i >= count:
            self.s.sent(self.sends.at[i % count], self.base + i - count)
        self.compute((k.dcxy, k.dcx, k.dcy, k.dc)[i], None, self.sends.at[i % count])
        self.s.start(self.sends.at[i % count], self.place(i), self.base + i, (k.dc, k.z))

    def own(self, i):
        k, b = self.s.links, self.base
        to_x, to_y = (k.dx, k.z), (k.dy, k.z)
        self.s.landed(self.place(i), b + i)
        kept = self.kept.at[i]
        self.compute((k.dxy, k.dx, k.dy, k.d)[i], self.land.at[i], kept)
        if i == 0:
            self.s.start(self.half(kept, 0), self.place(4), b + 4, to_x)
            self.s.start(self.half(kept, 1), self.place(7), b + 7, to_y)
        elif i == 1:
            self.s.start(self.half(kept, 0), self.place(6), b + 6, to_x)
        elif i == 2:
            self.s.start(self.half(kept, 1), self.place(5), b + 5, to_y)

    def first(self):
        self.partner(0)
        for i in range(3):
            self.partner(i + 1)
            self.own(i)
        self.own(3)

    def add(self, i, part, at):
        self.s.landed(self.place(at), self.base + at)
        start, size = self.halves[part]
        from_start = self.halves[at % 2][0] if at < 8 else self.halves[at - 8][0]
        slot = 4 + (at - 4) // 2
        step = 32 if size % 32 == 0 else 16

        def rows(n):
            r = pl.ds(pl.multiple_of(start + n * step, 16), step)
            g = pl.ds(pl.multiple_of(from_start + n * step, 16), step)
            self.kept[i, r] = (self.kept[i, r].astype(F32) + self.land[slot, g].astype(F32)).astype(BF16)

        loop(size // step, rows)

    def second(self):
        k, b = self.s.links, self.base
        self.add(2, 0, 4)
        self.s.start(self.half(self.kept.at[2], 0), self.place(8), b + 8, (k.dy, k.z))
        self.add(1, 1, 7)
        self.s.start(self.half(self.kept.at[1], 1), self.place(9), b + 9, (k.dx, k.z))

    def last(self):
        self.add(3, 0, 6)
        self.add(3, 1, 5)
        self.add(3, 0, 8)
        self.add(3, 1, 9)

    def drain(self):
        b, kept = self.base, self.kept
        count = self.sends.shape[0]
        for i in range(4 - count, 4):
            self.s.sent(self.sends.at[i % count], b + i)
        self.s.sent(self.half(kept.at[0], 0), b + 4)
        self.s.sent(self.half(kept.at[2], 1), b + 5)
        self.s.sent(self.half(kept.at[1], 0), b + 6)
        self.s.sent(self.half(kept.at[0], 1), b + 7)
        self.s.sent(self.half(kept.at[2], 0), b + 8)
        self.s.sent(self.half(kept.at[1], 1), b + 9)


class LineSum:
    def __init__(self, sender, local, part, sends, land, base):
        self.s, self.part, self.sends = sender, part, sends
        self.land, self.base = land, base
        self.rows = sends.shape[1]
        self.sem, self.first = local.sem, local.next
        local.next += 7

    def rows_of(self, t):
        return self.part.at[pl.ds(pl.multiple_of(t * self.rows, 16), self.rows)]

    def fetch(self, holds, slot, at):
        return pltpu.make_async_copy(self.rows_of(holds), self.sends.at[slot], self.sem.at[self.first + at])

    def begin(self):
        for s in (1, 2, 3):
            for sends, slot, place, holds, _, _ in self.ways(s):
                pl.when(sends)(lambda: self.fetch(holds, slot, place).start())
        self.fetch(self.s.links.z, 3, 6).start()
        self.step(1)

    def add(self, into, at):
        self.s.landed(self.land.at[at], self.base + at)

        def rows(n):
            r = pl.ds(pl.multiple_of(n * 32, 32), 32)
            self.sends[into, r] = (self.sends[into, r].astype(F32) + self.land[at, r].astype(F32)).astype(BF16)

        loop(self.rows // 32, rows)

    def ways(self, s):
        z = self.s.links.z
        right = (z <= s - 1, s - 1 - z, 2 * (s - 1), z + 4 - s, z >= 1, z + 1)
        left = (z >= 4 - s, s - 1, 2 * (s - 1) + 1, z - 4 + s, z <= 2, z - 1)
        return right, left

    def step(self, s):
        for sends, slot, place, holds, received, to in self.ways(s):

            @pl.when(sends)
            def _():
                self.fetch(holds, slot, place).wait()
                if s > 1:
                    pl.when(received)(lambda: self.add(slot, place - 2))
                self.s.start(self.sends.at[slot], self.land.at[place], self.base + place, (self.s.links.d, to))

    def finish(self, write):
        z = self.s.links.z
        self.fetch(z, 3, 6).wait()
        pl.when(z >= 1)(lambda: self.add(3, 4))
        pl.when(z <= 2)(lambda: self.add(3, 5))

        def rows(n):
            r = pl.ds(pl.multiple_of(n * 32, 32), 32)
            write(r, self.sends[3, r].astype(F32))

        loop(self.rows // 32, rows)

    def drain(self):
        for s in (1, 2, 3):
            for sends, slot, place, _, _, _ in self.ways(s):
                pl.when(sends)(functools.partial(self.s.sent, self.sends.at[slot], self.base + place))


def stream(local, count, source, bufs, body):
    first = local.next
    local.next += 2

    def copy(n, slot):
        return pltpu.make_async_copy(source(n), bufs.at[slot], local.sem.at[first + slot])

    copy(0, 0).start()

    def step(n):
        slot = n % 2
        copy(n, slot).wait()

        @pl.when(n + 1 < count)
        def _():
            copy(n + 1, 1 - slot).start()

        body(n, bufs.at[slot])

    loop(count, step)


def turned(ref):
    return jnp.transpose(ref[...].astype(F32)).astype(BF16)


def columns(ref, start, size):
    return ref.at[:, pl.ds(pl.multiple_of(start, 128), size)]


class Feeder:
    def __init__(self, local, source, bufs, block, dests):
        self.source, self.bufs, self.block, self.dests = source, bufs, block, dests
        self.sem, self.first, self.n = local.sem, local.next, 0
        local.next += 2
        self._copy(0).start()

    def _copy(self, n):
        return pltpu.make_async_copy(
            columns(self.source, self.dests[n] * self.block, self.block),
            self.bufs.at[n % 2],
            self.sem.at[self.first + n % 2],
        )

    def __call__(self, dest):
        n = self.n
        self.n += 1
        self._copy(n).wait()
        if n + 1 < len(self.dests):
            self._copy(n + 1).start()
        return self.bufs.at[n % 2]


def order_of(k):
    partner, own = (k.dcxy, k.dcx, k.dcy, k.dc), (k.dxy, k.dx, k.dy, k.d)
    return [partner[0], partner[1], own[0], partner[2], own[1], partner[3], own[2], own[3]]


def row_blocks(pick, left, right):
    width = right.shape[1]

    def compute(dest, add, out):
        left[...] = turned(pick(dest))

        def chunk(n):
            c = pl.ds(pl.multiple_of(n * 256, 256), 256)
            total = dot(left[...], right[:, c])
            if add is not None:
                total = total + add[:, c].astype(F32)
            out[:, c] = total.astype(BF16)

        loop(width // 256, chunk)

    return compute


def column_blocks(left, pick, chunks):
    size = left.shape[0] // chunks

    def compute(dest, add, out):
        picked = pick(dest)

        def chunk(n):
            r = pl.ds(pl.multiple_of(n * size, 16), size)
            total = dot(left[r], picked[...])
            if add is not None:
                total = total + add[r].astype(F32)
            out[r] = total.astype(BF16)

        loop(chunks, chunk)

    return compute


class Chunk:
    def __init__(self, sender, compute, sends, kept, land, base):
        self.s, self.compute, self.sends = sender, compute, sends
        self.kept, self.land, self.base = kept, land, base
        self.half = kept.shape[2] // 2

    def views(self, n):
        kept, land, h = self.kept.at[n], self.land.at[n], self.half
        top, low = pl.ds(0, h), pl.ds(h, h)
        return {
            "x1": (kept.at[pl.ds(0, 2), top], land.at[pl.ds(4, 2), top]),
            "y1": (kept.at[pl.ds(1, 2), low], land.at[pl.ds(4, 2), low]),
            "y2": (kept.at[2, top], land.at[6, top]),
            "x2": (kept.at[0, low], land.at[6, low]),
        }

    def partner(self, n):
        k = self.s.links
        for i, dest in enumerate((k.dcx, k.dcxy, k.dcy, k.dc)):
            self.compute(n, dest, None, self.sends.at[n, i])
        self.s.start(self.sends.at[n], self.land.at[n, pl.ds(0, 4)], self.base + 5 * n, (k.dc, k.z))

    def own(self, n):
        k, b, v = self.s.links, self.base + 5 * n, self.views(n)
        self.s.landed(self.land.at[n, pl.ds(0, 4)], b)
        for i, dest in enumerate((k.dx, k.dxy, k.dy, k.d)):
            self.compute(n, dest, self.land.at[n, i], self.kept.at[n, i])
        self.s.start(*v["x1"], b + 1, (k.dx, k.z))
        self.s.start(*v["y1"], b + 2, (k.dy, k.z))

    def add(self, n, i, start, got):
        kept, land = self.kept, self.land

        def rows(m):
            r = pl.ds(pl.multiple_of(start + m * 32, 32), 32)
            kept[n, i, r] = (kept[n, i, r].astype(F32) + land[n, got, r].astype(F32)).astype(BF16)

        loop(self.half // 32, rows)

    def second(self, n):
        k, b, v = self.s.links, self.base + 5 * n, self.views(n)
        self.s.landed(v["x1"][1], b + 1)
        self.add(n, 2, 0, 5)
        self.s.start(*v["y2"], b + 3, (k.dy, k.z))
        self.s.landed(v["y1"][1], b + 2)
        self.add(n, 0, self.half, 4)
        self.s.start(*v["x2"], b + 4, (k.dx, k.z))
        self.add(n, 3, 0, 4)
        self.add(n, 3, self.half, 5)

    def last(self, n):
        b, v = self.base + 5 * n, self.views(n)
        self.s.landed(v["y2"][1], b + 3)
        self.add(n, 3, 0, 6)
        self.s.landed(v["x2"][1], b + 4)
        self.add(n, 3, self.half, 6)

    def drain(self):
        for n in range(self.kept.shape[0]):
            b, v = self.base + 5 * n, self.views(n)
            self.s.sent(self.sends.at[n], b)
            for at, name in enumerate(("x1", "y1", "y2", "x2")):
                self.s.sent(v[name][0], b + 1 + at)


class Spread4:
    def __init__(self, sender, pick, land, base):
        self.s, self.pick, self.land, self.base = sender, pick, land, base

    def send(self):
        k = self.s.links
        for j in (1, 2, 3):
            to = (k.z + j) % 4
            self.s.start(self.pick(to), self.land.at[j - 1], self.base + j - 1, (k.d, to))

    def landed(self):
        for j in range(3):
            self.s.landed(self.land.at[j], self.base + j)

    def drain(self):
        z = self.s.links.z
        for j in (1, 2, 3):
            self.s.sent(self.pick((z + j) % 4), self.base + j - 1)


def feed_back_kernel(
    part_ref, n2_ref, dgu_ref, hidden_ref, top_ref, mid_ref,
    out_ref, ggu_out, gd_out,
    dgu, top_cols, n2_cols, left, sends, kept, land, hidden_cols, hidden_t, d_sends, d_kept, d_land,
    line_sends, line_land, send_sem, recv_sem, local_sem,
):
    links = Links()
    s = Sender(links, send_sem, recv_sem)
    local = Local(local_sem)
    block = left.shape[0]
    ff = hidden_t.shape[0]
    halves = lambda size: ((0, size // 2), (size // 2, size // 2))
    top_feed = Feeder(local, top_ref, top_cols, block, order_of(links))
    links.barrier()
    line = LineSum(s, local, part_ref, line_sends, line_land, 20)
    line.begin()
    fetch = local.start(dgu_ref, dgu)
    n2_feed = Feeder(local, n2_ref, n2_cols, block, order_of(links))

    def turn_hidden(n, buf):
        hidden_t[pl.ds(pl.multiple_of(n * 128, 128), 128)] = turned(buf)

    stream(local, ff // 128, lambda n: columns(hidden_ref, n * 128, 128), hidden_cols, turn_hidden)
    grad_d = Reduce(s, column_blocks(hidden_t, top_feed, 4), 10, d_sends, d_kept, d_land, halves(ff))
    grad_d.first()
    fetch.wait()
    line.step(2)
    grads = Reduce(s, row_blocks(n2_feed, left, dgu), 0, sends, kept, land, halves(block))
    grads.partner(0)
    grads.partner(1)
    grads.own(0)
    grad_d.second()
    grads.partner(2)
    grads.own(1)
    grads.partner(3)
    line.step(3)
    grads.own(2)
    grads.own(3)
    grad_d.last()
    to_down = local.start(d_kept.at[3], gd_out)
    grads.second()

    def write(r, total):
        out_ref[r] = mid_ref[r] + total

    line.finish(write)
    grads.last()
    local.load(kept.at[3], ggu_out)
    to_down.wait()
    grads.drain()
    grad_d.drain()
    line.drain()


def feed_back(part, n2, dgu, hidden, top, mid):
    rows, width = part.shape[0] // 4, part.shape[1]
    block, wide, ff = width // 8, dgu.shape[1], hidden.shape[1]
    vmem = pl.BlockSpec(memory_space=pltpu.VMEM)
    hbm = pl.BlockSpec(memory_space=pltpu.HBM)
    shape = jax.ShapeDtypeStruct
    return pl.pallas_call(
        feed_back_kernel,
        in_specs=[hbm] * 5 + [vmem],
        out_specs=[vmem, hbm, hbm],
        out_shape=[shape((rows, width), F32), shape((block, wide), BF16), shape((ff, block), BF16)],
        scratch_shapes=[
            pltpu.VMEM((4 * rows, wide), BF16),
            pltpu.VMEM((2, 4 * rows, block), BF16),
            pltpu.VMEM((2, 4 * rows, block), BF16),
            pltpu.VMEM((block, 4 * rows), BF16),
            pltpu.VMEM((2, block, wide), BF16),
            pltpu.VMEM((4, block, wide), BF16),
            pltpu.VMEM((7, block, wide), BF16),
            pltpu.VMEM((2, 4 * rows, 128), BF16),
            pltpu.VMEM((ff, 4 * rows), BF16),
            pltpu.VMEM((2, ff, block), BF16),
            pltpu.VMEM((4, ff, block), BF16),
            pltpu.VMEM((7, ff, block), BF16),
            pltpu.VMEM((4, rows, width), BF16),
            pltpu.VMEM((6, rows, width), BF16),
            pltpu.SemaphoreType.DMA((26,)),
            pltpu.SemaphoreType.DMA((26,)),
            pltpu.SemaphoreType.DMA((20,)),
        ],
        compiler_params=pltpu.CompilerParams(
            collective_id=1, has_side_effects=True, vmem_limit_bytes=65000 * 1024
        ),
        name="feed_back",
    )(part, n2, dgu, hidden, top, mid)


def norm_back_rows(rows_ref, at, gain, grad_normed):
    rows = rows_ref[at]
    inv = norm_scale(rows)
    weighted = grad_normed * gain
    scaled = grad_normed * rows * inv
    grad_rows = inv * weighted - rows * (inv * inv * inv) * jnp.mean(weighted * rows, -1, keepdims=True)
    return grad_rows, scaled


def attention_back_kernel(
    dn2_ref, mid_ref, x_ref, g_ref, gain_ref, cos_ref, sin_ref, q_ref, kv_ref, att_ref,
    wo_ref, wqkv_ref,
    grad_in_out, gq_out, gkv_out, go_out, gain_out,
    mid_bf, da, dqkv, dkv, dn1, n1, n1_t, att_t, w_chunk,
    row_sends, row_kept, land_row, o_sends, o_kept, land_o,
    gain_part, gain_land, z_q, z_kv, z_o,
    send_sem, recv_sem, local_sem,
):
    rows, width = x_ref.shape
    block = width // 8
    kv_width = 2 * KV * HD
    slot = width // 4
    links = Links()
    d, z = links.d, links.z
    s = Sender(links, send_sem, recv_sem)
    local = Local(local_sem)
    links.barrier(far=True)

    gain_part[...] = jnp.zeros_like(gain_part)
    dkv[...] = jnp.zeros_like(dkv)
    step = 32

    def add_gain(row, scaled):
        for b in range(8):
            total = jnp.sum(scaled[:, b * block : (b + 1) * block], 0, keepdims=True)
            at = (b % 2, b // 2 % 2 * 2 + b // 4)
            gain_part[at[0], at[1], row : row + 1] += total

    def middle(n):
        r = pl.ds(pl.multiple_of(n * step, step), step)
        grad_rows, scaled = norm_back_rows(mid_ref, r, gain_ref[1:2], dn2_ref[r])
        grad = g_ref[r] + grad_rows
        grad_in_out[r] = grad
        mid_bf[r] = grad.astype(BF16)
        add_gain(1, scaled)
        rows_x = x_ref[r]
        n1[r] = (rows_x * norm_scale(rows_x) * gain_ref[0:1]).astype(BF16)

    loop(rows // step, middle)

    def transpose_into(src, dst):
        def part(n):
            c = pl.ds(pl.multiple_of(n * 128, 128), 128)
            dst[c] = jnp.transpose(src[:, c].astype(F32)).astype(BF16)

        loop(src.shape[1] // 128, part)

    transpose_into(att_ref, att_t)
    halves = lambda size: ((0, size // 2), (size // 2, size // 2))
    pick_mid = lambda dest: columns(mid_bf, dest * block, block)
    grad_o = Reduce(s, column_blocks(att_t, pick_mid, 4), 0, o_sends, o_kept, land_o, halves(width))
    grad_o.first()
    transpose_into(n1, n1_t)

    def attended(n, buf):
        da[:, pl.ds(pl.multiple_of(n * 256, 256), 256)] = dot_nt(mid_bf[...], buf[...]).astype(BF16)

    row_chunk = lambda ref: lambda n: ref.at[pl.ds(pl.multiple_of(n * 256, 256), 256)]
    stream(local, width // 256, row_chunk(wo_ref), w_chunk.at[:, :, pl.ds(0, width)], attended)

    def group_of(n):
        return (z + 1 + n) % 4

    def row_compute(n, dest, add, out):
        left = n1_t[pl.ds(pl.multiple_of(dest * block, block), block)]
        start = group_of(n) * slot * (1 - n // 4) + width * (n // 4)
        for c in range(0, slot, 256):
            total = dot(left, dqkv[:, pl.ds(pl.multiple_of(start + c, 256), 256)])
            if add is not None:
                total = total + add[:, c : c + 256].astype(F32)
            out[:, c : c + 256] = total.astype(BF16)

    grad_row = Chunk(s, row_compute, row_sends, row_kept, land_row, 10)

    def final_q(n):
        grad_row.last(n)

        @pl.when(n < 3)
        def _():
            s.start(row_kept.at[n, 3], z_q.at[n], 35 + n, (d, group_of(n)))

    def group_step(n):
        group = group_of(n)

        def sequence(i):
            at = pl.ds(pl.multiple_of(i * SEQ, SEQ), SEQ)
            attend_back_group(cos_ref[at], sin_ref[at], group, q_ref, kv_ref, da, dqkv, dkv, at)

        loop(rows // SEQ, sequence)
        grad_row.partner(n)
        pl.when(n == 1)(grad_o.second)
        pl.when(n >= 1)(lambda: grad_row.own(n - 1))
        pl.when(n >= 2)(lambda: grad_row.second(n - 2))
        pl.when(n == 3)(lambda: final_q(0))

    loop(4, group_step)

    def key_value(i):
        at = pl.ds(pl.multiple_of(i * SEQ, SEQ), SEQ)
        first, _ = lane_masks()
        for tile in range(KV // 2):
            c = tile * LANES
            u = dkv[at, c : c + LANES]
            dqkv[at, width + c : width + c + LANES] = (
                u * cos_ref[at] - swap_halves(u, first) * sin_ref[at]
            ).astype(BF16)
        dqkv[at, width + KV * HD :] = dkv[at, KV * HD :].astype(BF16)

    loop(rows // SEQ, key_value)
    grad_row.partner(4)
    grad_o.last()
    send_o = Spread4(s, lambda p: o_kept.at[3, pl.ds(pl.multiple_of(p * slot, 16), slot)], z_o, 41)
    send_o.send()
    grad_row.own(3)
    grad_row.second(2)
    final_q(1)
    grad_row.own(4)
    grad_row.second(3)
    final_q(2)

    def projected(n, buf):
        dn1[:, pl.ds(pl.multiple_of(n * 256, 256), 256)] = dot_nt(dqkv[...], buf[...])

    stream(local, width // 256, row_chunk(wqkv_ref), w_chunk, projected)
    grad_row.second(4)
    final_q(3)

    def inward(n):
        r = pl.ds(pl.multiple_of(n * step, step), step)
        grad_rows, scaled = norm_back_rows(x_ref, r, gain_ref[0:1], dn1[r])
        grad_in_out[r] += grad_rows
        add_gain(0, scaled)

    loop(rows // step, inward)

    core, x_at, y_at = d % 2, d // 2 % 2, d // 4
    s.start(gain_part.at[1 - core], gain_land.at[pl.ds(0, 4)], 44, (links.dc, z))
    grad_row.last(4)
    send_kv = Spread4(
        s, lambda p: row_kept.at[4, 3, pl.ds(pl.multiple_of(p * KV_ROWS, 16), KV_ROWS)], z_kv, 38
    )
    send_kv.send()
    s.landed(gain_land.at[pl.ds(0, 4)], 44)
    gain_part[core] += gain_land[0:4]
    other_x = pl.multiple_of(2 - 2 * x_at, 2)
    s.start(gain_part.at[core, pl.ds(other_x, 2)], gain_land.at[pl.ds(4, 2)], 45, (links.dx, z))
    send_o.landed()

    def out_rows(n):
        r = pl.ds(pl.multiple_of(n * 16, 16), 16)
        mine = pl.ds(pl.multiple_of(z * slot + n * 16, 16), 16)
        go_out[r] = (
            o_kept[3, mine].astype(F32) + z_o[0, r].astype(F32) + z_o[1, r].astype(F32) + z_o[2, r].astype(F32)
        )

    loop(slot // 16, out_rows)
    s.landed(gain_land.at[pl.ds(4, 2)], 45)
    mine_x = 2 * x_at
    gain_part[core, pl.ds(mine_x, 2)] += gain_land[4:6]
    s.start(gain_part.at[core, mine_x + 1 - y_at], gain_land.at[6], 46, (links.dy, z))
    for n in range(3):
        s.landed(z_q.at[n], 35 + n)

    def query_rows(n):
        r = pl.ds(pl.multiple_of(n * 16, 16), 16)
        gq_out[r] = (
            row_kept[3, 3, r].astype(F32) + z_q[0, r].astype(F32) + z_q[1, r].astype(F32) + z_q[2, r].astype(F32)
        )

    loop(block // 16, query_rows)
    s.landed(gain_land.at[6], 46)
    gain_part[core, mine_x + y_at] += gain_land[6]
    send_g = Spread4(s, lambda p: gain_part.at[core, mine_x + y_at], gain_land.at[pl.ds(7, 3)], 47)
    send_g.send()
    send_kv.landed()
    mine_kv = pl.ds(pl.multiple_of(z * KV_ROWS, 16), KV_ROWS)
    gkv_out[...] = row_kept[4, 3, mine_kv].astype(F32) + (
        z_kv[0].astype(F32) + z_kv[1].astype(F32) + z_kv[2].astype(F32)
    )
    send_g.landed()
    gain_out[...] = gain_part[core, mine_x + y_at] + gain_land[7] + gain_land[8] + gain_land[9]

    for unit in (grad_o, grad_row, send_o, send_kv, send_g):
        unit.drain()
    for n in range(3):
        s.sent(row_kept.at[n, 3], 35 + n)
    s.sent(gain_part.at[1 - core], 44)
    s.sent(gain_part.at[core, pl.ds(other_x, 2)], 45)
    s.sent(gain_part.at[core, mine_x + 1 - y_at], 46)


def attention_back(dn2, mid, x, g, gains, cos, sin, query, key_val, attended, wo, wqkv):
    rows, width = x.shape
    block, slot = width // 8, width // 4
    kv_width = 2 * KV * HD
    wide = width + kv_width
    vmem = pl.BlockSpec(memory_space=pltpu.VMEM)
    hbm = pl.BlockSpec(memory_space=pltpu.HBM)
    shape = jax.ShapeDtypeStruct
    outs = [
        (vmem, shape((rows, width), F32)),
        (vmem, shape((block, slot), F32)),
        (vmem, shape((KV_ROWS, kv_width), F32)),
        (vmem, shape((slot, block), F32)),
        (vmem, shape((8, block), F32)),
    ]
    return pl.pallas_call(
        attention_back_kernel,
        in_specs=[vmem] * 10 + [hbm] * 2,
        out_specs=[o[0] for o in outs],
        out_shape=[o[1] for o in outs],
        scratch_shapes=[
            pltpu.VMEM((rows, width), BF16),
            pltpu.VMEM((rows, width), BF16),
            pltpu.VMEM((rows, wide), BF16),
            pltpu.VMEM((rows, kv_width), F32),
            pltpu.VMEM((rows, width), F32),
            pltpu.VMEM((rows, width), BF16),
            pltpu.VMEM((width, rows), BF16),
            pltpu.VMEM((width, rows), BF16),
            pltpu.VMEM((2, 256, wide), BF16),
            pltpu.VMEM((5, 4, block, slot), BF16),
            pltpu.VMEM((5, 4, block, slot), BF16),
            pltpu.VMEM((5, 7, block, slot), BF16),
            pltpu.VMEM((2, width, block), BF16),
            pltpu.VMEM((4, width, block), BF16),
            pltpu.VMEM((7, width, block), BF16),
            pltpu.VMEM((2, 4, 8, block), F32),
            pltpu.VMEM((10, 8, block), F32),
            pltpu.VMEM((3, block, slot), BF16),
            pltpu.VMEM((3, KV_ROWS, kv_width), BF16),
            pltpu.VMEM((3, slot, block), BF16),
            pltpu.SemaphoreType.DMA((50,)),
            pltpu.SemaphoreType.DMA((50,)),
            pltpu.SemaphoreType.DMA((60,)),
        ],
        compiler_params=pltpu.CompilerParams(
            collective_id=2, has_side_effects=True, vmem_limit_bytes=65000 * 1024
        ),
        name="attention_back",
    )(dn2, mid, x, g, gains, cos, sin, query, key_val, attended, wo, wqkv)


def plain_forward(x, g, cos, sin, w_query, w_kv, gains, w_out, w_gu, w_down):
    both = ("dp", "tensor")
    gather = lax.all_gather

    def whole(shard, dims):
        for dim, axis in dims:
            shard = gather(shard, axis, axis=dim, tiled=True)
        return shard

    wq = whole(w_query, ((1, "tensor"), (0, "dp")))
    wqkv = jnp.concatenate([wq, whole(w_kv, ((0, both),))], 1)
    gain = whole(gains, ((1, both),)).astype(F32)
    wo = whole(w_out, ((0, "tensor"), (1, "dp")))
    wgu = whole(w_gu, ((0, "dp"),))
    wd = whole(w_down, ((1, "dp"),))
    normed = (x * norm_scale(x) * gain[0]).astype(BF16)
    query, key_val, attended = attend(cos, sin, dot(normed, wqkv))
    middle = x + dot(attended, wo)
    normed_two = (middle * norm_scale(middle) * gain[1]).astype(BF16)
    n2 = gather(normed_two, "tensor", axis=0, tiled=True)
    top = gather(g.astype(BF16), "tensor", axis=0, tiled=True)
    return wqkv, gain, wo, wgu, wd, n2, top, query, key_val, attended, middle


def plain_backward(
    dn2_part, out_part, n2, grad_gu_pre, hidden, top,
    middle, x, g, gains, cos, sin, query, key_val, attended, wo, wqkv,
):
    width = x.shape[1]

    def scatter(part, axis, dim):
        return lax.psum_scatter(part.astype(BF16), axis, scatter_dimension=dim, tiled=True).astype(F32)

    output = middle + scatter(out_part, "tensor", 0)
    grad_mid_norm, gain_two = norm_back(middle, gains[1], scatter(dn2_part, "tensor", 0))
    grad_middle = g + grad_mid_norm
    mid_bf = grad_middle.astype(BF16)
    grad_qkv_rows = attend_back(cos, sin, query, key_val, dot_nt(mid_bf, wo).astype(BF16))
    grad_in_norm, gain_one = norm_back(x, gains[0], dot_nt(grad_qkv_rows, wqkv))
    normed_one = (x * norm_scale(x) * gains[0]).astype(BF16)
    grad_qkv = scatter(dot_tn(normed_one, grad_qkv_rows), "dp", 0)
    gain_parts = lax.psum_scatter(jnp.stack([gain_one, gain_two]), "dp", scatter_dimension=1, tiled=True)
    return (
        output,
        grad_middle + grad_in_norm,
        lax.psum_scatter(gain_parts, "tensor", scatter_dimension=1, tiled=True),
        scatter(grad_qkv[:, :width], "tensor", 1),
        scatter(grad_qkv[:, width:], "tensor", 0),
        scatter(scatter(dot_tn(attended, mid_bf), "dp", 1), "tensor", 0),
        scatter(dot_tn(n2, grad_gu_pre), "dp", 0),
        scatter(dot_tn(hidden, top), "dp", 1),
    )


def linked_layer(x, g, cos, sin, w_query, w_kv, gains, w_out, w_gu, w_down):
    slot = w_query.shape[1]
    padded = jnp.pad(gains, ((0, GAIN_ROWS - 2), (0, slot - gains.shape[1])))
    piece = jnp.concatenate([w_query, w_kv, padded])
    outs = forward_stage(x, g, cos, sin, piece, w_out, w_gu, w_down)
    wo, n2, top, wqkv, hidden, dgu, out_part = (outs[i] for i in (1, 4, 5, 6, 7, 8, 9))
    query, key_val, attended, middle, gain, dn2 = outs[11:]
    output, grad_gu, grad_down = feed_back(out_part, n2, dgu, hidden, top, middle)
    grad_in, grad_query, grad_kv, grad_out, gain_sum = attention_back(
        dn2, middle, x, g, gain, cos, sin, query, key_val, attended, wo, wqkv
    )
    own = gain_sum.shape[1] // 4
    grad_gains = lax.dynamic_slice(gain_sum, (0, lax.axis_index("tensor") * own), (2, own))
    return output, grad_in, grad_gains, grad_query, grad_kv, grad_out, grad_gu.astype(F32), grad_down.astype(F32)


def plain_layer(x, g, cos, sin, w_query, w_kv, gains, w_out, w_gu, w_down):
    wqkv, gains, wo, wgu, wd, n2, top, query, key_val, attended, middle = plain_forward(
        x, g, cos, sin, w_query, w_kv, gains, w_out, w_gu, w_down
    )
    ff = wd.shape[0]
    gate_up = dot(n2, wgu)
    gate_pre, up_pre = gate_up[:, :ff], gate_up[:, ff:]
    sig = jax.nn.sigmoid(gate_pre)
    hidden = (gate_pre * sig * up_pre).astype(BF16)
    grad_hidden = dot_nt(top, wd)
    grad_gate_pre = (grad_hidden * up_pre * sig * (1.0 + gate_pre * (1.0 - sig))).astype(BF16)
    grad_up_pre = (grad_hidden * gate_pre * sig).astype(BF16)
    grad_gu_pre = jnp.concatenate([grad_gate_pre, grad_up_pre], 1)
    return plain_backward(
        dot_nt(grad_gu_pre, wgu).astype(BF16), dot(hidden, wd).astype(BF16), n2, grad_gu_pre, hidden, top,
        middle, x, g, gains, cos, sin, query, key_val, attended, wo, wqkv,
    )


def on_device(
    linked,
    hidden_in, positions, norm_gains, w_query, w_key, w_value, w_out, w_gate, w_up, w_down, out_grad,
):
    x, g = hidden_in, out_grad
    rows, width = x.shape
    ff = w_gate.shape[2]
    kv_width = 2 * KV * HD
    z = lax.axis_index("tensor")

    cos, sin = rope_tables(lax.dynamic_slice_in_dim(positions, z * rows, rows))
    layer = linked_layer if linked else plain_layer
    output, grad_in, grad_gains, grad_query, grad_kv, grad_out, grad_gu, grad_down = layer(
        x, g, cos, sin,
        w_query[0],
        jnp.concatenate([w_key[0], w_value[0]], 1),
        norm_gains[0],
        w_out[0],
        jnp.concatenate([w_gate[0], w_up[0]], 1),
        w_down[0],
    )

    return (
        output,
        grad_in,
        grad_gains[None],
        grad_query[None],
        grad_kv[None, :, : KV * HD],
        grad_kv[None, :, KV * HD :],
        grad_out[None],
        grad_gu[None, :, :ff],
        grad_gu[None, :, ff:],
        grad_down[None],
    )


def solution(mesh):
    nd, nt = mesh.shape["dp"], mesh.shape["tensor"]
    rows = P(("dp", "tensor"), None)
    wide = P(None, "dp", "tensor")
    tall = P(None, "tensor", "dp")
    flat = P(None, ("dp", "tensor"), None)
    gain = P(None, None, ("dp", "tensor"))
    return jax.shard_map(
        functools.partial(on_device, (nd, nt) == (8, 4)),
        mesh=mesh,
        in_specs=(rows, P("dp"), gain, wide, flat, flat, tall, wide, wide, tall, rows),
        out_specs=(rows, rows, gain, wide, flat, flat, tall, wide, wide, tall),
        check_vma=False,
    )
```

```python
import functools

import jax
import jax.numpy as jnp
from jax import lax
from jax.experimental import pallas as pl
from jax.experimental.pallas import tpu as pltpu
from jax.sharding import PartitionSpec as P

H = 32
KV = 4
HD = 64
SEQ = 128
NORM_EPS = 1e-05
NEG_BIG = -1e30
SCALE = HD ** (-0.5)
LANES = 128
F32 = jnp.float32
BF16 = jnp.bfloat16


def dot(a, b):
    return jnp.dot(a, b, preferred_element_type=F32)


def dot_nt(a, b):
    return lax.dot_general(a, b, (((1,), (1,)), ((), ())), preferred_element_type=F32)


def dot_tn(a, b):
    return lax.dot_general(a, b, (((0,), (0,)), ((), ())), preferred_element_type=F32)


def lane_masks():
    lane = lax.broadcasted_iota(jnp.int32, (SEQ, LANES), 1)
    return lane % HD < HD // 2, lane < HD


def swap_halves(u, first):
    return jnp.where(first, pltpu.roll(u, LANES - HD // 2, 1), pltpu.roll(u, HD // 2, 1))


def twice(tile, index, low):
    turned = pltpu.roll(tile, HD, 1)
    return jnp.where(low, tile, turned) if index % 2 == 0 else jnp.where(low, turned, tile)


def causal_probs(query, key):
    scores = dot_nt(query, key) * SCALE
    rows = lax.broadcasted_iota(jnp.int32, scores.shape, 0)
    cols = lax.broadcasted_iota(jnp.int32, scores.shape, 1)
    scores = jnp.where(cols <= rows, scores, NEG_BIG)
    weights = jnp.exp(scores - jnp.max(scores, -1, keepdims=True))
    return weights * (1.0 / jnp.sum(weights, -1, keepdims=True))


def attend_sequence(cos, sin, load, kv_at, q_out, kv_out, o_out, at):
    first, low = lane_masks()

    def turn(u):
        return u * cos + swap_halves(u, first) * sin

    keys, vals_low, vals_high = [], [], []
    for tile in range(KV // 2):
        key = turn(load(kv_at + tile * LANES))
        val = load(kv_at + KV * HD + tile * LANES)
        kv_out[at, tile * LANES : (tile + 1) * LANES] = key.astype(BF16)
        kv_out[at, KV * HD + tile * LANES : KV * HD + (tile + 1) * LANES] = val.astype(BF16)
        for index in (0, 1):
            keys.append(twice(key, index, low).astype(BF16))
            both = twice(val, index, low)
            vals_low.append(jnp.where(low, both, 0.0).astype(BF16))
            vals_high.append(jnp.where(low, 0.0, both).astype(BF16))
    for pair in range(H // 2):
        group = pair * LANES // (H // KV * HD)
        query = turn(load(pair * LANES))
        p_low = causal_probs(jnp.where(low, query, 0.0).astype(BF16), keys[group])
        p_high = causal_probs(jnp.where(low, 0.0, query).astype(BF16), keys[group])
        q_out[at, pair * LANES : (pair + 1) * LANES] = query.astype(BF16)
        o_out[at, pair * LANES : (pair + 1) * LANES] = (
            dot(p_low.astype(BF16), vals_low[group]) + dot(p_high.astype(BF16), vals_high[group])
        ).astype(BF16)


def attend_back_sequence(cos, sin, q_ref, kv_ref, da_ref, dqkv_out, at):
    first, low = lane_masks()

    def turn_back(u):
        return (u * cos - swap_halves(u, first) * sin).astype(BF16)

    pair_total = H // KV * HD // LANES
    width = H * HD
    held = {}
    for group in range(KV):
        tile_at = group // 2 * LANES
        key = twice(kv_ref[at, tile_at : tile_at + LANES].astype(F32), group, low)
        val_at = KV * HD + tile_at
        val = twice(kv_ref[at, val_at : val_at + LANES].astype(F32), group, low).astype(BF16)
        key_low = jnp.where(low, key, 0.0).astype(BF16)
        key_high = jnp.where(low, 0.0, key).astype(BF16)
        key = key.astype(BF16)
        dk = jnp.zeros((SEQ, LANES), F32)
        dv = jnp.zeros((SEQ, LANES), F32)
        for pair in range(group * pair_total, (group + 1) * pair_total):
            query = q_ref[at, pair * LANES : (pair + 1) * LANES].astype(F32)
            grad = da_ref[at, pair * LANES : (pair + 1) * LANES].astype(F32)
            dq = None
            for is_low in (True, False):
                if is_low:
                    query_h = jnp.where(low, query, 0.0).astype(BF16)
                    grad_h = jnp.where(low, grad, 0.0).astype(BF16)
                else:
                    query_h = jnp.where(low, 0.0, query).astype(BF16)
                    grad_h = jnp.where(low, 0.0, grad).astype(BF16)
                prob = causal_probs(query_h, key)
                grad_prob = dot_nt(grad_h, val)
                delta = jnp.sum(prob * grad_prob, -1, keepdims=True)
                ds = (prob * (grad_prob - delta) * SCALE).astype(BF16)
                term = dot(ds, key_low if is_low else key_high)
                dq = term if dq is None else dq + term
                dk = dk + dot_tn(ds, query_h)
                dv = dv + dot_tn(prob.astype(BF16), grad_h)
            dqkv_out[at, pair * LANES : (pair + 1) * LANES] = turn_back(dq)
        held[group] = (dk + pltpu.roll(dk, HD, 1), dv + pltpu.roll(dv, HD, 1))
    for tile in range(KV // 2):
        col = width + tile * LANES
        dk = jnp.where(low, held[2 * tile][0], held[2 * tile + 1][0])
        dv = jnp.where(low, held[2 * tile][1], held[2 * tile + 1][1])
        dqkv_out[at, col : col + LANES] = turn_back(dk)
        dqkv_out[at, col + KV * HD : col + KV * HD + LANES] = dv.astype(BF16)


def attend_back_group(cos, sin, group, q_ref, kv_ref, da_ref, dqkv_out, dkv_out, at):
    first, low = lane_masks()
    head_width = H // KV * HD
    mine = low == (group % 2 == 0)

    def both(tile):
        kept = jnp.where(mine, tile.astype(F32), 0.0)
        return kept + pltpu.roll(kept, HD, 1)

    tile = pl.ds(pl.multiple_of(group // 2 * LANES, LANES), LANES)
    val_tile = pl.ds(pl.multiple_of(KV * HD + group // 2 * LANES, LANES), LANES)
    key = both(kv_ref[at, tile])
    val = both(kv_ref[at, val_tile]).astype(BF16)
    key_low = jnp.where(low, key, 0.0).astype(BF16)
    key_high = jnp.where(low, 0.0, key).astype(BF16)
    key = key.astype(BF16)
    dk = jnp.zeros((SEQ, LANES), F32)
    dv = jnp.zeros((SEQ, LANES), F32)
    for pair in range(head_width // LANES):
        c = pl.ds(pl.multiple_of(group * head_width + pair * LANES, LANES), LANES)
        query = q_ref[at, c].astype(F32)
        grad = da_ref[at, c].astype(F32)
        dq = None
        for is_low in (True, False):
            pick = low if is_low else jnp.logical_not(low)
            query_h = jnp.where(pick, query, 0.0).astype(BF16)
            grad_h = jnp.where(pick, grad, 0.0).astype(BF16)
            prob = causal_probs(query_h, key)
            grad_prob = dot_nt(grad_h, val)
            delta = jnp.sum(prob * grad_prob, -1, keepdims=True)
            ds = (prob * (grad_prob - delta) * SCALE).astype(BF16)
            term = dot(ds, key_low if is_low else key_high)
            dq = term if dq is None else dq + term
            dk = dk + dot_tn(ds, query_h)
            dv = dv + dot_tn(prob.astype(BF16), grad_h)
        dqkv_out[at, c] = (dq * cos - swap_halves(dq, first) * sin).astype(BF16)
    dkv_out[at, tile] += jnp.where(mine, dk + pltpu.roll(dk, HD, 1), 0.0)
    dkv_out[at, val_tile] += jnp.where(mine, dv + pltpu.roll(dv, HD, 1), 0.0)


def attend_kernel(cos_ref, sin_ref, qkv_ref, q_out, kv_out, o_out):
    attend_sequence(
        cos_ref[...], sin_ref[...], lambda c: qkv_ref[:, c : c + LANES], H * HD, q_out, kv_out, o_out, slice(None)
    )


def attend_back_kernel(cos_ref, sin_ref, q_ref, kv_ref, da_ref, dqkv_out):
    attend_back_sequence(cos_ref[...], sin_ref[...], q_ref, kv_ref, da_ref, dqkv_out, slice(None))


def by_sequence(body, name, ins, widths):
    rows = ins[0].shape[0]
    spec = lambda w: pl.BlockSpec((SEQ, w), lambda i: (i, 0))
    return pl.pallas_call(
        body,
        grid=(rows // SEQ,),
        in_specs=[spec(a.shape[1]) for a in ins],
        out_specs=[spec(w) for w in widths],
        out_shape=[jax.ShapeDtypeStruct((rows, w), BF16) for w in widths],
        name=name,
    )(*ins)


def attend(cos, sin, qkv):
    return by_sequence(attend_kernel, "attend", (cos, sin, qkv), (H * HD, 2 * KV * HD, H * HD))


def attend_back(cos, sin, query, key_val, grad):
    return by_sequence(
        attend_back_kernel, "attend_back", (cos, sin, query, key_val, grad), (H * HD + 2 * KV * HD,)
    )[0]


def norm_scale(rows):
    return lax.rsqrt(jnp.mean(rows * rows, -1, keepdims=True) + NORM_EPS)


def norm_back(rows, gain, grad_normed):
    inv = norm_scale(rows)
    weighted = grad_normed * gain
    grad_gain = jnp.sum(grad_normed * rows * inv, 0)
    grad_rows = inv * weighted - rows * inv**3 * jnp.mean(weighted * rows, -1, keepdims=True)
    return grad_rows, grad_gain


def rope_tables(positions):
    half = jnp.arange(LANES, dtype=jnp.int32) % (HD // 2)
    inv_freq = 10000.0 ** (-(half.astype(F32) * 2.0 / HD))
    angles = positions.astype(F32)[:, None] * inv_freq[None, :]
    sign = jnp.where(jnp.arange(LANES) % HD < HD // 2, -1.0, 1.0).astype(F32)
    return jnp.cos(angles), jnp.sin(angles) * sign[None, :]


MESH = pl.DeviceIdType.MESH
KV_ROWS = 64
GAIN_ROWS = 16


class Links:
    def __init__(self):
        self.d, self.z = lax.axis_index("dp"), lax.axis_index("tensor")
        core, x, y = self.d % 2, self.d // 2 % 2, self.d // 4
        self.dc = self.d + 1 - 2 * core
        step_x, step_y = 2 - 4 * x, 4 - 8 * y
        self.dx, self.dy, self.dxy = self.d + step_x, self.d + step_y, self.d + step_x + step_y
        self.dcx, self.dcy, self.dcxy = self.dc + step_x, self.dc + step_y, self.dc + step_x + step_y

    def barrier(self, far=False):
        z = self.z
        sem = pltpu.get_barrier_semaphore()

        def greet(d, zz):
            pl.semaphore_signal(sem, inc=1, device_id=(d, zz), device_id_type=MESH)

        for d in (self.dx, self.dy, self.dc):
            greet(d, z)
        if far:
            for j in (1, 2, 3):
                greet(self.d, (z + j) % 4)
            pl.semaphore_wait(sem, 6)
            return
        pl.when(z > 0)(lambda: greet(self.d, z - 1))
        pl.when(z < 3)(lambda: greet(self.d, z + 1))
        pl.semaphore_wait(sem, 3 + (z + 2) // 3 + (5 - z) // 3)


class Sender:
    def __init__(self, links, send_sem, recv_sem):
        self.links, self.send_sem, self.recv_sem = links, send_sem, recv_sem

    def copy(self, src, dst, at, to):
        return pltpu.make_async_remote_copy(
            src_ref=src,
            dst_ref=dst,
            send_sem=self.send_sem.at[at],
            recv_sem=self.recv_sem.at[at],
            device_id=to,
            device_id_type=MESH,
        )

    def start(self, src, dst, at, to):
        self.copy(src, dst, at, to).start()

    def landed(self, region, at):
        self.copy(region, region, at, (self.links.dc, self.links.z)).wait_recv()

    def sent(self, region, at):
        self.copy(region, region, at, (self.links.dc, self.links.z)).wait_send()


class Spread:
    def __init__(self, sender, region, base):
        self.s, self.region, self.base = sender, region, base

    def own(self, p, src):
        k, r, b = self.s.links, self.region, self.base + 9 * p
        mine = r(k.d, p, None)
        self.s.start(src, mine, b, (k.dx, k.z))
        self.s.start(src, mine, b + 1, (k.dy, k.z))
        self.s.start(src, mine, b + 2, (k.dc, k.z))

    def near(self, p):
        k, r, b = self.s.links, self.region, self.base + 9 * p
        self.s.landed(r(k.dx, p, None), b)
        self.s.start(r(k.dx, p, 0), r(k.dx, p, 0), b + 3, (k.dy, k.z))
        self.s.start(r(k.dx, p, None), r(k.dx, p, None), b + 5, (k.dc, k.z))
        self.s.landed(r(k.dy, p, None), b + 1)
        self.s.start(r(k.dy, p, 1), r(k.dy, p, 1), b + 4, (k.dx, k.z))
        self.s.start(r(k.dy, p, None), r(k.dy, p, None), b + 6, (k.dc, k.z))

    def far(self, p):
        k, r, b = self.s.links, self.region, self.base + 9 * p
        for part in (0, 1):
            self.s.landed(r(k.dxy, p, part), b + 3 + part)
            self.s.start(r(k.dxy, p, part), r(k.dxy, p, part), b + 7 + part, (k.dc, k.z))

    def finish(self, p):
        k, r, b = self.s.links, self.region, self.base + 9 * p
        self.s.landed(r(k.dc, p, None), b + 2)
        self.s.landed(r(k.dcx, p, None), b + 5)
        self.s.landed(r(k.dcy, p, None), b + 6)
        for part in (0, 1):
            self.s.landed(r(k.dcxy, p, part), b + 7 + part)

    def drain(self, p):
        k, r, b = self.s.links, self.region, self.base + 9 * p
        for i in (0, 1, 2):
            self.s.sent(r(k.d, p, None), b + i)
        self.s.sent(r(k.dx, p, 0), b + 3)
        self.s.sent(r(k.dy, p, 1), b + 4)
        self.s.sent(r(k.dx, p, None), b + 5)
        self.s.sent(r(k.dy, p, None), b + 6)
        for part in (0, 1):
            self.s.sent(r(k.dxy, p, part), b + 7 + part)


class Line:
    def __init__(self, sender, region, base):
        self.s, self.region, self.base = sender, region, base

    def _send(self, src, p, way, step):
        k = self.s.links
        self.s.start(src, self.region(p), self.base + 2 * (step - 1) + way, (k.d, k.z + 1 - 2 * way))

    def own(self, src):
        z = self.s.links.z
        pl.when(z < 3)(lambda: self._send(src, z, 0, 1))
        pl.when(z > 0)(lambda: self._send(src, z, 1, 1))

    def each(self, step, action):
        z = self.s.links.z
        pl.when(z >= step)(lambda: action(z - step, 0))
        pl.when(z + step <= 3)(lambda: action(z + step, 1))

    def arrive(self, step, then=None):
        z = self.s.links.z

        def action(p, way):
            self.s.landed(self.region(p), self.base + 2 * (step - 1) + way)
            if step < 3:
                ahead = z < 3 if way == 0 else z > 0
                pl.when(ahead)(lambda: self._send(self.region(p), p, way, step + 1))
            if then is not None:
                then(p)

        self.each(step, action)

    def drain(self):
        z = self.s.links.z
        for step in (1, 2, 3):
            for way in (0, 1):
                came = z - (step - 1) if way == 0 else z + (step - 1)
                ok = jnp.logical_and(z < 3, z >= step - 1) if way == 0 else jnp.logical_and(z > 0, z <= 4 - step)
                pl.when(ok)(
                    functools.partial(self.s.sent, self.region(came), self.base + 2 * (step - 1) + way)
                )


def forward_kernel(
    x_ref, g_ref, cos_ref, sin_ref, wq_in, wk_in, wv_in, gain_in, wo_ref, wg_in, wu_in, wd_ref,
    wa_all, wo_all, gu_all, wd_all, n2_all, top_all, wqkv_all, hidden_all, dgu_all, out_all, dn2_land,
    q_out, kv_out, o_out, mid_out, gain_out, dn2_out,
    att_ref, gu_ref, n1, qkv, w_buf, wkv_buf, gain_buf, wo_buf, n2, top,
    n2_rows, top_rows, gate_up, grad_hidden, hidden, dgu, dn2_sends, out_rows,
    send_sem, recv_sem, local_sem,
):
    rows, width = x_ref.shape
    slot_width = att_ref.shape[1]
    block = width // 8
    links = Links()
    d, z = links.d, links.z
    s = Sender(links, send_sem, recv_sem)
    ff = wd_ref.shape[0]
    cut_a = att_ref.shape[0] // 32 * 16
    cuts_a = ((0, cut_a), (cut_a, att_ref.shape[0] - cut_a))

    def at_a(dd, p, part):
        if part is None:
            return wa_all.at[dd, p]
        return wa_all.at[dd, p, pl.ds(*cuts_a[part])]

    def at_b(dd, p, part):
        start, size = (0, slot_width) if part is None else (part * slot_width // 2, slot_width // 2)
        return wo_all.at[
            pl.ds(pl.multiple_of(p * slot_width + start, 16), size),
            pl.ds(pl.multiple_of(dd * block, 128), block),
        ]

    def at_gu(dd, p, part):
        start, size = (0, block) if part is None else (part * block // 2, block // 2)
        return gu_all.at[pl.ds(pl.multiple_of(dd * block + start, 16), size)]

    def at_wd(dd, p, part):
        start, size = (0, ff) if part is None else (part * ff // 2, ff // 2)
        return wd_all.at[pl.ds(start, size), pl.ds(pl.multiple_of(dd * block, 128), block)]

    def rows_of(ref):
        return lambda p: ref.at[pl.ds(pl.multiple_of(p * rows, 16), rows)]

    spread_a, spread_b = Spread(s, at_a, 0), Spread(s, at_b, 36)
    spread_gu, spread_wd = Spread(s, at_gu, 72), Spread(s, at_wd, 81)
    line_a = Line(s, lambda p: at_a(d, p, None), 90)
    line_b = Line(s, lambda p: at_b(d, p, None), 96)
    line_n, line_t = Line(s, rows_of(n2_all), 102), Line(s, rows_of(top_all), 108)

    def keep(src, dst, at):
        pltpu.make_async_copy(src, dst, local_sem.at[at]).start()

    def kept(src, dst, at):
        pltpu.make_async_copy(src, dst, local_sem.at[at]).wait()

    kv_at = pl.ds(block, KV_ROWS)
    shards = [
        (wq_in, att_ref.at[pl.ds(0, block)], 78),
        (wk_in, att_ref.at[kv_at, pl.ds(0, KV * HD)], 79),
        (wv_in, att_ref.at[kv_at, pl.ds(KV * HD, KV * HD)], 80),
        (gain_in, att_ref.at[pl.ds(block + KV_ROWS, GAIN_ROWS), pl.ds(0, LANES)], 81),
    ]
    ffs = [(wg_in, gu_ref.at[:, pl.ds(0, ff)], 82), (wu_in, gu_ref.at[:, pl.ds(ff, ff)], 83)]
    for shard in shards + ffs:
        keep(*shard)
    att_ref[block + KV_ROWS :, LANES:] = jnp.zeros((GAIN_ROWS, slot_width - LANES), BF16)
    links.barrier(far=True)
    for shard in shards:
        kept(*shard)

    line_a.own(att_ref)
    spread_a.own(z, att_ref)
    keep(att_ref, at_a(d, z, None), 0)
    keep(wo_ref, at_b(d, z, None), 1)
    keep(wd_ref, at_wd(d, 0, None), 3)
    top[...] = g_ref[...].astype(BF16)
    line_a.arrive(1, lambda p: spread_a.own(p, at_a(d, p, None)))
    spread_a.near(z)
    line_a.arrive(2, lambda p: spread_a.own(p, at_a(d, p, None)))
    line_b.own(wo_ref)
    line_a.each(1, lambda p, way: spread_a.near(p))
    spread_a.far(z)
    line_a.arrive(3, lambda p: spread_a.own(p, at_a(d, p, None)))
    line_b.arrive(1)
    line_a.each(2, lambda p, way: spread_a.near(p))
    line_a.each(1, lambda p, way: spread_a.far(p))
    line_a.each(3, lambda p, way: spread_a.near(p))
    spread_b.own(z, wo_ref)
    line_b.each(1, lambda p, way: spread_b.own(p, at_b(d, p, None)))
    line_b.arrive(2, lambda p: spread_b.own(p, at_b(d, p, None)))
    line_a.each(2, lambda p, way: spread_a.far(p))
    line_a.each(3, lambda p, way: spread_a.far(p))
    for shard in ffs:
        kept(*shard)
    keep(gu_ref, at_gu(d, 0, None), 2)
    line_b.arrive(3, lambda p: spread_b.own(p, at_b(d, p, None)))
    line_t.own(top)
    kept(att_ref, at_a(d, z, None), 0)
    for p in range(4):
        spread_a.finish(p)

    def kv_copy(dd, p):
        return wkv_buf.at[dd, p], wqkv_all.at[pl.ds(dd * block + p * KV_ROWS, KV_ROWS), pl.ds(width, 2 * KV * HD)]

    for p in range(4):
        for dd in range(8):
            pltpu.make_async_copy(
                wa_all.at[dd, p, pl.ds(0, block)], w_buf.at[p, pl.ds(dd * block, block)], local_sem.at[14 + 8 * p + dd]
            ).start()
    keep(wa_all.at[:, :, pl.ds(block, KV_ROWS)], wkv_buf, 8)
    keep(wa_all.at[:, :, pl.ds(block + KV_ROWS, GAIN_ROWS), pl.ds(0, LANES)], gain_buf, 9)
    kept(wa_all.at[:, :, pl.ds(block + KV_ROWS, GAIN_ROWS), pl.ds(0, LANES)], gain_buf, 9)
    low_row = lax.broadcasted_iota(jnp.int32, (GAIN_ROWS, LANES), 1) < HD
    for dd in range(8):
        for half in (0, 1):
            first = gain_buf[dd, 2 * half].astype(F32)
            second = pltpu.roll(gain_buf[dd, 2 * half + 1].astype(F32), HD, 1)
            at = dd * block + half * LANES
            gain_out[:, at : at + LANES] = jnp.where(low_row, first, second)[:8]
    x = x_ref[...]
    n1[...] = (x * norm_scale(x) * gain_out[0:1]).astype(BF16)
    for p in range(4):
        for dd in range(8):
            kept(wa_all.at[dd, p, pl.ds(0, block)], w_buf.at[p, pl.ds(dd * block, block)], 14 + 8 * p + dd)
        for c in range(0, slot_width, 256):
            qkv[:, p * slot_width + c : p * slot_width + c + 256] = dot(n1[...], w_buf[p, :, c : c + 256])
        keep(w_buf.at[p], wqkv_all.at[:, pl.ds(p * slot_width, slot_width)], 4 + p)
    kept(wa_all.at[:, :, pl.ds(block, KV_ROWS)], wkv_buf, 8)
    qkv[:, width:] = dot(n1[...], wkv_buf[...].reshape(width, 2 * KV * HD))
    for p in range(4):
        for dd in range(8):
            pltpu.make_async_copy(*kv_copy(dd, p), local_sem.at[46 + 8 * p + dd]).start()

    line_b_pieces = lambda action: [action(z)] + [line_b.each(i, lambda p, way: action(p)) for i in (1, 2, 3)]

    def sequence(i, carry):
        at = pl.ds(pl.multiple_of(i * SEQ, SEQ), SEQ)
        attend_sequence(
            cos_ref[at], sin_ref[at], lambda c: qkv[at, c : c + LANES], width, q_out, kv_out, o_out, at
        )

        @pl.when(i == 0)
        def _():
            line_b_pieces(spread_b.near)
            spread_gu.own(0, gu_ref)
            line_t.arrive(1)

        return carry

    lax.fori_loop(0, rows // SEQ, sequence, 0)
    line_b_pieces(spread_b.far)
    kept(wo_ref, at_b(d, z, None), 1)
    for p in range(4):
        spread_b.finish(p)
    keep(wo_all, wo_buf, 0)
    kept(wo_all, wo_buf, 0)

    def column(i, carry):
        at = pl.ds(pl.multiple_of(i * 256, 256), 256)
        mid_out[:, at] = x_ref[:, at] + dot(o_out[...], wo_buf[:, at])
        return carry

    lax.fori_loop(0, width // 256, column, 0)
    mid = mid_out[...]
    n2[...] = (mid * norm_scale(mid) * gain_out[1:2]).astype(BF16)

    line_n.own(n2)
    keep(n2, n2_all.at[pl.ds(pl.multiple_of(z * rows, 16), rows)], 8)
    keep(top, top_all.at[pl.ds(pl.multiple_of(z * rows, 16), rows)], 9)
    line_t.arrive(2)
    for p in range(4):
        kept(w_buf.at[p], wqkv_all.at[:, pl.ds(p * slot_width, slot_width)], 4 + p)
        for dd in range(8):
            kept(*kv_copy(dd, p), 46 + 8 * p + dd)
    kept(gu_ref, at_gu(d, 0, None), 2)
    kept(wd_ref, at_wd(d, 0, None), 3)
    kept(n2, n2_all.at[pl.ds(pl.multiple_of(z * rows, 16), rows)], 8)
    kept(top, top_all.at[pl.ds(pl.multiple_of(z * rows, 16), rows)], 9)
    spread_gu.near(0)
    spread_wd.own(0, wd_ref)
    line_n.arrive(1)
    line_t.arrive(3)
    spread_gu.far(0)
    spread_gu.finish(0)

    wide = 2 * ff
    pieces = [(c, min(slot_width, wide - c)) for c in range(0, wide, slot_width)]
    gu_piece = lambda i, c, n: (columns(gu_all, c, n), w_buf.at[i, :, pl.ds(0, n)])
    for i, (c, n) in enumerate(pieces):
        keep(*gu_piece(i, c, n), 14 + i)
    wd_vmem = wo_buf.at[pl.ds(0, ff)]
    across, opposite, beside = 2 - z // 2, 3 - 3 * (z // 2), z + 1 - 2 * (z % 2)
    ends, inner = z % 3 == 0, z % 3 != 0
    chunks = [(c, min(256, ff - c)) for c in range(0, ff, 256)]

    def project(slot, source):
        for c, n in pieces:
            for h in range(0, n, 256):
                gate_up[slot, :, c + h : c + h + 256] = dot(source[...], w_buf[c // slot_width, :, h : h + 256])

    rows_at = lambda p: pl.ds(pl.multiple_of(p * rows, 16), rows)
    for i, (c, n) in enumerate(pieces):
        kept(*gu_piece(i, c, n), 14 + i)
    project(1, n2)
    spread_wd.near(0)
    line_n.arrive(2)
    keep(n2_all.at[rows_at(across)], n2_rows, 0)
    kept(n2_all.at[rows_at(across)], n2_rows, 0)
    project(0, n2_rows)
    spread_wd.far(0)
    spread_wd.finish(0)
    keep(wd_all, wd_vmem, 20)
    kept(wd_all, wd_vmem, 20)

    def place_of(p):
        return (p - z + 4) % 4 - 1

    def send_dn2(i, p):
        s.start(dn2_sends.at[i], dn2_land.at[place_of(p)], 114 + place_of(p), (d, p))

    def feed(i):
        pl.when(i == 1)(lambda: line_n.arrive(3))
        second = (i + 2) // 3 - i // 2
        p = across * ((3 - i) // 3) + opposite * second + beside * (i // 2 - i // 3) + z * (i // 3)
        at = rows_at(p)
        slot = i // 3
        keep(top_all.at[at], top_rows, 1)

        @pl.when(second + i // 2 - i // 3 == 1)
        def _():
            keep(n2_all.at[at], n2_rows, 0)
            kept(n2_all.at[at], n2_rows, 0)
            project(0, n2_rows)

        kept(top_all.at[at], top_rows, 1)
        for c, n in chunks:
            grad_hidden[:, c : c + n] = dot_nt(top_rows[...], wo_buf[c : c + n])

        @pl.when(i > 0)
        def _():
            kept(hidden, hidden_all.at[at], 2)
            kept(dgu, dgu_all.at[at], 3)

        def act(m):
            r = pl.ds(pl.multiple_of(m * 16, 16), 16)
            for c, n in chunks:
                gate, up = gate_up[slot, r, c : c + n], gate_up[slot, r, ff + c : ff + c + n]
                grad = grad_hidden[r, c : c + n]
                sig = 1.0 / (1.0 + jnp.exp(-gate))
                silu = gate * sig
                hidden[r, c : c + n] = (silu * up).astype(BF16)
                dgu[r, c : c + n] = (grad * up * sig * (1.0 + gate * (1.0 - sig))).astype(BF16)
                dgu[r, ff + c : ff + c + n] = (grad * silu).astype(BF16)

        loop(rows // 16, act)
        keep(hidden, hidden_all.at[at], 2)
        keep(dgu, dgu_all.at[at], 3)

        def back(m):
            r = pl.ds(pl.multiple_of(m * 256, 256), 256)
            total = None
            for j, (c, n) in enumerate(pieces):
                term = dot_nt(dgu[:, c : c + n], w_buf[j, r, :n])
                total = term if total is None else total + term

            @pl.when(i < 3)
            def _():
                dn2_sends[i, :, r] = total.astype(BF16)

            @pl.when(i == 3)
            def _():
                dn2_out[:, r] = total

        loop(width // 256, back)

        @pl.when(i % 2 == 0)
        def _():
            send_dn2(i, p)

        @pl.when(jnp.logical_and(i == 1, ends))
        def _():
            s.start(dn2_sends.at[1], dn2_land.at[3], 117, (d, 1 + z // 3))

        pl.when(i > 0)(lambda: kept(out_rows, out_all.at[at], 7))

        def down(m):
            r = pl.ds(pl.multiple_of(m * 256, 256), 256)
            out_rows[:, r] = dot(hidden[...], wo_buf[:ff, r]).astype(BF16)

        loop(width // 256, down)
        keep(out_rows, out_all.at[at], 7)

    loop(4, feed)
    kept(hidden, hidden_all.at[pl.ds(0, rows)], 2)
    kept(dgu, dgu_all.at[pl.ds(0, rows)], 3)
    kept(out_rows, out_all.at[pl.ds(0, rows)], 7)

    @pl.when(inner)
    def _():
        s.landed(dn2_land.at[3], 117)
        keep(dn2_land.at[3], n2_rows, 0)
        kept(dn2_land.at[3], n2_rows, 0)

        def add(m):
            r = pl.ds(pl.multiple_of(m * 32, 32), 32)
            dn2_sends[1, r] = (dn2_sends[1, r].astype(F32) + n2_rows[r].astype(F32)).astype(BF16)

        loop(rows // 32, add)
        send_dn2(1, opposite)

    def arrived(j):
        s.landed(dn2_land.at[j], 114 + j)
        keep(dn2_land.at[j], n2_rows, 0)
        kept(dn2_land.at[j], n2_rows, 0)

        def add(m):
            r = pl.ds(pl.multiple_of(m * 32, 32), 32)
            dn2_out[r] += n2_rows[r].astype(F32)

        loop(rows // 32, add)

    pl.when(z >= 1)(lambda: arrived(0))
    pl.when(z <= 2)(lambda: arrived(2))
    arrived(1)
    for i, p in ((0, across), (2, beside)):
        s.sent(dn2_sends.at[i], 114 + place_of(p))
    pl.when(ends)(lambda: s.sent(dn2_sends.at[1], 117))
    pl.when(inner)(lambda: s.sent(dn2_sends.at[1], 114 + place_of(opposite)))
    for p in range(4):
        spread_a.drain(p)
        spread_b.drain(p)
    spread_gu.drain(0)
    spread_wd.drain(0)
    for line in (line_a, line_b, line_n, line_t):
        line.drain()


def forward_stage(x, g, cos, sin, wq, wk, wv, gains, wo, wg, wu, wd):
    rows, width = x.shape
    slot_width = wq.shape[1]
    block = width // 8
    kv_width = 2 * KV * HD
    ff = wd.shape[0]
    vmem = pl.BlockSpec(memory_space=pltpu.VMEM)
    hbm = pl.BlockSpec(memory_space=pltpu.HBM)
    shape = jax.ShapeDtypeStruct
    outs = [
        (hbm, shape((8, 4, block + KV_ROWS + GAIN_ROWS, slot_width), BF16)),
        (hbm, shape((width, width), BF16)),
        (hbm, shape((width, 2 * ff), BF16)),
        (hbm, shape((ff, width), BF16)),
        (hbm, shape((4 * rows, width), BF16)),
        (hbm, shape((4 * rows, width), BF16)),
        (hbm, shape((width, width + kv_width), BF16)),
        (hbm, shape((4 * rows, ff), BF16)),
        (hbm, shape((4 * rows, 2 * ff), BF16)),
        (hbm, shape((4 * rows, width), BF16)),
        (hbm, shape((4, rows, width), BF16)),
        (vmem, shape((rows, width), BF16)),
        (vmem, shape((rows, kv_width), BF16)),
        (vmem, shape((rows, width), BF16)),
        (vmem, shape((rows, width), F32)),
        (vmem, shape((8, width), F32)),
        (vmem, shape((rows, width), F32)),
    ]
    return pl.pallas_call(
        forward_kernel,
        in_specs=[vmem] * 4 + [hbm] * 4 + [vmem] + [hbm] * 2 + [vmem],
        out_specs=[o[0] for o in outs],
        out_shape=[o[1] for o in outs],
        scratch_shapes=[
            pltpu.VMEM((block + KV_ROWS + GAIN_ROWS, slot_width), BF16),
            pltpu.VMEM((block, 2 * ff), BF16),
            pltpu.VMEM((rows, width), BF16),
            pltpu.VMEM((rows, width + kv_width), F32),
            pltpu.VMEM((-(-2 * ff // slot_width), width, slot_width), BF16),
            pltpu.VMEM((8, 4, KV_ROWS, kv_width), BF16),
            pltpu.VMEM((8, 4, GAIN_ROWS, LANES), BF16),
            pltpu.VMEM((width, width), BF16),
            pltpu.VMEM((rows, width), BF16),
            pltpu.VMEM((rows, width), BF16),
            pltpu.VMEM((rows, width), BF16),
            pltpu.VMEM((rows, width), BF16),
            pltpu.VMEM((2, rows, 2 * ff), F32),
            pltpu.VMEM((rows, ff), F32),
            pltpu.VMEM((rows, ff), BF16),
            pltpu.VMEM((rows, 2 * ff), BF16),
            pltpu.VMEM((3, rows, width), BF16),
            pltpu.VMEM((rows, width), BF16),
            pltpu.SemaphoreType.DMA((118,)),
            pltpu.SemaphoreType.DMA((118,)),
            pltpu.SemaphoreType.DMA((84,)),
        ],
        compiler_params=pltpu.CompilerParams(
            collective_id=0, has_side_effects=True, vmem_limit_bytes=65000 * 1024
        ),
        name="forward",
    )(x, g, cos, sin, wq, wk, wv, gains, wo, wg, wu, wd)


def loop(count, body):
    def step(i, carry):
        body(i)
        return carry

    lax.fori_loop(0, count, step, 0)


class Local:
    def __init__(self, sem):
        self.sem, self.next = sem, 0

    def start(self, src, dst):
        copy = pltpu.make_async_copy(src, dst, self.sem.at[self.next])
        self.next += 1
        copy.start()
        return copy

    def load(self, src, dst):
        self.start(src, dst).wait()


class Reduce:
    def __init__(self, sender, compute, base, sends, kept, land, halves):
        self.s, self.compute, self.base = sender, compute, base
        self.sends, self.kept, self.land, self.halves = sends, kept, land, halves

    def half(self, ref, part):
        return ref.at[pl.ds(*self.halves[part])]

    def place(self, i):
        if i < 4:
            return self.land.at[i]
        return self.half(self.land.at[4 + (i - 4) // 2], i % 2)

    def partner(self, i):
        k = self.s.links
        count = self.sends.shape[0]
        if i >= count:
            self.s.sent(self.sends.at[i % count], self.base + i - count)
        self.compute((k.dcxy, k.dcx, k.dcy, k.dc)[i], None, self.sends.at[i % count])
        self.s.start(self.sends.at[i % count], self.place(i), self.base + i, (k.dc, k.z))

    def own(self, i):
        k, b = self.s.links, self.base
        to_x, to_y = (k.dx, k.z), (k.dy, k.z)
        self.s.landed(self.place(i), b + i)
        kept = self.kept.at[i]
        self.compute((k.dxy, k.dx, k.dy, k.d)[i], self.land.at[i], kept)
        if i == 0:
            self.s.start(self.half(kept, 0), self.place(4), b + 4, to_x)
            self.s.start(self.half(kept, 1), self.place(7), b + 7, to_y)
        elif i == 1:
            self.s.start(self.half(kept, 0), self.place(6), b + 6, to_x)
        elif i == 2:
            self.s.start(self.half(kept, 1), self.place(5), b + 5, to_y)

    def first(self):
        self.partner(0)
        for i in range(3):
            self.partner(i + 1)
            self.own(i)
        self.own(3)

    def add(self, i, part, at):
        self.s.landed(self.place(at), self.base + at)
        start, size = self.halves[part]
        from_start = self.halves[at % 2][0] if at < 8 else self.halves[at - 8][0]
        slot = 4 + (at - 4) // 2
        step = 32 if size % 32 == 0 else 16

        def rows(n):
            r = pl.ds(pl.multiple_of(start + n * step, 16), step)
            g = pl.ds(pl.multiple_of(from_start + n * step, 16), step)
            self.kept[i, r] = (self.kept[i, r].astype(F32) + self.land[slot, g].astype(F32)).astype(BF16)

        loop(size // step, rows)

    def second(self):
        k, b = self.s.links, self.base
        self.add(2, 0, 4)
        self.s.start(self.half(self.kept.at[2], 0), self.place(8), b + 8, (k.dy, k.z))
        self.add(1, 1, 7)
        self.s.start(self.half(self.kept.at[1], 1), self.place(9), b + 9, (k.dx, k.z))

    def last(self):
        self.add(3, 0, 6)
        self.add(3, 1, 5)
        self.add(3, 0, 8)
        self.add(3, 1, 9)

    def drain(self):
        b, kept = self.base, self.kept
        count = self.sends.shape[0]
        for i in range(4 - count, 4):
            self.s.sent(self.sends.at[i % count], b + i)
        self.s.sent(self.half(kept.at[0], 0), b + 4)
        self.s.sent(self.half(kept.at[2], 1), b + 5)
        self.s.sent(self.half(kept.at[1], 0), b + 6)
        self.s.sent(self.half(kept.at[0], 1), b + 7)
        self.s.sent(self.half(kept.at[2], 0), b + 8)
        self.s.sent(self.half(kept.at[1], 1), b + 9)


class LineSum:
    def __init__(self, sender, local, part, sends, land, base):
        self.s, self.part, self.sends = sender, part, sends
        self.land, self.base = land, base
        self.rows = sends.shape[1]
        self.sem, self.first = local.sem, local.next
        local.next += 7

    def rows_of(self, t):
        return self.part.at[pl.ds(pl.multiple_of(t * self.rows, 16), self.rows)]

    def fetch(self, holds, slot, at):
        return pltpu.make_async_copy(self.rows_of(holds), self.sends.at[slot], self.sem.at[self.first + at])

    def begin(self):
        for s in (1, 2, 3):
            for sends, slot, place, holds, _, _ in self.ways(s):
                pl.when(sends)(lambda: self.fetch(holds, slot, place).start())
        self.fetch(self.s.links.z, 3, 6).start()
        self.step(1)

    def add(self, into, at):
        self.s.landed(self.land.at[at], self.base + at)

        def rows(n):
            r = pl.ds(pl.multiple_of(n * 32, 32), 32)
            self.sends[into, r] = (self.sends[into, r].astype(F32) + self.land[at, r].astype(F32)).astype(BF16)

        loop(self.rows // 32, rows)

    def ways(self, s):
        z = self.s.links.z
        right = (z <= s - 1, s - 1 - z, 2 * (s - 1), z + 4 - s, z >= 1, z + 1)
        left = (z >= 4 - s, s - 1, 2 * (s - 1) + 1, z - 4 + s, z <= 2, z - 1)
        return right, left

    def step(self, s):
        for sends, slot, place, holds, received, to in self.ways(s):

            @pl.when(sends)
            def _():
                self.fetch(holds, slot, place).wait()
                if s > 1:
                    pl.when(received)(lambda: self.add(slot, place - 2))
                self.s.start(self.sends.at[slot], self.land.at[place], self.base + place, (self.s.links.d, to))

    def finish(self, write):
        z = self.s.links.z
        self.fetch(z, 3, 6).wait()
        pl.when(z >= 1)(lambda: self.add(3, 4))
        pl.when(z <= 2)(lambda: self.add(3, 5))

        def rows(n):
            r = pl.ds(pl.multiple_of(n * 32, 32), 32)
            write(r, self.sends[3, r].astype(F32))

        loop(self.rows // 32, rows)

    def drain(self):
        for s in (1, 2, 3):
            for sends, slot, place, _, _, _ in self.ways(s):
                pl.when(sends)(functools.partial(self.s.sent, self.sends.at[slot], self.base + place))


def stream(local, count, source, bufs, body):
    first = local.next
    local.next += 2

    def copy(n, slot):
        return pltpu.make_async_copy(source(n), bufs.at[slot], local.sem.at[first + slot])

    copy(0, 0).start()

    def step(n):
        slot = n % 2
        copy(n, slot).wait()

        @pl.when(n + 1 < count)
        def _():
            copy(n + 1, 1 - slot).start()

        body(n, bufs.at[slot])

    loop(count, step)


def turned(ref):
    return jnp.transpose(ref[...].astype(F32)).astype(BF16)


def columns(ref, start, size):
    return ref.at[:, pl.ds(pl.multiple_of(start, 128), size)]


class Feeder:
    def __init__(self, local, source, bufs, block, dests):
        self.source, self.bufs, self.block, self.dests = source, bufs, block, dests
        self.sem, self.first, self.n = local.sem, local.next, 0
        local.next += 2
        self._copy(0).start()

    def _copy(self, n):
        return pltpu.make_async_copy(
            columns(self.source, self.dests[n] * self.block, self.block),
            self.bufs.at[n % 2],
            self.sem.at[self.first + n % 2],
        )

    def __call__(self, dest):
        n = self.n
        self.n += 1
        self._copy(n).wait()
        if n + 1 < len(self.dests):
            self._copy(n + 1).start()
        return self.bufs.at[n % 2]


def order_of(k):
    partner, own = (k.dcxy, k.dcx, k.dcy, k.dc), (k.dxy, k.dx, k.dy, k.d)
    return [partner[0], partner[1], own[0], partner[2], own[1], partner[3], own[2], own[3]]


def row_blocks(pick, left, right):
    width = right.shape[1]

    def compute(dest, add, out):
        left[...] = turned(pick(dest))

        def chunk(n):
            c = pl.ds(pl.multiple_of(n * 256, 256), 256)
            total = dot(left[...], right[:, c])
            if add is not None:
                total = total + add[:, c].astype(F32)
            out[:, c] = total.astype(BF16)

        loop(width // 256, chunk)

    return compute


def column_blocks(left, pick, chunks):
    size = left.shape[0] // chunks

    def compute(dest, add, out):
        picked = pick(dest)

        def chunk(n):
            r = pl.ds(pl.multiple_of(n * size, 16), size)
            total = dot(left[r], picked[...])
            if add is not None:
                total = total + add[r].astype(F32)
            out[r] = total.astype(BF16)

        loop(chunks, chunk)

    return compute


class Chunk:
    def __init__(self, sender, compute, sends, kept, land, base):
        self.s, self.compute, self.sends = sender, compute, sends
        self.kept, self.land, self.base = kept, land, base
        self.half = kept.shape[2] // 2

    def views(self, n):
        kept, land, h = self.kept.at[n], self.land.at[n], self.half
        top, low = pl.ds(0, h), pl.ds(h, h)
        return {
            "x1": (kept.at[pl.ds(0, 2), top], land.at[pl.ds(4, 2), top]),
            "y1": (kept.at[pl.ds(1, 2), low], land.at[pl.ds(4, 2), low]),
            "y2": (kept.at[2, top], land.at[6, top]),
            "x2": (kept.at[0, low], land.at[6, low]),
        }

    def partner(self, n):
        k = self.s.links
        for i, dest in enumerate((k.dcx, k.dcxy, k.dcy, k.dc)):
            self.compute(n, dest, None, self.sends.at[n, i])
        self.s.start(self.sends.at[n], self.land.at[n, pl.ds(0, 4)], self.base + 5 * n, (k.dc, k.z))

    def own(self, n):
        k, b, v = self.s.links, self.base + 5 * n, self.views(n)
        self.s.landed(self.land.at[n, pl.ds(0, 4)], b)
        for i, dest in enumerate((k.dx, k.dxy, k.dy, k.d)):
            self.compute(n, dest, self.land.at[n, i], self.kept.at[n, i])
        self.s.start(*v["x1"], b + 1, (k.dx, k.z))
        self.s.start(*v["y1"], b + 2, (k.dy, k.z))

    def add(self, n, i, start, got):
        kept, land = self.kept, self.land

        def rows(m):
            r = pl.ds(pl.multiple_of(start + m * 32, 32), 32)
            kept[n, i, r] = (kept[n, i, r].astype(F32) + land[n, got, r].astype(F32)).astype(BF16)

        loop(self.half // 32, rows)

    def second(self, n):
        k, b, v = self.s.links, self.base + 5 * n, self.views(n)
        self.s.landed(v["x1"][1], b + 1)
        self.add(n, 2, 0, 5)
        self.s.start(*v["y2"], b + 3, (k.dy, k.z))
        self.s.landed(v["y1"][1], b + 2)
        self.add(n, 0, self.half, 4)
        self.s.start(*v["x2"], b + 4, (k.dx, k.z))
        self.add(n, 3, 0, 4)
        self.add(n, 3, self.half, 5)

    def last(self, n):
        b, v = self.base + 5 * n, self.views(n)
        self.s.landed(v["y2"][1], b + 3)
        self.add(n, 3, 0, 6)
        self.s.landed(v["x2"][1], b + 4)
        self.add(n, 3, self.half, 6)

    def drain(self):
        for n in range(self.kept.shape[0]):
            b, v = self.base + 5 * n, self.views(n)
            self.s.sent(self.sends.at[n], b)
            for at, name in enumerate(("x1", "y1", "y2", "x2")):
                self.s.sent(v[name][0], b + 1 + at)


class Spread4:
    def __init__(self, sender, pick, land, base):
        self.s, self.pick, self.land, self.base = sender, pick, land, base

    def send(self):
        k = self.s.links
        for j in (1, 2, 3):
            to = (k.z + j) % 4
            self.s.start(self.pick(to), self.land.at[j - 1], self.base + j - 1, (k.d, to))

    def landed(self):
        for j in range(3):
            self.s.landed(self.land.at[j], self.base + j)

    def drain(self):
        z = self.s.links.z
        for j in (1, 2, 3):
            self.s.sent(self.pick((z + j) % 4), self.base + j - 1)


def feed_back_kernel(
    part_ref, n2_ref, dgu_ref, hidden_ref, top_ref, mid_ref,
    out_ref, ggu_out, gd_out,
    dgu, top_cols, n2_cols, left, sends, kept, land, hidden_cols, hidden_t, d_sends, d_kept, d_land,
    line_sends, line_land, send_sem, recv_sem, local_sem,
):
    links = Links()
    s = Sender(links, send_sem, recv_sem)
    local = Local(local_sem)
    block = left.shape[0]
    ff = hidden_t.shape[0]
    halves = lambda size: ((0, size // 2), (size // 2, size // 2))
    top_feed = Feeder(local, top_ref, top_cols, block, order_of(links))
    links.barrier()
    line = LineSum(s, local, part_ref, line_sends, line_land, 20)
    line.begin()
    fetch = local.start(dgu_ref, dgu)
    n2_feed = Feeder(local, n2_ref, n2_cols, block, order_of(links))

    def turn_hidden(n, buf):
        hidden_t[pl.ds(pl.multiple_of(n * 128, 128), 128)] = turned(buf)

    stream(local, ff // 128, lambda n: columns(hidden_ref, n * 128, 128), hidden_cols, turn_hidden)
    grad_d = Reduce(s, column_blocks(hidden_t, top_feed, 4), 10, d_sends, d_kept, d_land, halves(ff))
    grad_d.first()
    fetch.wait()
    line.step(2)
    grads = Reduce(s, row_blocks(n2_feed, left, dgu), 0, sends, kept, land, halves(block))
    grads.partner(0)
    grads.partner(1)
    grads.own(0)
    grad_d.second()
    grads.partner(2)
    grads.own(1)
    grads.partner(3)
    line.step(3)
    grads.own(2)
    grads.own(3)
    grad_d.last()
    to_down = local.start(d_kept.at[3], gd_out)
    grads.second()

    def write(r, total):
        out_ref[r] = mid_ref[r] + total

    line.finish(write)
    grads.last()
    local.load(kept.at[3], ggu_out)
    to_down.wait()
    grads.drain()
    grad_d.drain()
    line.drain()


def feed_back(part, n2, dgu, hidden, top, mid):
    rows, width = part.shape[0] // 4, part.shape[1]
    block, wide, ff = width // 8, dgu.shape[1], hidden.shape[1]
    vmem = pl.BlockSpec(memory_space=pltpu.VMEM)
    hbm = pl.BlockSpec(memory_space=pltpu.HBM)
    shape = jax.ShapeDtypeStruct
    return pl.pallas_call(
        feed_back_kernel,
        in_specs=[hbm] * 5 + [vmem],
        out_specs=[vmem, hbm, hbm],
        out_shape=[shape((rows, width), F32), shape((block, wide), BF16), shape((ff, block), BF16)],
        scratch_shapes=[
            pltpu.VMEM((4 * rows, wide), BF16),
            pltpu.VMEM((2, 4 * rows, block), BF16),
            pltpu.VMEM((2, 4 * rows, block), BF16),
            pltpu.VMEM((block, 4 * rows), BF16),
            pltpu.VMEM((2, block, wide), BF16),
            pltpu.VMEM((4, block, wide), BF16),
            pltpu.VMEM((7, block, wide), BF16),
            pltpu.VMEM((2, 4 * rows, 128), BF16),
            pltpu.VMEM((ff, 4 * rows), BF16),
            pltpu.VMEM((2, ff, block), BF16),
            pltpu.VMEM((4, ff, block), BF16),
            pltpu.VMEM((7, ff, block), BF16),
            pltpu.VMEM((4, rows, width), BF16),
            pltpu.VMEM((6, rows, width), BF16),
            pltpu.SemaphoreType.DMA((26,)),
            pltpu.SemaphoreType.DMA((26,)),
            pltpu.SemaphoreType.DMA((20,)),
        ],
        compiler_params=pltpu.CompilerParams(
            collective_id=1, has_side_effects=True, vmem_limit_bytes=65000 * 1024
        ),
        name="feed_back",
    )(part, n2, dgu, hidden, top, mid)


def norm_back_rows(rows_ref, at, gain, grad_normed):
    rows = rows_ref[at]
    inv = norm_scale(rows)
    weighted = grad_normed * gain
    scaled = grad_normed * rows * inv
    grad_rows = inv * weighted - rows * (inv * inv * inv) * jnp.mean(weighted * rows, -1, keepdims=True)
    return grad_rows, scaled


def attention_back_kernel(
    dn2_ref, mid_ref, x_ref, g_ref, gain_ref, cos_ref, sin_ref, q_ref, kv_ref, att_ref,
    wo_ref, wqkv_ref,
    grad_in_out, gq_out, gkv_out, go_out, gain_out,
    mid_bf, da, dqkv, dkv, dn1, n1, n1_t, att_t, w_chunk,
    row_sends, row_kept, land_row, o_sends, o_kept, land_o,
    gain_part, gain_land, z_q, z_kv, z_o,
    send_sem, recv_sem, local_sem,
):
    rows, width = x_ref.shape
    block = width // 8
    kv_width = 2 * KV * HD
    slot = width // 4
    links = Links()
    d, z = links.d, links.z
    s = Sender(links, send_sem, recv_sem)
    local = Local(local_sem)
    links.barrier(far=True)

    gain_part[...] = jnp.zeros_like(gain_part)
    dkv[...] = jnp.zeros_like(dkv)
    step = 32

    def add_gain(row, scaled):
        for b in range(8):
            total = jnp.sum(scaled[:, b * block : (b + 1) * block], 0, keepdims=True)
            at = (b % 2, b // 2 % 2 * 2 + b // 4)
            gain_part[at[0], at[1], row : row + 1] += total

    def middle(n):
        r = pl.ds(pl.multiple_of(n * step, step), step)
        grad_rows, scaled = norm_back_rows(mid_ref, r, gain_ref[1:2], dn2_ref[r])
        grad = g_ref[r] + grad_rows
        grad_in_out[r] = grad
        mid_bf[r] = grad.astype(BF16)
        add_gain(1, scaled)
        rows_x = x_ref[r]
        n1[r] = (rows_x * norm_scale(rows_x) * gain_ref[0:1]).astype(BF16)

    loop(rows // step, middle)

    def transpose_into(src, dst):
        def part(n):
            c = pl.ds(pl.multiple_of(n * 128, 128), 128)
            dst[c] = jnp.transpose(src[:, c].astype(F32)).astype(BF16)

        loop(src.shape[1] // 128, part)

    transpose_into(att_ref, att_t)
    halves = lambda size: ((0, size // 2), (size // 2, size // 2))
    pick_mid = lambda dest: columns(mid_bf, dest * block, block)
    grad_o = Reduce(s, column_blocks(att_t, pick_mid, 4), 0, o_sends, o_kept, land_o, halves(width))
    grad_o.first()
    transpose_into(n1, n1_t)

    def attended(n, buf):
        da[:, pl.ds(pl.multiple_of(n * 256, 256), 256)] = dot_nt(mid_bf[...], buf[...]).astype(BF16)

    row_chunk = lambda ref: lambda n: ref.at[pl.ds(pl.multiple_of(n * 256, 256), 256)]
    stream(local, width // 256, row_chunk(wo_ref), w_chunk.at[:, :, pl.ds(0, width)], attended)

    def group_of(n):
        return (z + 1 + n) % 4

    def row_compute(n, dest, add, out):
        left = n1_t[pl.ds(pl.multiple_of(dest * block, block), block)]
        start = group_of(n) * slot * (1 - n // 4) + width * (n // 4)
        for c in range(0, slot, 256):
            total = dot(left, dqkv[:, pl.ds(pl.multiple_of(start + c, 256), 256)])
            if add is not None:
                total = total + add[:, c : c + 256].astype(F32)
            out[:, c : c + 256] = total.astype(BF16)

    grad_row = Chunk(s, row_compute, row_sends, row_kept, land_row, 10)

    def final_q(n):
        grad_row.last(n)

        @pl.when(n < 3)
        def _():
            s.start(row_kept.at[n, 3], z_q.at[n], 35 + n, (d, group_of(n)))

    def group_step(n):
        group = group_of(n)

        def sequence(i):
            at = pl.ds(pl.multiple_of(i * SEQ, SEQ), SEQ)
            attend_back_group(cos_ref[at], sin_ref[at], group, q_ref, kv_ref, da, dqkv, dkv, at)

        loop(rows // SEQ, sequence)
        grad_row.partner(n)
        pl.when(n == 1)(grad_o.second)
        pl.when(n >= 1)(lambda: grad_row.own(n - 1))
        pl.when(n >= 2)(lambda: grad_row.second(n - 2))
        pl.when(n == 3)(lambda: final_q(0))

    loop(4, group_step)

    def key_value(i):
        at = pl.ds(pl.multiple_of(i * SEQ, SEQ), SEQ)
        first, _ = lane_masks()
        for tile in range(KV // 2):
            c = tile * LANES
            u = dkv[at, c : c + LANES]
            dqkv[at, width + c : width + c + LANES] = (
                u * cos_ref[at] - swap_halves(u, first) * sin_ref[at]
            ).astype(BF16)
        dqkv[at, width + KV * HD :] = dkv[at, KV * HD :].astype(BF16)

    loop(rows // SEQ, key_value)
    grad_row.partner(4)
    grad_o.last()
    send_o = Spread4(s, lambda p: o_kept.at[3, pl.ds(pl.multiple_of(p * slot, 16), slot)], z_o, 41)
    send_o.send()
    grad_row.own(3)
    grad_row.second(2)
    final_q(1)
    grad_row.own(4)
    grad_row.second(3)
    final_q(2)

    def projected(n, buf):
        dn1[:, pl.ds(pl.multiple_of(n * 256, 256), 256)] = dot_nt(dqkv[...], buf[...])

    stream(local, width // 256, row_chunk(wqkv_ref), w_chunk, projected)
    grad_row.second(4)
    final_q(3)

    def inward(n):
        r = pl.ds(pl.multiple_of(n * step, step), step)
        grad_rows, scaled = norm_back_rows(x_ref, r, gain_ref[0:1], dn1[r])
        grad_in_out[r] += grad_rows
        add_gain(0, scaled)

    loop(rows // step, inward)

    core, x_at, y_at = d % 2, d // 2 % 2, d // 4
    s.start(gain_part.at[1 - core], gain_land.at[pl.ds(0, 4)], 44, (links.dc, z))
    grad_row.last(4)
    send_kv = Spread4(
        s, lambda p: row_kept.at[4, 3, pl.ds(pl.multiple_of(p * KV_ROWS, 16), KV_ROWS)], z_kv, 38
    )
    send_kv.send()
    s.landed(gain_land.at[pl.ds(0, 4)], 44)
    gain_part[core] += gain_land[0:4]
    other_x = pl.multiple_of(2 - 2 * x_at, 2)
    s.start(gain_part.at[core, pl.ds(other_x, 2)], gain_land.at[pl.ds(4, 2)], 45, (links.dx, z))
    send_o.landed()

    def out_rows(n):
        r = pl.ds(pl.multiple_of(n * 16, 16), 16)
        mine = pl.ds(pl.multiple_of(z * slot + n * 16, 16), 16)
        go_out[r] = (
            o_kept[3, mine].astype(F32) + z_o[0, r].astype(F32) + z_o[1, r].astype(F32) + z_o[2, r].astype(F32)
        )

    loop(slot // 16, out_rows)
    s.landed(gain_land.at[pl.ds(4, 2)], 45)
    mine_x = 2 * x_at
    gain_part[core, pl.ds(mine_x, 2)] += gain_land[4:6]
    s.start(gain_part.at[core, mine_x + 1 - y_at], gain_land.at[6], 46, (links.dy, z))
    for n in range(3):
        s.landed(z_q.at[n], 35 + n)

    def query_rows(n):
        r = pl.ds(pl.multiple_of(n * 16, 16), 16)
        gq_out[r] = (
            row_kept[3, 3, r].astype(F32) + z_q[0, r].astype(F32) + z_q[1, r].astype(F32) + z_q[2, r].astype(F32)
        )

    loop(block // 16, query_rows)
    s.landed(gain_land.at[6], 46)
    gain_part[core, mine_x + y_at] += gain_land[6]
    send_g = Spread4(s, lambda p: gain_part.at[core, mine_x + y_at], gain_land.at[pl.ds(7, 3)], 47)
    send_g.send()
    send_kv.landed()
    mine_kv = pl.ds(pl.multiple_of(z * KV_ROWS, 16), KV_ROWS)
    gkv_out[...] = row_kept[4, 3, mine_kv].astype(F32) + (
        z_kv[0].astype(F32) + z_kv[1].astype(F32) + z_kv[2].astype(F32)
    )
    send_g.landed()
    gain_out[...] = gain_part[core, mine_x + y_at] + gain_land[7] + gain_land[8] + gain_land[9]

    for unit in (grad_o, grad_row, send_o, send_kv, send_g):
        unit.drain()
    for n in range(3):
        s.sent(row_kept.at[n, 3], 35 + n)
    s.sent(gain_part.at[1 - core], 44)
    s.sent(gain_part.at[core, pl.ds(other_x, 2)], 45)
    s.sent(gain_part.at[core, mine_x + 1 - y_at], 46)


def attention_back(dn2, mid, x, g, gains, cos, sin, query, key_val, attended, wo, wqkv):
    rows, width = x.shape
    block, slot = width // 8, width // 4
    kv_width = 2 * KV * HD
    wide = width + kv_width
    vmem = pl.BlockSpec(memory_space=pltpu.VMEM)
    hbm = pl.BlockSpec(memory_space=pltpu.HBM)
    shape = jax.ShapeDtypeStruct
    outs = [
        (vmem, shape((rows, width), F32)),
        (vmem, shape((block, slot), F32)),
        (vmem, shape((KV_ROWS, kv_width), F32)),
        (vmem, shape((slot, block), F32)),
        (vmem, shape((8, block), F32)),
    ]
    return pl.pallas_call(
        attention_back_kernel,
        in_specs=[vmem] * 10 + [hbm] * 2,
        out_specs=[o[0] for o in outs],
        out_shape=[o[1] for o in outs],
        scratch_shapes=[
            pltpu.VMEM((rows, width), BF16),
            pltpu.VMEM((rows, width), BF16),
            pltpu.VMEM((rows, wide), BF16),
            pltpu.VMEM((rows, kv_width), F32),
            pltpu.VMEM((rows, width), F32),
            pltpu.VMEM((rows, width), BF16),
            pltpu.VMEM((width, rows), BF16),
            pltpu.VMEM((width, rows), BF16),
            pltpu.VMEM((2, 256, wide), BF16),
            pltpu.VMEM((5, 4, block, slot), BF16),
            pltpu.VMEM((5, 4, block, slot), BF16),
            pltpu.VMEM((5, 7, block, slot), BF16),
            pltpu.VMEM((2, width, block), BF16),
            pltpu.VMEM((4, width, block), BF16),
            pltpu.VMEM((7, width, block), BF16),
            pltpu.VMEM((2, 4, 8, block), F32),
            pltpu.VMEM((10, 8, block), F32),
            pltpu.VMEM((3, block, slot), BF16),
            pltpu.VMEM((3, KV_ROWS, kv_width), BF16),
            pltpu.VMEM((3, slot, block), BF16),
            pltpu.SemaphoreType.DMA((50,)),
            pltpu.SemaphoreType.DMA((50,)),
            pltpu.SemaphoreType.DMA((60,)),
        ],
        compiler_params=pltpu.CompilerParams(
            collective_id=2, has_side_effects=True, vmem_limit_bytes=65000 * 1024
        ),
        name="attention_back",
    )(dn2, mid, x, g, gains, cos, sin, query, key_val, attended, wo, wqkv)


def plain_forward(x, g, cos, sin, w_query, w_kv, gains, w_out, w_gu, w_down):
    both = ("dp", "tensor")
    gather = lax.all_gather

    def whole(shard, dims):
        for dim, axis in dims:
            shard = gather(shard, axis, axis=dim, tiled=True)
        return shard

    wq = whole(w_query, ((1, "tensor"), (0, "dp")))
    wqkv = jnp.concatenate([wq, whole(w_kv, ((0, both),))], 1)
    gain = whole(gains, ((1, both),)).astype(F32)
    wo = whole(w_out, ((0, "tensor"), (1, "dp")))
    wgu = whole(w_gu, ((0, "dp"),))
    wd = whole(w_down, ((1, "dp"),))
    normed = (x * norm_scale(x) * gain[0]).astype(BF16)
    query, key_val, attended = attend(cos, sin, dot(normed, wqkv))
    middle = x + dot(attended, wo)
    normed_two = (middle * norm_scale(middle) * gain[1]).astype(BF16)
    n2 = gather(normed_two, "tensor", axis=0, tiled=True)
    top = gather(g.astype(BF16), "tensor", axis=0, tiled=True)
    return wqkv, gain, wo, wgu, wd, n2, top, query, key_val, attended, middle


def plain_backward(
    dn2_part, out_part, n2, grad_gu_pre, hidden, top,
    middle, x, g, gains, cos, sin, query, key_val, attended, wo, wqkv,
):
    width = x.shape[1]

    def scatter(part, axis, dim):
        return lax.psum_scatter(part.astype(BF16), axis, scatter_dimension=dim, tiled=True).astype(F32)

    output = middle + scatter(out_part, "tensor", 0)
    grad_mid_norm, gain_two = norm_back(middle, gains[1], scatter(dn2_part, "tensor", 0))
    grad_middle = g + grad_mid_norm
    mid_bf = grad_middle.astype(BF16)
    grad_qkv_rows = attend_back(cos, sin, query, key_val, dot_nt(mid_bf, wo).astype(BF16))
    grad_in_norm, gain_one = norm_back(x, gains[0], dot_nt(grad_qkv_rows, wqkv))
    normed_one = (x * norm_scale(x) * gains[0]).astype(BF16)
    grad_qkv = scatter(dot_tn(normed_one, grad_qkv_rows), "dp", 0)
    gain_parts = lax.psum_scatter(jnp.stack([gain_one, gain_two]), "dp", scatter_dimension=1, tiled=True)
    return (
        output,
        grad_middle + grad_in_norm,
        lax.psum_scatter(gain_parts, "tensor", scatter_dimension=1, tiled=True),
        scatter(grad_qkv[:, :width], "tensor", 1),
        scatter(grad_qkv[:, width:], "tensor", 0),
        scatter(scatter(dot_tn(attended, mid_bf), "dp", 1), "tensor", 0),
        scatter(dot_tn(n2, grad_gu_pre), "dp", 0),
        scatter(dot_tn(hidden, top), "dp", 1),
    )


def linked_layer(x, g, cos, sin, w_query, w_key, w_value, gains, w_out, w_gate, w_up, w_down):
    padded = jnp.pad(gains, ((0, GAIN_ROWS - 2), (0, LANES - gains.shape[1])))
    outs = forward_stage(x, g, cos, sin, w_query, w_key, w_value, padded, w_out, w_gate, w_up, w_down)
    wo, n2, top, wqkv, hidden, dgu, out_part = (outs[i] for i in (1, 4, 5, 6, 7, 8, 9))
    query, key_val, attended, middle, gain, dn2 = outs[11:]
    output, grad_gu, grad_down = feed_back(out_part, n2, dgu, hidden, top, middle)
    grad_in, grad_query, grad_kv, grad_out, gain_sum = attention_back(
        dn2, middle, x, g, gain, cos, sin, query, key_val, attended, wo, wqkv
    )
    own = gain_sum.shape[1] // 4
    grad_gains = lax.dynamic_slice(gain_sum, (0, lax.axis_index("tensor") * own), (2, own))
    return output, grad_in, grad_gains, grad_query, grad_kv, grad_out, grad_gu.astype(F32), grad_down.astype(F32)


def plain_layer(x, g, cos, sin, w_query, w_key, w_value, gains, w_out, w_gate, w_up, w_down):
    w_kv = jnp.concatenate([w_key, w_value], 1)
    w_gu = jnp.concatenate([w_gate, w_up], 1)
    wqkv, gains, wo, wgu, wd, n2, top, query, key_val, attended, middle = plain_forward(
        x, g, cos, sin, w_query, w_kv, gains, w_out, w_gu, w_down
    )
    ff = wd.shape[0]
    gate_up = dot(n2, wgu)
    gate_pre, up_pre = gate_up[:, :ff], gate_up[:, ff:]
    sig = jax.nn.sigmoid(gate_pre)
    hidden = (gate_pre * sig * up_pre).astype(BF16)
    grad_hidden = dot_nt(top, wd)
    grad_gate_pre = (grad_hidden * up_pre * sig * (1.0 + gate_pre * (1.0 - sig))).astype(BF16)
    grad_up_pre = (grad_hidden * gate_pre * sig).astype(BF16)
    grad_gu_pre = jnp.concatenate([grad_gate_pre, grad_up_pre], 1)
    return plain_backward(
        dot_nt(grad_gu_pre, wgu).astype(BF16), dot(hidden, wd).astype(BF16), n2, grad_gu_pre, hidden, top,
        middle, x, g, gains, cos, sin, query, key_val, attended, wo, wqkv,
    )


def on_device(
    linked,
    hidden_in, positions, norm_gains, w_query, w_key, w_value, w_out, w_gate, w_up, w_down, out_grad,
):
    x, g = hidden_in, out_grad
    rows, width = x.shape
    ff = w_gate.shape[2]
    kv_width = 2 * KV * HD
    z = lax.axis_index("tensor")

    cos, sin = rope_tables(lax.dynamic_slice_in_dim(positions, z * rows, rows))
    layer = linked_layer if linked else plain_layer
    output, grad_in, grad_gains, grad_query, grad_kv, grad_out, grad_gu, grad_down = layer(
        x, g, cos, sin,
        w_query[0], w_key[0], w_value[0], norm_gains[0], w_out[0], w_gate[0], w_up[0], w_down[0],
    )

    return (
        output,
        grad_in,
        grad_gains[None],
        grad_query[None],
        grad_kv[None, :, : KV * HD],
        grad_kv[None, :, KV * HD :],
        grad_out[None],
        grad_gu[None, :, :ff],
        grad_gu[None, :, ff:],
        grad_down[None],
    )


def solution(mesh):
    nd, nt = mesh.shape["dp"], mesh.shape["tensor"]
    rows = P(("dp", "tensor"), None)
    wide = P(None, "dp", "tensor")
    tall = P(None, "tensor", "dp")
    flat = P(None, ("dp", "tensor"), None)
    gain = P(None, None, ("dp", "tensor"))
    return jax.shard_map(
        functools.partial(on_device, (nd, nt) == (8, 4)),
        mesh=mesh,
        in_specs=(rows, P("dp"), gain, wide, flat, flat, tall, wide, wide, tall, rows),
        out_specs=(rows, rows, gain, wide, flat, flat, tall, wide, wide, tall),
        check_vma=False,
    )
```

```python
import functools

import jax
import jax.numpy as jnp
from jax import lax
from jax.experimental import pallas as pl
from jax.experimental.pallas import tpu as pltpu
from jax.sharding import PartitionSpec as P

H = 32
KV = 4
HD = 64
SEQ = 128
NORM_EPS = 1e-05
NEG_BIG = -1e30
SCALE = HD ** (-0.5)
LANES = 128
F32 = jnp.float32
BF16 = jnp.bfloat16


def dot(a, b):
    return jnp.dot(a, b, preferred_element_type=F32)


def dot_nt(a, b):
    return lax.dot_general(a, b, (((1,), (1,)), ((), ())), preferred_element_type=F32)


def dot_tn(a, b):
    return lax.dot_general(a, b, (((0,), (0,)), ((), ())), preferred_element_type=F32)


def lane_masks():
    lane = lax.broadcasted_iota(jnp.int32, (SEQ, LANES), 1)
    return lane % HD < HD // 2, lane < HD


def swap_halves(u, first):
    return jnp.where(first, pltpu.roll(u, LANES - HD // 2, 1), pltpu.roll(u, HD // 2, 1))


def twice(tile, index, low):
    turned = pltpu.roll(tile, HD, 1)
    return jnp.where(low, tile, turned) if index % 2 == 0 else jnp.where(low, turned, tile)


def causal_probs(query, key):
    scores = dot_nt(query, key) * SCALE
    rows = lax.broadcasted_iota(jnp.int32, scores.shape, 0)
    cols = lax.broadcasted_iota(jnp.int32, scores.shape, 1)
    scores = jnp.where(cols <= rows, scores, NEG_BIG)
    weights = jnp.exp(scores - jnp.max(scores, -1, keepdims=True))
    return weights * (1.0 / jnp.sum(weights, -1, keepdims=True))


def attend_sequence(cos, sin, load, kv_at, q_out, kv_out, o_out, at):
    first, low = lane_masks()

    def turn(u):
        return u * cos + swap_halves(u, first) * sin

    keys, vals_low, vals_high = [], [], []
    for tile in range(KV // 2):
        key = turn(load(kv_at + tile * LANES))
        val = load(kv_at + KV * HD + tile * LANES)
        kv_out[at, tile * LANES : (tile + 1) * LANES] = key.astype(BF16)
        kv_out[at, KV * HD + tile * LANES : KV * HD + (tile + 1) * LANES] = val.astype(BF16)
        for index in (0, 1):
            keys.append(twice(key, index, low).astype(BF16))
            both = twice(val, index, low)
            vals_low.append(jnp.where(low, both, 0.0).astype(BF16))
            vals_high.append(jnp.where(low, 0.0, both).astype(BF16))
    for pair in range(H // 2):
        group = pair * LANES // (H // KV * HD)
        query = turn(load(pair * LANES))
        p_low = causal_probs(jnp.where(low, query, 0.0).astype(BF16), keys[group])
        p_high = causal_probs(jnp.where(low, 0.0, query).astype(BF16), keys[group])
        q_out[at, pair * LANES : (pair + 1) * LANES] = query.astype(BF16)
        o_out[at, pair * LANES : (pair + 1) * LANES] = (
            dot(p_low.astype(BF16), vals_low[group]) + dot(p_high.astype(BF16), vals_high[group])
        ).astype(BF16)


def attend_back_sequence(cos, sin, q_ref, kv_ref, da_ref, dqkv_out, at):
    first, low = lane_masks()

    def turn_back(u):
        return (u * cos - swap_halves(u, first) * sin).astype(BF16)

    pair_total = H // KV * HD // LANES
    width = H * HD
    held = {}
    for group in range(KV):
        tile_at = group // 2 * LANES
        key = twice(kv_ref[at, tile_at : tile_at + LANES].astype(F32), group, low)
        val_at = KV * HD + tile_at
        val = twice(kv_ref[at, val_at : val_at + LANES].astype(F32), group, low).astype(BF16)
        key_low = jnp.where(low, key, 0.0).astype(BF16)
        key_high = jnp.where(low, 0.0, key).astype(BF16)
        key = key.astype(BF16)
        dk = jnp.zeros((SEQ, LANES), F32)
        dv = jnp.zeros((SEQ, LANES), F32)
        for pair in range(group * pair_total, (group + 1) * pair_total):
            query = q_ref[at, pair * LANES : (pair + 1) * LANES].astype(F32)
            grad = da_ref[at, pair * LANES : (pair + 1) * LANES].astype(F32)
            dq = None
            for is_low in (True, False):
                if is_low:
                    query_h = jnp.where(low, query, 0.0).astype(BF16)
                    grad_h = jnp.where(low, grad, 0.0).astype(BF16)
                else:
                    query_h = jnp.where(low, 0.0, query).astype(BF16)
                    grad_h = jnp.where(low, 0.0, grad).astype(BF16)
                prob = causal_probs(query_h, key)
                grad_prob = dot_nt(grad_h, val)
                delta = jnp.sum(prob * grad_prob, -1, keepdims=True)
                ds = (prob * (grad_prob - delta) * SCALE).astype(BF16)
                term = dot(ds, key_low if is_low else key_high)
                dq = term if dq is None else dq + term
                dk = dk + dot_tn(ds, query_h)
                dv = dv + dot_tn(prob.astype(BF16), grad_h)
            dqkv_out[at, pair * LANES : (pair + 1) * LANES] = turn_back(dq)
        held[group] = (dk + pltpu.roll(dk, HD, 1), dv + pltpu.roll(dv, HD, 1))
    for tile in range(KV // 2):
        col = width + tile * LANES
        dk = jnp.where(low, held[2 * tile][0], held[2 * tile + 1][0])
        dv = jnp.where(low, held[2 * tile][1], held[2 * tile + 1][1])
        dqkv_out[at, col : col + LANES] = turn_back(dk)
        dqkv_out[at, col + KV * HD : col + KV * HD + LANES] = dv.astype(BF16)


def causal_probs_turned(key, query):
    scores = dot_nt(key, query) * SCALE
    rows = lax.broadcasted_iota(jnp.int32, scores.shape, 0)
    cols = lax.broadcasted_iota(jnp.int32, scores.shape, 1)
    scores = jnp.where(rows <= cols, scores, NEG_BIG)
    weights = jnp.exp(scores - jnp.max(scores, 0, keepdims=True))
    return weights * (1.0 / jnp.sum(weights, 0, keepdims=True))


def attend_back_group(cos, sin, group, q_ref, kv_ref, da_ref, dqkv_out, dkv_out, at):
    first, low = lane_masks()
    head_width = H // KV * HD
    mine = low == (group % 2 == 0)

    def both(tile):
        kept = jnp.where(mine, tile.astype(F32), 0.0)
        return kept + pltpu.roll(kept, HD, 1)

    tile = pl.ds(pl.multiple_of(group // 2 * LANES, LANES), LANES)
    val_tile = pl.ds(pl.multiple_of(KV * HD + group // 2 * LANES, LANES), LANES)
    key = both(kv_ref[at, tile])
    val = both(kv_ref[at, val_tile]).astype(BF16)
    key_low = jnp.where(low, key, 0.0).astype(BF16)
    key_high = jnp.where(low, 0.0, key).astype(BF16)
    key = key.astype(BF16)
    dk = jnp.zeros((SEQ, LANES), F32)
    dv = jnp.zeros((SEQ, LANES), F32)
    for pair in range(head_width // LANES):
        c = pl.ds(pl.multiple_of(group * head_width + pair * LANES, LANES), LANES)
        query = q_ref[at, c].astype(F32)
        grad = da_ref[at, c].astype(F32)
        dq = None
        for is_low in (True, False):
            pick = low if is_low else jnp.logical_not(low)
            query_h = jnp.where(pick, query, 0.0).astype(BF16)
            grad_h = jnp.where(pick, grad, 0.0).astype(BF16)
            prob = causal_probs_turned(key, query_h)
            grad_prob = dot_nt(val, grad_h)
            delta = jnp.sum(prob * grad_prob, 0, keepdims=True)
            ds = (prob * (grad_prob - delta) * SCALE).astype(BF16)
            term = dot_tn(ds, key_low if is_low else key_high)
            dq = term if dq is None else dq + term
            dk = dk + dot(ds, query_h)
            dv = dv + dot(prob.astype(BF16), grad_h)
        dqkv_out[at, c] = (dq * cos - swap_halves(dq, first) * sin).astype(BF16)
    dkv_out[at, tile] += jnp.where(mine, dk + pltpu.roll(dk, HD, 1), 0.0)
    dkv_out[at, val_tile] += jnp.where(mine, dv + pltpu.roll(dv, HD, 1), 0.0)


def attend_kernel(cos_ref, sin_ref, qkv_ref, q_out, kv_out, o_out):
    attend_sequence(
        cos_ref[...], sin_ref[...], lambda c: qkv_ref[:, c : c + LANES], H * HD, q_out, kv_out, o_out, slice(None)
    )


def attend_back_kernel(cos_ref, sin_ref, q_ref, kv_ref, da_ref, dqkv_out):
    attend_back_sequence(cos_ref[...], sin_ref[...], q_ref, kv_ref, da_ref, dqkv_out, slice(None))


def by_sequence(body, name, ins, widths):
    rows = ins[0].shape[0]
    spec = lambda w: pl.BlockSpec((SEQ, w), lambda i: (i, 0))
    return pl.pallas_call(
        body,
        grid=(rows // SEQ,),
        in_specs=[spec(a.shape[1]) for a in ins],
        out_specs=[spec(w) for w in widths],
        out_shape=[jax.ShapeDtypeStruct((rows, w), BF16) for w in widths],
        name=name,
    )(*ins)


def attend(cos, sin, qkv):
    return by_sequence(attend_kernel, "attend", (cos, sin, qkv), (H * HD, 2 * KV * HD, H * HD))


def attend_back(cos, sin, query, key_val, grad):
    return by_sequence(
        attend_back_kernel, "attend_back", (cos, sin, query, key_val, grad), (H * HD + 2 * KV * HD,)
    )[0]


def norm_scale(rows):
    return lax.rsqrt(jnp.mean(rows * rows, -1, keepdims=True) + NORM_EPS)


def norm_back(rows, gain, grad_normed):
    inv = norm_scale(rows)
    weighted = grad_normed * gain
    grad_gain = jnp.sum(grad_normed * rows * inv, 0)
    grad_rows = inv * weighted - rows * inv**3 * jnp.mean(weighted * rows, -1, keepdims=True)
    return grad_rows, grad_gain


def rope_tables(positions):
    half = jnp.arange(LANES, dtype=jnp.int32) % (HD // 2)
    inv_freq = 10000.0 ** (-(half.astype(F32) * 2.0 / HD))
    angles = positions.astype(F32)[:, None] * inv_freq[None, :]
    sign = jnp.where(jnp.arange(LANES) % HD < HD // 2, -1.0, 1.0).astype(F32)
    return jnp.cos(angles), jnp.sin(angles) * sign[None, :]


MESH = pl.DeviceIdType.MESH
KV_ROWS = 64
GAIN_ROWS = 16


class Links:
    def __init__(self):
        self.d, self.z = lax.axis_index("dp"), lax.axis_index("tensor")
        core, x, y = self.d % 2, self.d // 2 % 2, self.d // 4
        self.dc = self.d + 1 - 2 * core
        step_x, step_y = 2 - 4 * x, 4 - 8 * y
        self.dx, self.dy, self.dxy = self.d + step_x, self.d + step_y, self.d + step_x + step_y
        self.dcx, self.dcy, self.dcxy = self.dc + step_x, self.dc + step_y, self.dc + step_x + step_y

    def barrier(self, far=False):
        z = self.z
        sem = pltpu.get_barrier_semaphore()

        def greet(d, zz):
            pl.semaphore_signal(sem, inc=1, device_id=(d, zz), device_id_type=MESH)

        for d in (self.dx, self.dy, self.dc):
            greet(d, z)
        if far:
            for j in (1, 2, 3):
                greet(self.d, (z + j) % 4)
            pl.semaphore_wait(sem, 6)
            return
        pl.when(z > 0)(lambda: greet(self.d, z - 1))
        pl.when(z < 3)(lambda: greet(self.d, z + 1))
        pl.semaphore_wait(sem, 3 + (z + 2) // 3 + (5 - z) // 3)


class Sender:
    def __init__(self, links, send_sem, recv_sem):
        self.links, self.send_sem, self.recv_sem = links, send_sem, recv_sem

    def copy(self, src, dst, at, to):
        return pltpu.make_async_remote_copy(
            src_ref=src,
            dst_ref=dst,
            send_sem=self.send_sem.at[at],
            recv_sem=self.recv_sem.at[at],
            device_id=to,
            device_id_type=MESH,
        )

    def start(self, src, dst, at, to):
        self.copy(src, dst, at, to).start()

    def landed(self, region, at):
        self.copy(region, region, at, (self.links.dc, self.links.z)).wait_recv()

    def sent(self, region, at):
        self.copy(region, region, at, (self.links.dc, self.links.z)).wait_send()


class Spread:
    def __init__(self, sender, region, base):
        self.s, self.region, self.base = sender, region, base

    def own(self, p, src):
        k, r, b = self.s.links, self.region, self.base + 9 * p
        mine = r(k.d, p, None)
        self.s.start(src, mine, b, (k.dx, k.z))
        self.s.start(src, mine, b + 1, (k.dy, k.z))
        self.s.start(src, mine, b + 2, (k.dc, k.z))

    def near(self, p):
        k, r, b = self.s.links, self.region, self.base + 9 * p
        self.s.landed(r(k.dx, p, None), b)
        self.s.start(r(k.dx, p, 0), r(k.dx, p, 0), b + 3, (k.dy, k.z))
        self.s.start(r(k.dx, p, None), r(k.dx, p, None), b + 5, (k.dc, k.z))
        self.s.landed(r(k.dy, p, None), b + 1)
        self.s.start(r(k.dy, p, 1), r(k.dy, p, 1), b + 4, (k.dx, k.z))
        self.s.start(r(k.dy, p, None), r(k.dy, p, None), b + 6, (k.dc, k.z))

    def far(self, p):
        k, r, b = self.s.links, self.region, self.base + 9 * p
        for part in (0, 1):
            self.s.landed(r(k.dxy, p, part), b + 3 + part)
            self.s.start(r(k.dxy, p, part), r(k.dxy, p, part), b + 7 + part, (k.dc, k.z))

    def finish(self, p):
        k, r, b = self.s.links, self.region, self.base + 9 * p
        self.s.landed(r(k.dc, p, None), b + 2)
        self.s.landed(r(k.dcx, p, None), b + 5)
        self.s.landed(r(k.dcy, p, None), b + 6)
        for part in (0, 1):
            self.s.landed(r(k.dcxy, p, part), b + 7 + part)

    def drain(self, p):
        k, r, b = self.s.links, self.region, self.base + 9 * p
        for i in (0, 1, 2):
            self.s.sent(r(k.d, p, None), b + i)
        self.s.sent(r(k.dx, p, 0), b + 3)
        self.s.sent(r(k.dy, p, 1), b + 4)
        self.s.sent(r(k.dx, p, None), b + 5)
        self.s.sent(r(k.dy, p, None), b + 6)
        for part in (0, 1):
            self.s.sent(r(k.dxy, p, part), b + 7 + part)


class Line:
    def __init__(self, sender, region, base):
        self.s, self.region, self.base = sender, region, base

    def _send(self, src, p, way, step):
        k = self.s.links
        self.s.start(src, self.region(p), self.base + 2 * (step - 1) + way, (k.d, k.z + 1 - 2 * way))

    def own(self, src):
        z = self.s.links.z
        pl.when(z < 3)(lambda: self._send(src, z, 0, 1))
        pl.when(z > 0)(lambda: self._send(src, z, 1, 1))

    def each(self, step, action):
        z = self.s.links.z
        pl.when(z >= step)(lambda: action(z - step, 0))
        pl.when(z + step <= 3)(lambda: action(z + step, 1))

    def arrive(self, step, then=None):
        z = self.s.links.z

        def action(p, way):
            self.s.landed(self.region(p), self.base + 2 * (step - 1) + way)
            if step < 3:
                ahead = z < 3 if way == 0 else z > 0
                pl.when(ahead)(lambda: self._send(self.region(p), p, way, step + 1))
            if then is not None:
                then(p)

        self.each(step, action)

    def drain(self):
        z = self.s.links.z
        for step in (1, 2, 3):
            for way in (0, 1):
                came = z - (step - 1) if way == 0 else z + (step - 1)
                ok = jnp.logical_and(z < 3, z >= step - 1) if way == 0 else jnp.logical_and(z > 0, z <= 4 - step)
                pl.when(ok)(
                    functools.partial(self.s.sent, self.region(came), self.base + 2 * (step - 1) + way)
                )


def forward_kernel(
    x_ref, g_ref, cos_ref, sin_ref, wq_in, wk_in, wv_in, gain_in, wo_ref, wg_in, wu_in, wd_ref,
    wa_all, wo_all, gu_all, wd_all, n2_all, top_all, wqkv_all, hidden_all, dgu_all, out_all, dn2_land,
    q_out, kv_out, o_out, mid_out, gain_out, dn2_out,
    att_ref, gu_ref, n1, qkv, w_buf, wkv_buf, gain_buf, wo_buf, n2, top,
    n2_rows, top_rows, gate_up, grad_hidden, hidden, dgu, dn2_sends, out_rows, relay,
    send_sem, recv_sem, local_sem,
):
    rows, width = x_ref.shape
    slot_width = att_ref.shape[1]
    block = width // 8
    links = Links()
    d, z = links.d, links.z
    s = Sender(links, send_sem, recv_sem)
    ff = wd_ref.shape[0]
    cut_a = att_ref.shape[0] // 32 * 16
    cuts_a = ((0, cut_a), (cut_a, att_ref.shape[0] - cut_a))

    def at_a(dd, p, part):
        if part is None:
            return wa_all.at[dd, p]
        return wa_all.at[dd, p, pl.ds(*cuts_a[part])]

    def at_b(dd, p, part):
        start, size = (0, slot_width) if part is None else (part * slot_width // 2, slot_width // 2)
        return wo_all.at[
            pl.ds(pl.multiple_of(p * slot_width + start, 16), size),
            pl.ds(pl.multiple_of(dd * block, 128), block),
        ]

    def at_gu(dd, p, part):
        start, size = (0, block) if part is None else (part * block // 2, block // 2)
        return gu_all.at[pl.ds(pl.multiple_of(dd * block + start, 16), size)]

    def at_wd(dd, p, part):
        start, size = (0, ff) if part is None else (part * ff // 2, ff // 2)
        return wd_all.at[pl.ds(start, size), pl.ds(pl.multiple_of(dd * block, 128), block)]

    def rows_of(ref):
        return lambda p: ref.at[pl.ds(pl.multiple_of(p * rows, 16), rows)]

    spread_a, spread_b = Spread(s, at_a, 0), Spread(s, at_b, 36)
    spread_gu, spread_wd = Spread(s, at_gu, 72), Spread(s, at_wd, 81)
    line_a = Line(s, lambda p: at_a(d, p, None), 90)
    line_b = Line(s, lambda p: at_b(d, p, None), 96)
    line_n, line_t = Line(s, rows_of(n2_all), 102), Line(s, rows_of(top_all), 108)

    def keep(src, dst, at):
        pltpu.make_async_copy(src, dst, local_sem.at[at]).start()

    def kept(src, dst, at):
        pltpu.make_async_copy(src, dst, local_sem.at[at]).wait()

    kv_at = pl.ds(block, KV_ROWS)
    shards = [
        (wq_in, att_ref.at[pl.ds(0, block)], 78),
        (wk_in, att_ref.at[kv_at, pl.ds(0, KV * HD)], 79),
        (wv_in, att_ref.at[kv_at, pl.ds(KV * HD, KV * HD)], 80),
        (gain_in, att_ref.at[pl.ds(block + KV_ROWS, GAIN_ROWS), pl.ds(0, LANES)], 81),
    ]
    ffs = [(wg_in, gu_ref.at[:, pl.ds(0, ff)], 82), (wu_in, gu_ref.at[:, pl.ds(ff, ff)], 83)]
    for shard in shards + ffs:
        keep(*shard)
    att_ref[block + KV_ROWS :, LANES:] = jnp.zeros((GAIN_ROWS, slot_width - LANES), BF16)
    links.barrier(far=True)
    for shard in shards:
        kept(*shard)

    line_a.own(att_ref)
    spread_a.own(z, att_ref)
    keep(att_ref, at_a(d, z, None), 0)
    keep(wo_ref, at_b(d, z, None), 1)
    keep(wd_ref, at_wd(d, 0, None), 3)
    top[...] = g_ref[...].astype(BF16)
    line_a.arrive(1, lambda p: spread_a.own(p, at_a(d, p, None)))
    spread_a.near(z)
    line_a.arrive(2, lambda p: spread_a.own(p, at_a(d, p, None)))
    line_b.own(wo_ref)
    line_a.each(1, lambda p, way: spread_a.near(p))
    spread_a.far(z)
    line_a.arrive(3, lambda p: spread_a.own(p, at_a(d, p, None)))
    line_b.arrive(1)
    line_a.each(2, lambda p, way: spread_a.near(p))
    line_a.each(1, lambda p, way: spread_a.far(p))
    line_a.each(3, lambda p, way: spread_a.near(p))
    spread_b.own(z, wo_ref)
    line_b.each(1, lambda p, way: spread_b.own(p, at_b(d, p, None)))
    line_b.arrive(2, lambda p: spread_b.own(p, at_b(d, p, None)))
    line_a.each(2, lambda p, way: spread_a.far(p))
    line_a.each(3, lambda p, way: spread_a.far(p))
    for shard in ffs:
        kept(*shard)
    keep(gu_ref, at_gu(d, 0, None), 2)
    line_b.arrive(3, lambda p: spread_b.own(p, at_b(d, p, None)))
    line_t.own(top)
    kept(att_ref, at_a(d, z, None), 0)
    for p in range(4):
        spread_a.finish(p)

    def kv_copy(dd, p):
        return wkv_buf.at[dd, p], wqkv_all.at[pl.ds(dd * block + p * KV_ROWS, KV_ROWS), pl.ds(width, 2 * KV * HD)]

    for p in range(4):
        for dd in range(8):
            pltpu.make_async_copy(
                wa_all.at[dd, p, pl.ds(0, block)], w_buf.at[p, pl.ds(dd * block, block)], local_sem.at[14 + 8 * p + dd]
            ).start()
    keep(wa_all.at[:, :, pl.ds(block, KV_ROWS)], wkv_buf, 8)
    keep(wa_all.at[:, :, pl.ds(block + KV_ROWS, GAIN_ROWS), pl.ds(0, LANES)], gain_buf, 9)
    kept(wa_all.at[:, :, pl.ds(block + KV_ROWS, GAIN_ROWS), pl.ds(0, LANES)], gain_buf, 9)
    low_row = lax.broadcasted_iota(jnp.int32, (GAIN_ROWS, LANES), 1) < HD
    for dd in range(8):
        for half in (0, 1):
            first = gain_buf[dd, 2 * half].astype(F32)
            second = pltpu.roll(gain_buf[dd, 2 * half + 1].astype(F32), HD, 1)
            at = dd * block + half * LANES
            gain_out[:, at : at + LANES] = jnp.where(low_row, first, second)[:8]
    x = x_ref[...]
    n1[...] = (x * norm_scale(x) * gain_out[0:1]).astype(BF16)
    for p in range(4):
        for dd in range(8):
            kept(wa_all.at[dd, p, pl.ds(0, block)], w_buf.at[p, pl.ds(dd * block, block)], 14 + 8 * p + dd)
        for c in range(0, slot_width, 256):
            qkv[:, p * slot_width + c : p * slot_width + c + 256] = dot(n1[...], w_buf[p, :, c : c + 256])
        keep(w_buf.at[p], wqkv_all.at[:, pl.ds(p * slot_width, slot_width)], 4 + p)
    kept(wa_all.at[:, :, pl.ds(block, KV_ROWS)], wkv_buf, 8)
    qkv[:, width:] = dot(n1[...], wkv_buf[...].reshape(width, 2 * KV * HD))
    for p in range(4):
        for dd in range(8):
            pltpu.make_async_copy(*kv_copy(dd, p), local_sem.at[46 + 8 * p + dd]).start()

    line_b_pieces = lambda action: [action(z)] + [line_b.each(i, lambda p, way: action(p)) for i in (1, 2, 3)]

    def sequence(i, carry):
        at = pl.ds(pl.multiple_of(i * SEQ, SEQ), SEQ)
        attend_sequence(
            cos_ref[at], sin_ref[at], lambda c: qkv[at, c : c + LANES], width, q_out, kv_out, o_out, at
        )

        @pl.when(i == 0)
        def _():
            line_b_pieces(spread_b.near)
            spread_gu.own(0, gu_ref)
            line_t.arrive(1)

        return carry

    lax.fori_loop(0, rows // SEQ, sequence, 0)
    line_b_pieces(spread_b.far)
    kept(wo_ref, at_b(d, z, None), 1)
    for p in range(4):
        spread_b.finish(p)
    keep(wo_all, wo_buf, 0)
    kept(wo_all, wo_buf, 0)

    def column(i, carry):
        at = pl.ds(pl.multiple_of(i * 256, 256), 256)
        mid_out[:, at] = x_ref[:, at] + dot(o_out[...], wo_buf[:, at])
        return carry

    lax.fori_loop(0, width // 256, column, 0)
    mid = mid_out[...]
    n2[...] = (mid * norm_scale(mid) * gain_out[1:2]).astype(BF16)

    line_n.own(n2)
    keep(n2, n2_all.at[pl.ds(pl.multiple_of(z * rows, 16), rows)], 8)
    keep(top, top_all.at[pl.ds(pl.multiple_of(z * rows, 16), rows)], 9)
    line_t.arrive(2)
    for p in range(4):
        kept(w_buf.at[p], wqkv_all.at[:, pl.ds(p * slot_width, slot_width)], 4 + p)
        for dd in range(8):
            kept(*kv_copy(dd, p), 46 + 8 * p + dd)
    kept(gu_ref, at_gu(d, 0, None), 2)
    kept(wd_ref, at_wd(d, 0, None), 3)
    kept(n2, n2_all.at[pl.ds(pl.multiple_of(z * rows, 16), rows)], 8)
    kept(top, top_all.at[pl.ds(pl.multiple_of(z * rows, 16), rows)], 9)
    spread_gu.near(0)
    spread_wd.own(0, wd_ref)
    line_n.arrive(1)
    line_t.arrive(3)
    spread_gu.far(0)
    spread_gu.finish(0)

    wide = 2 * ff
    pieces = [(c, min(slot_width, wide - c)) for c in range(0, wide, slot_width)]
    gu_piece = lambda i, c, n: (columns(gu_all, c, n), w_buf.at[i, :, pl.ds(0, n)])
    for i, (c, n) in enumerate(pieces):
        keep(*gu_piece(i, c, n), 14 + i)
    wd_vmem = wo_buf.at[pl.ds(0, ff)]
    across, opposite, beside = 2 - z // 2, 3 - 3 * (z // 2), z + 1 - 2 * (z % 2)
    ends, inner = z % 3 == 0, z % 3 != 0
    chunks = [(c, min(256, ff - c)) for c in range(0, ff, 256)]

    def project(slot, source):
        for c, n in pieces:
            for h in range(0, n, 256):
                gate_up[slot, :, c + h : c + h + 256] = dot(source[...], w_buf[c // slot_width, :, h : h + 256])

    rows_at = lambda p: pl.ds(pl.multiple_of(p * rows, 16), rows)
    for i, (c, n) in enumerate(pieces):
        kept(*gu_piece(i, c, n), 14 + i)
    project(1, n2)
    spread_wd.near(0)
    line_n.arrive(2)
    keep(n2_all.at[rows_at(across)], n2_rows, 0)
    kept(n2_all.at[rows_at(across)], n2_rows, 0)
    project(0, n2_rows)
    spread_wd.far(0)
    spread_wd.finish(0)
    keep(wd_all, wd_vmem, 20)
    kept(wd_all, wd_vmem, 20)

    def place_of(p):
        return (p - z + 4) % 4 - 1

    def send_dn2(i, p):
        s.start(dn2_sends.at[i], dn2_land.at[place_of(p)], 114 + place_of(p), (d, p))

    def half_of(ref, h):
        return columns(ref, h * (width // 2), width // 2)

    def opposite_half(h):
        return half_of(dn2_land.at[1], h), 115 + 4 * h

    def pass_on(h):
        s.landed(half_of(relay, h), 117 + h)

        def add(m):
            r = pl.ds(pl.multiple_of(m * 32, 32), 32)
            c = pl.ds(h * (width // 2), width // 2)
            dn2_sends[1, r, c] = (dn2_sends[1, r, c].astype(F32) + relay[r, c].astype(F32)).astype(BF16)

        loop(rows // 32, add)
        to, at = opposite_half(h)
        s.start(half_of(dn2_sends.at[1], h), to, at, (d, opposite))

    def feed(i):
        pl.when(i == 1)(lambda: line_n.arrive(3))
        second = (i + 2) // 3 - i // 2
        p = across * ((3 - i) // 3) + opposite * second + beside * (i // 2 - i // 3) + z * (i // 3)
        at = rows_at(p)
        slot = i // 3
        keep(top_all.at[at], top_rows, 1)

        @pl.when(second + i // 2 - i // 3 == 1)
        def _():
            keep(n2_all.at[at], n2_rows, 0)
            kept(n2_all.at[at], n2_rows, 0)
            project(0, n2_rows)

        kept(top_all.at[at], top_rows, 1)
        for c, n in chunks:
            grad_hidden[:, c : c + n] = dot_nt(top_rows[...], wo_buf[c : c + n])

        @pl.when(i > 0)
        def _():
            kept(hidden, hidden_all.at[at], 2)
            kept(dgu, dgu_all.at[at], 3)

        def act(m):
            r = pl.ds(pl.multiple_of(m * 16, 16), 16)
            for c, n in chunks:
                gate, up = gate_up[slot, r, c : c + n], gate_up[slot, r, ff + c : ff + c + n]
                grad = grad_hidden[r, c : c + n]
                sig = 1.0 / (1.0 + jnp.exp(-gate))
                silu = gate * sig
                hidden[r, c : c + n] = (silu * up).astype(BF16)
                dgu[r, c : c + n] = (grad * up * sig * (1.0 + gate * (1.0 - sig))).astype(BF16)
                dgu[r, ff + c : ff + c + n] = (grad * silu).astype(BF16)

        loop(rows // 16, act)
        pl.when(jnp.logical_and(i == 3, inner))(lambda: pass_on(1))
        keep(hidden, hidden_all.at[at], 2)
        keep(dgu, dgu_all.at[at], 3)

        def back(m):
            r = pl.ds(pl.multiple_of(m * 256, 256), 256)
            total = None
            for j, (c, n) in enumerate(pieces):
                term = dot_nt(dgu[:, c : c + n], w_buf[j, r, :n])
                total = term if total is None else total + term

            @pl.when(i < 3)
            def _():
                dn2_sends[i, :, r] = total.astype(BF16)

            @pl.when(i == 3)
            def _():
                dn2_out[:, r] = total

            for h in (0, 1):

                @pl.when(jnp.logical_and(jnp.logical_and(i == 1, m == 4 * h + 3), ends))
                def _():
                    s.start(half_of(dn2_sends.at[1], h), half_of(relay, h), 117 + h, (d, 1 + z // 3))

        loop(width // 256, back)

        @pl.when(i % 2 == 0)
        def _():
            send_dn2(i, p)


        pl.when(i > 0)(lambda: kept(out_rows, out_all.at[at], 7))

        def down(m):
            r = pl.ds(pl.multiple_of(m * 256, 256), 256)
            out_rows[:, r] = dot(hidden[...], wo_buf[:ff, r]).astype(BF16)

        loop(width // 256, down)
        keep(out_rows, out_all.at[at], 7)
        pl.when(jnp.logical_and(i == 2, inner))(lambda: pass_on(0))

    loop(4, feed)
    kept(hidden, hidden_all.at[pl.ds(0, rows)], 2)
    kept(dgu, dgu_all.at[pl.ds(0, rows)], 3)
    kept(out_rows, out_all.at[pl.ds(0, rows)], 7)

    def collect(region, at, h=None):
        s.landed(region, at)
        c = pl.ds(0, width) if h is None else pl.ds(h * (width // 2), width // 2)
        keep(region, n2_rows.at[:, c], 0)
        kept(region, n2_rows.at[:, c], 0)

        def add(m):
            r = pl.ds(pl.multiple_of(m * 32, 32), 32)
            dn2_out[r, c] += n2_rows[r, c].astype(F32)

        loop(rows // 32, add)

    pl.when(z >= 1)(lambda: collect(dn2_land.at[0], 114))
    pl.when(z <= 2)(lambda: collect(dn2_land.at[2], 116))
    pl.when(inner)(lambda: collect(dn2_land.at[1], 115))
    for h in (0, 1):
        to, at = opposite_half(h)
        pl.when(ends)(functools.partial(collect, to, at, h))
    for i, p in ((0, across), (2, beside)):
        s.sent(dn2_sends.at[i], 114 + place_of(p))
    for h in (0, 1):
        to, at = opposite_half(h)
        pl.when(ends)(functools.partial(s.sent, half_of(dn2_sends.at[1], h), 117 + h))
        pl.when(inner)(functools.partial(s.sent, half_of(dn2_sends.at[1], h), at))
    for p in range(4):
        spread_a.drain(p)
        spread_b.drain(p)
    spread_gu.drain(0)
    spread_wd.drain(0)
    for line in (line_a, line_b, line_n, line_t):
        line.drain()


def forward_stage(x, g, cos, sin, wq, wk, wv, gains, wo, wg, wu, wd):
    rows, width = x.shape
    slot_width = wq.shape[1]
    block = width // 8
    kv_width = 2 * KV * HD
    ff = wd.shape[0]
    vmem = pl.BlockSpec(memory_space=pltpu.VMEM)
    hbm = pl.BlockSpec(memory_space=pltpu.HBM)
    shape = jax.ShapeDtypeStruct
    outs = [
        (hbm, shape((8, 4, block + KV_ROWS + GAIN_ROWS, slot_width), BF16)),
        (hbm, shape((width, width), BF16)),
        (hbm, shape((width, 2 * ff), BF16)),
        (hbm, shape((ff, width), BF16)),
        (hbm, shape((4 * rows, width), BF16)),
        (hbm, shape((4 * rows, width), BF16)),
        (hbm, shape((width, width + kv_width), BF16)),
        (hbm, shape((4 * rows, ff), BF16)),
        (hbm, shape((4 * rows, 2 * ff), BF16)),
        (hbm, shape((4 * rows, width), BF16)),
        (hbm, shape((3, rows, width), BF16)),
        (vmem, shape((rows, width), BF16)),
        (vmem, shape((rows, kv_width), BF16)),
        (vmem, shape((rows, width), BF16)),
        (vmem, shape((rows, width), F32)),
        (vmem, shape((8, width), F32)),
        (vmem, shape((rows, width), F32)),
    ]
    return pl.pallas_call(
        forward_kernel,
        in_specs=[vmem] * 4 + [hbm] * 4 + [vmem] + [hbm] * 2 + [vmem],
        out_specs=[o[0] for o in outs],
        out_shape=[o[1] for o in outs],
        scratch_shapes=[
            pltpu.VMEM((block + KV_ROWS + GAIN_ROWS, slot_width), BF16),
            pltpu.VMEM((block, 2 * ff), BF16),
            pltpu.VMEM((rows, width), BF16),
            pltpu.VMEM((rows, width + kv_width), F32),
            pltpu.VMEM((-(-2 * ff // slot_width), width, slot_width), BF16),
            pltpu.VMEM((8, 4, KV_ROWS, kv_width), BF16),
            pltpu.VMEM((8, 4, GAIN_ROWS, LANES), BF16),
            pltpu.VMEM((width, width), BF16),
            pltpu.VMEM((rows, width), BF16),
            pltpu.VMEM((rows, width), BF16),
            pltpu.VMEM((rows, width), BF16),
            pltpu.VMEM((rows, width), BF16),
            pltpu.VMEM((2, rows, 2 * ff), F32),
            pltpu.VMEM((rows, ff), F32),
            pltpu.VMEM((rows, ff), BF16),
            pltpu.VMEM((rows, 2 * ff), BF16),
            pltpu.VMEM((3, rows, width), BF16),
            pltpu.VMEM((rows, width), BF16),
            pltpu.VMEM((rows, width), BF16),
            pltpu.SemaphoreType.DMA((120,)),
            pltpu.SemaphoreType.DMA((120,)),
            pltpu.SemaphoreType.DMA((84,)),
        ],
        compiler_params=pltpu.CompilerParams(
            collective_id=0, has_side_effects=True, vmem_limit_bytes=65000 * 1024
        ),
        name="forward",
    )(x, g, cos, sin, wq, wk, wv, gains, wo, wg, wu, wd)


def loop(count, body):
    def step(i, carry):
        body(i)
        return carry

    lax.fori_loop(0, count, step, 0)


class Local:
    def __init__(self, sem):
        self.sem, self.next = sem, 0

    def start(self, src, dst):
        copy = pltpu.make_async_copy(src, dst, self.sem.at[self.next])
        self.next += 1
        copy.start()
        return copy

    def load(self, src, dst):
        self.start(src, dst).wait()


class Reduce:
    def __init__(self, sender, compute, base, sends, kept, land, halves):
        self.s, self.compute, self.base = sender, compute, base
        self.sends, self.kept, self.land, self.halves = sends, kept, land, halves

    def half(self, ref, part):
        return ref.at[pl.ds(*self.halves[part])]

    def place(self, i):
        if i < 4:
            return self.land.at[i]
        return self.half(self.land.at[4 + (i - 4) // 2], i % 2)

    def partner(self, i):
        k = self.s.links
        count = self.sends.shape[0]
        if i >= count:
            self.s.sent(self.sends.at[i % count], self.base + i - count)
        self.compute((k.dcxy, k.dcx, k.dcy, k.dc)[i], None, self.sends.at[i % count])
        self.s.start(self.sends.at[i % count], self.place(i), self.base + i, (k.dc, k.z))

    def own(self, i):
        k, b = self.s.links, self.base
        to_x, to_y = (k.dx, k.z), (k.dy, k.z)
        self.s.landed(self.place(i), b + i)
        kept = self.kept.at[i]
        self.compute((k.dxy, k.dx, k.dy, k.d)[i], self.land.at[i], kept)
        if i == 0:
            self.s.start(self.half(kept, 0), self.place(4), b + 4, to_x)
            self.s.start(self.half(kept, 1), self.place(7), b + 7, to_y)
        elif i == 1:
            self.s.start(self.half(kept, 0), self.place(6), b + 6, to_x)
        elif i == 2:
            self.s.start(self.half(kept, 1), self.place(5), b + 5, to_y)

    def first(self):
        self.partner(0)
        for i in range(3):
            self.partner(i + 1)
            self.own(i)
        self.own(3)

    def add(self, i, part, at):
        self.s.landed(self.place(at), self.base + at)
        start, size = self.halves[part]
        from_start = self.halves[at % 2][0] if at < 8 else self.halves[at - 8][0]
        slot = 4 + (at - 4) // 2
        step = 32 if size % 32 == 0 else 16

        def rows(n):
            r = pl.ds(pl.multiple_of(start + n * step, 16), step)
            g = pl.ds(pl.multiple_of(from_start + n * step, 16), step)
            self.kept[i, r] = (self.kept[i, r].astype(F32) + self.land[slot, g].astype(F32)).astype(BF16)

        loop(size // step, rows)

    def second(self):
        k, b = self.s.links, self.base
        self.add(2, 0, 4)
        self.s.start(self.half(self.kept.at[2], 0), self.place(8), b + 8, (k.dy, k.z))
        self.add(1, 1, 7)
        self.s.start(self.half(self.kept.at[1], 1), self.place(9), b + 9, (k.dx, k.z))

    def last(self):
        self.add(3, 0, 6)
        self.add(3, 1, 5)
        self.add(3, 0, 8)
        self.add(3, 1, 9)

    def drain(self):
        b, kept = self.base, self.kept
        count = self.sends.shape[0]
        for i in range(4 - count, 4):
            self.s.sent(self.sends.at[i % count], b + i)
        self.s.sent(self.half(kept.at[0], 0), b + 4)
        self.s.sent(self.half(kept.at[2], 1), b + 5)
        self.s.sent(self.half(kept.at[1], 0), b + 6)
        self.s.sent(self.half(kept.at[0], 1), b + 7)
        self.s.sent(self.half(kept.at[2], 0), b + 8)
        self.s.sent(self.half(kept.at[1], 1), b + 9)


class LineSum:
    def __init__(self, sender, local, part, sends, land, base):
        self.s, self.part, self.sends = sender, part, sends
        self.land, self.base = land, base
        self.rows = sends.shape[1]
        self.sem, self.first = local.sem, local.next
        local.next += 7

    def rows_of(self, t):
        return self.part.at[pl.ds(pl.multiple_of(t * self.rows, 16), self.rows)]

    def fetch(self, holds, slot, at):
        return pltpu.make_async_copy(self.rows_of(holds), self.sends.at[slot], self.sem.at[self.first + at])

    def begin(self):
        for s in (1, 2, 3):
            for sends, slot, place, holds, _, _ in self.ways(s):
                pl.when(sends)(lambda: self.fetch(holds, slot, place).start())
        self.fetch(self.s.links.z, 3, 6).start()
        self.step(1)

    def add(self, into, at):
        self.s.landed(self.land.at[at], self.base + at)

        def rows(n):
            r = pl.ds(pl.multiple_of(n * 32, 32), 32)
            self.sends[into, r] = (self.sends[into, r].astype(F32) + self.land[at, r].astype(F32)).astype(BF16)

        loop(self.rows // 32, rows)

    def ways(self, s):
        z = self.s.links.z
        right = (z <= s - 1, s - 1 - z, 2 * (s - 1), z + 4 - s, z >= 1, z + 1)
        left = (z >= 4 - s, s - 1, 2 * (s - 1) + 1, z - 4 + s, z <= 2, z - 1)
        return right, left

    def step(self, s):
        for sends, slot, place, holds, received, to in self.ways(s):

            @pl.when(sends)
            def _():
                self.fetch(holds, slot, place).wait()
                if s > 1:
                    pl.when(received)(lambda: self.add(slot, place - 2))
                self.s.start(self.sends.at[slot], self.land.at[place], self.base + place, (self.s.links.d, to))

    def finish(self, write):
        z = self.s.links.z
        self.fetch(z, 3, 6).wait()
        pl.when(z >= 1)(lambda: self.add(3, 4))
        pl.when(z <= 2)(lambda: self.add(3, 5))

        def rows(n):
            r = pl.ds(pl.multiple_of(n * 32, 32), 32)
            write(r, self.sends[3, r].astype(F32))

        loop(self.rows // 32, rows)

    def drain(self):
        for s in (1, 2, 3):
            for sends, slot, place, _, _, _ in self.ways(s):
                pl.when(sends)(functools.partial(self.s.sent, self.sends.at[slot], self.base + place))


def stream(local, count, source, bufs, body):
    first = local.next
    local.next += 2

    def copy(n, slot):
        return pltpu.make_async_copy(source(n), bufs.at[slot], local.sem.at[first + slot])

    copy(0, 0).start()

    def step(n):
        slot = n % 2
        copy(n, slot).wait()

        @pl.when(n + 1 < count)
        def _():
            copy(n + 1, 1 - slot).start()

        body(n, bufs.at[slot])

    loop(count, step)


def turned(ref):
    return jnp.transpose(ref[...].astype(F32)).astype(BF16)


def columns(ref, start, size):
    return ref.at[:, pl.ds(pl.multiple_of(start, 128), size)]


class Feeder:
    def __init__(self, local, source, bufs, block, dests):
        self.source, self.bufs, self.block, self.dests = source, bufs, block, dests
        self.sem, self.first, self.n = local.sem, local.next, 0
        local.next += 2
        self._copy(0).start()

    def _copy(self, n):
        return pltpu.make_async_copy(
            columns(self.source, self.dests[n] * self.block, self.block),
            self.bufs.at[n % 2],
            self.sem.at[self.first + n % 2],
        )

    def __call__(self, dest):
        n = self.n
        self.n += 1
        self._copy(n).wait()
        if n + 1 < len(self.dests):
            self._copy(n + 1).start()
        return self.bufs.at[n % 2]


def order_of(k):
    partner, own = (k.dcxy, k.dcx, k.dcy, k.dc), (k.dxy, k.dx, k.dy, k.d)
    return [partner[0], partner[1], own[0], partner[2], own[1], partner[3], own[2], own[3]]


def row_blocks(pick, left, right):
    width = right.shape[1]

    def compute(dest, add, out):
        left[...] = turned(pick(dest))

        def chunk(n):
            c = pl.ds(pl.multiple_of(n * 256, 256), 256)
            total = dot(left[...], right[:, c])
            if add is not None:
                total = total + add[:, c].astype(F32)
            out[:, c] = total.astype(BF16)

        loop(width // 256, chunk)

    return compute


def column_blocks(left, pick, chunks):
    size = left.shape[0] // chunks

    def compute(dest, add, out):
        picked = pick(dest)

        def chunk(n):
            r = pl.ds(pl.multiple_of(n * size, 16), size)
            total = dot(left[r], picked[...])
            if add is not None:
                total = total + add[r].astype(F32)
            out[r] = total.astype(BF16)

        loop(chunks, chunk)

    return compute


class Chunk:
    def __init__(self, sender, compute, sends, kept, land, base):
        self.s, self.compute, self.sends = sender, compute, sends
        self.kept, self.land, self.base = kept, land, base
        self.half = kept.shape[2] // 2

    def views(self, n):
        kept, land, h = self.kept.at[n], self.land.at[n], self.half
        top, low = pl.ds(0, h), pl.ds(h, h)
        return {
            "x1": (kept.at[pl.ds(0, 2), top], land.at[pl.ds(4, 2), top]),
            "y1": (kept.at[pl.ds(1, 2), low], land.at[pl.ds(4, 2), low]),
            "y2": (kept.at[2, top], land.at[6, top]),
            "x2": (kept.at[0, low], land.at[6, low]),
        }

    def partner(self, n):
        k = self.s.links
        slot = n % self.sends.shape[0]
        if n != slot:
            self.s.sent(self.sends.at[slot], self.base + 5 * (n - self.sends.shape[0]))
        for i, dest in enumerate((k.dcx, k.dcxy, k.dcy, k.dc)):
            self.compute(n, dest, None, self.sends.at[slot, i])
        self.s.start(self.sends.at[slot], self.land.at[n, pl.ds(0, 4)], self.base + 5 * n, (k.dc, k.z))

    def own(self, n):
        k, b, v = self.s.links, self.base + 5 * n, self.views(n)
        self.s.landed(self.land.at[n, pl.ds(0, 4)], b)
        for i, dest in enumerate((k.dx, k.dxy, k.dy, k.d)):
            self.compute(n, dest, self.land.at[n, i], self.kept.at[n, i])
        self.s.start(*v["x1"], b + 1, (k.dx, k.z))
        self.s.start(*v["y1"], b + 2, (k.dy, k.z))

    def add(self, n, i, start, got):
        kept, land = self.kept, self.land

        def rows(m):
            r = pl.ds(pl.multiple_of(start + m * 32, 32), 32)
            kept[n, i, r] = (kept[n, i, r].astype(F32) + land[n, got, r].astype(F32)).astype(BF16)

        loop(self.half // 32, rows)

    def second(self, n):
        k, b, v = self.s.links, self.base + 5 * n, self.views(n)
        self.s.landed(v["x1"][1], b + 1)
        self.add(n, 2, 0, 5)
        self.s.start(*v["y2"], b + 3, (k.dy, k.z))
        self.s.landed(v["y1"][1], b + 2)
        self.add(n, 0, self.half, 4)
        self.s.start(*v["x2"], b + 4, (k.dx, k.z))
        self.add(n, 3, 0, 4)
        self.add(n, 3, self.half, 5)

    def last(self, n):
        b, v = self.base + 5 * n, self.views(n)
        self.s.landed(v["y2"][1], b + 3)
        self.add(n, 3, 0, 6)
        self.s.landed(v["x2"][1], b + 4)
        self.add(n, 3, self.half, 6)

    def drain(self):
        for n in range(self.kept.shape[0]):
            b, v = self.base + 5 * n, self.views(n)
            if n + self.sends.shape[0] >= self.kept.shape[0]:
                self.s.sent(self.sends.at[0], b)
            for at, name in enumerate(("x1", "y1", "y2", "x2")):
                self.s.sent(v[name][0], b + 1 + at)


class Spread4:
    def __init__(self, sender, pick, land, base):
        self.s, self.pick, self.land, self.base = sender, pick, land, base

    def send(self):
        k = self.s.links
        for j in (1, 2, 3):
            to = (k.z + j) % 4
            self.s.start(self.pick(to), self.land.at[j - 1], self.base + j - 1, (k.d, to))

    def landed(self):
        for j in range(3):
            self.s.landed(self.land.at[j], self.base + j)

    def drain(self):
        z = self.s.links.z
        for j in (1, 2, 3):
            self.s.sent(self.pick((z + j) % 4), self.base + j - 1)


def norm_back_rows(rows_ref, at, gain, grad_normed):
    rows = rows_ref[at]
    inv = norm_scale(rows)
    weighted = grad_normed * gain
    scaled = grad_normed * rows * inv
    grad_rows = inv * weighted - rows * (inv * inv * inv) * jnp.mean(weighted * rows, -1, keepdims=True)
    return grad_rows, scaled


def halves(size):
    return (0, size // 2), (size // 2, size // 2)


def add_gain(gain_part, block, row, scaled):
    for b in range(8):
        total = jnp.sum(scaled[:, b * block : (b + 1) * block], 0, keepdims=True)
        gain_part[b % 2, b // 2 % 2 * 2 + b // 4, row : row + 1] += total


def transpose_into(src, dst):
    def part(n):
        c = pl.ds(pl.multiple_of(n * 128, 128), 128)
        dst[c] = jnp.transpose(src[:, c].astype(F32)).astype(BF16)

    loop(src.shape[1] // 128, part)


def row_chunk(ref):
    return lambda n: ref.at[pl.ds(pl.multiple_of(n * 256, 256), 256)]


def attention_back_kernel(
    dn2_ref, mid_ref, g_ref, gain_ref, cos_ref, sin_ref, q_ref, kv_ref, att_ref,
    part_ref, hidden_ref, top_ref, wo_ref,
    gm_out, dqkv, out_ref, gain_part, gd_out, go_out,
    mid_bf, da, dkv, att_t, w_chunk, top_cols, hidden_cols, hidden_t,
    d_sends, d_kept, d_land, o_sends, o_kept, o_land, line_sends, line_land,
    send_sem, recv_sem, local_sem,
):
    rows, width = mid_ref.shape
    block = width // 8
    ff = hidden_t.shape[0]
    links = Links()
    s = Sender(links, send_sem, recv_sem)
    local = Local(local_sem)
    top_feed = Feeder(local, top_ref, top_cols, block, order_of(links))
    links.barrier()
    line = LineSum(s, local, part_ref, line_sends, line_land, 20)
    line.begin()

    def turn_hidden(n, buf):
        hidden_t[pl.ds(pl.multiple_of(n * 128, 128), 128)] = turned(buf)

    stream(local, ff // 128, lambda n: columns(hidden_ref, n * 128, 128), hidden_cols, turn_hidden)
    grad_d = Reduce(s, column_blocks(hidden_t, top_feed, 4), 0, d_sends, d_kept, d_land, halves(ff))
    grad_d.first()
    line.step(2)

    gain_part[...] = jnp.zeros_like(gain_part)
    dkv[...] = jnp.zeros_like(dkv)
    step = 32

    def middle(n):
        r = pl.ds(pl.multiple_of(n * step, step), step)
        grad_rows, scaled = norm_back_rows(mid_ref, r, gain_ref[1:2], dn2_ref[r])
        grad = g_ref[r] + grad_rows
        gm_out[r] = grad
        mid_bf[r] = grad.astype(BF16)
        add_gain(gain_part, block, 1, scaled)

    loop(rows // step, middle)
    transpose_into(att_ref, att_t)
    pick_mid = lambda dest: columns(mid_bf, dest * block, block)
    grad_o = Reduce(s, column_blocks(att_t, pick_mid, 4), 10, o_sends, o_kept, o_land, halves(width))
    grad_o.first()
    grad_d.second()

    def attended(n, buf):
        da[:, pl.ds(pl.multiple_of(n * 256, 256), 256)] = dot_nt(mid_bf[...], buf[...]).astype(BF16)

    stream(local, width // 256, row_chunk(wo_ref), w_chunk, attended)
    line.step(3)

    def group_step(n):
        def sequence(i):
            at = pl.ds(pl.multiple_of(i * SEQ, SEQ), SEQ)
            attend_back_group(cos_ref[at], sin_ref[at], n, q_ref, kv_ref, da, dqkv, dkv, at)

        loop(rows // SEQ, sequence)
        pl.when(n == 1)(grad_o.second)
        pl.when(n == 2)(grad_d.last)

    loop(KV, group_step)
    to_down = local.start(d_kept.at[3], gd_out)

    def key_value(i):
        at = pl.ds(pl.multiple_of(i * SEQ, SEQ), SEQ)
        first, _ = lane_masks()
        for tile in range(KV // 2):
            c = tile * LANES
            u = dkv[at, c : c + LANES]
            dqkv[at, width + c : width + c + LANES] = (
                u * cos_ref[at] - swap_halves(u, first) * sin_ref[at]
            ).astype(BF16)
        dqkv[at, width + KV * HD :] = dkv[at, KV * HD :].astype(BF16)

    loop(rows // SEQ, key_value)
    grad_o.last()
    to_out = local.start(o_kept.at[3], go_out)

    def write(r, total):
        out_ref[r] = mid_ref[r] + total

    line.finish(write)
    to_down.wait()
    to_out.wait()
    grad_o.drain()
    grad_d.drain()
    line.drain()


def attention_back(dn2, mid, g, gains, cos, sin, query, key_val, attended, part, hidden, top, wo):
    rows, width = mid.shape
    block, ff = width // 8, hidden.shape[1]
    kv_width = 2 * KV * HD
    vmem = pl.BlockSpec(memory_space=pltpu.VMEM)
    hbm = pl.BlockSpec(memory_space=pltpu.HBM)
    shape = jax.ShapeDtypeStruct
    return pl.pallas_call(
        attention_back_kernel,
        in_specs=[vmem] * 9 + [hbm] * 4,
        out_specs=[vmem] * 4 + [hbm] * 2,
        out_shape=[
            shape((rows, width), F32),
            shape((rows, width + kv_width), BF16),
            shape((rows, width), F32),
            shape((2, 4, 8, block), F32),
            shape((ff, block), BF16),
            shape((width, block), BF16),
        ],
        scratch_shapes=[
            pltpu.VMEM((rows, width), BF16),
            pltpu.VMEM((rows, width), BF16),
            pltpu.VMEM((rows, kv_width), F32),
            pltpu.VMEM((width, rows), BF16),
            pltpu.VMEM((2, 256, width), BF16),
            pltpu.VMEM((2, 4 * rows, block), BF16),
            pltpu.VMEM((2, 4 * rows, 128), BF16),
            pltpu.VMEM((ff, 4 * rows), BF16),
            pltpu.VMEM((2, ff, block), BF16),
            pltpu.VMEM((4, ff, block), BF16),
            pltpu.VMEM((7, ff, block), BF16),
            pltpu.VMEM((2, width, block), BF16),
            pltpu.VMEM((4, width, block), BF16),
            pltpu.VMEM((7, width, block), BF16),
            pltpu.VMEM((4, rows, width), BF16),
            pltpu.VMEM((6, rows, width), BF16),
            pltpu.SemaphoreType.DMA((26,)),
            pltpu.SemaphoreType.DMA((26,)),
            pltpu.SemaphoreType.DMA((20,)),
        ],
        compiler_params=pltpu.CompilerParams(
            collective_id=1, has_side_effects=True, vmem_limit_bytes=65000 * 1024
        ),
        name="attention_back",
    )(dn2, mid, g, gains, cos, sin, query, key_val, attended, part, hidden, top, wo)


def project_back_kernel(
    x_ref, gain_ref, dqkv, gain_in, gm_ref, n2_ref, dgu_ref, wqkv_ref, go_in,
    grad_in_out, gq_out, gkv_out, go_out, gain_out, ggu_out,
    dn1, n1, n1_t, w_chunk, dgu, n2_cols, left, sends, kept, land,
    row_sends, row_kept, row_land, o_block, gain_part, gain_land, z_q, z_kv, z_o,
    send_sem, recv_sem, local_sem,
):
    rows, width = x_ref.shape
    block, slot = width // 8, width // 4
    kv_width = 2 * KV * HD
    step = 32
    links = Links()
    d, z = links.d, links.z
    s = Sender(links, send_sem, recv_sem)
    local = Local(local_sem)
    n2_feed = Feeder(local, n2_ref, n2_cols, block, order_of(links))
    fetch_dgu = local.start(dgu_ref, dgu)
    fetch_o = local.start(go_in, o_block)
    fetch_gm = local.start(gm_ref, grad_in_out)
    links.barrier(far=True)
    fetch_o.wait()
    send_o = Spread4(s, lambda p: o_block.at[pl.ds(pl.multiple_of(p * slot, 16), slot)], z_o, 35)
    send_o.send()
    gain_part[...] = gain_in[...]

    def normed(n):
        r = pl.ds(pl.multiple_of(n * step, step), step)
        rows_x = x_ref[r]
        n1[r] = (rows_x * norm_scale(rows_x) * gain_ref[0:1]).astype(BF16)

    loop(rows // step, normed)
    transpose_into(n1, n1_t)

    group_of = lambda n: (z + n) % 4

    def row_compute(n, dest, add, out):
        picked = n1_t[pl.ds(pl.multiple_of(dest * block, block), block)]
        start = width if n == 0 else group_of(n) * slot
        for c in range(0, slot, 256):
            total = dot(picked, dqkv[:, pl.ds(pl.multiple_of(start + c, 256), 256)])
            if add is not None:
                total = total + add[:, c : c + 256].astype(F32)
            out[:, c : c + 256] = total.astype(BF16)

    row = Chunk(s, row_compute, row_sends, row_kept, row_land, 10)
    row.partner(0)
    for n in range(4):
        row.partner(n + 1)
        row.own(n)
    row.own(4)

    send_kv = Spread4(
        s, lambda p: row_kept.at[0, 3, pl.ds(pl.multiple_of(p * KV_ROWS, 16), KV_ROWS)], z_kv, 38
    )

    def final_q(n):
        row.last(n)
        s.start(row_kept.at[n, 3], z_q.at[n - 1], 40 + n, (d, group_of(n)))

    fetch_dgu.wait()
    grads = Reduce(s, row_blocks(n2_feed, left, dgu), 0, sends, kept, land, halves(block))
    grads.partner(0)
    row.second(0)
    grads.partner(1)
    row.second(1)
    row.second(2)
    grads.own(0)
    row.second(3)
    row.second(4)
    grads.partner(2)
    row.last(0)
    send_kv.send()
    final_q(1)
    grads.own(1)
    final_q(2)
    grads.partner(3)
    final_q(3)
    grads.own(2)
    row.last(4)
    grads.own(3)
    grads.second()

    def projected(n, buf):
        dn1[:, pl.ds(pl.multiple_of(n * 256, 256), 256)] = dot_nt(dqkv[...], buf[...])

    stream(local, width // 256, row_chunk(wqkv_ref), w_chunk, projected)
    fetch_gm.wait()

    def inward(n):
        r = pl.ds(pl.multiple_of(n * step, step), step)
        grad_rows, scaled = norm_back_rows(x_ref, r, gain_ref[0:1], dn1[r])
        grad_in_out[r] += grad_rows
        add_gain(gain_part, block, 0, scaled)

    loop(rows // step, inward)
    core, x_at, y_at = d % 2, d // 2 % 2, d // 4
    s.start(gain_part.at[1 - core], gain_land.at[pl.ds(0, 4)], 44, (links.dc, z))
    s.landed(gain_land.at[pl.ds(0, 4)], 44)
    gain_part[core] += gain_land[0:4]
    other_x = pl.multiple_of(2 - 2 * x_at, 2)
    s.start(gain_part.at[core, pl.ds(other_x, 2)], gain_land.at[pl.ds(4, 2)], 45, (links.dx, z))
    send_o.landed()

    def out_rows(n):
        r = pl.ds(pl.multiple_of(n * 16, 16), 16)
        mine = pl.ds(pl.multiple_of(z * slot + n * 16, 16), 16)
        go_out[r] = (
            o_block[mine].astype(F32) + z_o[0, r].astype(F32) + z_o[1, r].astype(F32) + z_o[2, r].astype(F32)
        )

    loop(slot // 16, out_rows)
    for n in range(3):
        s.landed(z_q.at[n], 41 + n)

    def query_rows(n):
        r = pl.ds(pl.multiple_of(n * 16, 16), 16)
        gq_out[r] = (
            row_kept[4, 3, r].astype(F32) + z_q[0, r].astype(F32) + z_q[1, r].astype(F32) + z_q[2, r].astype(F32)
        )

    loop(block // 16, query_rows)
    send_kv.landed()
    mine_kv = pl.ds(pl.multiple_of(z * KV_ROWS, 16), KV_ROWS)
    gkv_out[...] = row_kept[0, 3, mine_kv].astype(F32) + (
        z_kv[0].astype(F32) + z_kv[1].astype(F32) + z_kv[2].astype(F32)
    )
    s.landed(gain_land.at[pl.ds(4, 2)], 45)
    mine_x = 2 * x_at
    gain_part[core, pl.ds(mine_x, 2)] += gain_land[4:6]
    s.start(gain_part.at[core, mine_x + 1 - y_at], gain_land.at[6], 46, (links.dy, z))
    s.landed(gain_land.at[6], 46)
    gain_part[core, mine_x + y_at] += gain_land[6]
    send_g = Spread4(s, lambda p: gain_part.at[core, mine_x + y_at], gain_land.at[pl.ds(7, 3)], 47)
    send_g.send()
    grads.last()
    to_gu = local.start(kept.at[3], ggu_out)
    send_g.landed()
    gain_out[...] = gain_part[core, mine_x + y_at] + gain_land[7] + gain_land[8] + gain_land[9]
    to_gu.wait()
    for unit in (grads, row, send_o, send_kv, send_g):
        unit.drain()
    for n in range(3):
        s.sent(row_kept.at[n + 1, 3], 41 + n)
    s.sent(gain_part.at[1 - core], 44)
    s.sent(gain_part.at[core, pl.ds(other_x, 2)], 45)
    s.sent(gain_part.at[core, mine_x + 1 - y_at], 46)


def project_back(x, gains, dqkv, gain_in, gm, n2, dgu, wqkv, grad_o):
    rows, width = x.shape
    block, slot = width // 8, width // 4
    kv_width = 2 * KV * HD
    wide = dgu.shape[1]
    vmem = pl.BlockSpec(memory_space=pltpu.VMEM)
    hbm = pl.BlockSpec(memory_space=pltpu.HBM)
    shape = jax.ShapeDtypeStruct
    return pl.pallas_call(
        project_back_kernel,
        in_specs=[vmem] * 4 + [hbm] * 5,
        out_specs=[vmem] * 5 + [hbm],
        out_shape=[
            shape((rows, width), F32),
            shape((block, slot), F32),
            shape((KV_ROWS, kv_width), F32),
            shape((slot, block), F32),
            shape((8, block), F32),
            shape((block, wide), BF16),
        ],
        scratch_shapes=[
            pltpu.VMEM((rows, width), F32),
            pltpu.VMEM((rows, width), BF16),
            pltpu.VMEM((width, rows), BF16),
            pltpu.VMEM((2, 256, width + kv_width), BF16),
            pltpu.VMEM((4 * rows, wide), BF16),
            pltpu.VMEM((2, 4 * rows, block), BF16),
            pltpu.VMEM((block, 4 * rows), BF16),
            pltpu.VMEM((2, block, wide), BF16),
            pltpu.VMEM((4, block, wide), BF16),
            pltpu.VMEM((7, block, wide), BF16),
            pltpu.VMEM((3, 4, block, slot), BF16),
            pltpu.VMEM((5, 4, block, slot), BF16),
            pltpu.VMEM((5, 7, block, slot), BF16),
            pltpu.VMEM((width, block), BF16),
            pltpu.VMEM((2, 4, 8, block), F32),
            pltpu.VMEM((10, 8, block), F32),
            pltpu.VMEM((3, block, slot), BF16),
            pltpu.VMEM((3, KV_ROWS, kv_width), BF16),
            pltpu.VMEM((3, slot, block), BF16),
            pltpu.SemaphoreType.DMA((50,)),
            pltpu.SemaphoreType.DMA((50,)),
            pltpu.SemaphoreType.DMA((20,)),
        ],
        compiler_params=pltpu.CompilerParams(
            collective_id=2, has_side_effects=True, vmem_limit_bytes=65000 * 1024
        ),
        name="project_back",
    )(x, gains, dqkv, gain_in, gm, n2, dgu, wqkv, grad_o)


def plain_forward(x, g, cos, sin, w_query, w_kv, gains, w_out, w_gu, w_down):
    both = ("dp", "tensor")
    gather = lax.all_gather

    def whole(shard, dims):
        for dim, axis in dims:
            shard = gather(shard, axis, axis=dim, tiled=True)
        return shard

    wq = whole(w_query, ((1, "tensor"), (0, "dp")))
    wqkv = jnp.concatenate([wq, whole(w_kv, ((0, both),))], 1)
    gain = whole(gains, ((1, both),)).astype(F32)
    wo = whole(w_out, ((0, "tensor"), (1, "dp")))
    wgu = whole(w_gu, ((0, "dp"),))
    wd = whole(w_down, ((1, "dp"),))
    normed = (x * norm_scale(x) * gain[0]).astype(BF16)
    query, key_val, attended = attend(cos, sin, dot(normed, wqkv))
    middle = x + dot(attended, wo)
    normed_two = (middle * norm_scale(middle) * gain[1]).astype(BF16)
    n2 = gather(normed_two, "tensor", axis=0, tiled=True)
    top = gather(g.astype(BF16), "tensor", axis=0, tiled=True)
    return wqkv, gain, wo, wgu, wd, n2, top, query, key_val, attended, middle


def plain_backward(
    dn2_part, out_part, n2, grad_gu_pre, hidden, top,
    middle, x, g, gains, cos, sin, query, key_val, attended, wo, wqkv,
):
    width = x.shape[1]

    def scatter(part, axis, dim):
        return lax.psum_scatter(part.astype(BF16), axis, scatter_dimension=dim, tiled=True).astype(F32)

    output = middle + scatter(out_part, "tensor", 0)
    grad_mid_norm, gain_two = norm_back(middle, gains[1], scatter(dn2_part, "tensor", 0))
    grad_middle = g + grad_mid_norm
    mid_bf = grad_middle.astype(BF16)
    grad_qkv_rows = attend_back(cos, sin, query, key_val, dot_nt(mid_bf, wo).astype(BF16))
    grad_in_norm, gain_one = norm_back(x, gains[0], dot_nt(grad_qkv_rows, wqkv))
    normed_one = (x * norm_scale(x) * gains[0]).astype(BF16)
    grad_qkv = scatter(dot_tn(normed_one, grad_qkv_rows), "dp", 0)
    gain_parts = lax.psum_scatter(jnp.stack([gain_one, gain_two]), "dp", scatter_dimension=1, tiled=True)
    return (
        output,
        grad_middle + grad_in_norm,
        lax.psum_scatter(gain_parts, "tensor", scatter_dimension=1, tiled=True),
        scatter(grad_qkv[:, :width], "tensor", 1),
        scatter(grad_qkv[:, width:], "tensor", 0),
        scatter(scatter(dot_tn(attended, mid_bf), "dp", 1), "tensor", 0),
        scatter(dot_tn(n2, grad_gu_pre), "dp", 0),
        scatter(dot_tn(hidden, top), "dp", 1),
    )


def linked_layer(x, g, cos, sin, w_query, w_key, w_value, gains, w_out, w_gate, w_up, w_down):
    padded = jnp.pad(gains, ((0, GAIN_ROWS - 2), (0, LANES - gains.shape[1])))
    outs = forward_stage(x, g, cos, sin, w_query, w_key, w_value, padded, w_out, w_gate, w_up, w_down)
    wo, n2, top, wqkv, hidden, dgu, out_part = (outs[i] for i in (1, 4, 5, 6, 7, 8, 9))
    query, key_val, attended, middle, gain, dn2 = outs[11:]
    grad_middle, grad_qkv, output, gain_part, grad_down, grad_o = attention_back(
        dn2, middle, g, gain, cos, sin, query, key_val, attended, out_part, hidden, top, wo
    )
    grad_in, grad_query, grad_kv, grad_out, gain_sum, grad_gu = project_back(
        x, gain, grad_qkv, gain_part, grad_middle, n2, dgu, wqkv, grad_o
    )
    own = gain_sum.shape[1] // 4
    grad_gains = lax.dynamic_slice(gain_sum, (0, lax.axis_index("tensor") * own), (2, own))
    return output, grad_in, grad_gains, grad_query, grad_kv, grad_out, grad_gu.astype(F32), grad_down.astype(F32)


def plain_layer(x, g, cos, sin, w_query, w_key, w_value, gains, w_out, w_gate, w_up, w_down):
    w_kv = jnp.concatenate([w_key, w_value], 1)
    w_gu = jnp.concatenate([w_gate, w_up], 1)
    wqkv, gains, wo, wgu, wd, n2, top, query, key_val, attended, middle = plain_forward(
        x, g, cos, sin, w_query, w_kv, gains, w_out, w_gu, w_down
    )
    ff = wd.shape[0]
    gate_up = dot(n2, wgu)
    gate_pre, up_pre = gate_up[:, :ff], gate_up[:, ff:]
    sig = jax.nn.sigmoid(gate_pre)
    hidden = (gate_pre * sig * up_pre).astype(BF16)
    grad_hidden = dot_nt(top, wd)
    grad_gate_pre = (grad_hidden * up_pre * sig * (1.0 + gate_pre * (1.0 - sig))).astype(BF16)
    grad_up_pre = (grad_hidden * gate_pre * sig).astype(BF16)
    grad_gu_pre = jnp.concatenate([grad_gate_pre, grad_up_pre], 1)
    return plain_backward(
        dot_nt(grad_gu_pre, wgu).astype(BF16), dot(hidden, wd).astype(BF16), n2, grad_gu_pre, hidden, top,
        middle, x, g, gains, cos, sin, query, key_val, attended, wo, wqkv,
    )


def on_device(
    linked,
    hidden_in, positions, norm_gains, w_query, w_key, w_value, w_out, w_gate, w_up, w_down, out_grad,
):
    x, g = hidden_in, out_grad
    rows, width = x.shape
    ff = w_gate.shape[2]
    kv_width = 2 * KV * HD
    z = lax.axis_index("tensor")

    cos, sin = rope_tables(lax.dynamic_slice_in_dim(positions, z * rows, rows))
    layer = linked_layer if linked else plain_layer
    output, grad_in, grad_gains, grad_query, grad_kv, grad_out, grad_gu, grad_down = layer(
        x, g, cos, sin,
        w_query[0], w_key[0], w_value[0], norm_gains[0], w_out[0], w_gate[0], w_up[0], w_down[0],
    )

    return (
        output,
        grad_in,
        grad_gains[None],
        grad_query[None],
        grad_kv[None, :, : KV * HD],
        grad_kv[None, :, KV * HD :],
        grad_out[None],
        grad_gu[None, :, :ff],
        grad_gu[None, :, ff:],
        grad_down[None],
    )


def solution(mesh):
    nd, nt = mesh.shape["dp"], mesh.shape["tensor"]
    rows = P(("dp", "tensor"), None)
    wide = P(None, "dp", "tensor")
    tall = P(None, "tensor", "dp")
    flat = P(None, ("dp", "tensor"), None)
    gain = P(None, None, ("dp", "tensor"))
    return jax.shard_map(
        functools.partial(on_device, (nd, nt) == (8, 4)),
        mesh=mesh,
        in_specs=(rows, P("dp"), gain, wide, flat, flat, tall, wide, wide, tall, rows),
        out_specs=(rows, rows, gain, wide, flat, flat, tall, wide, wide, tall),
        check_vma=False,
    )
```

```python
import functools

import jax
import jax.numpy as jnp
from jax import lax
from jax.experimental import pallas as pl
from jax.experimental.pallas import tpu as pltpu
from jax.sharding import PartitionSpec as P

H = 32
KV = 4
HD = 64
SEQ = 128
NORM_EPS = 1e-05
NEG_BIG = -1e30
SCALE = HD ** (-0.5)
LANES = 128
F32 = jnp.float32
BF16 = jnp.bfloat16


def dot(a, b):
    return jnp.dot(a, b, preferred_element_type=F32)


def dot_nt(a, b):
    return lax.dot_general(a, b, (((1,), (1,)), ((), ())), preferred_element_type=F32)


def dot_tn(a, b):
    return lax.dot_general(a, b, (((0,), (0,)), ((), ())), preferred_element_type=F32)


def lane_masks():
    lane = lax.broadcasted_iota(jnp.int32, (SEQ, LANES), 1)
    return lane % HD < HD // 2, lane < HD


def swap_halves(u, first):
    return jnp.where(first, pltpu.roll(u, LANES - HD // 2, 1), pltpu.roll(u, HD // 2, 1))


def twice(tile, index, low):
    turned = pltpu.roll(tile, HD, 1)
    return jnp.where(low, tile, turned) if index % 2 == 0 else jnp.where(low, turned, tile)


def causal_probs(query, key):
    scores = dot_nt(query, key) * SCALE
    rows = lax.broadcasted_iota(jnp.int32, scores.shape, 0)
    cols = lax.broadcasted_iota(jnp.int32, scores.shape, 1)
    scores = jnp.where(cols <= rows, scores, NEG_BIG)
    weights = jnp.exp(scores - jnp.max(scores, -1, keepdims=True))
    return weights * (1.0 / jnp.sum(weights, -1, keepdims=True))


def attend_sequence(cos, sin, load, kv_at, q_out, kv_out, o_out, at):
    first, low = lane_masks()

    def turn(u):
        return u * cos + swap_halves(u, first) * sin

    keys, vals_low, vals_high = [], [], []
    for tile in range(KV // 2):
        key = turn(load(kv_at + tile * LANES))
        val = load(kv_at + KV * HD + tile * LANES)
        kv_out[at, tile * LANES : (tile + 1) * LANES] = key.astype(BF16)
        kv_out[at, KV * HD + tile * LANES : KV * HD + (tile + 1) * LANES] = val.astype(BF16)
        for index in (0, 1):
            keys.append(twice(key, index, low).astype(BF16))
            both = twice(val, index, low)
            vals_low.append(jnp.where(low, both, 0.0).astype(BF16))
            vals_high.append(jnp.where(low, 0.0, both).astype(BF16))
    for pair in range(H // 2):
        group = pair * LANES // (H // KV * HD)
        query = turn(load(pair * LANES))
        p_low = causal_probs(jnp.where(low, query, 0.0).astype(BF16), keys[group])
        p_high = causal_probs(jnp.where(low, 0.0, query).astype(BF16), keys[group])
        q_out[at, pair * LANES : (pair + 1) * LANES] = query.astype(BF16)
        o_out[at, pair * LANES : (pair + 1) * LANES] = (
            dot(p_low.astype(BF16), vals_low[group]) + dot(p_high.astype(BF16), vals_high[group])
        ).astype(BF16)


def attend_back_sequence(cos, sin, q_ref, kv_ref, da_ref, dqkv_out, at):
    first, low = lane_masks()

    def turn_back(u):
        return (u * cos - swap_halves(u, first) * sin).astype(BF16)

    pair_total = H // KV * HD // LANES
    width = H * HD
    held = {}
    for group in range(KV):
        tile_at = group // 2 * LANES
        key = twice(kv_ref[at, tile_at : tile_at + LANES].astype(F32), group, low)
        val_at = KV * HD + tile_at
        val = twice(kv_ref[at, val_at : val_at + LANES].astype(F32), group, low).astype(BF16)
        key_low = jnp.where(low, key, 0.0).astype(BF16)
        key_high = jnp.where(low, 0.0, key).astype(BF16)
        key = key.astype(BF16)
        dk = jnp.zeros((SEQ, LANES), F32)
        dv = jnp.zeros((SEQ, LANES), F32)
        for pair in range(group * pair_total, (group + 1) * pair_total):
            query = q_ref[at, pair * LANES : (pair + 1) * LANES].astype(F32)
            grad = da_ref[at, pair * LANES : (pair + 1) * LANES].astype(F32)
            dq = None
            for is_low in (True, False):
                if is_low:
                    query_h = jnp.where(low, query, 0.0).astype(BF16)
                    grad_h = jnp.where(low, grad, 0.0).astype(BF16)
                else:
                    query_h = jnp.where(low, 0.0, query).astype(BF16)
                    grad_h = jnp.where(low, 0.0, grad).astype(BF16)
                prob = causal_probs(query_h, key)
                grad_prob = dot_nt(grad_h, val)
                delta = jnp.sum(prob * grad_prob, -1, keepdims=True)
                ds = (prob * (grad_prob - delta) * SCALE).astype(BF16)
                term = dot(ds, key_low if is_low else key_high)
                dq = term if dq is None else dq + term
                dk = dk + dot_tn(ds, query_h)
                dv = dv + dot_tn(prob.astype(BF16), grad_h)
            dqkv_out[at, pair * LANES : (pair + 1) * LANES] = turn_back(dq)
        held[group] = (dk + pltpu.roll(dk, HD, 1), dv + pltpu.roll(dv, HD, 1))
    for tile in range(KV // 2):
        col = width + tile * LANES
        dk = jnp.where(low, held[2 * tile][0], held[2 * tile + 1][0])
        dv = jnp.where(low, held[2 * tile][1], held[2 * tile + 1][1])
        dqkv_out[at, col : col + LANES] = turn_back(dk)
        dqkv_out[at, col + KV * HD : col + KV * HD + LANES] = dv.astype(BF16)


def causal_probs_turned(key, query):
    scores = dot_nt(key, query) * SCALE
    rows = lax.broadcasted_iota(jnp.int32, scores.shape, 0)
    cols = lax.broadcasted_iota(jnp.int32, scores.shape, 1)
    scores = jnp.where(rows <= cols, scores, NEG_BIG)
    weights = jnp.exp(scores - jnp.max(scores, 0, keepdims=True))
    return weights * (1.0 / jnp.sum(weights, 0, keepdims=True))


def attend_back_group(cos, sin, group, q_ref, kv_ref, da_ref, dqkv_out, dkv_out, at):
    first, low = lane_masks()
    head_width = H // KV * HD
    mine = low == (group % 2 == 0)

    def both(tile):
        kept = jnp.where(mine, tile.astype(F32), 0.0)
        return kept + pltpu.roll(kept, HD, 1)

    tile = pl.ds(pl.multiple_of(group // 2 * LANES, LANES), LANES)
    val_tile = pl.ds(pl.multiple_of(KV * HD + group // 2 * LANES, LANES), LANES)
    key = both(kv_ref[at, tile])
    val = both(kv_ref[at, val_tile]).astype(BF16)
    key_low = jnp.where(low, key, 0.0).astype(BF16)
    key_high = jnp.where(low, 0.0, key).astype(BF16)
    key = key.astype(BF16)
    dk = jnp.zeros((SEQ, LANES), F32)
    dv = jnp.zeros((SEQ, LANES), F32)
    for pair in range(head_width // LANES):
        c = pl.ds(pl.multiple_of(group * head_width + pair * LANES, LANES), LANES)
        query = q_ref[at, c].astype(F32)
        grad = da_ref[at, c].astype(F32)
        dq = None
        for is_low in (True, False):
            pick = low if is_low else jnp.logical_not(low)
            query_h = jnp.where(pick, query, 0.0).astype(BF16)
            grad_h = jnp.where(pick, grad, 0.0).astype(BF16)
            prob = causal_probs_turned(key, query_h)
            grad_prob = dot_nt(val, grad_h)
            delta = jnp.sum(prob * grad_prob, 0, keepdims=True)
            ds = (prob * (grad_prob - delta) * SCALE).astype(BF16)
            term = dot_tn(ds, key_low if is_low else key_high)
            dq = term if dq is None else dq + term
            dk = dk + dot(ds, query_h)
            dv = dv + dot(prob.astype(BF16), grad_h)
        dqkv_out[at, c] = (dq * cos - swap_halves(dq, first) * sin).astype(BF16)
    dkv_out[at, tile] += jnp.where(mine, dk + pltpu.roll(dk, HD, 1), 0.0)
    dkv_out[at, val_tile] += jnp.where(mine, dv + pltpu.roll(dv, HD, 1), 0.0)


def attend_kernel(cos_ref, sin_ref, qkv_ref, q_out, kv_out, o_out):
    attend_sequence(
        cos_ref[...], sin_ref[...], lambda c: qkv_ref[:, c : c + LANES], H * HD, q_out, kv_out, o_out, slice(None)
    )


def attend_back_kernel(cos_ref, sin_ref, q_ref, kv_ref, da_ref, dqkv_out):
    attend_back_sequence(cos_ref[...], sin_ref[...], q_ref, kv_ref, da_ref, dqkv_out, slice(None))


def by_sequence(body, name, ins, widths):
    rows = ins[0].shape[0]
    spec = lambda w: pl.BlockSpec((SEQ, w), lambda i: (i, 0))
    return pl.pallas_call(
        body,
        grid=(rows // SEQ,),
        in_specs=[spec(a.shape[1]) for a in ins],
        out_specs=[spec(w) for w in widths],
        out_shape=[jax.ShapeDtypeStruct((rows, w), BF16) for w in widths],
        name=name,
    )(*ins)


def attend(cos, sin, qkv):
    return by_sequence(attend_kernel, "attend", (cos, sin, qkv), (H * HD, 2 * KV * HD, H * HD))


def attend_back(cos, sin, query, key_val, grad):
    return by_sequence(
        attend_back_kernel, "attend_back", (cos, sin, query, key_val, grad), (H * HD + 2 * KV * HD,)
    )[0]


def norm_scale(rows):
    return lax.rsqrt(jnp.mean(rows * rows, -1, keepdims=True) + NORM_EPS)


def norm_back(rows, gain, grad_normed):
    inv = norm_scale(rows)
    weighted = grad_normed * gain
    grad_gain = jnp.sum(grad_normed * rows * inv, 0)
    grad_rows = inv * weighted - rows * inv**3 * jnp.mean(weighted * rows, -1, keepdims=True)
    return grad_rows, grad_gain


def rope_tables(positions):
    half = jnp.arange(LANES, dtype=jnp.int32) % (HD // 2)
    inv_freq = 10000.0 ** (-(half.astype(F32) * 2.0 / HD))
    angles = positions.astype(F32)[:, None] * inv_freq[None, :]
    sign = jnp.where(jnp.arange(LANES) % HD < HD // 2, -1.0, 1.0).astype(F32)
    return jnp.cos(angles), jnp.sin(angles) * sign[None, :]


MESH = pl.DeviceIdType.MESH
KV_ROWS = 64
GAIN_ROWS = 16


class Links:
    def __init__(self):
        self.d, self.z = lax.axis_index("dp"), lax.axis_index("tensor")
        core, x, y = self.d % 2, self.d // 2 % 2, self.d // 4
        self.dc = self.d + 1 - 2 * core
        step_x, step_y = 2 - 4 * x, 4 - 8 * y
        self.dx, self.dy, self.dxy = self.d + step_x, self.d + step_y, self.d + step_x + step_y
        self.dcx, self.dcy, self.dcxy = self.dc + step_x, self.dc + step_y, self.dc + step_x + step_y

    def barrier(self, far=False):
        z = self.z
        sem = pltpu.get_barrier_semaphore()

        def greet(d, zz):
            pl.semaphore_signal(sem, inc=1, device_id=(d, zz), device_id_type=MESH)

        for d in (self.dx, self.dy, self.dc):
            greet(d, z)
        if far:
            for j in (1, 2, 3):
                greet(self.d, (z + j) % 4)
            pl.semaphore_wait(sem, 6)
            return
        pl.when(z > 0)(lambda: greet(self.d, z - 1))
        pl.when(z < 3)(lambda: greet(self.d, z + 1))
        pl.semaphore_wait(sem, 3 + (z + 2) // 3 + (5 - z) // 3)


class Sender:
    def __init__(self, links, send_sem, recv_sem):
        self.links, self.send_sem, self.recv_sem = links, send_sem, recv_sem

    def copy(self, src, dst, at, to):
        return pltpu.make_async_remote_copy(
            src_ref=src,
            dst_ref=dst,
            send_sem=self.send_sem.at[at],
            recv_sem=self.recv_sem.at[at],
            device_id=to,
            device_id_type=MESH,
        )

    def start(self, src, dst, at, to):
        self.copy(src, dst, at, to).start()

    def landed(self, region, at):
        self.copy(region, region, at, (self.links.dc, self.links.z)).wait_recv()

    def sent(self, region, at):
        self.copy(region, region, at, (self.links.dc, self.links.z)).wait_send()


class Spread:
    def __init__(self, sender, region, base):
        self.s, self.region, self.base = sender, region, base

    def own(self, p, src):
        k, r, b = self.s.links, self.region, self.base + 9 * p
        mine = r(k.d, p, None)
        self.s.start(src, mine, b, (k.dx, k.z))
        self.s.start(src, mine, b + 1, (k.dy, k.z))
        self.s.start(src, mine, b + 2, (k.dc, k.z))

    def near(self, p):
        k, r, b = self.s.links, self.region, self.base + 9 * p
        self.s.landed(r(k.dx, p, None), b)
        self.s.start(r(k.dx, p, 0), r(k.dx, p, 0), b + 3, (k.dy, k.z))
        self.s.start(r(k.dx, p, None), r(k.dx, p, None), b + 5, (k.dc, k.z))
        self.s.landed(r(k.dy, p, None), b + 1)
        self.s.start(r(k.dy, p, 1), r(k.dy, p, 1), b + 4, (k.dx, k.z))
        self.s.start(r(k.dy, p, None), r(k.dy, p, None), b + 6, (k.dc, k.z))

    def far(self, p):
        k, r, b = self.s.links, self.region, self.base + 9 * p
        for part in (0, 1):
            self.s.landed(r(k.dxy, p, part), b + 3 + part)
            self.s.start(r(k.dxy, p, part), r(k.dxy, p, part), b + 7 + part, (k.dc, k.z))

    def finish(self, p):
        k, r, b = self.s.links, self.region, self.base + 9 * p
        self.s.landed(r(k.dc, p, None), b + 2)
        self.s.landed(r(k.dcx, p, None), b + 5)
        self.s.landed(r(k.dcy, p, None), b + 6)
        for part in (0, 1):
            self.s.landed(r(k.dcxy, p, part), b + 7 + part)

    def drain(self, p):
        k, r, b = self.s.links, self.region, self.base + 9 * p
        for i in (0, 1, 2):
            self.s.sent(r(k.d, p, None), b + i)
        self.s.sent(r(k.dx, p, 0), b + 3)
        self.s.sent(r(k.dy, p, 1), b + 4)
        self.s.sent(r(k.dx, p, None), b + 5)
        self.s.sent(r(k.dy, p, None), b + 6)
        for part in (0, 1):
            self.s.sent(r(k.dxy, p, part), b + 7 + part)


class Line:
    def __init__(self, sender, region, base):
        self.s, self.region, self.base = sender, region, base

    def _send(self, src, p, way, step):
        k = self.s.links
        self.s.start(src, self.region(p), self.base + 2 * (step - 1) + way, (k.d, k.z + 1 - 2 * way))

    def own(self, src):
        z = self.s.links.z
        pl.when(z < 3)(lambda: self._send(src, z, 0, 1))
        pl.when(z > 0)(lambda: self._send(src, z, 1, 1))

    def each(self, step, action):
        z = self.s.links.z
        pl.when(z >= step)(lambda: action(z - step, 0))
        pl.when(z + step <= 3)(lambda: action(z + step, 1))

    def arrive(self, step, then=None):
        z = self.s.links.z

        def action(p, way):
            self.s.landed(self.region(p), self.base + 2 * (step - 1) + way)
            if step < 3:
                ahead = z < 3 if way == 0 else z > 0
                pl.when(ahead)(lambda: self._send(self.region(p), p, way, step + 1))
            if then is not None:
                then(p)

        self.each(step, action)

    def drain(self):
        z = self.s.links.z
        for step in (1, 2, 3):
            for way in (0, 1):
                came = z - (step - 1) if way == 0 else z + (step - 1)
                ok = jnp.logical_and(z < 3, z >= step - 1) if way == 0 else jnp.logical_and(z > 0, z <= 4 - step)
                pl.when(ok)(
                    functools.partial(self.s.sent, self.region(came), self.base + 2 * (step - 1) + way)
                )


def forward_kernel(
    x_ref, g_ref, cos_ref, sin_ref, wq_in, wk_in, wv_in, gain_in, wo_ref, wg_in, wu_in, wd_ref,
    wa_all, wo_all, gu_all, wd_all, n2_all, top_all, wqkv_all, hidden_all, dgu_all, out_all, dn2_land,
    q_all, kv_all, mid_all, n1_t_all, o_t_all, gain_out, dn2_out,
    q_out, kv_out, o_out, mid_out, att_ref, gu_ref, n1, qkv, w_buf, wkv_buf, gain_buf, wo_buf, n2, top,
    n2_rows, top_rows, gate_up, grad_hidden, hidden, dgu, dn2_sends, out_rows, relay,
    send_sem, recv_sem, local_sem,
):
    rows, width = x_ref.shape
    slot_width = att_ref.shape[1]
    block = width // 8
    links = Links()
    d, z = links.d, links.z
    s = Sender(links, send_sem, recv_sem)
    ff = wd_ref.shape[0]
    cut_a = att_ref.shape[0] // 32 * 16
    cuts_a = ((0, cut_a), (cut_a, att_ref.shape[0] - cut_a))

    def at_a(dd, p, part):
        if part is None:
            return wa_all.at[dd, p]
        return wa_all.at[dd, p, pl.ds(*cuts_a[part])]

    def at_b(dd, p, part):
        start, size = (0, slot_width) if part is None else (part * slot_width // 2, slot_width // 2)
        return wo_all.at[
            pl.ds(pl.multiple_of(p * slot_width + start, 16), size),
            pl.ds(pl.multiple_of(dd * block, 128), block),
        ]

    def at_gu(dd, p, part):
        start, size = (0, block) if part is None else (part * block // 2, block // 2)
        return gu_all.at[pl.ds(pl.multiple_of(dd * block + start, 16), size)]

    def at_wd(dd, p, part):
        start, size = (0, ff) if part is None else (part * ff // 2, ff // 2)
        return wd_all.at[pl.ds(start, size), pl.ds(pl.multiple_of(dd * block, 128), block)]

    def rows_of(ref):
        return lambda p: ref.at[pl.ds(pl.multiple_of(p * rows, 16), rows)]

    spread_a, spread_b = Spread(s, at_a, 0), Spread(s, at_b, 36)
    spread_gu, spread_wd = Spread(s, at_gu, 72), Spread(s, at_wd, 81)
    line_a = Line(s, lambda p: at_a(d, p, None), 90)
    line_b = Line(s, lambda p: at_b(d, p, None), 96)
    line_n, line_t = Line(s, rows_of(n2_all), 102), Line(s, rows_of(top_all), 108)

    def keep(src, dst, at):
        pltpu.make_async_copy(src, dst, local_sem.at[at]).start()

    def kept(src, dst, at):
        pltpu.make_async_copy(src, dst, local_sem.at[at]).wait()

    kv_at = pl.ds(block, KV_ROWS)
    shards = [
        (wq_in, att_ref.at[pl.ds(0, block)], 78),
        (wk_in, att_ref.at[kv_at, pl.ds(0, KV * HD)], 79),
        (wv_in, att_ref.at[kv_at, pl.ds(KV * HD, KV * HD)], 80),
        (gain_in, att_ref.at[pl.ds(block + KV_ROWS, GAIN_ROWS), pl.ds(0, LANES)], 81),
    ]
    ffs = [(wg_in, gu_ref.at[:, pl.ds(0, ff)], 82), (wu_in, gu_ref.at[:, pl.ds(ff, ff)], 83)]
    for shard in shards + ffs:
        keep(*shard)
    att_ref[block + KV_ROWS :, LANES:] = jnp.zeros((GAIN_ROWS, slot_width - LANES), BF16)
    links.barrier(far=True)
    for shard in shards:
        kept(*shard)

    line_a.own(att_ref)
    spread_a.own(z, att_ref)
    keep(att_ref, at_a(d, z, None), 0)
    keep(wo_ref, at_b(d, z, None), 1)
    keep(wd_ref, at_wd(d, 0, None), 3)
    top[...] = g_ref[...].astype(BF16)
    line_a.arrive(1, lambda p: spread_a.own(p, at_a(d, p, None)))
    spread_a.near(z)
    line_a.arrive(2, lambda p: spread_a.own(p, at_a(d, p, None)))
    line_b.own(wo_ref)
    line_a.each(1, lambda p, way: spread_a.near(p))
    spread_a.far(z)
    line_a.arrive(3, lambda p: spread_a.own(p, at_a(d, p, None)))
    line_b.arrive(1)
    line_a.each(2, lambda p, way: spread_a.near(p))
    line_a.each(1, lambda p, way: spread_a.far(p))
    line_a.each(3, lambda p, way: spread_a.near(p))
    spread_b.own(z, wo_ref)
    line_b.each(1, lambda p, way: spread_b.own(p, at_b(d, p, None)))
    line_b.arrive(2, lambda p: spread_b.own(p, at_b(d, p, None)))
    line_a.each(2, lambda p, way: spread_a.far(p))
    line_a.each(3, lambda p, way: spread_a.far(p))
    for shard in ffs:
        kept(*shard)
    keep(gu_ref, at_gu(d, 0, None), 2)
    line_b.arrive(3, lambda p: spread_b.own(p, at_b(d, p, None)))
    line_t.own(top)
    kept(att_ref, at_a(d, z, None), 0)
    for p in range(4):
        spread_a.finish(p)

    def kv_copy(dd, p):
        return wkv_buf.at[dd, p], wqkv_all.at[pl.ds(dd * block + p * KV_ROWS, KV_ROWS), pl.ds(width, 2 * KV * HD)]

    for p in range(4):
        for dd in range(8):
            pltpu.make_async_copy(
                wa_all.at[dd, p, pl.ds(0, block)], w_buf.at[p, pl.ds(dd * block, block)], local_sem.at[14 + 8 * p + dd]
            ).start()
    keep(wa_all.at[:, :, pl.ds(block, KV_ROWS)], wkv_buf, 8)
    keep(wa_all.at[:, :, pl.ds(block + KV_ROWS, GAIN_ROWS), pl.ds(0, LANES)], gain_buf, 9)
    kept(wa_all.at[:, :, pl.ds(block + KV_ROWS, GAIN_ROWS), pl.ds(0, LANES)], gain_buf, 9)
    low_row = lax.broadcasted_iota(jnp.int32, (GAIN_ROWS, LANES), 1) < HD
    for dd in range(8):
        for half in (0, 1):
            first = gain_buf[dd, 2 * half].astype(F32)
            second = pltpu.roll(gain_buf[dd, 2 * half + 1].astype(F32), HD, 1)
            at = dd * block + half * LANES
            gain_out[:, at : at + LANES] = jnp.where(low_row, first, second)[:8]
    x = x_ref[...]
    n1[...] = (x * norm_scale(x) * gain_out[0:1]).astype(BF16)
    for p in range(4):
        for dd in range(8):
            kept(wa_all.at[dd, p, pl.ds(0, block)], w_buf.at[p, pl.ds(dd * block, block)], 14 + 8 * p + dd)
        for c in range(0, slot_width, 256):
            qkv[:, p * slot_width + c : p * slot_width + c + 256] = dot(n1[...], w_buf[p, :, c : c + 256])
        keep(w_buf.at[p], wqkv_all.at[:, pl.ds(p * slot_width, slot_width)], 4 + p)
    kept(wa_all.at[:, :, pl.ds(block, KV_ROWS)], wkv_buf, 8)
    qkv[:, width:] = dot(n1[...], wkv_buf[...].reshape(width, 2 * KV * HD))
    for p in range(4):
        for dd in range(8):
            pltpu.make_async_copy(*kv_copy(dd, p), local_sem.at[46 + 8 * p + dd]).start()

    line_b_pieces = lambda action: [action(z)] + [line_b.each(i, lambda p, way: action(p)) for i in (1, 2, 3)]

    def sequence(i, carry):
        at = pl.ds(pl.multiple_of(i * SEQ, SEQ), SEQ)
        attend_sequence(
            cos_ref[at], sin_ref[at], lambda c: qkv[at, c : c + LANES], width, q_out, kv_out, o_out, at
        )

        @pl.when(i == 0)
        def _():
            line_b_pieces(spread_b.near)
            spread_gu.own(0, gu_ref)
            line_t.arrive(1)

        return carry

    lax.fori_loop(0, rows // SEQ, sequence, 0)
    line_b_pieces(spread_b.far)
    kept(wo_ref, at_b(d, z, None), 1)
    for p in range(4):
        spread_b.finish(p)
    keep(wo_all, wo_buf, 0)
    kept(wo_all, wo_buf, 0)

    def column(i, carry):
        at = pl.ds(pl.multiple_of(i * 256, 256), 256)
        mid_out[:, at] = x_ref[:, at] + dot(o_out[...], wo_buf[:, at])
        return carry

    lax.fori_loop(0, width // 256, column, 0)
    mid = mid_out[...]
    n2[...] = (mid * norm_scale(mid) * gain_out[1:2]).astype(BF16)

    line_n.own(n2)
    keep(n2, n2_all.at[pl.ds(pl.multiple_of(z * rows, 16), rows)], 8)
    keep(top, top_all.at[pl.ds(pl.multiple_of(z * rows, 16), rows)], 9)
    line_t.arrive(2)
    results = [(q_out, q_all, 84), (kv_out, kv_all, 85), (mid_out, mid_all, 86)]
    for result in results:
        keep(*result)
    turns = []
    for i, (src, buf, dst) in enumerate(((n1, out_rows, n1_t_all), (o_out, dn2_sends.at[0], o_t_all))):
        for b in range(8):
            part = pl.ds(b * block, block)
            buf[:, part] = jnp.transpose(src[:, part].astype(F32)).astype(BF16)
            turns.append((buf.at[:, part], dst.at[part], 87 + 8 * i + b))
            keep(*turns[-1])
    for p in range(4):
        kept(w_buf.at[p], wqkv_all.at[:, pl.ds(p * slot_width, slot_width)], 4 + p)
        for dd in range(8):
            kept(*kv_copy(dd, p), 46 + 8 * p + dd)
    kept(gu_ref, at_gu(d, 0, None), 2)
    kept(wd_ref, at_wd(d, 0, None), 3)
    kept(n2, n2_all.at[pl.ds(pl.multiple_of(z * rows, 16), rows)], 8)
    kept(top, top_all.at[pl.ds(pl.multiple_of(z * rows, 16), rows)], 9)
    spread_gu.near(0)
    spread_wd.own(0, wd_ref)
    line_n.arrive(1)
    line_t.arrive(3)
    spread_gu.far(0)
    spread_gu.finish(0)

    wide = 2 * ff
    pieces = [(c, min(slot_width, wide - c)) for c in range(0, wide, slot_width)]
    gu_piece = lambda i, c, n: (columns(gu_all, c, n), w_buf.at[i, :, pl.ds(0, n)])
    for i, (c, n) in enumerate(pieces):
        keep(*gu_piece(i, c, n), 14 + i)
    wd_vmem = wo_buf.at[pl.ds(0, ff)]
    for turn in turns + results:
        kept(*turn)
    across, opposite, beside = 2 - z // 2, 3 - 3 * (z // 2), z + 1 - 2 * (z % 2)
    ends, inner = z % 3 == 0, z % 3 != 0
    chunks = [(c, min(256, ff - c)) for c in range(0, ff, 256)]

    def project(slot, source):
        for c, n in pieces:
            for h in range(0, n, 256):
                gate_up[slot, :, c + h : c + h + 256] = dot(source[...], w_buf[c // slot_width, :, h : h + 256])

    rows_at = lambda p: pl.ds(pl.multiple_of(p * rows, 16), rows)
    for i, (c, n) in enumerate(pieces):
        kept(*gu_piece(i, c, n), 14 + i)
    project(1, n2)
    spread_wd.near(0)
    line_n.arrive(2)
    keep(n2_all.at[rows_at(across)], n2_rows, 0)
    kept(n2_all.at[rows_at(across)], n2_rows, 0)
    project(0, n2_rows)
    spread_wd.far(0)
    spread_wd.finish(0)
    keep(wd_all, wd_vmem, 20)
    kept(wd_all, wd_vmem, 20)

    def place_of(p):
        return (p - z + 4) % 4 - 1

    def send_dn2(i, p):
        s.start(dn2_sends.at[i], dn2_land.at[place_of(p)], 114 + place_of(p), (d, p))

    def half_of(ref, h):
        return columns(ref, h * (width // 2), width // 2)

    def opposite_half(h):
        return half_of(dn2_land.at[1], h), 115 + 4 * h

    def pass_on(h):
        s.landed(half_of(relay, h), 117 + h)

        def add(m):
            r = pl.ds(pl.multiple_of(m * 32, 32), 32)
            c = pl.ds(h * (width // 2), width // 2)
            dn2_sends[1, r, c] = (dn2_sends[1, r, c].astype(F32) + relay[r, c].astype(F32)).astype(BF16)

        loop(rows // 32, add)
        to, at = opposite_half(h)
        s.start(half_of(dn2_sends.at[1], h), to, at, (d, opposite))

    def feed(i):
        pl.when(i == 1)(lambda: line_n.arrive(3))
        second = (i + 2) // 3 - i // 2
        p = across * ((3 - i) // 3) + opposite * second + beside * (i // 2 - i // 3) + z * (i // 3)
        at = rows_at(p)
        slot = i // 3
        keep(top_all.at[at], top_rows, 1)

        @pl.when(second + i // 2 - i // 3 == 1)
        def _():
            keep(n2_all.at[at], n2_rows, 0)
            kept(n2_all.at[at], n2_rows, 0)
            project(0, n2_rows)

        kept(top_all.at[at], top_rows, 1)
        for c, n in chunks:
            grad_hidden[:, c : c + n] = dot_nt(top_rows[...], wo_buf[c : c + n])

        @pl.when(i > 0)
        def _():
            kept(hidden, hidden_all.at[at], 2)
            kept(dgu, dgu_all.at[at], 3)

        def act(m):
            r = pl.ds(pl.multiple_of(m * 16, 16), 16)
            for c, n in chunks:
                gate, up = gate_up[slot, r, c : c + n], gate_up[slot, r, ff + c : ff + c + n]
                grad = grad_hidden[r, c : c + n]
                sig = 1.0 / (1.0 + jnp.exp(-gate))
                silu = gate * sig
                hidden[r, c : c + n] = (silu * up).astype(BF16)
                dgu[r, c : c + n] = (grad * up * sig * (1.0 + gate * (1.0 - sig))).astype(BF16)
                dgu[r, ff + c : ff + c + n] = (grad * silu).astype(BF16)

        loop(rows // 16, act)
        pl.when(jnp.logical_and(i == 3, inner))(lambda: pass_on(1))
        keep(hidden, hidden_all.at[at], 2)
        keep(dgu, dgu_all.at[at], 3)

        def back(m):
            r = pl.ds(pl.multiple_of(m * 256, 256), 256)
            total = None
            for j, (c, n) in enumerate(pieces):
                term = dot_nt(dgu[:, c : c + n], w_buf[j, r, :n])
                total = term if total is None else total + term

            @pl.when(i < 3)
            def _():
                dn2_sends[i, :, r] = total.astype(BF16)

            @pl.when(i == 3)
            def _():
                dn2_out[:, r] = total

            for h in (0, 1):

                @pl.when(jnp.logical_and(jnp.logical_and(i == 1, m == 4 * h + 3), ends))
                def _():
                    s.start(half_of(dn2_sends.at[1], h), half_of(relay, h), 117 + h, (d, 1 + z // 3))

        loop(width // 256, back)

        @pl.when(i % 2 == 0)
        def _():
            send_dn2(i, p)


        pl.when(i > 0)(lambda: kept(out_rows, out_all.at[at], 7))

        def down(m):
            r = pl.ds(pl.multiple_of(m * 256, 256), 256)
            out_rows[:, r] = dot(hidden[...], wo_buf[:ff, r]).astype(BF16)

        loop(width // 256, down)
        keep(out_rows, out_all.at[at], 7)
        pl.when(jnp.logical_and(i == 2, inner))(lambda: pass_on(0))

    loop(4, feed)
    kept(hidden, hidden_all.at[pl.ds(0, rows)], 2)
    kept(dgu, dgu_all.at[pl.ds(0, rows)], 3)
    kept(out_rows, out_all.at[pl.ds(0, rows)], 7)

    def collect(region, at, h=None):
        s.landed(region, at)
        c = pl.ds(0, width) if h is None else pl.ds(h * (width // 2), width // 2)
        keep(region, n2_rows.at[:, c], 0)
        kept(region, n2_rows.at[:, c], 0)

        def add(m):
            r = pl.ds(pl.multiple_of(m * 32, 32), 32)
            dn2_out[r, c] += n2_rows[r, c].astype(F32)

        loop(rows // 32, add)

    pl.when(z >= 1)(lambda: collect(dn2_land.at[0], 114))
    pl.when(z <= 2)(lambda: collect(dn2_land.at[2], 116))
    pl.when(inner)(lambda: collect(dn2_land.at[1], 115))
    for h in (0, 1):
        to, at = opposite_half(h)
        pl.when(ends)(functools.partial(collect, to, at, h))
    for i, p in ((0, across), (2, beside)):
        s.sent(dn2_sends.at[i], 114 + place_of(p))
    for h in (0, 1):
        to, at = opposite_half(h)
        pl.when(ends)(functools.partial(s.sent, half_of(dn2_sends.at[1], h), 117 + h))
        pl.when(inner)(functools.partial(s.sent, half_of(dn2_sends.at[1], h), at))
    for p in range(4):
        spread_a.drain(p)
        spread_b.drain(p)
    spread_gu.drain(0)
    spread_wd.drain(0)
    for line in (line_a, line_b, line_n, line_t):
        line.drain()


def forward_stage(x, g, cos, sin, wq, wk, wv, gains, wo, wg, wu, wd):
    rows, width = x.shape
    slot_width = wq.shape[1]
    block = width // 8
    kv_width = 2 * KV * HD
    ff = wd.shape[0]
    vmem = pl.BlockSpec(memory_space=pltpu.VMEM)
    hbm = pl.BlockSpec(memory_space=pltpu.HBM)
    shape = jax.ShapeDtypeStruct
    outs = [
        (hbm, shape((8, 4, block + KV_ROWS + GAIN_ROWS, slot_width), BF16)),
        (hbm, shape((width, width), BF16)),
        (hbm, shape((width, 2 * ff), BF16)),
        (hbm, shape((ff, width), BF16)),
        (hbm, shape((4 * rows, width), BF16)),
        (hbm, shape((4 * rows, width), BF16)),
        (hbm, shape((width, width + kv_width), BF16)),
        (hbm, shape((4 * rows, ff), BF16)),
        (hbm, shape((4 * rows, 2 * ff), BF16)),
        (hbm, shape((4 * rows, width), BF16)),
        (hbm, shape((3, rows, width), BF16)),
        (hbm, shape((rows, width), BF16)),
        (hbm, shape((rows, kv_width), BF16)),
        (hbm, shape((rows, width), F32)),
        (hbm, shape((width, rows), BF16)),
        (hbm, shape((width, rows), BF16)),
        (vmem, shape((8, width), F32)),
        (vmem, shape((rows, width), F32)),
    ]
    return pl.pallas_call(
        forward_kernel,
        in_specs=[vmem] * 4 + [hbm] * 4 + [vmem] + [hbm] * 2 + [vmem],
        out_specs=[o[0] for o in outs],
        out_shape=[o[1] for o in outs],
        scratch_shapes=[
            pltpu.VMEM((rows, width), BF16),
            pltpu.VMEM((rows, kv_width), BF16),
            pltpu.VMEM((rows, width), BF16),
            pltpu.VMEM((rows, width), F32),
            pltpu.VMEM((block + KV_ROWS + GAIN_ROWS, slot_width), BF16),
            pltpu.VMEM((block, 2 * ff), BF16),
            pltpu.VMEM((rows, width), BF16),
            pltpu.VMEM((rows, width + kv_width), F32),
            pltpu.VMEM((-(-2 * ff // slot_width), width, slot_width), BF16),
            pltpu.VMEM((8, 4, KV_ROWS, kv_width), BF16),
            pltpu.VMEM((8, 4, GAIN_ROWS, LANES), BF16),
            pltpu.VMEM((width, width), BF16),
            pltpu.VMEM((rows, width), BF16),
            pltpu.VMEM((rows, width), BF16),
            pltpu.VMEM((rows, width), BF16),
            pltpu.VMEM((rows, width), BF16),
            pltpu.VMEM((2, rows, 2 * ff), F32),
            pltpu.VMEM((rows, ff), F32),
            pltpu.VMEM((rows, ff), BF16),
            pltpu.VMEM((rows, 2 * ff), BF16),
            pltpu.VMEM((3, rows, width), BF16),
            pltpu.VMEM((rows, width), BF16),
            pltpu.VMEM((rows, width), BF16),
            pltpu.SemaphoreType.DMA((120,)),
            pltpu.SemaphoreType.DMA((120,)),
            pltpu.SemaphoreType.DMA((103,)),
        ],
        compiler_params=pltpu.CompilerParams(
            collective_id=0, has_side_effects=True, vmem_limit_bytes=65000 * 1024
        ),
        name="forward",
    )(x, g, cos, sin, wq, wk, wv, gains, wo, wg, wu, wd)


def loop(count, body):
    def step(i, carry):
        body(i)
        return carry

    lax.fori_loop(0, count, step, 0)


class Local:
    def __init__(self, sem):
        self.sem, self.next = sem, 0

    def start(self, src, dst):
        copy = pltpu.make_async_copy(src, dst, self.sem.at[self.next])
        self.next += 1
        copy.start()
        return copy

    def load(self, src, dst):
        self.start(src, dst).wait()


class Reduce:
    def __init__(self, sender, compute, base, sends, kept, land, halves):
        self.s, self.compute, self.base = sender, compute, base
        self.sends, self.kept, self.land, self.halves = sends, kept, land, halves

    def half(self, ref, part):
        return ref.at[pl.ds(*self.halves[part])]

    def place(self, i):
        if i < 4:
            return self.land.at[i]
        return self.half(self.land.at[4 + (i - 4) // 2], i % 2)

    def partner(self, i):
        k = self.s.links
        count = self.sends.shape[0]
        if i >= count:
            self.s.sent(self.sends.at[i % count], self.base + i - count)
        self.compute((k.dcxy, k.dcx, k.dcy, k.dc)[i], None, self.sends.at[i % count])
        self.s.start(self.sends.at[i % count], self.place(i), self.base + i, (k.dc, k.z))

    def own(self, i):
        k, b = self.s.links, self.base
        to_x, to_y = (k.dx, k.z), (k.dy, k.z)
        self.s.landed(self.place(i), b + i)
        kept = self.kept.at[i]
        self.compute((k.dxy, k.dx, k.dy, k.d)[i], self.land.at[i], kept)
        if i == 0:
            self.s.start(self.half(kept, 0), self.place(4), b + 4, to_x)
            self.s.start(self.half(kept, 1), self.place(7), b + 7, to_y)
        elif i == 1:
            self.s.start(self.half(kept, 0), self.place(6), b + 6, to_x)
        elif i == 2:
            self.s.start(self.half(kept, 1), self.place(5), b + 5, to_y)

    def first(self):
        self.partner(0)
        for i in range(3):
            self.partner(i + 1)
            self.own(i)
        self.own(3)

    def add(self, i, part, at):
        self.s.landed(self.place(at), self.base + at)
        start, size = self.halves[part]
        from_start = self.halves[at % 2][0] if at < 8 else self.halves[at - 8][0]
        slot = 4 + (at - 4) // 2
        step = 32 if size % 32 == 0 else 16

        def rows(n):
            r = pl.ds(pl.multiple_of(start + n * step, 16), step)
            g = pl.ds(pl.multiple_of(from_start + n * step, 16), step)
            self.kept[i, r] = (self.kept[i, r].astype(F32) + self.land[slot, g].astype(F32)).astype(BF16)

        loop(size // step, rows)

    def second(self):
        k, b = self.s.links, self.base
        self.add(2, 0, 4)
        self.s.start(self.half(self.kept.at[2], 0), self.place(8), b + 8, (k.dy, k.z))
        self.add(1, 1, 7)
        self.s.start(self.half(self.kept.at[1], 1), self.place(9), b + 9, (k.dx, k.z))

    def third(self):
        self.add(3, 0, 6)
        self.add(3, 1, 5)

    def last(self):
        self.add(3, 0, 8)
        self.add(3, 1, 9)

    def drain(self):
        b, kept = self.base, self.kept
        count = self.sends.shape[0]
        for i in range(4 - count, 4):
            self.s.sent(self.sends.at[i % count], b + i)
        self.s.sent(self.half(kept.at[0], 0), b + 4)
        self.s.sent(self.half(kept.at[2], 1), b + 5)
        self.s.sent(self.half(kept.at[1], 0), b + 6)
        self.s.sent(self.half(kept.at[0], 1), b + 7)
        self.s.sent(self.half(kept.at[2], 0), b + 8)
        self.s.sent(self.half(kept.at[1], 1), b + 9)


class LineSum:
    def __init__(self, sender, local, part, sends, land, base):
        self.s, self.part, self.sends = sender, part, sends
        self.land, self.base = land, base
        self.rows = sends.shape[1]
        self.sem, self.first = local.sem, local.next
        local.next += 7

    def rows_of(self, t):
        return self.part.at[pl.ds(pl.multiple_of(t * self.rows, 16), self.rows)]

    def fetch(self, holds, slot, at):
        return pltpu.make_async_copy(self.rows_of(holds), self.sends.at[slot], self.sem.at[self.first + at])

    def begin(self):
        for s in (1, 2, 3):
            for sends, slot, place, holds, _, _ in self.ways(s):
                pl.when(sends)(lambda: self.fetch(holds, slot, place).start())
        self.fetch(self.s.links.z, 3, 6).start()
        self.step(1)

    def add(self, into, at):
        self.s.landed(self.land.at[at], self.base + at)

        def rows(n):
            r = pl.ds(pl.multiple_of(n * 32, 32), 32)
            self.sends[into, r] = (self.sends[into, r].astype(F32) + self.land[at, r].astype(F32)).astype(BF16)

        loop(self.rows // 32, rows)

    def ways(self, s):
        z = self.s.links.z
        right = (z <= s - 1, s - 1 - z, 2 * (s - 1), z + 4 - s, z >= 1, z + 1)
        left = (z >= 4 - s, s - 1, 2 * (s - 1) + 1, z - 4 + s, z <= 2, z - 1)
        return right, left

    def step(self, s):
        for sends, slot, place, holds, received, to in self.ways(s):

            @pl.when(sends)
            def _():
                self.fetch(holds, slot, place).wait()
                if s > 1:
                    pl.when(received)(lambda: self.add(slot, place - 2))
                self.s.start(self.sends.at[slot], self.land.at[place], self.base + place, (self.s.links.d, to))

    def finish(self, write):
        z = self.s.links.z
        self.fetch(z, 3, 6).wait()
        pl.when(z >= 1)(lambda: self.add(3, 4))
        pl.when(z <= 2)(lambda: self.add(3, 5))

        def rows(n):
            r = pl.ds(pl.multiple_of(n * 32, 32), 32)
            write(r, self.sends[3, r].astype(F32))

        loop(self.rows // 32, rows)

    def drain(self):
        for s in (1, 2, 3):
            for sends, slot, place, _, _, _ in self.ways(s):
                pl.when(sends)(functools.partial(self.s.sent, self.sends.at[slot], self.base + place))


def stream(local, count, source, bufs, body):
    first = local.next
    local.next += 2

    def copy(n, slot):
        return pltpu.make_async_copy(source(n), bufs.at[slot], local.sem.at[first + slot])

    copy(0, 0).start()

    def step(n):
        slot = n % 2
        copy(n, slot).wait()

        @pl.when(n + 1 < count)
        def _():
            copy(n + 1, 1 - slot).start()

        body(n, bufs.at[slot])

    loop(count, step)


def turned(ref):
    return jnp.transpose(ref[...].astype(F32)).astype(BF16)


def columns(ref, start, size):
    return ref.at[:, pl.ds(pl.multiple_of(start, 128), size)]


class Feeder:
    def __init__(self, local, source, bufs, block, dests):
        self.source, self.bufs, self.block, self.dests = source, bufs, block, dests
        self.sem, self.first, self.n = local.sem, local.next, 0
        local.next += 2
        self._copy(0).start()

    def _copy(self, n):
        return pltpu.make_async_copy(
            columns(self.source, self.dests[n] * self.block, self.block),
            self.bufs.at[n % 2],
            self.sem.at[self.first + n % 2],
        )

    def __call__(self, dest):
        n = self.n
        self.n += 1
        self._copy(n).wait()
        if n + 1 < len(self.dests):
            self._copy(n + 1).start()
        return self.bufs.at[n % 2]


def order_of(k):
    partner, own = (k.dcxy, k.dcx, k.dcy, k.dc), (k.dxy, k.dx, k.dy, k.d)
    return [partner[0], partner[1], own[0], partner[2], own[1], partner[3], own[2], own[3]]


def row_blocks(pick, left, right):
    width = right.shape[1]

    def compute(dest, add, out):
        left[...] = turned(pick(dest))

        def chunk(n):
            c = pl.ds(pl.multiple_of(n * 256, 256), 256)
            total = dot(left[...], right[:, c])
            if add is not None:
                total = total + add[:, c].astype(F32)
            out[:, c] = total.astype(BF16)

        loop(width // 256, chunk)

    return compute


def column_blocks(left, pick, chunks):
    size = left.shape[0] // chunks

    def compute(dest, add, out):
        picked = pick(dest)

        def chunk(n):
            r = pl.ds(pl.multiple_of(n * size, 16), size)
            total = dot(left[r], picked[...])
            if add is not None:
                total = total + add[r].astype(F32)
            out[r] = total.astype(BF16)

        loop(chunks, chunk)

    return compute


class Chunk:
    def __init__(self, sender, compute, sends, kept, land, base):
        self.s, self.compute, self.sends = sender, compute, sends
        self.kept, self.land, self.base = kept, land, base
        self.half = kept.shape[2] // 2

    def views(self, n):
        kept, land, h = self.kept.at[n], self.land.at[n], self.half
        top, low = pl.ds(0, h), pl.ds(h, h)
        return {
            "x1": (kept.at[pl.ds(0, 2), top], land.at[pl.ds(4, 2), top]),
            "y1": (kept.at[pl.ds(1, 2), low], land.at[pl.ds(4, 2), low]),
            "y2": (kept.at[2, top], land.at[6, top]),
            "x2": (kept.at[0, low], land.at[6, low]),
        }

    def partner(self, n):
        k = self.s.links
        slot = n % self.sends.shape[0]
        if n != slot:
            self.s.sent(self.sends.at[slot], self.base + 5 * (n - self.sends.shape[0]))
        for i, dest in enumerate((k.dcx, k.dcxy, k.dcy, k.dc)):
            self.compute(n, dest, None, self.sends.at[slot, i])
        self.s.start(self.sends.at[slot], self.land.at[n, pl.ds(0, 4)], self.base + 5 * n, (k.dc, k.z))

    def own(self, n):
        k, b, v = self.s.links, self.base + 5 * n, self.views(n)
        self.s.landed(self.land.at[n, pl.ds(0, 4)], b)
        for i, dest in enumerate((k.dx, k.dxy, k.dy, k.d)):
            self.compute(n, dest, self.land.at[n, i], self.kept.at[n, i])
        self.s.start(*v["x1"], b + 1, (k.dx, k.z))
        self.s.start(*v["y1"], b + 2, (k.dy, k.z))

    def add(self, n, i, start, got):
        kept, land = self.kept, self.land

        def rows(m):
            r = pl.ds(pl.multiple_of(start + m * 32, 32), 32)
            kept[n, i, r] = (kept[n, i, r].astype(F32) + land[n, got, r].astype(F32)).astype(BF16)

        loop(self.half // 32, rows)

    def second(self, n):
        k, b, v = self.s.links, self.base + 5 * n, self.views(n)
        self.s.landed(v["x1"][1], b + 1)
        self.add(n, 2, 0, 5)
        self.s.start(*v["y2"], b + 3, (k.dy, k.z))
        self.s.landed(v["y1"][1], b + 2)
        self.add(n, 0, self.half, 4)
        self.s.start(*v["x2"], b + 4, (k.dx, k.z))
        self.add(n, 3, 0, 4)
        self.add(n, 3, self.half, 5)

    def last(self, n):
        b, v = self.base + 5 * n, self.views(n)
        self.s.landed(v["y2"][1], b + 3)
        self.add(n, 3, 0, 6)
        self.s.landed(v["x2"][1], b + 4)
        self.add(n, 3, self.half, 6)

    def drain(self):
        for n in range(self.kept.shape[0]):
            b, v = self.base + 5 * n, self.views(n)
            if n + self.sends.shape[0] >= self.kept.shape[0]:
                self.s.sent(self.sends.at[0], b)
            for at, name in enumerate(("x1", "y1", "y2", "x2")):
                self.s.sent(v[name][0], b + 1 + at)


class Spread4:
    def __init__(self, sender, pick, land, base):
        self.s, self.pick, self.land, self.base = sender, pick, land, base

    def send(self):
        k = self.s.links
        for j in (1, 2, 3):
            to = (k.z + j) % 4
            self.s.start(self.pick(to), self.land.at[j - 1], self.base + j - 1, (k.d, to))

    def landed(self):
        for j in range(3):
            self.s.landed(self.land.at[j], self.base + j)

    def drain(self):
        z = self.s.links.z
        for j in (1, 2, 3):
            self.s.sent(self.pick((z + j) % 4), self.base + j - 1)


def norm_back_rows(rows_ref, at, gain, grad_normed):
    rows = rows_ref[at]
    inv = norm_scale(rows)
    weighted = grad_normed * gain
    scaled = grad_normed * rows * inv
    grad_rows = inv * weighted - rows * (inv * inv * inv) * jnp.mean(weighted * rows, -1, keepdims=True)
    return grad_rows, scaled


def halves(size):
    return (0, size // 2), (size // 2, size // 2)


def add_gain(gain_part, block, row, scaled):
    for b in range(8):
        total = jnp.sum(scaled[:, b * block : (b + 1) * block], 0, keepdims=True)
        gain_part[b % 2, b // 2 % 2 * 2 + b // 4, row : row + 1] += total


def transpose_into(src, dst):
    def part(n):
        c = pl.ds(pl.multiple_of(n * 128, 128), 128)
        dst[c] = jnp.transpose(src[:, c].astype(F32)).astype(BF16)

    loop(src.shape[1] // 128, part)


def row_chunk(ref):
    return lambda n: ref.at[pl.ds(pl.multiple_of(n * 256, 256), 256)]


def attention_back_kernel(
    gain_ref, cos_ref, sin_ref, dn2_in, mid_in, g_in, q_in, kv_in, att_in,
    part_ref, hidden_ref, top_ref, wo_ref,
    out_ref, gain_part, gd_out, go_out, gm_all, dqkv_all,
    dn2_ref, mid_ref, g_ref, q_ref, kv_ref, att_t, gm_out, dqkv, mid_bf, da, dkv, w_chunk, top_cols, hidden_cols, hidden_t,
    d_sends, d_kept, d_land, o_sends, o_kept, o_land, line_sends, line_land,
    send_sem, recv_sem, local_sem,
):
    rows, width = mid_ref.shape
    block = width // 8
    ff = hidden_t.shape[0]
    links = Links()
    s = Sender(links, send_sem, recv_sem)
    local = Local(local_sem)
    top_feed = Feeder(local, top_ref, top_cols, block, order_of(links))
    links.barrier()
    line = LineSum(s, local, part_ref, line_sends, line_land, 20)
    line.begin()
    ins = [
        local.start(src, dst)
        for src, dst in (
            (dn2_in, dn2_ref), (mid_in, mid_ref), (g_in, g_ref), (att_in, att_t), (q_in, q_ref), (kv_in, kv_ref)
        )
    ]

    def turn_hidden(n, buf):
        hidden_t[pl.ds(pl.multiple_of(n * 128, 128), 128)] = turned(buf)

    stream(local, ff // 128, lambda n: columns(hidden_ref, n * 128, 128), hidden_cols, turn_hidden)
    grad_d = Reduce(s, column_blocks(hidden_t, top_feed, 4), 0, d_sends, d_kept, d_land, halves(ff))
    grad_d.first()
    line.step(2)

    gain_part[...] = jnp.zeros_like(gain_part)
    dkv[...] = jnp.zeros_like(dkv)
    step = 32

    def middle(n):
        r = pl.ds(pl.multiple_of(n * step, step), step)
        grad_rows, scaled = norm_back_rows(mid_ref, r, gain_ref[1:2], dn2_ref[r])
        grad = g_ref[r] + grad_rows
        gm_out[r] = grad
        mid_bf[r] = grad.astype(BF16)
        add_gain(gain_part, block, 1, scaled)

    for copy in ins:
        copy.wait()
    loop(rows // step, middle)
    to_gm = local.start(gm_out, gm_all)
    pick_mid = lambda dest: columns(mid_bf, dest * block, block)
    grad_o = Reduce(s, column_blocks(att_t, pick_mid, 4), 10, o_sends, o_kept, o_land, halves(width))
    grad_o.first()
    grad_d.second()

    def attended(n, buf):
        da[:, pl.ds(pl.multiple_of(n * 256, 256), 256)] = dot_nt(mid_bf[...], buf[...]).astype(BF16)

    stream(local, width // 256, row_chunk(wo_ref), w_chunk, attended)
    line.step(3)

    def group_step(n):
        def sequence(i):
            at = pl.ds(pl.multiple_of(i * SEQ, SEQ), SEQ)
            attend_back_group(cos_ref[at], sin_ref[at], n, q_ref, kv_ref, da, dqkv, dkv, at)

        loop(rows // SEQ, sequence)
        pl.when(n == 1)(grad_o.second)
        pl.when(n == 2)(grad_d.third)
        pl.when(n == 2)(grad_d.last)
        pl.when(n == 3)(grad_o.third)

    loop(KV, group_step)
    to_down = local.start(d_kept.at[3], gd_out)

    def key_value(i):
        at = pl.ds(pl.multiple_of(i * SEQ, SEQ), SEQ)
        first, _ = lane_masks()
        for tile in range(KV // 2):
            c = tile * LANES
            u = dkv[at, c : c + LANES]
            dqkv[at, width + c : width + c + LANES] = (
                u * cos_ref[at] - swap_halves(u, first) * sin_ref[at]
            ).astype(BF16)
        dqkv[at, width + KV * HD :] = dkv[at, KV * HD :].astype(BF16)

    loop(rows // SEQ, key_value)
    to_dqkv = local.start(dqkv, dqkv_all)
    grad_o.last()
    to_out = local.start(o_kept.at[3], go_out)

    def write(r, total):
        out_ref[r] = mid_ref[r] + total

    line.finish(write)
    for copy in (to_down, to_out, to_gm, to_dqkv):
        copy.wait()
    grad_o.drain()
    grad_d.drain()
    line.drain()


def attention_back(gains, cos, sin, dn2, mid, g, query, key_val, attended_t, part, hidden, top, wo):
    rows, width = mid.shape
    block, ff = width // 8, hidden.shape[1]
    kv_width = 2 * KV * HD
    vmem = pl.BlockSpec(memory_space=pltpu.VMEM)
    hbm = pl.BlockSpec(memory_space=pltpu.HBM)
    shape = jax.ShapeDtypeStruct
    return pl.pallas_call(
        attention_back_kernel,
        in_specs=[vmem] * 3 + [hbm] * 10,
        out_specs=[vmem] * 2 + [hbm] * 4,
        out_shape=[
            shape((rows, width), F32),
            shape((2, 4, 8, block), F32),
            shape((ff, block), BF16),
            shape((width, block), BF16),
            shape((rows, width), F32),
            shape((rows, width + kv_width), BF16),
        ],
        scratch_shapes=[
            pltpu.VMEM((rows, width), F32),
            pltpu.VMEM((rows, width), F32),
            pltpu.VMEM((rows, width), F32),
            pltpu.VMEM((rows, width), BF16),
            pltpu.VMEM((rows, kv_width), BF16),
            pltpu.VMEM((width, rows), BF16),
            pltpu.VMEM((rows, width), F32),
            pltpu.VMEM((rows, width + kv_width), BF16),
            pltpu.VMEM((rows, width), BF16),
            pltpu.VMEM((rows, width), BF16),
            pltpu.VMEM((rows, kv_width), F32),
            pltpu.VMEM((2, 256, width), BF16),
            pltpu.VMEM((2, 4 * rows, block), BF16),
            pltpu.VMEM((2, 4 * rows, 128), BF16),
            pltpu.VMEM((ff, 4 * rows), BF16),
            pltpu.VMEM((2, ff, block), BF16),
            pltpu.VMEM((4, ff, block), BF16),
            pltpu.VMEM((7, ff, block), BF16),
            pltpu.VMEM((2, width, block), BF16),
            pltpu.VMEM((4, width, block), BF16),
            pltpu.VMEM((7, width, block), BF16),
            pltpu.VMEM((4, rows, width), BF16),
            pltpu.VMEM((6, rows, width), BF16),
            pltpu.SemaphoreType.DMA((26,)),
            pltpu.SemaphoreType.DMA((26,)),
            pltpu.SemaphoreType.DMA((40,)),
        ],
        compiler_params=pltpu.CompilerParams(
            collective_id=1, has_side_effects=True, vmem_limit_bytes=65000 * 1024
        ),
        name="attention_back",
    )(gains, cos, sin, dn2, mid, g, query, key_val, attended_t, part, hidden, top, wo)


def project_back_kernel(
    gain_ref, gain_in, x_in, dqkv_in, n1_in, gm_ref, n2_ref, dgu_ref, wqkv_ref, go_in,
    gq_out, gkv_out, go_out, gain_out, grad_in_all, ggu_out,
    x_ref, dqkv, grad_in_out, dn1, n1_t, w_chunk, dgu, n2_cols, left, sends, kept, land,
    row_sends, row_kept, row_land, o_block, gain_part, gain_land, z_q, z_kv, z_o,
    send_sem, recv_sem, local_sem,
):
    rows, width = x_ref.shape
    block, slot = width // 8, width // 4
    kv_width = 2 * KV * HD
    step = 32
    links = Links()
    d, z = links.d, links.z
    s = Sender(links, send_sem, recv_sem)
    local = Local(local_sem)
    firsts = [local.start(dqkv_in, dqkv), local.start(n1_in, n1_t)]
    n2_feed = Feeder(local, n2_ref, n2_cols, block, order_of(links))
    fetch_dgu = local.start(dgu_ref, dgu)
    fetch_x = local.start(x_in, x_ref)
    fetch_o = local.start(go_in, o_block)
    fetch_gm = local.start(gm_ref, grad_in_out)
    links.barrier(far=True)
    fetch_o.wait()
    send_o = Spread4(s, lambda p: o_block.at[pl.ds(pl.multiple_of(p * slot, 16), slot)], z_o, 35)
    send_o.send()
    gain_part[...] = gain_in[...]

    for copy in firsts:
        copy.wait()

    group_of = lambda n: (z + n) % 4

    def row_compute(n, dest, add, out):
        picked = n1_t[pl.ds(pl.multiple_of(dest * block, block), block)]
        start = width if n == 0 else group_of(n) * slot
        for c in range(0, slot, 256):
            total = dot(picked, dqkv[:, pl.ds(pl.multiple_of(start + c, 256), 256)])
            if add is not None:
                total = total + add[:, c : c + 256].astype(F32)
            out[:, c : c + 256] = total.astype(BF16)

    row = Chunk(s, row_compute, row_sends, row_kept, row_land, 10)
    row.partner(0)
    for n in range(4):
        row.partner(n + 1)
        row.own(n)
    row.own(4)

    send_kv = Spread4(
        s, lambda p: row_kept.at[0, 3, pl.ds(pl.multiple_of(p * KV_ROWS, 16), KV_ROWS)], z_kv, 38
    )

    def final_q(n):
        row.last(n)
        s.start(row_kept.at[n, 3], z_q.at[n - 1], 40 + n, (d, group_of(n)))

    fetch_dgu.wait()
    grads = Reduce(s, row_blocks(n2_feed, left, dgu), 0, sends, kept, land, halves(block))
    grads.partner(0)
    row.second(0)
    grads.partner(1)
    row.second(1)
    row.second(2)
    grads.own(0)
    row.second(3)
    row.second(4)
    grads.partner(2)
    row.last(0)
    send_kv.send()
    final_q(1)
    grads.own(1)
    final_q(2)
    grads.partner(3)
    final_q(3)
    grads.own(2)
    row.last(4)
    grads.own(3)
    grads.second()

    def projected(n, buf):
        dn1[:, pl.ds(pl.multiple_of(n * 256, 256), 256)] = dot_nt(dqkv[...], buf[...])

    stream(local, width // 256, row_chunk(wqkv_ref), w_chunk, projected)
    fetch_gm.wait()
    fetch_x.wait()

    def inward(n):
        r = pl.ds(pl.multiple_of(n * step, step), step)
        grad_rows, scaled = norm_back_rows(x_ref, r, gain_ref[0:1], dn1[r])
        grad_in_out[r] += grad_rows
        add_gain(gain_part, block, 0, scaled)

    loop(rows // step, inward)
    to_in = local.start(grad_in_out, grad_in_all)
    grads.third()
    core, x_at, y_at = d % 2, d // 2 % 2, d // 4
    s.start(gain_part.at[1 - core], gain_land.at[pl.ds(0, 4)], 44, (links.dc, z))
    s.landed(gain_land.at[pl.ds(0, 4)], 44)
    gain_part[core] += gain_land[0:4]
    other_x = pl.multiple_of(2 - 2 * x_at, 2)
    s.start(gain_part.at[core, pl.ds(other_x, 2)], gain_land.at[pl.ds(4, 2)], 45, (links.dx, z))
    send_o.landed()

    def out_rows(n):
        r = pl.ds(pl.multiple_of(n * 16, 16), 16)
        mine = pl.ds(pl.multiple_of(z * slot + n * 16, 16), 16)
        go_out[r] = (
            o_block[mine].astype(F32) + z_o[0, r].astype(F32) + z_o[1, r].astype(F32) + z_o[2, r].astype(F32)
        )

    loop(slot // 16, out_rows)
    for n in range(3):
        s.landed(z_q.at[n], 41 + n)

    def query_rows(n):
        r = pl.ds(pl.multiple_of(n * 16, 16), 16)
        gq_out[r] = (
            row_kept[4, 3, r].astype(F32) + z_q[0, r].astype(F32) + z_q[1, r].astype(F32) + z_q[2, r].astype(F32)
        )

    loop(block // 16, query_rows)
    send_kv.landed()
    mine_kv = pl.ds(pl.multiple_of(z * KV_ROWS, 16), KV_ROWS)
    gkv_out[...] = row_kept[0, 3, mine_kv].astype(F32) + (
        z_kv[0].astype(F32) + z_kv[1].astype(F32) + z_kv[2].astype(F32)
    )
    s.landed(gain_land.at[pl.ds(4, 2)], 45)
    mine_x = 2 * x_at
    gain_part[core, pl.ds(mine_x, 2)] += gain_land[4:6]
    s.start(gain_part.at[core, mine_x + 1 - y_at], gain_land.at[6], 46, (links.dy, z))
    s.landed(gain_land.at[6], 46)
    gain_part[core, mine_x + y_at] += gain_land[6]
    send_g = Spread4(s, lambda p: gain_part.at[core, mine_x + y_at], gain_land.at[pl.ds(7, 3)], 47)
    send_g.send()
    grads.last()
    to_gu = local.start(kept.at[3], ggu_out)
    send_g.landed()
    gain = gain_part[core, mine_x + y_at] + gain_land[7] + gain_land[8] + gain_land[9]
    gain_out[...] = pltpu.roll(gain, (4 - z) % 4 * (block // 4), 1)
    to_gu.wait()
    to_in.wait()
    for unit in (grads, row, send_o, send_kv, send_g):
        unit.drain()
    for n in range(3):
        s.sent(row_kept.at[n + 1, 3], 41 + n)
    s.sent(gain_part.at[1 - core], 44)
    s.sent(gain_part.at[core, pl.ds(other_x, 2)], 45)
    s.sent(gain_part.at[core, mine_x + 1 - y_at], 46)


def project_back(gains, gain_in, x, dqkv, normed_t, gm, n2, dgu, wqkv, grad_o):
    rows, width = x.shape
    block, slot = width // 8, width // 4
    kv_width = 2 * KV * HD
    wide = dgu.shape[1]
    vmem = pl.BlockSpec(memory_space=pltpu.VMEM)
    hbm = pl.BlockSpec(memory_space=pltpu.HBM)
    shape = jax.ShapeDtypeStruct
    return pl.pallas_call(
        project_back_kernel,
        in_specs=[vmem] * 2 + [hbm] * 8,
        out_specs=[vmem] * 4 + [hbm] * 2,
        out_shape=[
            shape((block, slot), F32),
            shape((KV_ROWS, kv_width), F32),
            shape((slot, block), F32),
            shape((8, block), F32),
            shape((rows, width), F32),
            shape((block, wide), BF16),
        ],
        scratch_shapes=[
            pltpu.VMEM((rows, width), F32),
            pltpu.VMEM((rows, width + kv_width), BF16),
            pltpu.VMEM((rows, width), F32),
            pltpu.VMEM((rows, width), F32),
            pltpu.VMEM((width, rows), BF16),
            pltpu.VMEM((2, 256, width + kv_width), BF16),
            pltpu.VMEM((4 * rows, wide), BF16),
            pltpu.VMEM((2, 4 * rows, block), BF16),
            pltpu.VMEM((block, 4 * rows), BF16),
            pltpu.VMEM((2, block, wide), BF16),
            pltpu.VMEM((4, block, wide), BF16),
            pltpu.VMEM((7, block, wide), BF16),
            pltpu.VMEM((3, 4, block, slot), BF16),
            pltpu.VMEM((5, 4, block, slot), BF16),
            pltpu.VMEM((5, 7, block, slot), BF16),
            pltpu.VMEM((width, block), BF16),
            pltpu.VMEM((2, 4, 8, block), F32),
            pltpu.VMEM((10, 8, block), F32),
            pltpu.VMEM((3, block, slot), BF16),
            pltpu.VMEM((3, KV_ROWS, kv_width), BF16),
            pltpu.VMEM((3, slot, block), BF16),
            pltpu.SemaphoreType.DMA((50,)),
            pltpu.SemaphoreType.DMA((50,)),
            pltpu.SemaphoreType.DMA((40,)),
        ],
        compiler_params=pltpu.CompilerParams(
            collective_id=2, has_side_effects=True, vmem_limit_bytes=65000 * 1024
        ),
        name="project_back",
    )(gains, gain_in, x, dqkv, normed_t, gm, n2, dgu, wqkv, grad_o)


def results_kernel(
    hidden_in, grad_in, gq_in, gkv_in, go_in, gain_in, gu_in, gd_in,
    hidden_out, grad_out, gain_out, gq_out, gk_out, gv_out, go_out, gate_out, up_out, gd_out,
    hidden, grad, gq, gkv, go, gu, gd, gate, up, down, in_sem, out_sem,
):
    loads = [
        pltpu.make_async_copy(src, dst, in_sem.at[i])
        for i, (src, dst) in enumerate(
            ((gu_in, gu), (gd_in, gd), (hidden_in, hidden), (grad_in, grad), (gq_in, gq), (go_in, go), (gkv_in, gkv))
        )
    ]
    for load in loads:
        load.start()
    stores = []

    def store(src, dst):
        stores.append(pltpu.make_async_copy(src, dst, out_sem.at[len(stores)]))
        stores[-1].start()

    ff = gate.shape[1]
    gain_out[...] = gain_in[0:2, : gain_out.shape[1]]
    loads[0].wait()

    def widen(src, dst, start):
        def rows(n):
            r = pl.ds(pl.multiple_of(n * 32, 32), 32)
            dst[r] = src[r, start : start + dst.shape[1]].astype(F32)

        loop(dst.shape[0] // 32, rows)

    widen(gu, gate, 0)
    store(gate, gate_out)
    widen(gu, up, ff)
    store(up, up_out)
    loads[1].wait()
    widen(gd, down, 0)
    store(down, gd_out)
    for load, src, dst in zip(loads[2:6], (hidden, grad, gq, go), (hidden_out, grad_out, gq_out, go_out)):
        load.wait()
        store(src, dst)
    loads[6].wait()
    half = gk_out.shape[1]
    store(gkv.at[:, pl.ds(0, half)], gk_out)
    store(gkv.at[:, pl.ds(half, half)], gv_out)
    for copy in stores:
        copy.wait()


def results(hidden, grad, gq, gkv, go, gain, gu, gd):
    vmem = pl.BlockSpec(memory_space=pltpu.VMEM)
    hbm = pl.BlockSpec(memory_space=pltpu.HBM)
    shape = lambda *dims: jax.ShapeDtypeStruct(dims, F32)
    ff = gu.shape[1] // 2
    outs = [
        shape(*hidden.shape), shape(*grad.shape), shape(2, gain.shape[1] // 4), shape(*gq.shape),
        shape(gkv.shape[0], gkv.shape[1] // 2), shape(gkv.shape[0], gkv.shape[1] // 2), shape(*go.shape),
        shape(gu.shape[0], ff), shape(gu.shape[0], ff), shape(*gd.shape),
    ]
    return pl.pallas_call(
        results_kernel,
        in_specs=[hbm] * 5 + [vmem] + [hbm] * 2,
        out_specs=[vmem if i == 2 else hbm for i in range(10)],
        out_shape=outs,
        scratch_shapes=[pltpu.VMEM(a.shape, a.dtype) for a in (hidden, grad, gq, gkv, go, gu, gd)]
        + [pltpu.VMEM((gu.shape[0], ff), F32)] * 2
        + [pltpu.VMEM(gd.shape, F32), pltpu.SemaphoreType.DMA((7,)), pltpu.SemaphoreType.DMA((9,))],
        name="results",
    )(hidden, grad, gq, gkv, go, gain, gu, gd)


def plain_forward(x, g, cos, sin, w_query, w_kv, gains, w_out, w_gu, w_down):
    both = ("dp", "tensor")
    gather = lax.all_gather

    def whole(shard, dims):
        for dim, axis in dims:
            shard = gather(shard, axis, axis=dim, tiled=True)
        return shard

    wq = whole(w_query, ((1, "tensor"), (0, "dp")))
    wqkv = jnp.concatenate([wq, whole(w_kv, ((0, both),))], 1)
    gain = whole(gains, ((1, both),)).astype(F32)
    wo = whole(w_out, ((0, "tensor"), (1, "dp")))
    wgu = whole(w_gu, ((0, "dp"),))
    wd = whole(w_down, ((1, "dp"),))
    normed = (x * norm_scale(x) * gain[0]).astype(BF16)
    query, key_val, attended = attend(cos, sin, dot(normed, wqkv))
    middle = x + dot(attended, wo)
    normed_two = (middle * norm_scale(middle) * gain[1]).astype(BF16)
    n2 = gather(normed_two, "tensor", axis=0, tiled=True)
    top = gather(g.astype(BF16), "tensor", axis=0, tiled=True)
    return wqkv, gain, wo, wgu, wd, n2, top, query, key_val, attended, middle


def plain_backward(
    dn2_part, out_part, n2, grad_gu_pre, hidden, top,
    middle, x, g, gains, cos, sin, query, key_val, attended, wo, wqkv,
):
    width = x.shape[1]

    def scatter(part, axis, dim):
        return lax.psum_scatter(part.astype(BF16), axis, scatter_dimension=dim, tiled=True).astype(F32)

    output = middle + scatter(out_part, "tensor", 0)
    grad_mid_norm, gain_two = norm_back(middle, gains[1], scatter(dn2_part, "tensor", 0))
    grad_middle = g + grad_mid_norm
    mid_bf = grad_middle.astype(BF16)
    grad_qkv_rows = attend_back(cos, sin, query, key_val, dot_nt(mid_bf, wo).astype(BF16))
    grad_in_norm, gain_one = norm_back(x, gains[0], dot_nt(grad_qkv_rows, wqkv))
    normed_one = (x * norm_scale(x) * gains[0]).astype(BF16)
    grad_qkv = scatter(dot_tn(normed_one, grad_qkv_rows), "dp", 0)
    gain_parts = lax.psum_scatter(jnp.stack([gain_one, gain_two]), "dp", scatter_dimension=1, tiled=True)
    return (
        output,
        grad_middle + grad_in_norm,
        lax.psum_scatter(gain_parts, "tensor", scatter_dimension=1, tiled=True),
        scatter(grad_qkv[:, :width], "tensor", 1),
        scatter(grad_qkv[:, width:], "tensor", 0),
        scatter(scatter(dot_tn(attended, mid_bf), "dp", 1), "tensor", 0),
        scatter(dot_tn(n2, grad_gu_pre), "dp", 0),
        scatter(dot_tn(hidden, top), "dp", 1),
    )


def linked_layer(x, g, cos, sin, w_query, w_key, w_value, gains, w_out, w_gate, w_up, w_down):
    padded = jnp.pad(gains, ((0, GAIN_ROWS - 2), (0, LANES - gains.shape[1])))
    outs = forward_stage(x, g, cos, sin, w_query, w_key, w_value, padded, w_out, w_gate, w_up, w_down)
    wo, n2, top, wqkv, hidden, dgu, out_part = (outs[i] for i in (1, 4, 5, 6, 7, 8, 9))
    query, key_val, middle, normed_t, attended_t, gain, dn2 = outs[11:]
    output, gain_part, grad_down, grad_o, grad_middle, grad_qkv = attention_back(
        gain, cos, sin, dn2, middle, g, query, key_val, attended_t, out_part, hidden, top, wo
    )
    grad_query, grad_kv, grad_out, gain_sum, grad_in, grad_gu = project_back(
        gain, gain_part, x, grad_qkv, normed_t, grad_middle, n2, dgu, wqkv, grad_o
    )
    return results(output, grad_in, grad_query, grad_kv, grad_out, gain_sum, grad_gu, grad_down)


def plain_layer(x, g, cos, sin, w_query, w_key, w_value, gains, w_out, w_gate, w_up, w_down):
    w_kv = jnp.concatenate([w_key, w_value], 1)
    w_gu = jnp.concatenate([w_gate, w_up], 1)
    wqkv, gains, wo, wgu, wd, n2, top, query, key_val, attended, middle = plain_forward(
        x, g, cos, sin, w_query, w_kv, gains, w_out, w_gu, w_down
    )
    ff = wd.shape[0]
    gate_up = dot(n2, wgu)
    gate_pre, up_pre = gate_up[:, :ff], gate_up[:, ff:]
    sig = jax.nn.sigmoid(gate_pre)
    hidden = (gate_pre * sig * up_pre).astype(BF16)
    grad_hidden = dot_nt(top, wd)
    grad_gate_pre = (grad_hidden * up_pre * sig * (1.0 + gate_pre * (1.0 - sig))).astype(BF16)
    grad_up_pre = (grad_hidden * gate_pre * sig).astype(BF16)
    grad_gu_pre = jnp.concatenate([grad_gate_pre, grad_up_pre], 1)
    output, grad_in, grad_gains, grad_query, grad_kv, grad_out, grad_gu, grad_down = plain_backward(
        dot_nt(grad_gu_pre, wgu).astype(BF16), dot(hidden, wd).astype(BF16), n2, grad_gu_pre, hidden, top,
        middle, x, g, gains, cos, sin, query, key_val, attended, wo, wqkv,
    )
    half = KV * HD
    return (
        output, grad_in, grad_gains, grad_query, grad_kv[:, :half], grad_kv[:, half:], grad_out,
        grad_gu[:, :ff], grad_gu[:, ff:], grad_down,
    )


def on_device(
    linked,
    hidden_in, positions, norm_gains, w_query, w_key, w_value, w_out, w_gate, w_up, w_down, out_grad,
):
    x, g = hidden_in, out_grad
    rows, width = x.shape
    ff = w_gate.shape[2]
    kv_width = 2 * KV * HD
    z = lax.axis_index("tensor")

    cos, sin = rope_tables(lax.dynamic_slice_in_dim(positions, z * rows, rows))
    layer = linked_layer if linked else plain_layer
    outs = layer(
        x, g, cos, sin,
        w_query[0], w_key[0], w_value[0], norm_gains[0], w_out[0], w_gate[0], w_up[0], w_down[0],
    )
    return tuple(outs[:2]) + tuple(out[None] for out in outs[2:])


def solution(mesh):
    nd, nt = mesh.shape["dp"], mesh.shape["tensor"]
    rows = P(("dp", "tensor"), None)
    wide = P(None, "dp", "tensor")
    tall = P(None, "tensor", "dp")
    flat = P(None, ("dp", "tensor"), None)
    gain = P(None, None, ("dp", "tensor"))
    return jax.shard_map(
        functools.partial(on_device, (nd, nt) == (8, 4)),
        mesh=mesh,
        in_specs=(rows, P("dp"), gain, wide, flat, flat, tall, wide, wide, tall, rows),
        out_specs=(rows, rows, gain, wide, flat, flat, tall, wide, wide, tall),
        check_vma=False,
    )
```

```python
import functools

import jax
import jax.numpy as jnp
from jax import lax
from jax.experimental import pallas as pl
from jax.experimental.pallas import tpu as pltpu
from jax.sharding import PartitionSpec as P

H = 32
KV = 4
HD = 64
SEQ = 128
NORM_EPS = 1e-05
NEG_BIG = -1e30
SCALE = HD ** (-0.5)
LANES = 128
F32 = jnp.float32
BF16 = jnp.bfloat16


def dot(a, b):
    return jnp.dot(a, b, preferred_element_type=F32)


def dot_nt(a, b):
    return lax.dot_general(a, b, (((1,), (1,)), ((), ())), preferred_element_type=F32)


def dot_tn(a, b):
    return lax.dot_general(a, b, (((0,), (0,)), ((), ())), preferred_element_type=F32)


def lane_masks():
    lane = lax.broadcasted_iota(jnp.int32, (SEQ, LANES), 1)
    return lane % HD < HD // 2, lane < HD


def swap_halves(u, first):
    return jnp.where(first, pltpu.roll(u, LANES - HD // 2, 1), pltpu.roll(u, HD // 2, 1))


def twice(tile, index, low):
    turned = pltpu.roll(tile, HD, 1)
    return jnp.where(low, tile, turned) if index % 2 == 0 else jnp.where(low, turned, tile)


def causal_probs(query, key):
    scores = dot_nt(query, key) * SCALE
    rows = lax.broadcasted_iota(jnp.int32, scores.shape, 0)
    cols = lax.broadcasted_iota(jnp.int32, scores.shape, 1)
    scores = jnp.where(cols <= rows, scores, NEG_BIG)
    weights = jnp.exp(scores - jnp.max(scores, -1, keepdims=True))
    return weights * (1.0 / jnp.sum(weights, -1, keepdims=True))


def attend_sequence(cos, sin, load, kv_at, q_out, kv_out, o_out, at):
    first, low = lane_masks()

    def turn(u):
        return u * cos + swap_halves(u, first) * sin

    keys, vals_low, vals_high = [], [], []
    for tile in range(KV // 2):
        key = turn(load(kv_at + tile * LANES))
        val = load(kv_at + KV * HD + tile * LANES)
        kv_out[at, tile * LANES : (tile + 1) * LANES] = key.astype(BF16)
        kv_out[at, KV * HD + tile * LANES : KV * HD + (tile + 1) * LANES] = val.astype(BF16)
        for index in (0, 1):
            keys.append(twice(key, index, low).astype(BF16))
            both = twice(val, index, low)
            vals_low.append(jnp.where(low, both, 0.0).astype(BF16))
            vals_high.append(jnp.where(low, 0.0, both).astype(BF16))
    for pair in range(H // 2):
        group = pair * LANES // (H // KV * HD)
        query = turn(load(pair * LANES))
        p_low = causal_probs(jnp.where(low, query, 0.0).astype(BF16), keys[group])
        p_high = causal_probs(jnp.where(low, 0.0, query).astype(BF16), keys[group])
        q_out[at, pair * LANES : (pair + 1) * LANES] = query.astype(BF16)
        o_out[at, pair * LANES : (pair + 1) * LANES] = (
            dot(p_low.astype(BF16), vals_low[group]) + dot(p_high.astype(BF16), vals_high[group])
        ).astype(BF16)


def attend_back_sequence(cos, sin, q_ref, kv_ref, da_ref, dqkv_out, at):
    first, low = lane_masks()

    def turn_back(u):
        return (u * cos - swap_halves(u, first) * sin).astype(BF16)

    pair_total = H // KV * HD // LANES
    width = H * HD
    held = {}
    for group in range(KV):
        tile_at = group // 2 * LANES
        key = twice(kv_ref[at, tile_at : tile_at + LANES].astype(F32), group, low)
        val_at = KV * HD + tile_at
        val = twice(kv_ref[at, val_at : val_at + LANES].astype(F32), group, low).astype(BF16)
        key_low = jnp.where(low, key, 0.0).astype(BF16)
        key_high = jnp.where(low, 0.0, key).astype(BF16)
        key = key.astype(BF16)
        dk = jnp.zeros((SEQ, LANES), F32)
        dv = jnp.zeros((SEQ, LANES), F32)
        for pair in range(group * pair_total, (group + 1) * pair_total):
            query = q_ref[at, pair * LANES : (pair + 1) * LANES].astype(F32)
            grad = da_ref[at, pair * LANES : (pair + 1) * LANES].astype(F32)
            dq = None
            for is_low in (True, False):
                if is_low:
                    query_h = jnp.where(low, query, 0.0).astype(BF16)
                    grad_h = jnp.where(low, grad, 0.0).astype(BF16)
                else:
                    query_h = jnp.where(low, 0.0, query).astype(BF16)
                    grad_h = jnp.where(low, 0.0, grad).astype(BF16)
                prob = causal_probs(query_h, key)
                grad_prob = dot_nt(grad_h, val)
                delta = jnp.sum(prob * grad_prob, -1, keepdims=True)
                ds = (prob * (grad_prob - delta) * SCALE).astype(BF16)
                term = dot(ds, key_low if is_low else key_high)
                dq = term if dq is None else dq + term
                dk = dk + dot_tn(ds, query_h)
                dv = dv + dot_tn(prob.astype(BF16), grad_h)
            dqkv_out[at, pair * LANES : (pair + 1) * LANES] = turn_back(dq)
        held[group] = (dk + pltpu.roll(dk, HD, 1), dv + pltpu.roll(dv, HD, 1))
    for tile in range(KV // 2):
        col = width + tile * LANES
        dk = jnp.where(low, held[2 * tile][0], held[2 * tile + 1][0])
        dv = jnp.where(low, held[2 * tile][1], held[2 * tile + 1][1])
        dqkv_out[at, col : col + LANES] = turn_back(dk)
        dqkv_out[at, col + KV * HD : col + KV * HD + LANES] = dv.astype(BF16)


def causal_probs_turned(key, query):
    scores = dot_nt(key, query) * SCALE
    rows = lax.broadcasted_iota(jnp.int32, scores.shape, 0)
    cols = lax.broadcasted_iota(jnp.int32, scores.shape, 1)
    scores = jnp.where(rows <= cols, scores, NEG_BIG)
    weights = jnp.exp(scores - jnp.max(scores, 0, keepdims=True))
    return weights * (1.0 / jnp.sum(weights, 0, keepdims=True))


def attend_back_group(cos, sin, group, q_ref, kv_ref, da_ref, dqkv_out, dkv_out, at):
    first, low = lane_masks()
    head_width = H // KV * HD
    mine = low == (group % 2 == 0)

    def both(tile):
        kept = jnp.where(mine, tile.astype(F32), 0.0)
        return kept + pltpu.roll(kept, HD, 1)

    tile = pl.ds(pl.multiple_of(group // 2 * LANES, LANES), LANES)
    val_tile = pl.ds(pl.multiple_of(KV * HD + group // 2 * LANES, LANES), LANES)
    key = both(kv_ref[at, tile])
    val = both(kv_ref[at, val_tile]).astype(BF16)
    key_low = jnp.where(low, key, 0.0).astype(BF16)
    key_high = jnp.where(low, 0.0, key).astype(BF16)
    key = key.astype(BF16)
    dk = jnp.zeros((SEQ, LANES), F32)
    dv = jnp.zeros((SEQ, LANES), F32)
    for pair in range(head_width // LANES):
        c = pl.ds(pl.multiple_of(group * head_width + pair * LANES, LANES), LANES)
        query = q_ref[at, c].astype(F32)
        grad = da_ref[at, c].astype(F32)
        dq = None
        for is_low in (True, False):
            pick = low if is_low else jnp.logical_not(low)
            query_h = jnp.where(pick, query, 0.0).astype(BF16)
            grad_h = jnp.where(pick, grad, 0.0).astype(BF16)
            prob = causal_probs_turned(key, query_h)
            grad_prob = dot_nt(val, grad_h)
            delta = jnp.sum(prob * grad_prob, 0, keepdims=True)
            ds = (prob * (grad_prob - delta) * SCALE).astype(BF16)
            term = dot_tn(ds, key_low if is_low else key_high)
            dq = term if dq is None else dq + term
            dk = dk + dot(ds, query_h)
            dv = dv + dot(prob.astype(BF16), grad_h)
        dqkv_out[at, c] = (dq * cos - swap_halves(dq, first) * sin).astype(BF16)
    dkv_out[at, tile] += jnp.where(mine, dk + pltpu.roll(dk, HD, 1), 0.0)
    dkv_out[at, val_tile] += jnp.where(mine, dv + pltpu.roll(dv, HD, 1), 0.0)


def attend_kernel(cos_ref, sin_ref, qkv_ref, q_out, kv_out, o_out):
    attend_sequence(
        cos_ref[...], sin_ref[...], lambda c: qkv_ref[:, c : c + LANES], H * HD, q_out, kv_out, o_out, slice(None)
    )


def attend_back_kernel(cos_ref, sin_ref, q_ref, kv_ref, da_ref, dqkv_out):
    attend_back_sequence(cos_ref[...], sin_ref[...], q_ref, kv_ref, da_ref, dqkv_out, slice(None))


def by_sequence(body, name, ins, widths):
    rows = ins[0].shape[0]
    spec = lambda w: pl.BlockSpec((SEQ, w), lambda i: (i, 0))
    return pl.pallas_call(
        body,
        grid=(rows // SEQ,),
        in_specs=[spec(a.shape[1]) for a in ins],
        out_specs=[spec(w) for w in widths],
        out_shape=[jax.ShapeDtypeStruct((rows, w), BF16) for w in widths],
        name=name,
    )(*ins)


def attend(cos, sin, qkv):
    return by_sequence(attend_kernel, "attend", (cos, sin, qkv), (H * HD, 2 * KV * HD, H * HD))


def attend_back(cos, sin, query, key_val, grad):
    return by_sequence(
        attend_back_kernel, "attend_back", (cos, sin, query, key_val, grad), (H * HD + 2 * KV * HD,)
    )[0]


def norm_scale(rows):
    return lax.rsqrt(jnp.mean(rows * rows, -1, keepdims=True) + NORM_EPS)


def norm_back(rows, gain, grad_normed):
    inv = norm_scale(rows)
    weighted = grad_normed * gain
    grad_gain = jnp.sum(grad_normed * rows * inv, 0)
    grad_rows = inv * weighted - rows * inv**3 * jnp.mean(weighted * rows, -1, keepdims=True)
    return grad_rows, grad_gain


def rope_tables(positions):
    half = jnp.arange(LANES, dtype=jnp.int32) % (HD // 2)
    inv_freq = 10000.0 ** (-(half.astype(F32) * 2.0 / HD))
    angles = positions.astype(F32)[:, None] * inv_freq[None, :]
    sign = jnp.where(jnp.arange(LANES) % HD < HD // 2, -1.0, 1.0).astype(F32)
    return jnp.cos(angles), jnp.sin(angles) * sign[None, :]


MESH = pl.DeviceIdType.MESH
KV_ROWS = 64
GAIN_ROWS = 16


class Links:
    def __init__(self):
        self.d, self.z = lax.axis_index("dp"), lax.axis_index("tensor")
        core, x, y = self.d % 2, self.d // 2 % 2, self.d // 4
        self.dc = self.d + 1 - 2 * core
        step_x, step_y = 2 - 4 * x, 4 - 8 * y
        self.dx, self.dy, self.dxy = self.d + step_x, self.d + step_y, self.d + step_x + step_y
        self.dcx, self.dcy, self.dcxy = self.dc + step_x, self.dc + step_y, self.dc + step_x + step_y

    def barrier(self, far=False):
        z = self.z
        sem = pltpu.get_barrier_semaphore()

        def greet(d, zz):
            pl.semaphore_signal(sem, inc=1, device_id=(d, zz), device_id_type=MESH)

        for d in (self.dx, self.dy, self.dc):
            greet(d, z)
        if far:
            for j in (1, 2, 3):
                greet(self.d, (z + j) % 4)
            pl.semaphore_wait(sem, 6)
            return
        pl.when(z > 0)(lambda: greet(self.d, z - 1))
        pl.when(z < 3)(lambda: greet(self.d, z + 1))
        pl.semaphore_wait(sem, 3 + (z + 2) // 3 + (5 - z) // 3)


class Sender:
    def __init__(self, links, send_sem, recv_sem):
        self.links, self.send_sem, self.recv_sem = links, send_sem, recv_sem

    def copy(self, src, dst, at, to):
        return pltpu.make_async_remote_copy(
            src_ref=src,
            dst_ref=dst,
            send_sem=self.send_sem.at[at],
            recv_sem=self.recv_sem.at[at],
            device_id=to,
            device_id_type=MESH,
        )

    def start(self, src, dst, at, to):
        self.copy(src, dst, at, to).start()

    def landed(self, region, at):
        self.copy(region, region, at, (self.links.dc, self.links.z)).wait_recv()

    def sent(self, region, at):
        self.copy(region, region, at, (self.links.dc, self.links.z)).wait_send()


class Spread:
    def __init__(self, sender, region, base):
        self.s, self.region, self.base = sender, region, base

    def own(self, p, src):
        k, r, b = self.s.links, self.region, self.base + 9 * p
        mine = r(k.d, p, None)
        self.s.start(src, mine, b, (k.dx, k.z))
        self.s.start(src, mine, b + 1, (k.dy, k.z))
        self.s.start(src, mine, b + 2, (k.dc, k.z))

    def near(self, p):
        k, r, b = self.s.links, self.region, self.base + 9 * p
        self.s.landed(r(k.dx, p, None), b)
        self.s.start(r(k.dx, p, 0), r(k.dx, p, 0), b + 3, (k.dy, k.z))
        self.s.start(r(k.dx, p, None), r(k.dx, p, None), b + 5, (k.dc, k.z))
        self.s.landed(r(k.dy, p, None), b + 1)
        self.s.start(r(k.dy, p, 1), r(k.dy, p, 1), b + 4, (k.dx, k.z))
        self.s.start(r(k.dy, p, None), r(k.dy, p, None), b + 6, (k.dc, k.z))

    def far(self, p):
        k, r, b = self.s.links, self.region, self.base + 9 * p
        for part in (0, 1):
            self.s.landed(r(k.dxy, p, part), b + 3 + part)
            self.s.start(r(k.dxy, p, part), r(k.dxy, p, part), b + 7 + part, (k.dc, k.z))

    def finish(self, p):
        k, r, b = self.s.links, self.region, self.base + 9 * p
        self.s.landed(r(k.dc, p, None), b + 2)
        self.s.landed(r(k.dcx, p, None), b + 5)
        self.s.landed(r(k.dcy, p, None), b + 6)
        for part in (0, 1):
            self.s.landed(r(k.dcxy, p, part), b + 7 + part)

    def drain(self, p):
        k, r, b = self.s.links, self.region, self.base + 9 * p
        for i in (0, 1, 2):
            self.s.sent(r(k.d, p, None), b + i)
        self.s.sent(r(k.dx, p, 0), b + 3)
        self.s.sent(r(k.dy, p, 1), b + 4)
        self.s.sent(r(k.dx, p, None), b + 5)
        self.s.sent(r(k.dy, p, None), b + 6)
        for part in (0, 1):
            self.s.sent(r(k.dxy, p, part), b + 7 + part)


class Line:
    def __init__(self, sender, region, base):
        self.s, self.region, self.base = sender, region, base

    def _send(self, src, p, way, step):
        k = self.s.links
        self.s.start(src, self.region(p), self.base + 2 * (step - 1) + way, (k.d, k.z + 1 - 2 * way))

    def own(self, src):
        z = self.s.links.z
        pl.when(z < 3)(lambda: self._send(src, z, 0, 1))
        pl.when(z > 0)(lambda: self._send(src, z, 1, 1))

    def each(self, step, action):
        z = self.s.links.z
        pl.when(z >= step)(lambda: action(z - step, 0))
        pl.when(z + step <= 3)(lambda: action(z + step, 1))

    def arrive(self, step, then=None):
        z = self.s.links.z

        def action(p, way):
            self.s.landed(self.region(p), self.base + 2 * (step - 1) + way)
            if step < 3:
                ahead = z < 3 if way == 0 else z > 0
                pl.when(ahead)(lambda: self._send(self.region(p), p, way, step + 1))
            if then is not None:
                then(p)

        self.each(step, action)

    def drain(self):
        z = self.s.links.z
        for step in (1, 2, 3):
            for way in (0, 1):
                came = z - (step - 1) if way == 0 else z + (step - 1)
                ok = jnp.logical_and(z < 3, z >= step - 1) if way == 0 else jnp.logical_and(z > 0, z <= 4 - step)
                pl.when(ok)(
                    functools.partial(self.s.sent, self.region(came), self.base + 2 * (step - 1) + way)
                )


def forward_kernel(
    x_ref, g_ref, cos_ref, sin_ref, wq_in, wk_in, wv_in, gain_in, wo_ref, wg_in, wu_in, wd_ref,
    wa_all, wo_all, gu_all, wd_all, n2_all, top_all, wqkv_all, hidden_all, dgu_all, out_all, dn2_land,
    q_all, kv_all, mid_all, n1_t_all, o_t_all, gain_out, dn2_out,
    q_out, kv_out, o_out, mid_out, att_ref, gu_ref, n1, qkv, w_buf, wkv_buf, gain_buf, wo_buf, n2, top,
    n2_rows, top_rows, gate_up, grad_hidden, hidden, dgu, dn2_sends, out_rows, relay,
    send_sem, recv_sem, local_sem,
):
    rows, width = x_ref.shape
    slot_width = att_ref.shape[1]
    block = width // 8
    links = Links()
    d, z = links.d, links.z
    s = Sender(links, send_sem, recv_sem)
    ff = wd_ref.shape[0]
    cut_a = att_ref.shape[0] // 32 * 16
    cuts_a = ((0, cut_a), (cut_a, att_ref.shape[0] - cut_a))

    def at_a(dd, p, part):
        if part is None:
            return wa_all.at[dd, p]
        return wa_all.at[dd, p, pl.ds(*cuts_a[part])]

    def at_b(dd, p, part):
        start, size = (0, slot_width) if part is None else (part * slot_width // 2, slot_width // 2)
        return wo_all.at[
            pl.ds(pl.multiple_of(p * slot_width + start, 16), size),
            pl.ds(pl.multiple_of(dd * block, 128), block),
        ]

    def at_gu(dd, p, part):
        start, size = (0, block) if part is None else (part * block // 2, block // 2)
        return gu_all.at[pl.ds(pl.multiple_of(dd * block + start, 16), size)]

    def at_wd(dd, p, part):
        start, size = (0, ff) if part is None else (part * ff // 2, ff // 2)
        return wd_all.at[pl.ds(start, size), pl.ds(pl.multiple_of(dd * block, 128), block)]

    def rows_of(ref):
        return lambda p: ref.at[pl.ds(pl.multiple_of(p * rows, 16), rows)]

    spread_a, spread_b = Spread(s, at_a, 0), Spread(s, at_b, 36)
    spread_gu, spread_wd = Spread(s, at_gu, 72), Spread(s, at_wd, 81)
    line_a = Line(s, lambda p: at_a(d, p, None), 90)
    line_b = Line(s, lambda p: at_b(d, p, None), 96)
    line_n, line_t = Line(s, rows_of(n2_all), 102), Line(s, rows_of(top_all), 108)

    def keep(src, dst, at):
        pltpu.make_async_copy(src, dst, local_sem.at[at]).start()

    def kept(src, dst, at):
        pltpu.make_async_copy(src, dst, local_sem.at[at]).wait()

    kv_at = pl.ds(block, KV_ROWS)
    shards = [
        (wq_in, att_ref.at[pl.ds(0, block)], 78),
        (wk_in, att_ref.at[kv_at, pl.ds(0, KV * HD)], 79),
        (wv_in, att_ref.at[kv_at, pl.ds(KV * HD, KV * HD)], 80),
        (gain_in, att_ref.at[pl.ds(block + KV_ROWS, GAIN_ROWS), pl.ds(0, LANES)], 81),
    ]
    ffs = [(wg_in, gu_ref.at[:, pl.ds(0, ff)], 82), (wu_in, gu_ref.at[:, pl.ds(ff, ff)], 83)]
    for shard in shards + ffs:
        keep(*shard)
    att_ref[block + KV_ROWS :, LANES:] = jnp.zeros((GAIN_ROWS, slot_width - LANES), BF16)
    links.barrier(far=True)
    for shard in shards:
        kept(*shard)

    line_a.own(att_ref)
    spread_a.own(z, att_ref)
    keep(att_ref, at_a(d, z, None), 0)
    keep(wo_ref, at_b(d, z, None), 1)
    keep(wd_ref, at_wd(d, 0, None), 3)
    top[...] = g_ref[...].astype(BF16)
    line_a.arrive(1, lambda p: spread_a.own(p, at_a(d, p, None)))
    spread_a.near(z)
    line_a.arrive(2, lambda p: spread_a.own(p, at_a(d, p, None)))
    line_b.own(wo_ref)
    line_a.each(1, lambda p, way: spread_a.near(p))
    spread_a.far(z)
    line_a.arrive(3, lambda p: spread_a.own(p, at_a(d, p, None)))
    line_b.arrive(1)
    line_a.each(2, lambda p, way: spread_a.near(p))
    line_a.each(1, lambda p, way: spread_a.far(p))
    line_a.each(3, lambda p, way: spread_a.near(p))
    spread_b.own(z, wo_ref)
    line_b.each(1, lambda p, way: spread_b.own(p, at_b(d, p, None)))
    line_b.arrive(2, lambda p: spread_b.own(p, at_b(d, p, None)))
    line_a.each(2, lambda p, way: spread_a.far(p))
    line_a.each(3, lambda p, way: spread_a.far(p))
    for shard in ffs:
        kept(*shard)
    keep(gu_ref, at_gu(d, 0, None), 2)
    line_b.arrive(3, lambda p: spread_b.own(p, at_b(d, p, None)))
    line_t.own(top)
    kept(att_ref, at_a(d, z, None), 0)
    for p in range(4):
        spread_a.finish(p)

    def kv_copy(dd, p):
        return wkv_buf.at[dd, p], wqkv_all.at[pl.ds(dd * block + p * KV_ROWS, KV_ROWS), pl.ds(width, 2 * KV * HD)]

    for p in range(4):
        for dd in range(8):
            pltpu.make_async_copy(
                wa_all.at[dd, p, pl.ds(0, block)], w_buf.at[p, pl.ds(dd * block, block)], local_sem.at[14 + 8 * p + dd]
            ).start()
    keep(wa_all.at[:, :, pl.ds(block, KV_ROWS)], wkv_buf, 8)
    keep(wa_all.at[:, :, pl.ds(block + KV_ROWS, GAIN_ROWS), pl.ds(0, LANES)], gain_buf, 9)
    kept(wa_all.at[:, :, pl.ds(block + KV_ROWS, GAIN_ROWS), pl.ds(0, LANES)], gain_buf, 9)
    low_row = lax.broadcasted_iota(jnp.int32, (GAIN_ROWS, LANES), 1) < HD
    for dd in range(8):
        for half in (0, 1):
            first = gain_buf[dd, 2 * half].astype(F32)
            second = pltpu.roll(gain_buf[dd, 2 * half + 1].astype(F32), HD, 1)
            at = dd * block + half * LANES
            gain_out[:, at : at + LANES] = jnp.where(low_row, first, second)[:8]
    x = x_ref[...]
    n1[...] = (x * norm_scale(x) * gain_out[0:1]).astype(BF16)
    for p in range(4):
        for dd in range(8):
            kept(wa_all.at[dd, p, pl.ds(0, block)], w_buf.at[p, pl.ds(dd * block, block)], 14 + 8 * p + dd)
        for c in range(0, slot_width, 256):
            qkv[:, p * slot_width + c : p * slot_width + c + 256] = dot(n1[...], w_buf[p, :, c : c + 256])
        keep(w_buf.at[p], wqkv_all.at[:, pl.ds(p * slot_width, slot_width)], 4 + p)
    kept(wa_all.at[:, :, pl.ds(block, KV_ROWS)], wkv_buf, 8)
    qkv[:, width:] = dot(n1[...], wkv_buf[...].reshape(width, 2 * KV * HD))
    for p in range(4):
        for dd in range(8):
            pltpu.make_async_copy(*kv_copy(dd, p), local_sem.at[46 + 8 * p + dd]).start()

    line_b_pieces = lambda action: [action(z)] + [line_b.each(i, lambda p, way: action(p)) for i in (1, 2, 3)]

    def sequence(i, carry):
        at = pl.ds(pl.multiple_of(i * SEQ, SEQ), SEQ)
        attend_sequence(
            cos_ref[at], sin_ref[at], lambda c: qkv[at, c : c + LANES], width, q_out, kv_out, o_out, at
        )

        @pl.when(i == 0)
        def _():
            line_b_pieces(spread_b.near)
            spread_gu.own(0, gu_ref)
            line_t.arrive(1)

        return carry

    lax.fori_loop(0, rows // SEQ, sequence, 0)
    line_b_pieces(spread_b.far)
    kept(wo_ref, at_b(d, z, None), 1)
    for p in range(4):
        spread_b.finish(p)
    keep(wo_all, wo_buf, 0)
    kept(wo_all, wo_buf, 0)

    def column(i, carry):
        at = pl.ds(pl.multiple_of(i * 256, 256), 256)
        mid_out[:, at] = x_ref[:, at] + dot(o_out[...], wo_buf[:, at])
        return carry

    lax.fori_loop(0, width // 256, column, 0)
    mid = mid_out[...]
    n2[...] = (mid * norm_scale(mid) * gain_out[1:2]).astype(BF16)

    line_n.own(n2)
    keep(n2, n2_all.at[pl.ds(pl.multiple_of(z * rows, 16), rows)], 8)
    keep(top, top_all.at[pl.ds(pl.multiple_of(z * rows, 16), rows)], 9)
    results = [(q_out, q_all, 84), (kv_out, kv_all, 85), (mid_out, mid_all, 86)]
    for result in results:
        keep(*result)
    turns = []
    for i, (src, buf, dst) in enumerate(((n1, out_rows, n1_t_all), (o_out, dn2_sends.at[0], o_t_all))):
        for b in range(8):
            part = pl.ds(b * block, block)
            buf[:, part] = jnp.transpose(src[:, part].astype(F32)).astype(BF16)
            turns.append((buf.at[:, part], dst.at[part], 87 + 8 * i + b))
            keep(*turns[-1])
    for p in range(4):
        kept(w_buf.at[p], wqkv_all.at[:, pl.ds(p * slot_width, slot_width)], 4 + p)
        for dd in range(8):
            kept(*kv_copy(dd, p), 46 + 8 * p + dd)
    kept(gu_ref, at_gu(d, 0, None), 2)
    kept(wd_ref, at_wd(d, 0, None), 3)
    kept(n2, n2_all.at[pl.ds(pl.multiple_of(z * rows, 16), rows)], 8)
    kept(top, top_all.at[pl.ds(pl.multiple_of(z * rows, 16), rows)], 9)
    spread_gu.near(0)
    spread_wd.own(0, wd_ref)
    line_n.arrive(1)
    spread_gu.far(0)
    spread_gu.finish(0)

    wide = 2 * ff
    pieces = [(c, min(slot_width, wide - c)) for c in range(0, wide, slot_width)]
    gu_piece = lambda i, c, n: (columns(gu_all, c, n), w_buf.at[i, :, pl.ds(0, n)])
    for i, (c, n) in enumerate(pieces):
        keep(*gu_piece(i, c, n), 14 + i)
    wd_vmem = wo_buf.at[pl.ds(0, ff)]
    for turn in turns + results:
        kept(*turn)
    across, opposite, beside = 2 - z // 2, 3 - 3 * (z // 2), z + 1 - 2 * (z % 2)
    ends, inner = z % 3 == 0, z % 3 != 0
    chunks = [(c, min(256, ff - c)) for c in range(0, ff, 256)]

    def project(slot, source):
        for c, n in pieces:
            for h in range(0, n, 256):
                gate_up[slot, :, c + h : c + h + 256] = dot(source[...], w_buf[c // slot_width, :, h : h + 256])

    rows_at = lambda p: pl.ds(pl.multiple_of(p * rows, 16), rows)
    for i, (c, n) in enumerate(pieces):
        kept(*gu_piece(i, c, n), 14 + i)
    project(1, n2)
    line_n.arrive(2)
    line_t.arrive(2)
    spread_wd.near(0)
    keep(n2_all.at[rows_at(across)], n2_rows, 0)
    kept(n2_all.at[rows_at(across)], n2_rows, 0)
    project(0, n2_rows)
    spread_wd.far(0)
    spread_wd.finish(0)
    keep(wd_all, wd_vmem, 20)
    kept(wd_all, wd_vmem, 20)

    def place_of(p):
        return (p - z + 4) % 4 - 1

    def send_dn2(i, p):
        s.start(dn2_sends.at[i], dn2_land.at[place_of(p)], 114 + place_of(p), (d, p))

    def half_of(ref, h):
        return columns(ref, h * (width // 2), width // 2)

    def opposite_half(h):
        return half_of(dn2_land.at[1], h), 115 + 4 * h

    def pass_on(h):
        s.landed(half_of(relay, h), 117 + h)

        def add(m):
            r = pl.ds(pl.multiple_of(m * 32, 32), 32)
            c = pl.ds(h * (width // 2), width // 2)
            dn2_sends[1, r, c] = (dn2_sends[1, r, c].astype(F32) + relay[r, c].astype(F32)).astype(BF16)

        loop(rows // 32, add)
        to, at = opposite_half(h)
        s.start(half_of(dn2_sends.at[1], h), to, at, (d, opposite))

    def feed(i):
        pl.when(i == 1)(lambda: line_n.arrive(3))
        second = (i + 2) // 3 - i // 2
        p = across * ((3 - i) // 3) + opposite * second + beside * (i // 2 - i // 3) + z * (i // 3)
        at = rows_at(p)
        slot = i // 3
        pl.when(i != 1)(lambda: keep(top_all.at[at], top_rows, 1))

        @pl.when(second + i // 2 - i // 3 == 1)
        def _():
            keep(n2_all.at[at], n2_rows, 0)
            kept(n2_all.at[at], n2_rows, 0)
            project(0, n2_rows)

        @pl.when(i == 1)
        def _():
            line_t.arrive(3)
            keep(top_all.at[at], top_rows, 1)

        kept(top_all.at[at], top_rows, 1)
        for c, n in chunks:
            grad_hidden[:, c : c + n] = dot_nt(top_rows[...], wo_buf[c : c + n])

        @pl.when(i > 0)
        def _():
            kept(hidden, hidden_all.at[at], 2)
            kept(dgu, dgu_all.at[at], 3)

        def act(m):
            r = pl.ds(pl.multiple_of(m * 16, 16), 16)
            for c, n in chunks:
                gate, up = gate_up[slot, r, c : c + n], gate_up[slot, r, ff + c : ff + c + n]
                grad = grad_hidden[r, c : c + n]
                sig = 1.0 / (1.0 + jnp.exp(-gate))
                silu = gate * sig
                hidden[r, c : c + n] = (silu * up).astype(BF16)
                dgu[r, c : c + n] = (grad * up * sig * (1.0 + gate * (1.0 - sig))).astype(BF16)
                dgu[r, ff + c : ff + c + n] = (grad * silu).astype(BF16)

        loop(rows // 16, act)
        pl.when(jnp.logical_and(i == 3, inner))(lambda: pass_on(1))
        keep(hidden, hidden_all.at[at], 2)
        keep(dgu, dgu_all.at[at], 3)

        def back(m):
            r = pl.ds(pl.multiple_of(m * 256, 256), 256)
            total = None
            for j, (c, n) in enumerate(pieces):
                term = dot_nt(dgu[:, c : c + n], w_buf[j, r, :n])
                total = term if total is None else total + term

            @pl.when(i < 3)
            def _():
                dn2_sends[i, :, r] = total.astype(BF16)

            @pl.when(i == 3)
            def _():
                dn2_out[:, r] = total

            for h in (0, 1):

                @pl.when(jnp.logical_and(jnp.logical_and(i == 1, m == 4 * h + 3), ends))
                def _():
                    s.start(half_of(dn2_sends.at[1], h), half_of(relay, h), 117 + h, (d, 1 + z // 3))

        loop(width // 256, back)

        @pl.when(i % 2 == 0)
        def _():
            send_dn2(i, p)


        pl.when(i > 0)(lambda: kept(out_rows, out_all.at[at], 7))

        def down(m):
            r = pl.ds(pl.multiple_of(m * 256, 256), 256)
            out_rows[:, r] = dot(hidden[...], wo_buf[:ff, r]).astype(BF16)

        loop(width // 256, down)
        keep(out_rows, out_all.at[at], 7)
        pl.when(jnp.logical_and(i == 2, inner))(lambda: pass_on(0))

    loop(4, feed)
    kept(hidden, hidden_all.at[pl.ds(0, rows)], 2)
    kept(dgu, dgu_all.at[pl.ds(0, rows)], 3)
    kept(out_rows, out_all.at[pl.ds(0, rows)], 7)

    def collect(region, at, h=None):
        s.landed(region, at)
        c = pl.ds(0, width) if h is None else pl.ds(h * (width // 2), width // 2)
        keep(region, n2_rows.at[:, c], 0)
        kept(region, n2_rows.at[:, c], 0)

        def add(m):
            r = pl.ds(pl.multiple_of(m * 32, 32), 32)
            dn2_out[r, c] += n2_rows[r, c].astype(F32)

        loop(rows // 32, add)

    pl.when(z >= 1)(lambda: collect(dn2_land.at[0], 114))
    pl.when(z <= 2)(lambda: collect(dn2_land.at[2], 116))
    pl.when(inner)(lambda: collect(dn2_land.at[1], 115))
    for h in (0, 1):
        to, at = opposite_half(h)
        pl.when(ends)(functools.partial(collect, to, at, h))
    for i, p in ((0, across), (2, beside)):
        s.sent(dn2_sends.at[i], 114 + place_of(p))
    for h in (0, 1):
        to, at = opposite_half(h)
        pl.when(ends)(functools.partial(s.sent, half_of(dn2_sends.at[1], h), 117 + h))
        pl.when(inner)(functools.partial(s.sent, half_of(dn2_sends.at[1], h), at))
    for p in range(4):
        spread_a.drain(p)
        spread_b.drain(p)
    spread_gu.drain(0)
    spread_wd.drain(0)
    for line in (line_a, line_b, line_n, line_t):
        line.drain()


def forward_stage(x, g, cos, sin, wq, wk, wv, gains, wo, wg, wu, wd):
    rows, width = x.shape
    slot_width = wq.shape[1]
    block = width // 8
    kv_width = 2 * KV * HD
    ff = wd.shape[0]
    vmem = pl.BlockSpec(memory_space=pltpu.VMEM)
    hbm = pl.BlockSpec(memory_space=pltpu.HBM)
    shape = jax.ShapeDtypeStruct
    outs = [
        (hbm, shape((8, 4, block + KV_ROWS + GAIN_ROWS, slot_width), BF16)),
        (hbm, shape((width, width), BF16)),
        (hbm, shape((width, 2 * ff), BF16)),
        (hbm, shape((ff, width), BF16)),
        (hbm, shape((4 * rows, width), BF16)),
        (hbm, shape((4 * rows, width), BF16)),
        (hbm, shape((width, width + kv_width), BF16)),
        (hbm, shape((4 * rows, ff), BF16)),
        (hbm, shape((4 * rows, 2 * ff), BF16)),
        (hbm, shape((4 * rows, width), BF16)),
        (hbm, shape((3, rows, width), BF16)),
        (hbm, shape((rows, width), BF16)),
        (hbm, shape((rows, kv_width), BF16)),
        (hbm, shape((rows, width), F32)),
        (hbm, shape((width, rows), BF16)),
        (hbm, shape((width, rows), BF16)),
        (vmem, shape((8, width), F32)),
        (vmem, shape((rows, width), F32)),
    ]
    return pl.pallas_call(
        forward_kernel,
        in_specs=[vmem] * 4 + [hbm] * 4 + [vmem] + [hbm] * 2 + [vmem],
        out_specs=[o[0] for o in outs],
        out_shape=[o[1] for o in outs],
        scratch_shapes=[
            pltpu.VMEM((rows, width), BF16),
            pltpu.VMEM((rows, kv_width), BF16),
            pltpu.VMEM((rows, width), BF16),
            pltpu.VMEM((rows, width), F32),
            pltpu.VMEM((block + KV_ROWS + GAIN_ROWS, slot_width), BF16),
            pltpu.VMEM((block, 2 * ff), BF16),
            pltpu.VMEM((rows, width), BF16),
            pltpu.VMEM((rows, width + kv_width), F32),
            pltpu.VMEM((-(-2 * ff // slot_width), width, slot_width), BF16),
            pltpu.VMEM((8, 4, KV_ROWS, kv_width), BF16),
            pltpu.VMEM((8, 4, GAIN_ROWS, LANES), BF16),
            pltpu.VMEM((width, width), BF16),
            pltpu.VMEM((rows, width), BF16),
            pltpu.VMEM((rows, width), BF16),
            pltpu.VMEM((rows, width), BF16),
            pltpu.VMEM((rows, width), BF16),
            pltpu.VMEM((2, rows, 2 * ff), F32),
            pltpu.VMEM((rows, ff), F32),
            pltpu.VMEM((rows, ff), BF16),
            pltpu.VMEM((rows, 2 * ff), BF16),
            pltpu.VMEM((3, rows, width), BF16),
            pltpu.VMEM((rows, width), BF16),
            pltpu.VMEM((rows, width), BF16),
            pltpu.SemaphoreType.DMA((120,)),
            pltpu.SemaphoreType.DMA((120,)),
            pltpu.SemaphoreType.DMA((103,)),
        ],
        compiler_params=pltpu.CompilerParams(
            collective_id=0, has_side_effects=True, vmem_limit_bytes=65000 * 1024
        ),
        name="forward",
    )(x, g, cos, sin, wq, wk, wv, gains, wo, wg, wu, wd)


def loop(count, body):
    def step(i, carry):
        body(i)
        return carry

    lax.fori_loop(0, count, step, 0)


class Local:
    def __init__(self, sem):
        self.sem, self.next = sem, 0

    def start(self, src, dst):
        copy = pltpu.make_async_copy(src, dst, self.sem.at[self.next])
        self.next += 1
        copy.start()
        return copy

    def load(self, src, dst):
        self.start(src, dst).wait()


class Reduce:
    def __init__(self, sender, compute, base, sends, kept, land, halves):
        self.s, self.compute, self.base = sender, compute, base
        self.sends, self.kept, self.land, self.halves = sends, kept, land, halves

    def half(self, ref, part):
        return ref.at[pl.ds(*self.halves[part])]

    def place(self, i):
        if i < 4:
            return self.land.at[i]
        return self.half(self.land.at[4 + (i - 4) // 2], i % 2)

    def partner(self, i):
        k = self.s.links
        count = self.sends.shape[0]
        if i >= count:
            self.s.sent(self.sends.at[i % count], self.base + i - count)
        self.compute((k.dcxy, k.dcx, k.dcy, k.dc)[i], None, self.sends.at[i % count])
        self.s.start(self.sends.at[i % count], self.place(i), self.base + i, (k.dc, k.z))

    def own(self, i):
        k, b = self.s.links, self.base
        to_x, to_y = (k.dx, k.z), (k.dy, k.z)
        self.s.landed(self.place(i), b + i)
        kept = self.kept.at[i]
        self.compute((k.dxy, k.dx, k.dy, k.d)[i], self.land.at[i], kept)
        if i == 0:
            self.s.start(self.half(kept, 0), self.place(4), b + 4, to_x)
            self.s.start(self.half(kept, 1), self.place(7), b + 7, to_y)
        elif i == 1:
            self.s.start(self.half(kept, 0), self.place(6), b + 6, to_x)
        elif i == 2:
            self.s.start(self.half(kept, 1), self.place(5), b + 5, to_y)

    def first(self):
        self.partner(0)
        for i in range(3):
            self.partner(i + 1)
            self.own(i)
        self.own(3)

    def add(self, i, part, at):
        self.s.landed(self.place(at), self.base + at)
        start, size = self.halves[part]
        from_start = self.halves[at % 2][0] if at < 8 else self.halves[at - 8][0]
        slot = 4 + (at - 4) // 2
        step = 32 if size % 32 == 0 else 16

        def rows(n):
            r = pl.ds(pl.multiple_of(start + n * step, 16), step)
            g = pl.ds(pl.multiple_of(from_start + n * step, 16), step)
            self.kept[i, r] = (self.kept[i, r].astype(F32) + self.land[slot, g].astype(F32)).astype(BF16)

        loop(size // step, rows)

    def second(self):
        k, b = self.s.links, self.base
        self.add(2, 0, 4)
        self.s.start(self.half(self.kept.at[2], 0), self.place(8), b + 8, (k.dy, k.z))
        self.add(1, 1, 7)
        self.s.start(self.half(self.kept.at[1], 1), self.place(9), b + 9, (k.dx, k.z))

    def third(self):
        self.add(3, 0, 6)
        self.add(3, 1, 5)

    def last(self):
        self.add(3, 0, 8)
        self.add(3, 1, 9)

    def drain(self):
        b, kept = self.base, self.kept
        count = self.sends.shape[0]
        for i in range(4 - count, 4):
            self.s.sent(self.sends.at[i % count], b + i)
        self.s.sent(self.half(kept.at[0], 0), b + 4)
        self.s.sent(self.half(kept.at[2], 1), b + 5)
        self.s.sent(self.half(kept.at[1], 0), b + 6)
        self.s.sent(self.half(kept.at[0], 1), b + 7)
        self.s.sent(self.half(kept.at[2], 0), b + 8)
        self.s.sent(self.half(kept.at[1], 1), b + 9)


class LineSum:
    def __init__(self, sender, local, part, sends, land, base):
        self.s, self.part, self.sends = sender, part, sends
        self.land, self.base = land, base
        self.rows = sends.shape[1]
        self.sem, self.first = local.sem, local.next
        local.next += 7

    def rows_of(self, t):
        return self.part.at[pl.ds(pl.multiple_of(t * self.rows, 16), self.rows)]

    def fetch(self, holds, slot, at):
        return pltpu.make_async_copy(self.rows_of(holds), self.sends.at[slot], self.sem.at[self.first + at])

    def begin(self):
        for s in (1, 2, 3):
            for sends, slot, place, holds, _, _ in self.ways(s):
                pl.when(sends)(lambda: self.fetch(holds, slot, place).start())
        self.fetch(self.s.links.z, 3, 6).start()
        self.step(1)

    def add(self, into, at):
        self.s.landed(self.land.at[at], self.base + at)

        def rows(n):
            r = pl.ds(pl.multiple_of(n * 32, 32), 32)
            self.sends[into, r] = (self.sends[into, r].astype(F32) + self.land[at, r].astype(F32)).astype(BF16)

        loop(self.rows // 32, rows)

    def ways(self, s):
        z = self.s.links.z
        right = (z <= s - 1, s - 1 - z, 2 * (s - 1), z + 4 - s, z >= 1, z + 1)
        left = (z >= 4 - s, s - 1, 2 * (s - 1) + 1, z - 4 + s, z <= 2, z - 1)
        return right, left

    def step(self, s):
        for sends, slot, place, holds, received, to in self.ways(s):

            @pl.when(sends)
            def _():
                self.fetch(holds, slot, place).wait()
                if s > 1:
                    pl.when(received)(lambda: self.add(slot, place - 2))
                self.s.start(self.sends.at[slot], self.land.at[place], self.base + place, (self.s.links.d, to))

    def finish(self, write):
        z = self.s.links.z
        self.fetch(z, 3, 6).wait()
        pl.when(z >= 1)(lambda: self.add(3, 4))
        pl.when(z <= 2)(lambda: self.add(3, 5))

        def rows(n):
            r = pl.ds(pl.multiple_of(n * 32, 32), 32)
            write(r, self.sends[3, r].astype(F32))

        loop(self.rows // 32, rows)

    def drain(self):
        for s in (1, 2, 3):
            for sends, slot, place, _, _, _ in self.ways(s):
                pl.when(sends)(functools.partial(self.s.sent, self.sends.at[slot], self.base + place))


def stream(local, count, source, bufs, body):
    first = local.next
    local.next += 2

    def copy(n, slot):
        return pltpu.make_async_copy(source(n), bufs.at[slot], local.sem.at[first + slot])

    copy(0, 0).start()

    def step(n):
        slot = n % 2
        copy(n, slot).wait()

        @pl.when(n + 1 < count)
        def _():
            copy(n + 1, 1 - slot).start()

        body(n, bufs.at[slot])

    loop(count, step)


def turned(ref):
    return jnp.transpose(ref[...].astype(F32)).astype(BF16)


def columns(ref, start, size):
    return ref.at[:, pl.ds(pl.multiple_of(start, 128), size)]


class Feeder:
    def __init__(self, local, source, bufs, block, dests):
        self.source, self.bufs, self.block, self.dests = source, bufs, block, dests
        self.sem, self.first, self.n = local.sem, local.next, 0
        local.next += 2
        self._copy(0).start()

    def _copy(self, n):
        return pltpu.make_async_copy(
            columns(self.source, self.dests[n] * self.block, self.block),
            self.bufs.at[n % 2],
            self.sem.at[self.first + n % 2],
        )

    def __call__(self, dest):
        n = self.n
        self.n += 1
        self._copy(n).wait()
        if n + 1 < len(self.dests):
            self._copy(n + 1).start()
        return self.bufs.at[n % 2]


def order_of(k):
    partner, own = (k.dcxy, k.dcx, k.dcy, k.dc), (k.dxy, k.dx, k.dy, k.d)
    return [partner[0], partner[1], own[0], partner[2], own[1], partner[3], own[2], own[3]]


def row_blocks(pick, left, right):
    width = right.shape[1]

    def compute(dest, add, out):
        left[...] = turned(pick(dest))

        def chunk(n):
            c = pl.ds(pl.multiple_of(n * 256, 256), 256)
            total = dot(left[...], right[:, c])
            if add is not None:
                total = total + add[:, c].astype(F32)
            out[:, c] = total.astype(BF16)

        loop(width // 256, chunk)

    return compute


def column_blocks(left, pick, chunks):
    size = left.shape[0] // chunks

    def compute(dest, add, out):
        picked = pick(dest)

        def chunk(n):
            r = pl.ds(pl.multiple_of(n * size, 16), size)
            total = dot(left[r], picked[...])
            if add is not None:
                total = total + add[r].astype(F32)
            out[r] = total.astype(BF16)

        loop(chunks, chunk)

    return compute


class Chunk:
    def __init__(self, sender, compute, sends, kept, land, base):
        self.s, self.compute, self.sends = sender, compute, sends
        self.kept, self.land, self.base = kept, land, base
        self.half = kept.shape[2] // 2

    def views(self, n):
        kept, land, h = self.kept.at[n], self.land.at[n], self.half
        top, low = pl.ds(0, h), pl.ds(h, h)
        return {
            "x1": (kept.at[pl.ds(0, 2), top], land.at[pl.ds(4, 2), top]),
            "y1": (kept.at[pl.ds(1, 2), low], land.at[pl.ds(4, 2), low]),
            "y2": (kept.at[2, top], land.at[6, top]),
            "x2": (kept.at[0, low], land.at[6, low]),
        }

    def partner(self, n):
        k = self.s.links
        slot = n % self.sends.shape[0]
        if n != slot:
            self.s.sent(self.sends.at[slot], self.base + 5 * (n - self.sends.shape[0]))
        for i, dest in enumerate((k.dcx, k.dcxy, k.dcy, k.dc)):
            self.compute(n, dest, None, self.sends.at[slot, i])
        self.s.start(self.sends.at[slot], self.land.at[n, pl.ds(0, 4)], self.base + 5 * n, (k.dc, k.z))

    def own(self, n):
        k, b, v = self.s.links, self.base + 5 * n, self.views(n)
        self.s.landed(self.land.at[n, pl.ds(0, 4)], b)
        for i, dest in enumerate((k.dx, k.dxy, k.dy, k.d)):
            self.compute(n, dest, self.land.at[n, i], self.kept.at[n, i])
        self.s.start(*v["x1"], b + 1, (k.dx, k.z))
        self.s.start(*v["y1"], b + 2, (k.dy, k.z))

    def add(self, n, i, start, got):
        kept, land = self.kept, self.land

        def rows(m):
            r = pl.ds(pl.multiple_of(start + m * 32, 32), 32)
            kept[n, i, r] = (kept[n, i, r].astype(F32) + land[n, got, r].astype(F32)).astype(BF16)

        loop(self.half // 32, rows)

    def second(self, n):
        k, b, v = self.s.links, self.base + 5 * n, self.views(n)
        self.s.landed(v["x1"][1], b + 1)
        self.add(n, 2, 0, 5)
        self.s.start(*v["y2"], b + 3, (k.dy, k.z))
        self.s.landed(v["y1"][1], b + 2)
        self.add(n, 0, self.half, 4)
        self.s.start(*v["x2"], b + 4, (k.dx, k.z))
        self.add(n, 3, 0, 4)
        self.add(n, 3, self.half, 5)

    def last(self, n):
        b, v = self.base + 5 * n, self.views(n)
        self.s.landed(v["y2"][1], b + 3)
        self.add(n, 3, 0, 6)
        self.s.landed(v["x2"][1], b + 4)
        self.add(n, 3, self.half, 6)

    def drain(self):
        for n in range(self.kept.shape[0]):
            b, v = self.base + 5 * n, self.views(n)
            if n + self.sends.shape[0] >= self.kept.shape[0]:
                self.s.sent(self.sends.at[0], b)
            for at, name in enumerate(("x1", "y1", "y2", "x2")):
                self.s.sent(v[name][0], b + 1 + at)


class Spread4:
    def __init__(self, sender, pick, land, base):
        self.s, self.pick, self.land, self.base = sender, pick, land, base

    def send(self):
        k = self.s.links
        for j in (1, 2, 3):
            to = (k.z + j) % 4
            self.s.start(self.pick(to), self.land.at[j - 1], self.base + j - 1, (k.d, to))

    def landed(self):
        for j in range(3):
            self.s.landed(self.land.at[j], self.base + j)

    def drain(self):
        z = self.s.links.z
        for j in (1, 2, 3):
            self.s.sent(self.pick((z + j) % 4), self.base + j - 1)


def norm_back_rows(rows_ref, at, gain, grad_normed):
    rows = rows_ref[at]
    inv = norm_scale(rows)
    weighted = grad_normed * gain
    scaled = grad_normed * rows * inv
    grad_rows = inv * weighted - rows * (inv * inv * inv) * jnp.mean(weighted * rows, -1, keepdims=True)
    return grad_rows, scaled


def halves(size):
    return (0, size // 2), (size // 2, size // 2)


def add_gain(gain_part, block, row, scaled):
    for b in range(8):
        total = jnp.sum(scaled[:, b * block : (b + 1) * block], 0, keepdims=True)
        gain_part[b % 2, b // 2 % 2 * 2 + b // 4, row : row + 1] += total


def transpose_into(src, dst):
    def part(n):
        c = pl.ds(pl.multiple_of(n * 128, 128), 128)
        dst[c] = jnp.transpose(src[:, c].astype(F32)).astype(BF16)

    loop(src.shape[1] // 128, part)


def row_chunk(ref):
    return lambda n: ref.at[pl.ds(pl.multiple_of(n * 256, 256), 256)]


def attention_back_kernel(
    gain_ref, cos_ref, sin_ref, dn2_in, mid_in, g_in, q_in, kv_in, att_in,
    part_ref, hidden_ref, top_ref, wo_ref,
    out_ref, gain_part, gd_out, go_out, gm_all, dqkv_all,
    dn2_ref, mid_ref, g_ref, q_ref, kv_ref, att_t, gm_out, dqkv, mid_bf, da, dkv, w_chunk, top_cols, hidden_cols, hidden_t,
    d_sends, d_kept, d_land, o_sends, o_kept, o_land, line_sends, line_land,
    send_sem, recv_sem, local_sem,
):
    rows, width = mid_ref.shape
    block = width // 8
    ff = hidden_t.shape[0]
    links = Links()
    s = Sender(links, send_sem, recv_sem)
    local = Local(local_sem)
    top_feed = Feeder(local, top_ref, top_cols, block, order_of(links))
    links.barrier()
    line = LineSum(s, local, part_ref, line_sends, line_land, 20)
    line.begin()
    ins = [
        local.start(src, dst)
        for src, dst in (
            (dn2_in, dn2_ref), (mid_in, mid_ref), (g_in, g_ref), (att_in, att_t), (q_in, q_ref), (kv_in, kv_ref)
        )
    ]

    def turn_hidden(n, buf):
        hidden_t[pl.ds(pl.multiple_of(n * 128, 128), 128)] = turned(buf)

    stream(local, ff // 128, lambda n: columns(hidden_ref, n * 128, 128), hidden_cols, turn_hidden)
    grad_d = Reduce(s, column_blocks(hidden_t, top_feed, 4), 0, d_sends, d_kept, d_land, halves(ff))
    grad_d.first()
    line.step(2)

    gain_part[...] = jnp.zeros_like(gain_part)
    dkv[...] = jnp.zeros_like(dkv)
    step = 32

    def middle(n):
        r = pl.ds(pl.multiple_of(n * step, step), step)
        grad_rows, scaled = norm_back_rows(mid_ref, r, gain_ref[1:2], dn2_ref[r])
        grad = g_ref[r] + grad_rows
        gm_out[r] = grad
        mid_bf[r] = grad.astype(BF16)
        add_gain(gain_part, block, 1, scaled)

    for copy in ins:
        copy.wait()
    loop(rows // step, middle)
    to_gm = local.start(gm_out, gm_all)
    pick_mid = lambda dest: columns(mid_bf, dest * block, block)
    grad_o = Reduce(s, column_blocks(att_t, pick_mid, 4), 10, o_sends, o_kept, o_land, halves(width))
    grad_o.first()
    grad_d.second()

    def attended(n, buf):
        da[:, pl.ds(pl.multiple_of(n * 256, 256), 256)] = dot_nt(mid_bf[...], buf[...]).astype(BF16)

    stream(local, width // 256, row_chunk(wo_ref), w_chunk, attended)
    line.step(3)

    def group_step(n):
        def sequence(i):
            at = pl.ds(pl.multiple_of(i * SEQ, SEQ), SEQ)
            attend_back_group(cos_ref[at], sin_ref[at], n, q_ref, kv_ref, da, dqkv, dkv, at)

        loop(rows // SEQ, sequence)
        pl.when(n == 1)(grad_o.second)
        pl.when(n == 2)(grad_d.third)
        pl.when(n == 2)(grad_d.last)
        pl.when(n == 3)(grad_o.third)

    loop(KV, group_step)
    to_down = local.start(d_kept.at[3], gd_out)

    def key_value(i):
        at = pl.ds(pl.multiple_of(i * SEQ, SEQ), SEQ)
        first, _ = lane_masks()
        for tile in range(KV // 2):
            c = tile * LANES
            u = dkv[at, c : c + LANES]
            dqkv[at, width + c : width + c + LANES] = (
                u * cos_ref[at] - swap_halves(u, first) * sin_ref[at]
            ).astype(BF16)
        dqkv[at, width + KV * HD :] = dkv[at, KV * HD :].astype(BF16)

    loop(rows // SEQ, key_value)
    to_dqkv = local.start(dqkv, dqkv_all)
    grad_o.last()
    to_out = local.start(o_kept.at[3], go_out)

    def write(r, total):
        out_ref[r] = mid_ref[r] + total

    line.finish(write)
    for copy in (to_down, to_out, to_gm, to_dqkv):
        copy.wait()
    grad_o.drain()
    grad_d.drain()
    line.drain()


def attention_back(gains, cos, sin, dn2, mid, g, query, key_val, attended_t, part, hidden, top, wo):
    rows, width = mid.shape
    block, ff = width // 8, hidden.shape[1]
    kv_width = 2 * KV * HD
    vmem = pl.BlockSpec(memory_space=pltpu.VMEM)
    hbm = pl.BlockSpec(memory_space=pltpu.HBM)
    shape = jax.ShapeDtypeStruct
    return pl.pallas_call(
        attention_back_kernel,
        in_specs=[vmem] * 3 + [hbm] * 10,
        out_specs=[vmem] * 2 + [hbm] * 4,
        out_shape=[
            shape((rows, width), F32),
            shape((2, 4, 8, block), F32),
            shape((ff, block), BF16),
            shape((width, block), BF16),
            shape((rows, width), F32),
            shape((rows, width + kv_width), BF16),
        ],
        scratch_shapes=[
            pltpu.VMEM((rows, width), F32),
            pltpu.VMEM((rows, width), F32),
            pltpu.VMEM((rows, width), F32),
            pltpu.VMEM((rows, width), BF16),
            pltpu.VMEM((rows, kv_width), BF16),
            pltpu.VMEM((width, rows), BF16),
            pltpu.VMEM((rows, width), F32),
            pltpu.VMEM((rows, width + kv_width), BF16),
            pltpu.VMEM((rows, width), BF16),
            pltpu.VMEM((rows, width), BF16),
            pltpu.VMEM((rows, kv_width), F32),
            pltpu.VMEM((2, 256, width), BF16),
            pltpu.VMEM((2, 4 * rows, block), BF16),
            pltpu.VMEM((2, 4 * rows, 128), BF16),
            pltpu.VMEM((ff, 4 * rows), BF16),
            pltpu.VMEM((2, ff, block), BF16),
            pltpu.VMEM((4, ff, block), BF16),
            pltpu.VMEM((7, ff, block), BF16),
            pltpu.VMEM((2, width, block), BF16),
            pltpu.VMEM((4, width, block), BF16),
            pltpu.VMEM((7, width, block), BF16),
            pltpu.VMEM((4, rows, width), BF16),
            pltpu.VMEM((6, rows, width), BF16),
            pltpu.SemaphoreType.DMA((26,)),
            pltpu.SemaphoreType.DMA((26,)),
            pltpu.SemaphoreType.DMA((40,)),
        ],
        compiler_params=pltpu.CompilerParams(
            collective_id=1, has_side_effects=True, vmem_limit_bytes=65000 * 1024
        ),
        name="attention_back",
    )(gains, cos, sin, dn2, mid, g, query, key_val, attended_t, part, hidden, top, wo)


def project_back_kernel(
    gain_ref, gain_in, x_in, dqkv_in, n1_in, gm_ref, n2_ref, dgu_ref, wqkv_ref, go_in,
    gq_out, gkv_out, go_out, gain_out, grad_in_all, ggu_out,
    x_ref, dqkv, grad_in_out, dn1, n1_t, w_chunk, dgu, n2_cols, left, sends, kept, land,
    row_sends, row_kept, row_land, o_block, gain_part, gain_land, z_q, z_kv, z_o,
    send_sem, recv_sem, local_sem,
):
    rows, width = x_ref.shape
    block, slot = width // 8, width // 4
    kv_width = 2 * KV * HD
    step = 32
    links = Links()
    d, z = links.d, links.z
    s = Sender(links, send_sem, recv_sem)
    local = Local(local_sem)
    firsts = [local.start(dqkv_in, dqkv), local.start(n1_in, n1_t)]
    n2_feed = Feeder(local, n2_ref, n2_cols, block, order_of(links))
    fetch_dgu = local.start(dgu_ref, dgu)
    fetch_x = local.start(x_in, x_ref)
    fetch_o = local.start(go_in, o_block)
    fetch_gm = local.start(gm_ref, grad_in_out)
    links.barrier(far=True)
    fetch_o.wait()
    send_o = Spread4(s, lambda p: o_block.at[pl.ds(pl.multiple_of(p * slot, 16), slot)], z_o, 35)
    send_o.send()
    gain_part[...] = gain_in[...]

    for copy in firsts:
        copy.wait()

    group_of = lambda n: (z + n) % 4

    def row_compute(n, dest, add, out):
        picked = n1_t[pl.ds(pl.multiple_of(dest * block, block), block)]
        start = width if n == 0 else group_of(n) * slot
        for c in range(0, slot, 256):
            total = dot(picked, dqkv[:, pl.ds(pl.multiple_of(start + c, 256), 256)])
            if add is not None:
                total = total + add[:, c : c + 256].astype(F32)
            out[:, c : c + 256] = total.astype(BF16)

    row = Chunk(s, row_compute, row_sends, row_kept, row_land, 10)
    row.partner(0)
    for n in range(4):
        row.partner(n + 1)
        row.own(n)
    row.own(4)

    send_kv = Spread4(
        s, lambda p: row_kept.at[0, 3, pl.ds(pl.multiple_of(p * KV_ROWS, 16), KV_ROWS)], z_kv, 38
    )

    def final_q(n):
        row.last(n)
        s.start(row_kept.at[n, 3], z_q.at[n - 1], 40 + n, (d, group_of(n)))

    fetch_dgu.wait()
    grads = Reduce(s, row_blocks(n2_feed, left, dgu), 0, sends, kept, land, halves(block))
    grads.partner(0)
    row.second(0)
    grads.partner(1)
    row.second(1)
    row.second(2)
    grads.own(0)
    row.second(3)
    row.second(4)
    grads.partner(2)
    row.last(0)
    send_kv.send()
    final_q(1)
    grads.own(1)
    final_q(2)
    grads.partner(3)
    final_q(3)
    grads.own(2)
    row.last(4)
    grads.own(3)
    grads.second()

    def projected(n, buf):
        dn1[:, pl.ds(pl.multiple_of(n * 256, 256), 256)] = dot_nt(dqkv[...], buf[...])

    stream(local, width // 256, row_chunk(wqkv_ref), w_chunk, projected)
    fetch_gm.wait()
    fetch_x.wait()

    def inward(n):
        r = pl.ds(pl.multiple_of(n * step, step), step)
        grad_rows, scaled = norm_back_rows(x_ref, r, gain_ref[0:1], dn1[r])
        grad_in_out[r] += grad_rows
        add_gain(gain_part, block, 0, scaled)

    loop(rows // step, inward)
    to_in = local.start(grad_in_out, grad_in_all)
    grads.third()
    core, x_at, y_at = d % 2, d // 2 % 2, d // 4
    s.start(gain_part.at[1 - core], gain_land.at[pl.ds(0, 4)], 44, (links.dc, z))
    s.landed(gain_land.at[pl.ds(0, 4)], 44)
    gain_part[core] += gain_land[0:4]
    other_x = pl.multiple_of(2 - 2 * x_at, 2)
    s.start(gain_part.at[core, pl.ds(other_x, 2)], gain_land.at[pl.ds(4, 2)], 45, (links.dx, z))
    send_o.landed()

    def out_rows(n):
        r = pl.ds(pl.multiple_of(n * 16, 16), 16)
        mine = pl.ds(pl.multiple_of(z * slot + n * 16, 16), 16)
        go_out[r] = (
            o_block[mine].astype(F32) + z_o[0, r].astype(F32) + z_o[1, r].astype(F32) + z_o[2, r].astype(F32)
        )

    loop(slot // 16, out_rows)
    for n in range(3):
        s.landed(z_q.at[n], 41 + n)

    def query_rows(n):
        r = pl.ds(pl.multiple_of(n * 16, 16), 16)
        gq_out[r] = (
            row_kept[4, 3, r].astype(F32) + z_q[0, r].astype(F32) + z_q[1, r].astype(F32) + z_q[2, r].astype(F32)
        )

    loop(block // 16, query_rows)
    send_kv.landed()
    mine_kv = pl.ds(pl.multiple_of(z * KV_ROWS, 16), KV_ROWS)
    gkv_out[...] = row_kept[0, 3, mine_kv].astype(F32) + (
        z_kv[0].astype(F32) + z_kv[1].astype(F32) + z_kv[2].astype(F32)
    )
    s.landed(gain_land.at[pl.ds(4, 2)], 45)
    mine_x = 2 * x_at
    gain_part[core, pl.ds(mine_x, 2)] += gain_land[4:6]
    s.start(gain_part.at[core, mine_x + 1 - y_at], gain_land.at[6], 46, (links.dy, z))
    s.landed(gain_land.at[6], 46)
    gain_part[core, mine_x + y_at] += gain_land[6]
    send_g = Spread4(s, lambda p: gain_part.at[core, mine_x + y_at], gain_land.at[pl.ds(7, 3)], 47)
    send_g.send()
    grads.last()
    to_gu = local.start(kept.at[3], ggu_out)
    send_g.landed()
    gain = gain_part[core, mine_x + y_at] + gain_land[7] + gain_land[8] + gain_land[9]
    gain_out[...] = pltpu.roll(gain, (4 - z) % 4 * (block // 4), 1)
    to_gu.wait()
    to_in.wait()
    for unit in (grads, row, send_o, send_kv, send_g):
        unit.drain()
    for n in range(3):
        s.sent(row_kept.at[n + 1, 3], 41 + n)
    s.sent(gain_part.at[1 - core], 44)
    s.sent(gain_part.at[core, pl.ds(other_x, 2)], 45)
    s.sent(gain_part.at[core, mine_x + 1 - y_at], 46)


def project_back(gains, gain_in, x, dqkv, normed_t, gm, n2, dgu, wqkv, grad_o):
    rows, width = x.shape
    block, slot = width // 8, width // 4
    kv_width = 2 * KV * HD
    wide = dgu.shape[1]
    vmem = pl.BlockSpec(memory_space=pltpu.VMEM)
    hbm = pl.BlockSpec(memory_space=pltpu.HBM)
    shape = jax.ShapeDtypeStruct
    return pl.pallas_call(
        project_back_kernel,
        in_specs=[vmem] * 2 + [hbm] * 8,
        out_specs=[vmem] * 4 + [hbm] * 2,
        out_shape=[
            shape((block, slot), F32),
            shape((KV_ROWS, kv_width), F32),
            shape((slot, block), F32),
            shape((8, block), F32),
            shape((rows, width), F32),
            shape((block, wide), BF16),
        ],
        scratch_shapes=[
            pltpu.VMEM((rows, width), F32),
            pltpu.VMEM((rows, width + kv_width), BF16),
            pltpu.VMEM((rows, width), F32),
            pltpu.VMEM((rows, width), F32),
            pltpu.VMEM((width, rows), BF16),
            pltpu.VMEM((2, 256, width + kv_width), BF16),
            pltpu.VMEM((4 * rows, wide), BF16),
            pltpu.VMEM((2, 4 * rows, block), BF16),
            pltpu.VMEM((block, 4 * rows), BF16),
            pltpu.VMEM((2, block, wide), BF16),
            pltpu.VMEM((4, block, wide), BF16),
            pltpu.VMEM((7, block, wide), BF16),
            pltpu.VMEM((3, 4, block, slot), BF16),
            pltpu.VMEM((5, 4, block, slot), BF16),
            pltpu.VMEM((5, 7, block, slot), BF16),
            pltpu.VMEM((width, block), BF16),
            pltpu.VMEM((2, 4, 8, block), F32),
            pltpu.VMEM((10, 8, block), F32),
            pltpu.VMEM((3, block, slot), BF16),
            pltpu.VMEM((3, KV_ROWS, kv_width), BF16),
            pltpu.VMEM((3, slot, block), BF16),
            pltpu.SemaphoreType.DMA((50,)),
            pltpu.SemaphoreType.DMA((50,)),
            pltpu.SemaphoreType.DMA((40,)),
        ],
        compiler_params=pltpu.CompilerParams(
            collective_id=2, has_side_effects=True, vmem_limit_bytes=65000 * 1024
        ),
        name="project_back",
    )(gains, gain_in, x, dqkv, normed_t, gm, n2, dgu, wqkv, grad_o)


def results_kernel(
    hidden_in, grad_in, gq_in, gkv_in, go_in, gain_in, gu_in, gd_in,
    hidden_out, grad_out, gain_out, gq_out, gk_out, gv_out, go_out, gate_out, up_out, gd_out,
    hidden, grad, gq, gkv, go, gu, gd, gate, up, down, in_sem, out_sem,
):
    loads = [
        pltpu.make_async_copy(src, dst, in_sem.at[i])
        for i, (src, dst) in enumerate(
            ((gu_in, gu), (gd_in, gd), (hidden_in, hidden), (grad_in, grad), (gq_in, gq), (go_in, go), (gkv_in, gkv))
        )
    ]
    for load in loads:
        load.start()
    stores = []

    def store(src, dst):
        stores.append(pltpu.make_async_copy(src, dst, out_sem.at[len(stores)]))
        stores[-1].start()

    ff = gate.shape[1]
    gain_out[...] = gain_in[0:2, : gain_out.shape[1]]
    loads[0].wait()

    def widen(src, dst, start):
        def rows(n):
            r = pl.ds(pl.multiple_of(n * 32, 32), 32)
            dst[r] = src[r, start : start + dst.shape[1]].astype(F32)

        loop(dst.shape[0] // 32, rows)

    widen(gu, gate, 0)
    store(gate, gate_out)
    widen(gu, up, ff)
    store(up, up_out)
    loads[1].wait()
    widen(gd, down, 0)
    store(down, gd_out)
    for load, src, dst in zip(loads[2:6], (hidden, grad, gq, go), (hidden_out, grad_out, gq_out, go_out)):
        load.wait()
        store(src, dst)
    loads[6].wait()
    half = gk_out.shape[1]
    store(gkv.at[:, pl.ds(0, half)], gk_out)
    store(gkv.at[:, pl.ds(half, half)], gv_out)
    for copy in stores:
        copy.wait()


def results(hidden, grad, gq, gkv, go, gain, gu, gd):
    vmem = pl.BlockSpec(memory_space=pltpu.VMEM)
    hbm = pl.BlockSpec(memory_space=pltpu.HBM)
    shape = lambda *dims: jax.ShapeDtypeStruct(dims, F32)
    ff = gu.shape[1] // 2
    outs = [
        shape(*hidden.shape), shape(*grad.shape), shape(2, gain.shape[1] // 4), shape(*gq.shape),
        shape(gkv.shape[0], gkv.shape[1] // 2), shape(gkv.shape[0], gkv.shape[1] // 2), shape(*go.shape),
        shape(gu.shape[0], ff), shape(gu.shape[0], ff), shape(*gd.shape),
    ]
    return pl.pallas_call(
        results_kernel,
        in_specs=[hbm] * 5 + [vmem] + [hbm] * 2,
        out_specs=[vmem if i == 2 else hbm for i in range(10)],
        out_shape=outs,
        scratch_shapes=[pltpu.VMEM(a.shape, a.dtype) for a in (hidden, grad, gq, gkv, go, gu, gd)]
        + [pltpu.VMEM((gu.shape[0], ff), F32)] * 2
        + [pltpu.VMEM(gd.shape, F32), pltpu.SemaphoreType.DMA((7,)), pltpu.SemaphoreType.DMA((9,))],
        name="results",
    )(hidden, grad, gq, gkv, go, gain, gu, gd)


def plain_forward(x, g, cos, sin, w_query, w_kv, gains, w_out, w_gu, w_down):
    both = ("dp", "tensor")
    gather = lax.all_gather

    def whole(shard, dims):
        for dim, axis in dims:
            shard = gather(shard, axis, axis=dim, tiled=True)
        return shard

    wq = whole(w_query, ((1, "tensor"), (0, "dp")))
    wqkv = jnp.concatenate([wq, whole(w_kv, ((0, both),))], 1)
    gain = whole(gains, ((1, both),)).astype(F32)
    wo = whole(w_out, ((0, "tensor"), (1, "dp")))
    wgu = whole(w_gu, ((0, "dp"),))
    wd = whole(w_down, ((1, "dp"),))
    normed = (x * norm_scale(x) * gain[0]).astype(BF16)
    query, key_val, attended = attend(cos, sin, dot(normed, wqkv))
    middle = x + dot(attended, wo)
    normed_two = (middle * norm_scale(middle) * gain[1]).astype(BF16)
    n2 = gather(normed_two, "tensor", axis=0, tiled=True)
    top = gather(g.astype(BF16), "tensor", axis=0, tiled=True)
    return wqkv, gain, wo, wgu, wd, n2, top, query, key_val, attended, middle


def plain_backward(
    dn2_part, out_part, n2, grad_gu_pre, hidden, top,
    middle, x, g, gains, cos, sin, query, key_val, attended, wo, wqkv,
):
    width = x.shape[1]

    def scatter(part, axis, dim):
        return lax.psum_scatter(part.astype(BF16), axis, scatter_dimension=dim, tiled=True).astype(F32)

    output = middle + scatter(out_part, "tensor", 0)
    grad_mid_norm, gain_two = norm_back(middle, gains[1], scatter(dn2_part, "tensor", 0))
    grad_middle = g + grad_mid_norm
    mid_bf = grad_middle.astype(BF16)
    grad_qkv_rows = attend_back(cos, sin, query, key_val, dot_nt(mid_bf, wo).astype(BF16))
    grad_in_norm, gain_one = norm_back(x, gains[0], dot_nt(grad_qkv_rows, wqkv))
    normed_one = (x * norm_scale(x) * gains[0]).astype(BF16)
    grad_qkv = scatter(dot_tn(normed_one, grad_qkv_rows), "dp", 0)
    gain_parts = lax.psum_scatter(jnp.stack([gain_one, gain_two]), "dp", scatter_dimension=1, tiled=True)
    return (
        output,
        grad_middle + grad_in_norm,
        lax.psum_scatter(gain_parts, "tensor", scatter_dimension=1, tiled=True),
        scatter(grad_qkv[:, :width], "tensor", 1),
        scatter(grad_qkv[:, width:], "tensor", 0),
        scatter(scatter(dot_tn(attended, mid_bf), "dp", 1), "tensor", 0),
        scatter(dot_tn(n2, grad_gu_pre), "dp", 0),
        scatter(dot_tn(hidden, top), "dp", 1),
    )


def linked_layer(x, g, cos, sin, w_query, w_key, w_value, gains, w_out, w_gate, w_up, w_down):
    padded = jnp.pad(gains, ((0, GAIN_ROWS - 2), (0, LANES - gains.shape[1])))
    outs = forward_stage(x, g, cos, sin, w_query, w_key, w_value, padded, w_out, w_gate, w_up, w_down)
    wo, n2, top, wqkv, hidden, dgu, out_part = (outs[i] for i in (1, 4, 5, 6, 7, 8, 9))
    query, key_val, middle, normed_t, attended_t, gain, dn2 = outs[11:]
    output, gain_part, grad_down, grad_o, grad_middle, grad_qkv = attention_back(
        gain, cos, sin, dn2, middle, g, query, key_val, attended_t, out_part, hidden, top, wo
    )
    grad_query, grad_kv, grad_out, gain_sum, grad_in, grad_gu = project_back(
        gain, gain_part, x, grad_qkv, normed_t, grad_middle, n2, dgu, wqkv, grad_o
    )
    return results(output, grad_in, grad_query, grad_kv, grad_out, gain_sum, grad_gu, grad_down)


def plain_layer(x, g, cos, sin, w_query, w_key, w_value, gains, w_out, w_gate, w_up, w_down):
    w_kv = jnp.concatenate([w_key, w_value], 1)
    w_gu = jnp.concatenate([w_gate, w_up], 1)
    wqkv, gains, wo, wgu, wd, n2, top, query, key_val, attended, middle = plain_forward(
        x, g, cos, sin, w_query, w_kv, gains, w_out, w_gu, w_down
    )
    ff = wd.shape[0]
    gate_up = dot(n2, wgu)
    gate_pre, up_pre = gate_up[:, :ff], gate_up[:, ff:]
    sig = jax.nn.sigmoid(gate_pre)
    hidden = (gate_pre * sig * up_pre).astype(BF16)
    grad_hidden = dot_nt(top, wd)
    grad_gate_pre = (grad_hidden * up_pre * sig * (1.0 + gate_pre * (1.0 - sig))).astype(BF16)
    grad_up_pre = (grad_hidden * gate_pre * sig).astype(BF16)
    grad_gu_pre = jnp.concatenate([grad_gate_pre, grad_up_pre], 1)
    output, grad_in, grad_gains, grad_query, grad_kv, grad_out, grad_gu, grad_down = plain_backward(
        dot_nt(grad_gu_pre, wgu).astype(BF16), dot(hidden, wd).astype(BF16), n2, grad_gu_pre, hidden, top,
        middle, x, g, gains, cos, sin, query, key_val, attended, wo, wqkv,
    )
    half = KV * HD
    return (
        output, grad_in, grad_gains, grad_query, grad_kv[:, :half], grad_kv[:, half:], grad_out,
        grad_gu[:, :ff], grad_gu[:, ff:], grad_down,
    )


def on_device(
    linked,
    hidden_in, positions, norm_gains, w_query, w_key, w_value, w_out, w_gate, w_up, w_down, out_grad,
):
    x, g = hidden_in, out_grad
    rows, width = x.shape
    ff = w_gate.shape[2]
    kv_width = 2 * KV * HD
    z = lax.axis_index("tensor")

    cos, sin = rope_tables(lax.dynamic_slice_in_dim(positions, z * rows, rows))
    layer = linked_layer if linked else plain_layer
    outs = layer(
        x, g, cos, sin,
        w_query[0], w_key[0], w_value[0], norm_gains[0], w_out[0], w_gate[0], w_up[0], w_down[0],
    )
    return tuple(outs[:2]) + tuple(out[None] for out in outs[2:])


def solution(mesh):
    nd, nt = mesh.shape["dp"], mesh.shape["tensor"]
    rows = P(("dp", "tensor"), None)
    wide = P(None, "dp", "tensor")
    tall = P(None, "tensor", "dp")
    flat = P(None, ("dp", "tensor"), None)
    gain = P(None, None, ("dp", "tensor"))
    return jax.shard_map(
        functools.partial(on_device, (nd, nt) == (8, 4)),
        mesh=mesh,
        in_specs=(rows, P("dp"), gain, wide, flat, flat, tall, wide, wide, tall, rows),
        out_specs=(rows, rows, gain, wide, flat, flat, tall, wide, wide, tall),
        check_vma=False,
    )
```

```python
import functools

import jax
import jax.numpy as jnp
from jax import lax
from jax.experimental import pallas as pl
from jax.experimental.pallas import tpu as pltpu
from jax.sharding import PartitionSpec as P

H = 32
KV = 4
HD = 64
SEQ = 128
NORM_EPS = 1e-05
NEG_BIG = -1e30
SCALE = HD ** (-0.5)
LANES = 128
F32 = jnp.float32
BF16 = jnp.bfloat16


def dot(a, b):
    return jnp.dot(a, b, preferred_element_type=F32)


def dot_nt(a, b):
    return lax.dot_general(a, b, (((1,), (1,)), ((), ())), preferred_element_type=F32)


def dot_tn(a, b):
    return lax.dot_general(a, b, (((0,), (0,)), ((), ())), preferred_element_type=F32)


def lane_masks():
    lane = lax.broadcasted_iota(jnp.int32, (SEQ, LANES), 1)
    return lane % HD < HD // 2, lane < HD


def swap_halves(u, first):
    return jnp.where(first, pltpu.roll(u, LANES - HD // 2, 1), pltpu.roll(u, HD // 2, 1))


def twice(tile, index, low):
    turned = pltpu.roll(tile, HD, 1)
    return jnp.where(low, tile, turned) if index % 2 == 0 else jnp.where(low, turned, tile)


def causal_probs(query, key):
    scores = dot_nt(query, key) * SCALE
    rows = lax.broadcasted_iota(jnp.int32, scores.shape, 0)
    cols = lax.broadcasted_iota(jnp.int32, scores.shape, 1)
    scores = jnp.where(cols <= rows, scores, NEG_BIG)
    weights = jnp.exp(scores - jnp.max(scores, -1, keepdims=True))
    return weights * (1.0 / jnp.sum(weights, -1, keepdims=True))


def attend_sequence(cos, sin, load, kv_at, q_out, kv_out, o_out, at):
    first, low = lane_masks()

    def turn(u):
        return u * cos + swap_halves(u, first) * sin

    keys, vals_low, vals_high = [], [], []
    for tile in range(KV // 2):
        key = turn(load(kv_at + tile * LANES))
        val = load(kv_at + KV * HD + tile * LANES)
        kv_out[at, tile * LANES : (tile + 1) * LANES] = key.astype(BF16)
        kv_out[at, KV * HD + tile * LANES : KV * HD + (tile + 1) * LANES] = val.astype(BF16)
        for index in (0, 1):
            keys.append(twice(key, index, low).astype(BF16))
            both = twice(val, index, low)
            vals_low.append(jnp.where(low, both, 0.0).astype(BF16))
            vals_high.append(jnp.where(low, 0.0, both).astype(BF16))
    for pair in range(H // 2):
        group = pair * LANES // (H // KV * HD)
        query = turn(load(pair * LANES))
        p_low = causal_probs(jnp.where(low, query, 0.0).astype(BF16), keys[group])
        p_high = causal_probs(jnp.where(low, 0.0, query).astype(BF16), keys[group])
        q_out[at, pair * LANES : (pair + 1) * LANES] = query.astype(BF16)
        o_out[at, pair * LANES : (pair + 1) * LANES] = (
            dot(p_low.astype(BF16), vals_low[group]) + dot(p_high.astype(BF16), vals_high[group])
        ).astype(BF16)


def attend_back_sequence(cos, sin, q_ref, kv_ref, da_ref, dqkv_out, at):
    first, low = lane_masks()

    def turn_back(u):
        return (u * cos - swap_halves(u, first) * sin).astype(BF16)

    pair_total = H // KV * HD // LANES
    width = H * HD
    held = {}
    for group in range(KV):
        tile_at = group // 2 * LANES
        key = twice(kv_ref[at, tile_at : tile_at + LANES].astype(F32), group, low)
        val_at = KV * HD + tile_at
        val = twice(kv_ref[at, val_at : val_at + LANES].astype(F32), group, low).astype(BF16)
        key_low = jnp.where(low, key, 0.0).astype(BF16)
        key_high = jnp.where(low, 0.0, key).astype(BF16)
        key = key.astype(BF16)
        dk = jnp.zeros((SEQ, LANES), F32)
        dv = jnp.zeros((SEQ, LANES), F32)
        for pair in range(group * pair_total, (group + 1) * pair_total):
            query = q_ref[at, pair * LANES : (pair + 1) * LANES].astype(F32)
            grad = da_ref[at, pair * LANES : (pair + 1) * LANES].astype(F32)
            dq = None
            for is_low in (True, False):
                if is_low:
                    query_h = jnp.where(low, query, 0.0).astype(BF16)
                    grad_h = jnp.where(low, grad, 0.0).astype(BF16)
                else:
                    query_h = jnp.where(low, 0.0, query).astype(BF16)
                    grad_h = jnp.where(low, 0.0, grad).astype(BF16)
                prob = causal_probs(query_h, key)
                grad_prob = dot_nt(grad_h, val)
                delta = jnp.sum(prob * grad_prob, -1, keepdims=True)
                ds = (prob * (grad_prob - delta) * SCALE).astype(BF16)
                term = dot(ds, key_low if is_low else key_high)
                dq = term if dq is None else dq + term
                dk = dk + dot_tn(ds, query_h)
                dv = dv + dot_tn(prob.astype(BF16), grad_h)
            dqkv_out[at, pair * LANES : (pair + 1) * LANES] = turn_back(dq)
        held[group] = (dk + pltpu.roll(dk, HD, 1), dv + pltpu.roll(dv, HD, 1))
    for tile in range(KV // 2):
        col = width + tile * LANES
        dk = jnp.where(low, held[2 * tile][0], held[2 * tile + 1][0])
        dv = jnp.where(low, held[2 * tile][1], held[2 * tile + 1][1])
        dqkv_out[at, col : col + LANES] = turn_back(dk)
        dqkv_out[at, col + KV * HD : col + KV * HD + LANES] = dv.astype(BF16)


def causal_probs_turned(key, query):
    scores = dot_nt(key, query) * SCALE
    rows = lax.broadcasted_iota(jnp.int32, scores.shape, 0)
    cols = lax.broadcasted_iota(jnp.int32, scores.shape, 1)
    scores = jnp.where(rows <= cols, scores, NEG_BIG)
    weights = jnp.exp(scores - jnp.max(scores, 0, keepdims=True))
    return weights * (1.0 / jnp.sum(weights, 0, keepdims=True))


def attend_back_group(cos, sin, group, q_ref, kv_ref, da_ref, dqkv_out, dkv_out, at):
    first, low = lane_masks()
    head_width = H // KV * HD
    mine = low == (group % 2 == 0)

    def both(tile):
        kept = jnp.where(mine, tile.astype(F32), 0.0)
        return kept + pltpu.roll(kept, HD, 1)

    tile = pl.ds(pl.multiple_of(group // 2 * LANES, LANES), LANES)
    val_tile = pl.ds(pl.multiple_of(KV * HD + group // 2 * LANES, LANES), LANES)
    key = both(kv_ref[at, tile])
    val = both(kv_ref[at, val_tile]).astype(BF16)
    key_low = jnp.where(low, key, 0.0).astype(BF16)
    key_high = jnp.where(low, 0.0, key).astype(BF16)
    key = key.astype(BF16)
    dk = jnp.zeros((SEQ, LANES), F32)
    dv = jnp.zeros((SEQ, LANES), F32)
    for pair in range(head_width // LANES):
        c = pl.ds(pl.multiple_of(group * head_width + pair * LANES, LANES), LANES)
        query = q_ref[at, c].astype(F32)
        grad = da_ref[at, c].astype(F32)
        dq = None
        for is_low in (True, False):
            pick = low if is_low else jnp.logical_not(low)
            query_h = jnp.where(pick, query, 0.0).astype(BF16)
            grad_h = jnp.where(pick, grad, 0.0).astype(BF16)
            prob = causal_probs_turned(key, query_h)
            grad_prob = dot_nt(val, grad_h)
            delta = jnp.sum(prob * grad_prob, 0, keepdims=True)
            ds = (prob * (grad_prob - delta) * SCALE).astype(BF16)
            term = dot_tn(ds, key_low if is_low else key_high)
            dq = term if dq is None else dq + term
            dk = dk + dot(ds, query_h)
            dv = dv + dot(prob.astype(BF16), grad_h)
        dqkv_out[at, c] = (dq * cos - swap_halves(dq, first) * sin).astype(BF16)
    dkv_out[at, tile] += jnp.where(mine, dk + pltpu.roll(dk, HD, 1), 0.0)
    dkv_out[at, val_tile] += jnp.where(mine, dv + pltpu.roll(dv, HD, 1), 0.0)


def attend_kernel(cos_ref, sin_ref, qkv_ref, q_out, kv_out, o_out):
    attend_sequence(
        cos_ref[...], sin_ref[...], lambda c: qkv_ref[:, c : c + LANES], H * HD, q_out, kv_out, o_out, slice(None)
    )


def attend_back_kernel(cos_ref, sin_ref, q_ref, kv_ref, da_ref, dqkv_out):
    attend_back_sequence(cos_ref[...], sin_ref[...], q_ref, kv_ref, da_ref, dqkv_out, slice(None))


def by_sequence(body, name, ins, widths):
    rows = ins[0].shape[0]
    spec = lambda w: pl.BlockSpec((SEQ, w), lambda i: (i, 0))
    return pl.pallas_call(
        body,
        grid=(rows // SEQ,),
        in_specs=[spec(a.shape[1]) for a in ins],
        out_specs=[spec(w) for w in widths],
        out_shape=[jax.ShapeDtypeStruct((rows, w), BF16) for w in widths],
        name=name,
    )(*ins)


def attend(cos, sin, qkv):
    return by_sequence(attend_kernel, "attend", (cos, sin, qkv), (H * HD, 2 * KV * HD, H * HD))


def attend_back(cos, sin, query, key_val, grad):
    return by_sequence(
        attend_back_kernel, "attend_back", (cos, sin, query, key_val, grad), (H * HD + 2 * KV * HD,)
    )[0]


def norm_scale(rows):
    return lax.rsqrt(jnp.mean(rows * rows, -1, keepdims=True) + NORM_EPS)


def norm_back(rows, gain, grad_normed):
    inv = norm_scale(rows)
    weighted = grad_normed * gain
    grad_gain = jnp.sum(grad_normed * rows * inv, 0)
    grad_rows = inv * weighted - rows * inv**3 * jnp.mean(weighted * rows, -1, keepdims=True)
    return grad_rows, grad_gain


def rope_tables(positions):
    half = jnp.arange(LANES, dtype=jnp.int32) % (HD // 2)
    inv_freq = 10000.0 ** (-(half.astype(F32) * 2.0 / HD))
    angles = positions.astype(F32)[:, None] * inv_freq[None, :]
    sign = jnp.where(jnp.arange(LANES) % HD < HD // 2, -1.0, 1.0).astype(F32)
    return jnp.cos(angles), jnp.sin(angles) * sign[None, :]


MESH = pl.DeviceIdType.MESH
KV_ROWS = 64
GAIN_ROWS = 16


class Links:
    def __init__(self):
        self.d, self.z = lax.axis_index("dp"), lax.axis_index("tensor")
        core, x, y = self.d % 2, self.d // 2 % 2, self.d // 4
        self.dc = self.d + 1 - 2 * core
        step_x, step_y = 2 - 4 * x, 4 - 8 * y
        self.dx, self.dy, self.dxy = self.d + step_x, self.d + step_y, self.d + step_x + step_y
        self.dcx, self.dcy, self.dcxy = self.dc + step_x, self.dc + step_y, self.dc + step_x + step_y

    def barrier(self, far=False):
        z = self.z
        sem = pltpu.get_barrier_semaphore()

        def greet(d, zz):
            pl.semaphore_signal(sem, inc=1, device_id=(d, zz), device_id_type=MESH)

        for d in (self.dx, self.dy, self.dc):
            greet(d, z)
        if far:
            for j in (1, 2, 3):
                greet(self.d, (z + j) % 4)
            pl.semaphore_wait(sem, 6)
            return
        pl.when(z > 0)(lambda: greet(self.d, z - 1))
        pl.when(z < 3)(lambda: greet(self.d, z + 1))
        pl.semaphore_wait(sem, 3 + (z + 2) // 3 + (5 - z) // 3)


class Sender:
    def __init__(self, links, send_sem, recv_sem):
        self.links, self.send_sem, self.recv_sem = links, send_sem, recv_sem

    def copy(self, src, dst, at, to):
        return pltpu.make_async_remote_copy(
            src_ref=src,
            dst_ref=dst,
            send_sem=self.send_sem.at[at],
            recv_sem=self.recv_sem.at[at],
            device_id=to,
            device_id_type=MESH,
        )

    def start(self, src, dst, at, to):
        self.copy(src, dst, at, to).start()

    def landed(self, region, at):
        self.copy(region, region, at, (self.links.dc, self.links.z)).wait_recv()

    def sent(self, region, at):
        self.copy(region, region, at, (self.links.dc, self.links.z)).wait_send()


class Spread:
    def __init__(self, sender, region, base):
        self.s, self.region, self.base = sender, region, base

    def own(self, p, src):
        k, r, b = self.s.links, self.region, self.base + 9 * p
        mine = r(k.d, p, None)
        self.s.start(src, mine, b, (k.dx, k.z))
        self.s.start(src, mine, b + 1, (k.dy, k.z))
        self.s.start(src, mine, b + 2, (k.dc, k.z))

    def near(self, p):
        k, r, b = self.s.links, self.region, self.base + 9 * p
        self.s.landed(r(k.dx, p, None), b)
        self.s.start(r(k.dx, p, 0), r(k.dx, p, 0), b + 3, (k.dy, k.z))
        self.s.start(r(k.dx, p, None), r(k.dx, p, None), b + 5, (k.dc, k.z))
        self.s.landed(r(k.dy, p, None), b + 1)
        self.s.start(r(k.dy, p, 1), r(k.dy, p, 1), b + 4, (k.dx, k.z))
        self.s.start(r(k.dy, p, None), r(k.dy, p, None), b + 6, (k.dc, k.z))

    def far(self, p):
        k, r, b = self.s.links, self.region, self.base + 9 * p
        for part in (0, 1):
            self.s.landed(r(k.dxy, p, part), b + 3 + part)
            self.s.start(r(k.dxy, p, part), r(k.dxy, p, part), b + 7 + part, (k.dc, k.z))

    def finish(self, p):
        k, r, b = self.s.links, self.region, self.base + 9 * p
        self.s.landed(r(k.dc, p, None), b + 2)
        self.s.landed(r(k.dcx, p, None), b + 5)
        self.s.landed(r(k.dcy, p, None), b + 6)
        for part in (0, 1):
            self.s.landed(r(k.dcxy, p, part), b + 7 + part)

    def drain(self, p):
        k, r, b = self.s.links, self.region, self.base + 9 * p
        for i in (0, 1, 2):
            self.s.sent(r(k.d, p, None), b + i)
        self.s.sent(r(k.dx, p, 0), b + 3)
        self.s.sent(r(k.dy, p, 1), b + 4)
        self.s.sent(r(k.dx, p, None), b + 5)
        self.s.sent(r(k.dy, p, None), b + 6)
        for part in (0, 1):
            self.s.sent(r(k.dxy, p, part), b + 7 + part)


class Line:
    def __init__(self, sender, region, base):
        self.s, self.region, self.base = sender, region, base

    def _send(self, src, p, way, step):
        k = self.s.links
        self.s.start(src, self.region(p), self.base + 2 * (step - 1) + way, (k.d, k.z + 1 - 2 * way))

    def own(self, src):
        z = self.s.links.z
        pl.when(z < 3)(lambda: self._send(src, z, 0, 1))
        pl.when(z > 0)(lambda: self._send(src, z, 1, 1))

    def each(self, step, action):
        z = self.s.links.z
        pl.when(z >= step)(lambda: action(z - step, 0))
        pl.when(z + step <= 3)(lambda: action(z + step, 1))

    def arrive(self, step, then=None):
        z = self.s.links.z

        def action(p, way):
            self.s.landed(self.region(p), self.base + 2 * (step - 1) + way)
            if step < 3:
                ahead = z < 3 if way == 0 else z > 0
                pl.when(ahead)(lambda: self._send(self.region(p), p, way, step + 1))
            if then is not None:
                then(p)

        self.each(step, action)

    def drain(self):
        z = self.s.links.z
        for step in (1, 2, 3):
            for way in (0, 1):
                came = z - (step - 1) if way == 0 else z + (step - 1)
                ok = jnp.logical_and(z < 3, z >= step - 1) if way == 0 else jnp.logical_and(z > 0, z <= 4 - step)
                pl.when(ok)(
                    functools.partial(self.s.sent, self.region(came), self.base + 2 * (step - 1) + way)
                )


def forward_kernel(
    x_ref, g_ref, cos_ref, sin_ref, wq_in, wk_in, wv_in, gain_in, wo_ref, wg_in, wu_in, wd_ref,
    wa_all, wo_all, gu_all, wd_all, n2_all, top_all, wqkv_all, hidden_all, dgu_all, out_all, dn2_land,
    q_all, kv_all, mid_all, n1_t_all, o_t_all, gain_out, dn2_out,
    q_out, kv_out, o_out, mid_out, att_ref, gu_ref, n1, qkv, w_buf, wkv_buf, gain_buf, wo_buf, n2, top,
    n2_rows, top_rows, gate_up, grad_hidden, hidden, dgu, dn2_sends, out_rows, relay,
    send_sem, recv_sem, local_sem,
):
    rows, width = x_ref.shape
    slot_width = att_ref.shape[1]
    block = width // 8
    links = Links()
    d, z = links.d, links.z
    s = Sender(links, send_sem, recv_sem)
    ff = wd_ref.shape[0]
    cut_a = att_ref.shape[0] // 32 * 16
    cuts_a = ((0, cut_a), (cut_a, att_ref.shape[0] - cut_a))

    def at_a(dd, p, part):
        if part is None:
            return wa_all.at[dd, p]
        return wa_all.at[dd, p, pl.ds(*cuts_a[part])]

    def at_b(dd, p, part):
        start, size = (0, slot_width) if part is None else (part * slot_width // 2, slot_width // 2)
        return wo_all.at[
            pl.ds(pl.multiple_of(p * slot_width + start, 16), size),
            pl.ds(pl.multiple_of(dd * block, 128), block),
        ]

    def at_gu(dd, p, part):
        start, size = (0, block) if part is None else (part * block // 2, block // 2)
        return gu_all.at[pl.ds(pl.multiple_of(dd * block + start, 16), size)]

    def at_wd(dd, p, part):
        start, size = (0, ff) if part is None else (part * ff // 2, ff // 2)
        return wd_all.at[pl.ds(start, size), pl.ds(pl.multiple_of(dd * block, 128), block)]

    def rows_of(ref):
        return lambda p: ref.at[pl.ds(pl.multiple_of(p * rows, 16), rows)]

    spread_a, spread_b = Spread(s, at_a, 0), Spread(s, at_b, 36)
    spread_gu, spread_wd = Spread(s, at_gu, 72), Spread(s, at_wd, 81)
    line_a = Line(s, lambda p: at_a(d, p, None), 90)
    line_b = Line(s, lambda p: at_b(d, p, None), 96)
    line_n, line_t = Line(s, rows_of(n2_all), 102), Line(s, rows_of(top_all), 108)

    def keep(src, dst, at):
        pltpu.make_async_copy(src, dst, local_sem.at[at]).start()

    def kept(src, dst, at):
        pltpu.make_async_copy(src, dst, local_sem.at[at]).wait()

    kv_at = pl.ds(block, KV_ROWS)
    shards = [
        (wq_in, att_ref.at[pl.ds(0, block)], 78),
        (wk_in, att_ref.at[kv_at, pl.ds(0, KV * HD)], 79),
        (wv_in, att_ref.at[kv_at, pl.ds(KV * HD, KV * HD)], 80),
        (gain_in, att_ref.at[pl.ds(block + KV_ROWS, GAIN_ROWS), pl.ds(0, LANES)], 81),
    ]
    ffs = [(wg_in, gu_ref.at[:, pl.ds(0, ff)], 82), (wu_in, gu_ref.at[:, pl.ds(ff, ff)], 83)]
    for shard in shards + ffs:
        keep(*shard)
    att_ref[block + KV_ROWS :, LANES:] = jnp.zeros((GAIN_ROWS, slot_width - LANES), BF16)
    links.barrier(far=True)
    for shard in shards:
        kept(*shard)

    line_a.own(att_ref)
    spread_a.own(z, att_ref)
    keep(att_ref, at_a(d, z, None), 0)
    keep(wo_ref, at_b(d, z, None), 1)
    keep(wd_ref, at_wd(d, 0, None), 3)
    top[...] = g_ref[...].astype(BF16)
    line_a.arrive(1, lambda p: spread_a.own(p, at_a(d, p, None)))
    spread_a.near(z)
    line_a.arrive(2, lambda p: spread_a.own(p, at_a(d, p, None)))
    line_b.own(wo_ref)
    line_a.each(1, lambda p, way: spread_a.near(p))
    spread_a.far(z)
    line_a.arrive(3, lambda p: spread_a.own(p, at_a(d, p, None)))
    line_b.arrive(1)
    line_a.each(2, lambda p, way: spread_a.near(p))
    line_a.each(1, lambda p, way: spread_a.far(p))
    line_a.each(3, lambda p, way: spread_a.near(p))
    spread_b.own(z, wo_ref)
    line_b.each(1, lambda p, way: spread_b.own(p, at_b(d, p, None)))
    line_b.arrive(2, lambda p: spread_b.own(p, at_b(d, p, None)))
    line_a.each(2, lambda p, way: spread_a.far(p))
    line_a.each(3, lambda p, way: spread_a.far(p))
    for shard in ffs:
        kept(*shard)
    keep(gu_ref, at_gu(d, 0, None), 2)
    line_b.arrive(3, lambda p: spread_b.own(p, at_b(d, p, None)))
    line_t.own(top)
    kept(att_ref, at_a(d, z, None), 0)
    for p in range(4):
        spread_a.finish(p)

    def kv_copy(dd, p):
        return wkv_buf.at[dd, p], wqkv_all.at[pl.ds(dd * block + p * KV_ROWS, KV_ROWS), pl.ds(width, 2 * KV * HD)]

    for p in range(4):
        for dd in range(8):
            pltpu.make_async_copy(
                wa_all.at[dd, p, pl.ds(0, block)], w_buf.at[p, pl.ds(dd * block, block)], local_sem.at[14 + 8 * p + dd]
            ).start()
    keep(wa_all.at[:, :, pl.ds(block, KV_ROWS)], wkv_buf, 8)
    keep(wa_all.at[:, :, pl.ds(block + KV_ROWS, GAIN_ROWS), pl.ds(0, LANES)], gain_buf, 9)
    kept(wa_all.at[:, :, pl.ds(block + KV_ROWS, GAIN_ROWS), pl.ds(0, LANES)], gain_buf, 9)
    low_row = lax.broadcasted_iota(jnp.int32, (GAIN_ROWS, LANES), 1) < HD
    for dd in range(8):
        for half in (0, 1):
            first = gain_buf[dd, 2 * half].astype(F32)
            second = pltpu.roll(gain_buf[dd, 2 * half + 1].astype(F32), HD, 1)
            at = dd * block + half * LANES
            gain_out[:, at : at + LANES] = jnp.where(low_row, first, second)[:8]
    x = x_ref[...]
    n1[...] = (x * norm_scale(x) * gain_out[0:1]).astype(BF16)
    for p in range(4):
        for dd in range(8):
            kept(wa_all.at[dd, p, pl.ds(0, block)], w_buf.at[p, pl.ds(dd * block, block)], 14 + 8 * p + dd)
        for c in range(0, slot_width, 256):
            qkv[:, p * slot_width + c : p * slot_width + c + 256] = dot(n1[...], w_buf[p, :, c : c + 256])
        keep(w_buf.at[p], wqkv_all.at[:, pl.ds(p * slot_width, slot_width)], 4 + p)
    kept(wa_all.at[:, :, pl.ds(block, KV_ROWS)], wkv_buf, 8)
    qkv[:, width:] = dot(n1[...], wkv_buf[...].reshape(width, 2 * KV * HD))
    for p in range(4):
        for dd in range(8):
            pltpu.make_async_copy(*kv_copy(dd, p), local_sem.at[46 + 8 * p + dd]).start()

    line_b_pieces = lambda action: [action(z)] + [line_b.each(i, lambda p, way: action(p)) for i in (1, 2, 3)]

    def sequence(i, carry):
        at = pl.ds(pl.multiple_of(i * SEQ, SEQ), SEQ)
        attend_sequence(
            cos_ref[at], sin_ref[at], lambda c: qkv[at, c : c + LANES], width, q_out, kv_out, o_out, at
        )

        @pl.when(i == 0)
        def _():
            line_b_pieces(spread_b.near)
            spread_gu.own(0, gu_ref)
            line_t.arrive(1)

        return carry

    lax.fori_loop(0, rows // SEQ, sequence, 0)
    line_b_pieces(spread_b.far)
    kept(wo_ref, at_b(d, z, None), 1)
    for p in range(4):
        spread_b.finish(p)
    keep(wo_all, wo_buf, 0)
    kept(wo_all, wo_buf, 0)

    def column(i, carry):
        at = pl.ds(pl.multiple_of(i * 256, 256), 256)
        mid_out[:, at] = x_ref[:, at] + dot(o_out[...], wo_buf[:, at])
        return carry

    lax.fori_loop(0, width // 256, column, 0)
    mid = mid_out[...]
    n2[...] = (mid * norm_scale(mid) * gain_out[1:2]).astype(BF16)

    line_n.own(n2)
    keep(n2, n2_all.at[pl.ds(pl.multiple_of(z * rows, 16), rows)], 8)
    keep(top, top_all.at[pl.ds(pl.multiple_of(z * rows, 16), rows)], 9)
    results = [(q_out, q_all, 84), (kv_out, kv_all, 85), (mid_out, mid_all, 86)]
    for result in results:
        keep(*result)
    turns = []
    for i, (src, buf, dst) in enumerate(((n1, out_rows, n1_t_all), (o_out, dn2_sends.at[0], o_t_all))):
        for b in range(8):
            part = pl.ds(b * block, block)
            buf[:, part] = jnp.transpose(src[:, part].astype(F32)).astype(BF16)
            turns.append((buf.at[:, part], dst.at[part], 87 + 8 * i + b))
            keep(*turns[-1])
    for p in range(4):
        kept(w_buf.at[p], wqkv_all.at[:, pl.ds(p * slot_width, slot_width)], 4 + p)
        for dd in range(8):
            kept(*kv_copy(dd, p), 46 + 8 * p + dd)
    kept(gu_ref, at_gu(d, 0, None), 2)
    kept(wd_ref, at_wd(d, 0, None), 3)
    kept(n2, n2_all.at[pl.ds(pl.multiple_of(z * rows, 16), rows)], 8)
    kept(top, top_all.at[pl.ds(pl.multiple_of(z * rows, 16), rows)], 9)
    spread_gu.near(0)
    spread_wd.own(0, wd_ref)
    line_n.arrive(1)
    spread_gu.far(0)
    spread_gu.finish(0)

    wide = 2 * ff
    pieces = [(c, min(slot_width, wide - c)) for c in range(0, wide, slot_width)]
    gu_piece = lambda i, c, n: (columns(gu_all, c, n), w_buf.at[i, :, pl.ds(0, n)])
    for i, (c, n) in enumerate(pieces):
        keep(*gu_piece(i, c, n), 14 + i)
    wd_vmem = wo_buf.at[pl.ds(0, ff)]
    for turn in turns + results:
        kept(*turn)
    across, opposite, beside = 2 - z // 2, 3 - 3 * (z // 2), z + 1 - 2 * (z % 2)
    ends, inner = z % 3 == 0, z % 3 != 0
    chunks = [(c, min(256, ff - c)) for c in range(0, ff, 256)]

    def project(slot, source):
        for c, n in pieces:
            for h in range(0, n, 256):
                gate_up[slot, :, c + h : c + h + 256] = dot(source[...], w_buf[c // slot_width, :, h : h + 256])

    rows_at = lambda p: pl.ds(pl.multiple_of(p * rows, 16), rows)
    for i, (c, n) in enumerate(pieces):
        kept(*gu_piece(i, c, n), 14 + i)
    project(1, n2)
    line_n.arrive(2)
    line_t.arrive(2)
    spread_wd.near(0)
    keep(n2_all.at[rows_at(across)], n2_rows, 0)
    kept(n2_all.at[rows_at(across)], n2_rows, 0)
    project(0, n2_rows)
    spread_wd.far(0)
    spread_wd.finish(0)
    keep(wd_all, wd_vmem, 20)
    kept(wd_all, wd_vmem, 20)

    def place_of(p):
        return (p - z + 4) % 4 - 1

    def send_dn2(i, p):
        s.start(dn2_sends.at[i], dn2_land.at[place_of(p)], 114 + place_of(p), (d, p))

    def half_of(ref, h):
        return columns(ref, h * (width // 2), width // 2)

    def opposite_half(h):
        return half_of(dn2_land.at[1], h), 115 + 4 * h

    def pass_on(h):
        s.landed(half_of(relay, h), 117 + h)

        def add(m):
            r = pl.ds(pl.multiple_of(m * 32, 32), 32)
            c = pl.ds(h * (width // 2), width // 2)
            dn2_sends[1, r, c] = (dn2_sends[1, r, c].astype(F32) + relay[r, c].astype(F32)).astype(BF16)

        loop(rows // 32, add)
        to, at = opposite_half(h)
        s.start(half_of(dn2_sends.at[1], h), to, at, (d, opposite))

    def feed(i):
        pl.when(i == 1)(lambda: line_n.arrive(3))
        second = (i + 2) // 3 - i // 2
        p = across * ((3 - i) // 3) + opposite * second + beside * (i // 2 - i // 3) + z * (i // 3)
        at = rows_at(p)
        slot = i // 3
        pl.when(i != 1)(lambda: keep(top_all.at[at], top_rows, 1))

        @pl.when(second + i // 2 - i // 3 == 1)
        def _():
            keep(n2_all.at[at], n2_rows, 0)
            kept(n2_all.at[at], n2_rows, 0)
            project(0, n2_rows)

        @pl.when(i == 1)
        def _():
            line_t.arrive(3)
            keep(top_all.at[at], top_rows, 1)

        kept(top_all.at[at], top_rows, 1)
        for c, n in chunks:
            grad_hidden[:, c : c + n] = dot_nt(top_rows[...], wo_buf[c : c + n])

        @pl.when(i > 0)
        def _():
            kept(hidden, hidden_all.at[at], 2)
            kept(dgu, dgu_all.at[at], 3)

        def act(m):
            r = pl.ds(pl.multiple_of(m * 16, 16), 16)
            for c, n in chunks:
                gate, up = gate_up[slot, r, c : c + n], gate_up[slot, r, ff + c : ff + c + n]
                grad = grad_hidden[r, c : c + n]
                sig = 1.0 / (1.0 + jnp.exp(-gate))
                silu = gate * sig
                hidden[r, c : c + n] = (silu * up).astype(BF16)
                dgu[r, c : c + n] = (grad * up * sig * (1.0 + gate * (1.0 - sig))).astype(BF16)
                dgu[r, ff + c : ff + c + n] = (grad * silu).astype(BF16)

        loop(rows // 16, act)
        pl.when(jnp.logical_and(i == 3, inner))(lambda: pass_on(1))
        keep(hidden, hidden_all.at[at], 2)
        keep(dgu, dgu_all.at[at], 3)

        def back(m):
            r = pl.ds(pl.multiple_of(m * 256, 256), 256)
            total = None
            for j, (c, n) in enumerate(pieces):
                term = dot_nt(dgu[:, c : c + n], w_buf[j, r, :n])
                total = term if total is None else total + term

            @pl.when(i < 3)
            def _():
                dn2_sends[i, :, r] = total.astype(BF16)

            @pl.when(i == 3)
            def _():
                dn2_out[:, r] = total

            for h in (0, 1):

                @pl.when(jnp.logical_and(jnp.logical_and(i == 1, m == 4 * h + 3), ends))
                def _():
                    s.start(half_of(dn2_sends.at[1], h), half_of(relay, h), 117 + h, (d, 1 + z // 3))

        loop(width // 256, back)

        @pl.when(i % 2 == 0)
        def _():
            send_dn2(i, p)


        pl.when(i > 0)(lambda: kept(out_rows, out_all.at[at], 7))

        def down(m):
            r = pl.ds(pl.multiple_of(m * 256, 256), 256)
            out_rows[:, r] = dot(hidden[...], wo_buf[:ff, r]).astype(BF16)

        loop(width // 256, down)
        keep(out_rows, out_all.at[at], 7)
        pl.when(jnp.logical_and(i == 2, inner))(lambda: pass_on(0))

    loop(4, feed)
    kept(hidden, hidden_all.at[pl.ds(0, rows)], 2)
    kept(dgu, dgu_all.at[pl.ds(0, rows)], 3)
    kept(out_rows, out_all.at[pl.ds(0, rows)], 7)

    def collect(region, at, h=None):
        s.landed(region, at)
        c = pl.ds(0, width) if h is None else pl.ds(h * (width // 2), width // 2)
        keep(region, n2_rows.at[:, c], 0)
        kept(region, n2_rows.at[:, c], 0)

        def add(m):
            r = pl.ds(pl.multiple_of(m * 32, 32), 32)
            dn2_out[r, c] += n2_rows[r, c].astype(F32)

        loop(rows // 32, add)

    pl.when(z >= 1)(lambda: collect(dn2_land.at[0], 114))
    pl.when(z <= 2)(lambda: collect(dn2_land.at[2], 116))
    pl.when(inner)(lambda: collect(dn2_land.at[1], 115))
    for h in (0, 1):
        to, at = opposite_half(h)
        pl.when(ends)(functools.partial(collect, to, at, h))
    for i, p in ((0, across), (2, beside)):
        s.sent(dn2_sends.at[i], 114 + place_of(p))
    for h in (0, 1):
        to, at = opposite_half(h)
        pl.when(ends)(functools.partial(s.sent, half_of(dn2_sends.at[1], h), 117 + h))
        pl.when(inner)(functools.partial(s.sent, half_of(dn2_sends.at[1], h), at))
    for p in range(4):
        spread_a.drain(p)
        spread_b.drain(p)
    spread_gu.drain(0)
    spread_wd.drain(0)
    for line in (line_a, line_b, line_n, line_t):
        line.drain()


def forward_stage(x, g, cos, sin, wq, wk, wv, gains, wo, wg, wu, wd):
    rows, width = x.shape
    slot_width = wq.shape[1]
    block = width // 8
    kv_width = 2 * KV * HD
    ff = wd.shape[0]
    vmem = pl.BlockSpec(memory_space=pltpu.VMEM)
    hbm = pl.BlockSpec(memory_space=pltpu.HBM)
    shape = jax.ShapeDtypeStruct
    outs = [
        (hbm, shape((8, 4, block + KV_ROWS + GAIN_ROWS, slot_width), BF16)),
        (hbm, shape((width, width), BF16)),
        (hbm, shape((width, 2 * ff), BF16)),
        (hbm, shape((ff, width), BF16)),
        (hbm, shape((4 * rows, width), BF16)),
        (hbm, shape((4 * rows, width), BF16)),
        (hbm, shape((width, width + kv_width), BF16)),
        (hbm, shape((4 * rows, ff), BF16)),
        (hbm, shape((4 * rows, 2 * ff), BF16)),
        (hbm, shape((4 * rows, width), BF16)),
        (hbm, shape((3, rows, width), BF16)),
        (hbm, shape((rows, width), BF16)),
        (hbm, shape((rows, kv_width), BF16)),
        (hbm, shape((rows, width), F32)),
        (hbm, shape((width, rows), BF16)),
        (hbm, shape((width, rows), BF16)),
        (vmem, shape((8, width), F32)),
        (vmem, shape((rows, width), F32)),
    ]
    return pl.pallas_call(
        forward_kernel,
        in_specs=[vmem] * 4 + [hbm] * 4 + [vmem] + [hbm] * 2 + [vmem],
        out_specs=[o[0] for o in outs],
        out_shape=[o[1] for o in outs],
        scratch_shapes=[
            pltpu.VMEM((rows, width), BF16),
            pltpu.VMEM((rows, kv_width), BF16),
            pltpu.VMEM((rows, width), BF16),
            pltpu.VMEM((rows, width), F32),
            pltpu.VMEM((block + KV_ROWS + GAIN_ROWS, slot_width), BF16),
            pltpu.VMEM((block, 2 * ff), BF16),
            pltpu.VMEM((rows, width), BF16),
            pltpu.VMEM((rows, width + kv_width), F32),
            pltpu.VMEM((-(-2 * ff // slot_width), width, slot_width), BF16),
            pltpu.VMEM((8, 4, KV_ROWS, kv_width), BF16),
            pltpu.VMEM((8, 4, GAIN_ROWS, LANES), BF16),
            pltpu.VMEM((width, width), BF16),
            pltpu.VMEM((rows, width), BF16),
            pltpu.VMEM((rows, width), BF16),
            pltpu.VMEM((rows, width), BF16),
            pltpu.VMEM((rows, width), BF16),
            pltpu.VMEM((2, rows, 2 * ff), F32),
            pltpu.VMEM((rows, ff), F32),
            pltpu.VMEM((rows, ff), BF16),
            pltpu.VMEM((rows, 2 * ff), BF16),
            pltpu.VMEM((3, rows, width), BF16),
            pltpu.VMEM((rows, width), BF16),
            pltpu.VMEM((rows, width), BF16),
            pltpu.SemaphoreType.DMA((120,)),
            pltpu.SemaphoreType.DMA((120,)),
            pltpu.SemaphoreType.DMA((103,)),
        ],
        compiler_params=pltpu.CompilerParams(
            collective_id=0, has_side_effects=True, vmem_limit_bytes=65000 * 1024
        ),
        name="forward",
    )(x, g, cos, sin, wq, wk, wv, gains, wo, wg, wu, wd)


def loop(count, body):
    def step(i, carry):
        body(i)
        return carry

    lax.fori_loop(0, count, step, 0)


class Local:
    def __init__(self, sem):
        self.sem, self.next = sem, 0

    def start(self, src, dst):
        copy = pltpu.make_async_copy(src, dst, self.sem.at[self.next])
        self.next += 1
        copy.start()
        return copy

    def load(self, src, dst):
        self.start(src, dst).wait()


class Reduce:
    def __init__(self, sender, compute, base, sends, kept, land, halves):
        self.s, self.compute, self.base = sender, compute, base
        self.sends, self.kept, self.land, self.halves = sends, kept, land, halves

    def half(self, ref, part):
        return ref.at[pl.ds(*self.halves[part])]

    def place(self, i):
        if i < 4:
            return self.land.at[i]
        return self.half(self.land.at[4 + (i - 4) // 2], i % 2)

    def partner(self, i):
        k = self.s.links
        count = self.sends.shape[0]
        if i >= count:
            self.s.sent(self.sends.at[i % count], self.base + i - count)
        self.compute((k.dcxy, k.dcx, k.dcy, k.dc)[i], None, self.sends.at[i % count])
        self.s.start(self.sends.at[i % count], self.place(i), self.base + i, (k.dc, k.z))

    def own(self, i):
        k, b = self.s.links, self.base
        to_x, to_y = (k.dx, k.z), (k.dy, k.z)
        self.s.landed(self.place(i), b + i)
        kept = self.kept.at[i]
        self.compute((k.dxy, k.dx, k.dy, k.d)[i], self.land.at[i], kept)
        if i == 0:
            self.s.start(self.half(kept, 0), self.place(4), b + 4, to_x)
            self.s.start(self.half(kept, 1), self.place(7), b + 7, to_y)
        elif i == 1:
            self.s.start(self.half(kept, 0), self.place(6), b + 6, to_x)
        elif i == 2:
            self.s.start(self.half(kept, 1), self.place(5), b + 5, to_y)

    def first(self):
        self.partner(0)
        for i in range(3):
            self.partner(i + 1)
            self.own(i)
        self.own(3)

    def add(self, i, part, at):
        self.s.landed(self.place(at), self.base + at)
        start, size = self.halves[part]
        from_start = self.halves[at % 2][0] if at < 8 else self.halves[at - 8][0]
        slot = 4 + (at - 4) // 2
        step = 32 if size % 32 == 0 else 16

        def rows(n):
            r = pl.ds(pl.multiple_of(start + n * step, 16), step)
            g = pl.ds(pl.multiple_of(from_start + n * step, 16), step)
            self.kept[i, r] = (self.kept[i, r].astype(F32) + self.land[slot, g].astype(F32)).astype(BF16)

        loop(size // step, rows)

    def second(self):
        k, b = self.s.links, self.base
        self.add(2, 0, 4)
        self.s.start(self.half(self.kept.at[2], 0), self.place(8), b + 8, (k.dy, k.z))
        self.add(1, 1, 7)
        self.s.start(self.half(self.kept.at[1], 1), self.place(9), b + 9, (k.dx, k.z))

    def third(self):
        self.add(3, 0, 6)
        self.add(3, 1, 5)

    def last(self):
        self.add(3, 0, 8)
        self.add(3, 1, 9)

    def drain(self):
        b, kept = self.base, self.kept
        count = self.sends.shape[0]
        for i in range(4 - count, 4):
            self.s.sent(self.sends.at[i % count], b + i)
        self.s.sent(self.half(kept.at[0], 0), b + 4)
        self.s.sent(self.half(kept.at[2], 1), b + 5)
        self.s.sent(self.half(kept.at[1], 0), b + 6)
        self.s.sent(self.half(kept.at[0], 1), b + 7)
        self.s.sent(self.half(kept.at[2], 0), b + 8)
        self.s.sent(self.half(kept.at[1], 1), b + 9)


class LineSum:
    def __init__(self, sender, local, part, sends, land, base):
        self.s, self.part, self.sends = sender, part, sends
        self.land, self.base = land, base
        self.rows = sends.shape[1]
        self.sem, self.first = local.sem, local.next
        local.next += 7

    def rows_of(self, t):
        return self.part.at[pl.ds(pl.multiple_of(t * self.rows, 16), self.rows)]

    def fetch(self, holds, slot, at):
        return pltpu.make_async_copy(self.rows_of(holds), self.sends.at[slot], self.sem.at[self.first + at])

    def begin(self):
        for s in (1, 2, 3):
            for sends, slot, place, holds, _, _ in self.ways(s):
                pl.when(sends)(lambda: self.fetch(holds, slot, place).start())
        self.fetch(self.s.links.z, 3, 6).start()
        self.step(1)

    def add(self, into, at):
        self.s.landed(self.land.at[at], self.base + at)

        def rows(n):
            r = pl.ds(pl.multiple_of(n * 32, 32), 32)
            self.sends[into, r] = (self.sends[into, r].astype(F32) + self.land[at, r].astype(F32)).astype(BF16)

        loop(self.rows // 32, rows)

    def ways(self, s):
        z = self.s.links.z
        right = (z <= s - 1, s - 1 - z, 2 * (s - 1), z + 4 - s, z >= 1, z + 1)
        left = (z >= 4 - s, s - 1, 2 * (s - 1) + 1, z - 4 + s, z <= 2, z - 1)
        return right, left

    def step(self, s):
        for sends, slot, place, holds, received, to in self.ways(s):

            @pl.when(sends)
            def _():
                self.fetch(holds, slot, place).wait()
                if s > 1:
                    pl.when(received)(lambda: self.add(slot, place - 2))
                self.s.start(self.sends.at[slot], self.land.at[place], self.base + place, (self.s.links.d, to))

    def finish(self, write):
        z = self.s.links.z
        self.fetch(z, 3, 6).wait()
        pl.when(z >= 1)(lambda: self.add(3, 4))
        pl.when(z <= 2)(lambda: self.add(3, 5))

        def rows(n):
            r = pl.ds(pl.multiple_of(n * 32, 32), 32)
            write(r, self.sends[3, r].astype(F32))

        loop(self.rows // 32, rows)

    def drain(self):
        for s in (1, 2, 3):
            for sends, slot, place, _, _, _ in self.ways(s):
                pl.when(sends)(functools.partial(self.s.sent, self.sends.at[slot], self.base + place))


def stream(local, count, source, bufs, body):
    first = local.next
    local.next += 2

    def copy(n, slot):
        return pltpu.make_async_copy(source(n), bufs.at[slot], local.sem.at[first + slot])

    copy(0, 0).start()

    def step(n):
        slot = n % 2
        copy(n, slot).wait()

        @pl.when(n + 1 < count)
        def _():
            copy(n + 1, 1 - slot).start()

        body(n, bufs.at[slot])

    loop(count, step)


def turned(ref):
    return jnp.transpose(ref[...].astype(F32)).astype(BF16)


def columns(ref, start, size):
    return ref.at[:, pl.ds(pl.multiple_of(start, 128), size)]


class Feeder:
    def __init__(self, local, source, bufs, block, dests):
        self.source, self.bufs, self.block, self.dests = source, bufs, block, dests
        self.sem, self.first, self.n = local.sem, local.next, 0
        local.next += 2
        self._copy(0).start()

    def _copy(self, n):
        return pltpu.make_async_copy(
            columns(self.source, self.dests[n] * self.block, self.block),
            self.bufs.at[n % 2],
            self.sem.at[self.first + n % 2],
        )

    def __call__(self, dest):
        n = self.n
        self.n += 1
        self._copy(n).wait()
        if n + 1 < len(self.dests):
            self._copy(n + 1).start()
        return self.bufs.at[n % 2]


def order_of(k):
    partner, own = (k.dcxy, k.dcx, k.dcy, k.dc), (k.dxy, k.dx, k.dy, k.d)
    return [partner[0], partner[1], own[0], partner[2], own[1], partner[3], own[2], own[3]]


def row_blocks(pick, left, right):
    width = right.shape[1]

    def compute(dest, add, out):
        left[...] = turned(pick(dest))

        def chunk(n):
            c = pl.ds(pl.multiple_of(n * 256, 256), 256)
            total = dot(left[...], right[:, c])
            if add is not None:
                total = total + add[:, c].astype(F32)
            out[:, c] = total.astype(BF16)

        loop(width // 256, chunk)

    return compute


def column_blocks(left, pick, chunks):
    size = left.shape[0] // chunks

    def compute(dest, add, out):
        picked = pick(dest)

        def chunk(n):
            r = pl.ds(pl.multiple_of(n * size, 16), size)
            total = dot(left[r], picked[...])
            if add is not None:
                total = total + add[r].astype(F32)
            out[r] = total.astype(BF16)

        loop(chunks, chunk)

    return compute


class Chunk:
    def __init__(self, sender, compute, sends, kept, land, base):
        self.s, self.compute, self.sends = sender, compute, sends
        self.kept, self.land, self.base = kept, land, base
        self.half = kept.shape[2] // 2

    def views(self, n):
        kept, land, h = self.kept.at[n], self.land.at[n], self.half
        top, low = pl.ds(0, h), pl.ds(h, h)
        return {
            "x1": (kept.at[pl.ds(0, 2), top], land.at[pl.ds(4, 2), top]),
            "y1": (kept.at[pl.ds(1, 2), low], land.at[pl.ds(4, 2), low]),
            "y2": (kept.at[2, top], land.at[6, top]),
            "x2": (kept.at[0, low], land.at[6, low]),
        }

    def partner(self, n):
        k = self.s.links
        slot = n % self.sends.shape[0]
        if n != slot:
            self.s.sent(self.sends.at[slot], self.base + 5 * (n - self.sends.shape[0]))
        for i, dest in enumerate((k.dcx, k.dcxy, k.dcy, k.dc)):
            self.compute(n, dest, None, self.sends.at[slot, i])
        self.s.start(self.sends.at[slot], self.land.at[n, pl.ds(0, 4)], self.base + 5 * n, (k.dc, k.z))

    def own(self, n):
        k, b, v = self.s.links, self.base + 5 * n, self.views(n)
        self.s.landed(self.land.at[n, pl.ds(0, 4)], b)
        for i, dest in enumerate((k.dx, k.dxy, k.dy, k.d)):
            self.compute(n, dest, self.land.at[n, i], self.kept.at[n, i])
        self.s.start(*v["x1"], b + 1, (k.dx, k.z))
        self.s.start(*v["y1"], b + 2, (k.dy, k.z))

    def add(self, n, i, start, got):
        kept, land = self.kept, self.land

        def rows(m):
            r = pl.ds(pl.multiple_of(start + m * 32, 32), 32)
            kept[n, i, r] = (kept[n, i, r].astype(F32) + land[n, got, r].astype(F32)).astype(BF16)

        loop(self.half // 32, rows)

    def second(self, n):
        k, b, v = self.s.links, self.base + 5 * n, self.views(n)
        self.s.landed(v["x1"][1], b + 1)
        self.add(n, 2, 0, 5)
        self.s.start(*v["y2"], b + 3, (k.dy, k.z))
        self.s.landed(v["y1"][1], b + 2)
        self.add(n, 0, self.half, 4)
        self.s.start(*v["x2"], b + 4, (k.dx, k.z))
        self.add(n, 3, 0, 4)
        self.add(n, 3, self.half, 5)

    def last(self, n):
        b, v = self.base + 5 * n, self.views(n)
        self.s.landed(v["y2"][1], b + 3)
        self.add(n, 3, 0, 6)
        self.s.landed(v["x2"][1], b + 4)
        self.add(n, 3, self.half, 6)

    def drain(self):
        for n in range(self.kept.shape[0]):
            b, v = self.base + 5 * n, self.views(n)
            if n + self.sends.shape[0] >= self.kept.shape[0]:
                self.s.sent(self.sends.at[0], b)
            for at, name in enumerate(("x1", "y1", "y2", "x2")):
                self.s.sent(v[name][0], b + 1 + at)


class Spread4:
    def __init__(self, sender, pick, land, base):
        self.s, self.pick, self.land, self.base = sender, pick, land, base

    def send(self):
        k = self.s.links
        for j in (1, 2, 3):
            to = (k.z + j) % 4
            self.s.start(self.pick(to), self.land.at[j - 1], self.base + j - 1, (k.d, to))

    def landed(self):
        for j in range(3):
            self.s.landed(self.land.at[j], self.base + j)

    def drain(self):
        z = self.s.links.z
        for j in (1, 2, 3):
            self.s.sent(self.pick((z + j) % 4), self.base + j - 1)


def norm_back_rows(rows_ref, at, gain, grad_normed):
    rows = rows_ref[at]
    inv = norm_scale(rows)
    weighted = grad_normed * gain
    scaled = grad_normed * rows * inv
    grad_rows = inv * weighted - rows * (inv * inv * inv) * jnp.mean(weighted * rows, -1, keepdims=True)
    return grad_rows, scaled


def halves(size):
    return (0, size // 2), (size // 2, size // 2)


def add_gain(gain_part, block, row, scaled):
    for b in range(8):
        total = jnp.sum(scaled[:, b * block : (b + 1) * block], 0, keepdims=True)
        gain_part[b % 2, b // 2 % 2 * 2 + b // 4, row : row + 1] += total


def transpose_into(src, dst):
    def part(n):
        c = pl.ds(pl.multiple_of(n * 128, 128), 128)
        dst[c] = jnp.transpose(src[:, c].astype(F32)).astype(BF16)

    loop(src.shape[1] // 128, part)


def row_chunk(ref):
    return lambda n: ref.at[pl.ds(pl.multiple_of(n * 256, 256), 256)]


def attention_back_kernel(
    gain_ref, cos_ref, sin_ref, dn2_in, mid_in, g_in, q_in, kv_in, att_in,
    part_ref, hidden_ref, top_ref, wo_ref,
    out_ref, gain_part, gd_out, go_out, gm_all, dqkv_all,
    dn2_ref, mid_ref, g_ref, q_ref, kv_ref, att_t, gm_out, dqkv, mid_bf, da, dkv, w_chunk, top_cols, hidden_cols, hidden_t,
    d_sends, d_kept, d_land, o_sends, o_kept, o_land, line_sends, line_land,
    send_sem, recv_sem, local_sem,
):
    rows, width = mid_ref.shape
    block = width // 8
    ff = hidden_t.shape[0]
    links = Links()
    s = Sender(links, send_sem, recv_sem)
    local = Local(local_sem)
    top_feed = Feeder(local, top_ref, top_cols, block, order_of(links))
    links.barrier()
    line = LineSum(s, local, part_ref, line_sends, line_land, 20)
    line.begin()
    ins = [
        local.start(src, dst)
        for src, dst in (
            (dn2_in, dn2_ref), (mid_in, mid_ref), (g_in, g_ref), (att_in, att_t), (q_in, q_ref), (kv_in, kv_ref)
        )
    ]

    def turn_hidden(n, buf):
        hidden_t[pl.ds(pl.multiple_of(n * 128, 128), 128)] = turned(buf)

    stream(local, ff // 128, lambda n: columns(hidden_ref, n * 128, 128), hidden_cols, turn_hidden)
    grad_d = Reduce(s, column_blocks(hidden_t, top_feed, 4), 0, d_sends, d_kept, d_land, halves(ff))
    grad_d.first()
    line.step(2)

    gain_part[...] = jnp.zeros_like(gain_part)
    dkv[...] = jnp.zeros_like(dkv)
    step = 32

    def middle(n):
        r = pl.ds(pl.multiple_of(n * step, step), step)
        grad_rows, scaled = norm_back_rows(mid_ref, r, gain_ref[1:2], dn2_ref[r])
        grad = g_ref[r] + grad_rows
        gm_out[r] = grad
        mid_bf[r] = grad.astype(BF16)
        add_gain(gain_part, block, 1, scaled)

    for copy in ins:
        copy.wait()
    loop(rows // step, middle)
    to_gm = local.start(gm_out, gm_all)
    pick_mid = lambda dest: columns(mid_bf, dest * block, block)
    grad_o = Reduce(s, column_blocks(att_t, pick_mid, 4), 10, o_sends, o_kept, o_land, halves(width))
    grad_o.first()
    grad_d.second()

    def attended(n, buf):
        da[:, pl.ds(pl.multiple_of(n * 256, 256), 256)] = dot_nt(mid_bf[...], buf[...]).astype(BF16)

    stream(local, width // 256, row_chunk(wo_ref), w_chunk, attended)
    line.step(3)

    def group_step(n):
        def sequence(i):
            at = pl.ds(pl.multiple_of(i * SEQ, SEQ), SEQ)
            attend_back_group(cos_ref[at], sin_ref[at], n, q_ref, kv_ref, da, dqkv, dkv, at)

        loop(rows // SEQ, sequence)
        pl.when(n == 1)(grad_o.second)
        pl.when(n == 2)(grad_d.third)
        pl.when(n == 2)(grad_d.last)
        pl.when(n == 3)(grad_o.third)

    loop(KV, group_step)
    to_down = local.start(d_kept.at[3], gd_out)

    def key_value(i):
        at = pl.ds(pl.multiple_of(i * SEQ, SEQ), SEQ)
        first, _ = lane_masks()
        for tile in range(KV // 2):
            c = tile * LANES
            u = dkv[at, c : c + LANES]
            dqkv[at, width + c : width + c + LANES] = (
                u * cos_ref[at] - swap_halves(u, first) * sin_ref[at]
            ).astype(BF16)
        dqkv[at, width + KV * HD :] = dkv[at, KV * HD :].astype(BF16)

    loop(rows // SEQ, key_value)
    to_dqkv = local.start(dqkv, dqkv_all)
    grad_o.last()
    to_out = local.start(o_kept.at[3], go_out)

    def write(r, total):
        out_ref[r] = mid_ref[r] + total

    line.finish(write)
    for copy in (to_down, to_out, to_gm, to_dqkv):
        copy.wait()
    grad_o.drain()
    grad_d.drain()
    line.drain()


def attention_back(gains, cos, sin, dn2, mid, g, query, key_val, attended_t, part, hidden, top, wo):
    rows, width = mid.shape
    block, ff = width // 8, hidden.shape[1]
    kv_width = 2 * KV * HD
    vmem = pl.BlockSpec(memory_space=pltpu.VMEM)
    hbm = pl.BlockSpec(memory_space=pltpu.HBM)
    shape = jax.ShapeDtypeStruct
    return pl.pallas_call(
        attention_back_kernel,
        in_specs=[vmem] * 3 + [hbm] * 10,
        out_specs=[vmem] * 2 + [hbm] * 4,
        out_shape=[
            shape((rows, width), F32),
            shape((2, 4, 8, block), F32),
            shape((ff, block), BF16),
            shape((width, block), BF16),
            shape((rows, width), F32),
            shape((rows, width + kv_width), BF16),
        ],
        scratch_shapes=[
            pltpu.VMEM((rows, width), F32),
            pltpu.VMEM((rows, width), F32),
            pltpu.VMEM((rows, width), F32),
            pltpu.VMEM((rows, width), BF16),
            pltpu.VMEM((rows, kv_width), BF16),
            pltpu.VMEM((width, rows), BF16),
            pltpu.VMEM((rows, width), F32),
            pltpu.VMEM((rows, width + kv_width), BF16),
            pltpu.VMEM((rows, width), BF16),
            pltpu.VMEM((rows, width), BF16),
            pltpu.VMEM((rows, kv_width), F32),
            pltpu.VMEM((2, 256, width), BF16),
            pltpu.VMEM((2, 4 * rows, block), BF16),
            pltpu.VMEM((2, 4 * rows, 128), BF16),
            pltpu.VMEM((ff, 4 * rows), BF16),
            pltpu.VMEM((2, ff, block), BF16),
            pltpu.VMEM((4, ff, block), BF16),
            pltpu.VMEM((7, ff, block), BF16),
            pltpu.VMEM((2, width, block), BF16),
            pltpu.VMEM((4, width, block), BF16),
            pltpu.VMEM((7, width, block), BF16),
            pltpu.VMEM((4, rows, width), BF16),
            pltpu.VMEM((6, rows, width), BF16),
            pltpu.SemaphoreType.DMA((26,)),
            pltpu.SemaphoreType.DMA((26,)),
            pltpu.SemaphoreType.DMA((40,)),
        ],
        compiler_params=pltpu.CompilerParams(
            collective_id=1, has_side_effects=True, vmem_limit_bytes=65000 * 1024
        ),
        name="attention_back",
    )(gains, cos, sin, dn2, mid, g, query, key_val, attended_t, part, hidden, top, wo)


def project_back_kernel(
    gain_ref, gain_in, x_in, dqkv_in, n1_in, gm_ref, n2_ref, dgu_ref, wqkv_ref, go_in,
    gq_out, gkv_out, go_out, gain_out, grad_in_all, ggu_out,
    x_ref, dqkv, grad_in_out, dn1, n1_t, w_chunk, dgu, n2_cols, left, sends, kept, land,
    row_sends, row_kept, row_land, o_block, gain_part, gain_land, z_q, z_kv, z_o,
    send_sem, recv_sem, local_sem,
):
    rows, width = x_ref.shape
    block, slot = width // 8, width // 4
    kv_width = 2 * KV * HD
    step = 32
    links = Links()
    d, z = links.d, links.z
    s = Sender(links, send_sem, recv_sem)
    local = Local(local_sem)
    firsts = [local.start(dqkv_in, dqkv), local.start(n1_in, n1_t)]
    links.barrier(far=True)
    gain_part[...] = gain_in[...]
    for copy in firsts:
        copy.wait()
    fetch_o = local.start(go_in, o_block)
    n2_feed = Feeder(local, n2_ref, n2_cols, block, order_of(links))
    fetch_dgu = local.start(dgu_ref, dgu)
    fetch_x = local.start(x_in, x_ref)
    fetch_gm = local.start(gm_ref, grad_in_out)

    group_of = lambda n: (z + n) % 4

    def row_compute(n, dest, add, out):
        picked = n1_t[pl.ds(pl.multiple_of(dest * block, block), block)]
        start = width if n == 0 else group_of(n) * slot
        for c in range(0, slot, 256):
            total = dot(picked, dqkv[:, pl.ds(pl.multiple_of(start + c, 256), 256)])
            if add is not None:
                total = total + add[:, c : c + 256].astype(F32)
            out[:, c : c + 256] = total.astype(BF16)

    row = Chunk(s, row_compute, row_sends, row_kept, row_land, 10)
    row.partner(0)
    for n in range(4):
        row.partner(n + 1)
        row.own(n)
    row.own(4)
    fetch_o.wait()
    send_o = Spread4(s, lambda p: o_block.at[pl.ds(pl.multiple_of(p * slot, 16), slot)], z_o, 35)
    send_o.send()

    send_kv = Spread4(
        s, lambda p: row_kept.at[0, 3, pl.ds(pl.multiple_of(p * KV_ROWS, 16), KV_ROWS)], z_kv, 38
    )

    def final_q(n):
        row.last(n)
        s.start(row_kept.at[n, 3], z_q.at[n - 1], 40 + n, (d, group_of(n)))

    fetch_dgu.wait()
    grads = Reduce(s, row_blocks(n2_feed, left, dgu), 0, sends, kept, land, halves(block))
    grads.partner(0)
    row.second(0)
    grads.partner(1)
    row.second(1)
    row.second(2)
    grads.own(0)
    row.second(3)
    row.second(4)
    grads.partner(2)
    row.last(0)
    send_kv.send()
    final_q(1)
    grads.own(1)
    final_q(2)
    grads.partner(3)
    final_q(3)
    grads.own(2)
    row.last(4)
    grads.own(3)
    grads.second()

    def projected(n, buf):
        dn1[:, pl.ds(pl.multiple_of(n * 256, 256), 256)] = dot_nt(dqkv[...], buf[...])

    stream(local, width // 256, row_chunk(wqkv_ref), w_chunk, projected)
    fetch_gm.wait()
    fetch_x.wait()

    def inward(n):
        r = pl.ds(pl.multiple_of(n * step, step), step)
        grad_rows, scaled = norm_back_rows(x_ref, r, gain_ref[0:1], dn1[r])
        grad_in_out[r] += grad_rows
        add_gain(gain_part, block, 0, scaled)

    loop(rows // step, inward)
    to_in = local.start(grad_in_out, grad_in_all)
    grads.third()
    core, x_at, y_at = d % 2, d // 2 % 2, d // 4
    s.start(gain_part.at[1 - core], gain_land.at[pl.ds(0, 4)], 44, (links.dc, z))
    s.landed(gain_land.at[pl.ds(0, 4)], 44)
    gain_part[core] += gain_land[0:4]
    other_x = pl.multiple_of(2 - 2 * x_at, 2)
    s.start(gain_part.at[core, pl.ds(other_x, 2)], gain_land.at[pl.ds(4, 2)], 45, (links.dx, z))
    send_o.landed()

    def out_rows(n):
        r = pl.ds(pl.multiple_of(n * 16, 16), 16)
        mine = pl.ds(pl.multiple_of(z * slot + n * 16, 16), 16)
        go_out[r] = (
            o_block[mine].astype(F32) + z_o[0, r].astype(F32) + z_o[1, r].astype(F32) + z_o[2, r].astype(F32)
        )

    loop(slot // 16, out_rows)
    for n in range(3):
        s.landed(z_q.at[n], 41 + n)

    def query_rows(n):
        r = pl.ds(pl.multiple_of(n * 16, 16), 16)
        gq_out[r] = (
            row_kept[4, 3, r].astype(F32) + z_q[0, r].astype(F32) + z_q[1, r].astype(F32) + z_q[2, r].astype(F32)
        )

    loop(block // 16, query_rows)
    send_kv.landed()
    mine_kv = pl.ds(pl.multiple_of(z * KV_ROWS, 16), KV_ROWS)
    gkv_out[...] = row_kept[0, 3, mine_kv].astype(F32) + (
        z_kv[0].astype(F32) + z_kv[1].astype(F32) + z_kv[2].astype(F32)
    )
    s.landed(gain_land.at[pl.ds(4, 2)], 45)
    mine_x = 2 * x_at
    gain_part[core, pl.ds(mine_x, 2)] += gain_land[4:6]
    s.start(gain_part.at[core, mine_x + 1 - y_at], gain_land.at[6], 46, (links.dy, z))
    s.landed(gain_land.at[6], 46)
    gain_part[core, mine_x + y_at] += gain_land[6]
    send_g = Spread4(s, lambda p: gain_part.at[core, mine_x + y_at], gain_land.at[pl.ds(7, 3)], 47)
    send_g.send()
    grads.last()
    to_gu = local.start(kept.at[3], ggu_out)
    send_g.landed()
    gain = gain_part[core, mine_x + y_at] + gain_land[7] + gain_land[8] + gain_land[9]
    gain_out[...] = pltpu.roll(gain, (4 - z) % 4 * (block // 4), 1)
    to_gu.wait()
    to_in.wait()
    for unit in (grads, row, send_o, send_kv, send_g):
        unit.drain()
    for n in range(3):
        s.sent(row_kept.at[n + 1, 3], 41 + n)
    s.sent(gain_part.at[1 - core], 44)
    s.sent(gain_part.at[core, pl.ds(other_x, 2)], 45)
    s.sent(gain_part.at[core, mine_x + 1 - y_at], 46)


def project_back(gains, gain_in, x, dqkv, normed_t, gm, n2, dgu, wqkv, grad_o):
    rows, width = x.shape
    block, slot = width // 8, width // 4
    kv_width = 2 * KV * HD
    wide = dgu.shape[1]
    vmem = pl.BlockSpec(memory_space=pltpu.VMEM)
    hbm = pl.BlockSpec(memory_space=pltpu.HBM)
    shape = jax.ShapeDtypeStruct
    return pl.pallas_call(
        project_back_kernel,
        in_specs=[vmem] * 2 + [hbm] * 8,
        out_specs=[vmem] * 4 + [hbm] * 2,
        out_shape=[
            shape((block, slot), F32),
            shape((KV_ROWS, kv_width), F32),
            shape((slot, block), F32),
            shape((8, block), F32),
            shape((rows, width), F32),
            shape((block, wide), BF16),
        ],
        scratch_shapes=[
            pltpu.VMEM((rows, width), F32),
            pltpu.VMEM((rows, width + kv_width), BF16),
            pltpu.VMEM((rows, width), F32),
            pltpu.VMEM((rows, width), F32),
            pltpu.VMEM((width, rows), BF16),
            pltpu.VMEM((2, 256, width + kv_width), BF16),
            pltpu.VMEM((4 * rows, wide), BF16),
            pltpu.VMEM((2, 4 * rows, block), BF16),
            pltpu.VMEM((block, 4 * rows), BF16),
            pltpu.VMEM((2, block, wide), BF16),
            pltpu.VMEM((4, block, wide), BF16),
            pltpu.VMEM((7, block, wide), BF16),
            pltpu.VMEM((3, 4, block, slot), BF16),
            pltpu.VMEM((5, 4, block, slot), BF16),
            pltpu.VMEM((5, 7, block, slot), BF16),
            pltpu.VMEM((width, block), BF16),
            pltpu.VMEM((2, 4, 8, block), F32),
            pltpu.VMEM((10, 8, block), F32),
            pltpu.VMEM((3, block, slot), BF16),
            pltpu.VMEM((3, KV_ROWS, kv_width), BF16),
            pltpu.VMEM((3, slot, block), BF16),
            pltpu.SemaphoreType.DMA((50,)),
            pltpu.SemaphoreType.DMA((50,)),
            pltpu.SemaphoreType.DMA((40,)),
        ],
        compiler_params=pltpu.CompilerParams(
            collective_id=2, has_side_effects=True, vmem_limit_bytes=65000 * 1024
        ),
        name="project_back",
    )(gains, gain_in, x, dqkv, normed_t, gm, n2, dgu, wqkv, grad_o)


def results_kernel(
    hidden_in, grad_in, gq_in, gkv_in, go_in, gain_in, gu_in, gd_in,
    hidden_out, grad_out, gain_out, gq_out, gk_out, gv_out, go_out, gate_out, up_out, gd_out,
    hidden, grad, gq, gkv, go, gu, gd, gate, up, down, in_sem, out_sem,
):
    loads = [
        pltpu.make_async_copy(src, dst, in_sem.at[i])
        for i, (src, dst) in enumerate(
            ((gu_in, gu), (gd_in, gd), (hidden_in, hidden), (grad_in, grad), (gq_in, gq), (go_in, go), (gkv_in, gkv))
        )
    ]
    for load in loads:
        load.start()
    stores = []

    def store(src, dst):
        stores.append(pltpu.make_async_copy(src, dst, out_sem.at[len(stores)]))
        stores[-1].start()

    ff = gate.shape[1]
    gain_out[...] = gain_in[0:2, : gain_out.shape[1]]
    loads[0].wait()

    def widen(src, dst, start):
        def rows(n):
            r = pl.ds(pl.multiple_of(n * 32, 32), 32)
            dst[r] = src[r, start : start + dst.shape[1]].astype(F32)

        loop(dst.shape[0] // 32, rows)

    widen(gu, gate, 0)
    store(gate, gate_out)
    widen(gu, up, ff)
    store(up, up_out)
    loads[1].wait()
    widen(gd, down, 0)
    store(down, gd_out)
    for load, src, dst in zip(loads[2:6], (hidden, grad, gq, go), (hidden_out, grad_out, gq_out, go_out)):
        load.wait()
        store(src, dst)
    loads[6].wait()
    half = gk_out.shape[1]
    store(gkv.at[:, pl.ds(0, half)], gk_out)
    store(gkv.at[:, pl.ds(half, half)], gv_out)
    for copy in stores:
        copy.wait()


def results(hidden, grad, gq, gkv, go, gain, gu, gd):
    vmem = pl.BlockSpec(memory_space=pltpu.VMEM)
    hbm = pl.BlockSpec(memory_space=pltpu.HBM)
    shape = lambda *dims: jax.ShapeDtypeStruct(dims, F32)
    ff = gu.shape[1] // 2
    outs = [
        shape(*hidden.shape), shape(*grad.shape), shape(2, gain.shape[1] // 4), shape(*gq.shape),
        shape(gkv.shape[0], gkv.shape[1] // 2), shape(gkv.shape[0], gkv.shape[1] // 2), shape(*go.shape),
        shape(gu.shape[0], ff), shape(gu.shape[0], ff), shape(*gd.shape),
    ]
    return pl.pallas_call(
        results_kernel,
        in_specs=[hbm] * 5 + [vmem] + [hbm] * 2,
        out_specs=[vmem if i == 2 else hbm for i in range(10)],
        out_shape=outs,
        scratch_shapes=[pltpu.VMEM(a.shape, a.dtype) for a in (hidden, grad, gq, gkv, go, gu, gd)]
        + [pltpu.VMEM((gu.shape[0], ff), F32)] * 2
        + [pltpu.VMEM(gd.shape, F32), pltpu.SemaphoreType.DMA((7,)), pltpu.SemaphoreType.DMA((9,))],
        name="results",
    )(hidden, grad, gq, gkv, go, gain, gu, gd)


def plain_forward(x, g, cos, sin, w_query, w_kv, gains, w_out, w_gu, w_down):
    both = ("dp", "tensor")
    gather = lax.all_gather

    def whole(shard, dims):
        for dim, axis in dims:
            shard = gather(shard, axis, axis=dim, tiled=True)
        return shard

    wq = whole(w_query, ((1, "tensor"), (0, "dp")))
    wqkv = jnp.concatenate([wq, whole(w_kv, ((0, both),))], 1)
    gain = whole(gains, ((1, both),)).astype(F32)
    wo = whole(w_out, ((0, "tensor"), (1, "dp")))
    wgu = whole(w_gu, ((0, "dp"),))
    wd = whole(w_down, ((1, "dp"),))
    normed = (x * norm_scale(x) * gain[0]).astype(BF16)
    query, key_val, attended = attend(cos, sin, dot(normed, wqkv))
    middle = x + dot(attended, wo)
    normed_two = (middle * norm_scale(middle) * gain[1]).astype(BF16)
    n2 = gather(normed_two, "tensor", axis=0, tiled=True)
    top = gather(g.astype(BF16), "tensor", axis=0, tiled=True)
    return wqkv, gain, wo, wgu, wd, n2, top, query, key_val, attended, middle


def plain_backward(
    dn2_part, out_part, n2, grad_gu_pre, hidden, top,
    middle, x, g, gains, cos, sin, query, key_val, attended, wo, wqkv,
):
    width = x.shape[1]

    def scatter(part, axis, dim):
        return lax.psum_scatter(part.astype(BF16), axis, scatter_dimension=dim, tiled=True).astype(F32)

    output = middle + scatter(out_part, "tensor", 0)
    grad_mid_norm, gain_two = norm_back(middle, gains[1], scatter(dn2_part, "tensor", 0))
    grad_middle = g + grad_mid_norm
    mid_bf = grad_middle.astype(BF16)
    grad_qkv_rows = attend_back(cos, sin, query, key_val, dot_nt(mid_bf, wo).astype(BF16))
    grad_in_norm, gain_one = norm_back(x, gains[0], dot_nt(grad_qkv_rows, wqkv))
    normed_one = (x * norm_scale(x) * gains[0]).astype(BF16)
    grad_qkv = scatter(dot_tn(normed_one, grad_qkv_rows), "dp", 0)
    gain_parts = lax.psum_scatter(jnp.stack([gain_one, gain_two]), "dp", scatter_dimension=1, tiled=True)
    return (
        output,
        grad_middle + grad_in_norm,
        lax.psum_scatter(gain_parts, "tensor", scatter_dimension=1, tiled=True),
        scatter(grad_qkv[:, :width], "tensor", 1),
        scatter(grad_qkv[:, width:], "tensor", 0),
        scatter(scatter(dot_tn(attended, mid_bf), "dp", 1), "tensor", 0),
        scatter(dot_tn(n2, grad_gu_pre), "dp", 0),
        scatter(dot_tn(hidden, top), "dp", 1),
    )


def linked_layer(x, g, cos, sin, w_query, w_key, w_value, gains, w_out, w_gate, w_up, w_down):
    padded = jnp.pad(gains, ((0, GAIN_ROWS - 2), (0, LANES - gains.shape[1])))
    outs = forward_stage(x, g, cos, sin, w_query, w_key, w_value, padded, w_out, w_gate, w_up, w_down)
    wo, n2, top, wqkv, hidden, dgu, out_part = (outs[i] for i in (1, 4, 5, 6, 7, 8, 9))
    query, key_val, middle, normed_t, attended_t, gain, dn2 = outs[11:]
    output, gain_part, grad_down, grad_o, grad_middle, grad_qkv = attention_back(
        gain, cos, sin, dn2, middle, g, query, key_val, attended_t, out_part, hidden, top, wo
    )
    grad_query, grad_kv, grad_out, gain_sum, grad_in, grad_gu = project_back(
        gain, gain_part, x, grad_qkv, normed_t, grad_middle, n2, dgu, wqkv, grad_o
    )
    return results(output, grad_in, grad_query, grad_kv, grad_out, gain_sum, grad_gu, grad_down)


def plain_layer(x, g, cos, sin, w_query, w_key, w_value, gains, w_out, w_gate, w_up, w_down):
    w_kv = jnp.concatenate([w_key, w_value], 1)
    w_gu = jnp.concatenate([w_gate, w_up], 1)
    wqkv, gains, wo, wgu, wd, n2, top, query, key_val, attended, middle = plain_forward(
        x, g, cos, sin, w_query, w_kv, gains, w_out, w_gu, w_down
    )
    ff = wd.shape[0]
    gate_up = dot(n2, wgu)
    gate_pre, up_pre = gate_up[:, :ff], gate_up[:, ff:]
    sig = jax.nn.sigmoid(gate_pre)
    hidden = (gate_pre * sig * up_pre).astype(BF16)
    grad_hidden = dot_nt(top, wd)
    grad_gate_pre = (grad_hidden * up_pre * sig * (1.0 + gate_pre * (1.0 - sig))).astype(BF16)
    grad_up_pre = (grad_hidden * gate_pre * sig).astype(BF16)
    grad_gu_pre = jnp.concatenate([grad_gate_pre, grad_up_pre], 1)
    output, grad_in, grad_gains, grad_query, grad_kv, grad_out, grad_gu, grad_down = plain_backward(
        dot_nt(grad_gu_pre, wgu).astype(BF16), dot(hidden, wd).astype(BF16), n2, grad_gu_pre, hidden, top,
        middle, x, g, gains, cos, sin, query, key_val, attended, wo, wqkv,
    )
    half = KV * HD
    return (
        output, grad_in, grad_gains, grad_query, grad_kv[:, :half], grad_kv[:, half:], grad_out,
        grad_gu[:, :ff], grad_gu[:, ff:], grad_down,
    )


def on_device(
    linked,
    hidden_in, positions, norm_gains, w_query, w_key, w_value, w_out, w_gate, w_up, w_down, out_grad,
):
    x, g = hidden_in, out_grad
    rows, width = x.shape
    ff = w_gate.shape[2]
    kv_width = 2 * KV * HD
    z = lax.axis_index("tensor")

    cos, sin = rope_tables(lax.dynamic_slice_in_dim(positions, z * rows, rows))
    layer = linked_layer if linked else plain_layer
    outs = layer(
        x, g, cos, sin,
        w_query[0], w_key[0], w_value[0], norm_gains[0], w_out[0], w_gate[0], w_up[0], w_down[0],
    )
    return tuple(outs[:2]) + tuple(out[None] for out in outs[2:])


def solution(mesh):
    nd, nt = mesh.shape["dp"], mesh.shape["tensor"]
    rows = P(("dp", "tensor"), None)
    wide = P(None, "dp", "tensor")
    tall = P(None, "tensor", "dp")
    flat = P(None, ("dp", "tensor"), None)
    gain = P(None, None, ("dp", "tensor"))
    return jax.shard_map(
        functools.partial(on_device, (nd, nt) == (8, 4)),
        mesh=mesh,
        in_specs=(rows, P("dp"), gain, wide, flat, flat, tall, wide, wide, tall, rows),
        out_specs=(rows, rows, gain, wide, flat, flat, tall, wide, wide, tall),
        check_vma=False,
    )
```
